32 devices in a mesh: shard: 8 (over z, y), rep: 4 (over x, core).
Axes of the slice: x: 2, y: 2, z: 4, core: 2. Of those that a mesh axis runs over, the one named last changes fastest.
Arguments:
- tokens: bfloat16 [32768, 1024], P(('shard', 'rep')), may hold values from -6 to 6
- lengths: int32 [32], P(('shard', 'rep')), may hold values from 256 to 1024, as said below
- variate_ids: int32 [32, 1024], P(('shard', 'rep')), may hold values from 0 to 3
- time_ids: int32 [32, 1024], P(('shard', 'rep')), may hold values from 0 to 1023
- attn_gain: bfloat16 [1024], P('shard'), may hold values from 0.5 to 1.5
- w_qkv: bfloat16 [1024, 3072], P('shard'), may hold values from -0.1875 to 0.1875
- attn_bias: bfloat16 [2, 16], P(None, 'shard'), may hold values from -1 to 1
- w_out: bfloat16 [1024, 1024], P('shard'), may hold values from -0.75 to 0.75
- ffn_gain: bfloat16 [1024], P('shard'), may hold values from 0.5 to 1.5
- w_in: bfloat16 [1024, 8192], P('shard'), may hold values from -0.1875 to 0.1875
- w_down: bfloat16 [4096, 1024], P('shard'), may hold values from -0.09375 to 0.09375
- cotangent: bfloat16 [32768, 1024], P(('shard', 'rep')), may hold values from -6 to 6
Outputs:
- result: bfloat16 [32768, 1024], P(('shard', 'rep'))
- grad_tokens: float32 [32768, 1024], P(('shard', 'rep'))
- grad_attn_gain: float32 [1024], P('shard')
- grad_qkv: float32 [1024, 3072], P('shard')
- grad_bias: float32 [2, 16], P(None, 'shard')
- grad_out: float32 [1024, 1024], P('shard')
- grad_ffn_gain: float32 [1024], P('shard')
- grad_in: float32 [1024, 8192], P('shard')
- grad_down: float32 [4096, 1024], P('shard')
The draws below stay inside these ranges and needn't reach their ends.
Inputs may be any that keep to these rules, and one draw needn't show every extreme that they name: `lengths`: some sequence has all 1024 positions valid.
All inputs are finite; a program needn't handle non-finite values.
Results may differ from the reference program's by a relative error of at most 0.029.
Values may be sent and summed in bfloat16 or wider, within the bound.
A program may use at most 384 MiB of HBM per device.

```python
import jax
import jax.numpy as jnp
from jax import lax

D = 1024
HEADS = 16
HEAD_DIM = 64
FF = 4096
LEN = 1024
VARIATES = 4
SEQS = 32
TOKENS = 32768


def draw_lengths(key, part):
    first_key, second_key = jax.random.split(jax.random.fold_in(key, 7))
    drawn = jax.random.randint(first_key, (SEQS,), LEN // 4, LEN + 1)
    chosen = jax.random.randint(second_key, (), 0, SEQS)
    return jnp.where(jnp.arange(SEQS) == chosen, LEN, drawn).astype(jnp.int32)


def plant(values, key, least, largest):
    index_at = [jax.random.randint(jax.random.fold_in(key, axis), (), 0, length) for axis, length in enumerate(values.shape)]
    longest = values.shape.index(max(values.shape))
    neighbour = index_at[:longest] + [(index_at[longest] + 1) % values.shape[longest]] + index_at[longest + 1:]
    return values.at[tuple(index_at)].set(least).at[tuple(neighbour)].set(largest)


def level_of(rng, dims, shards, smallest, top_value):
    def one(axis_at, blocks):
        draws = jax.random.uniform(jax.random.fold_in(jax.random.fold_in(rng, 6), axis_at), (blocks,), jnp.float32, smallest / len(shards), top_value / len(shards))
        return jnp.repeat(jnp.exp(draws), dims[axis_at] // blocks).reshape((-1,) + (1,) * (len(dims) - axis_at - 1))

    factor_of = one(*shards[0])
    for cut in shards[1:]:
        factor_of = factor_of * one(*cut)
    return factor_of


def bell_draw(key, extent, deviation, limit, cuts=(), dtype=jnp.bfloat16):
    level = level_of(key, extent, cuts, -0.22, 0.18) if cuts else 1.0
    entries = jax.random.normal(key, extent, jnp.float32) * deviation * level
    return jnp.minimum(jnp.maximum(entries, -limit), limit).astype(dtype)


def setup_inputs(seed: int = 0) -> dict:
    streams_of = jax.random.split(jax.random.key(seed), 13)
    tokens = bell_draw(streams_of[0], (TOKENS, D), 1.0, 6.0, ((0, 32),))
    lengths = draw_lengths(jax.random.fold_in(streams_of[12], 71), 0)
    variate_ids = plant(jax.random.randint(streams_of[2], (SEQS, LEN), 0, VARIATES), jax.random.fold_in(streams_of[2], 1), 0, VARIATES - 1).astype(jnp.int32)
    time_ids = plant(jax.random.randint(streams_of[3], (SEQS, LEN), 0, LEN), jax.random.fold_in(streams_of[3], 1), 0, LEN - 1).astype(jnp.int32)
    attn_gain = jnp.clip(1.0 + 0.1 * jax.random.normal(streams_of[4], (D,), jnp.float32), 0.5, 1.5).astype(jnp.bfloat16)
    w_qkv = bell_draw(streams_of[5], (D, 3 * D), D ** -0.5, 0.1875, ((0, 8),))
    attn_bias = jnp.clip(jax.random.uniform(streams_of[6], (2, HEADS), jnp.float32, -1.0, 1.0) * level_of(streams_of[6], (2, HEADS), ((1, 8),), -0.4, 0.0), -1.0, 1.0).astype(jnp.bfloat16)
    w_out = bell_draw(streams_of[7], (D, D), (D // 16) ** -0.5, 0.75, ((0, 8),))
    ffn_gain = jnp.clip(1.0 + 0.1 * jax.random.normal(streams_of[8], (D,), jnp.float32), 0.5, 1.5).astype(jnp.bfloat16)
    w_in = bell_draw(streams_of[9], (D, 2 * FF), D ** -0.5, 0.1875, ((0, 8),))
    w_down = bell_draw(streams_of[10], (FF, D), FF ** -0.5, 0.09375, ((0, 8),))
    cotangent = bell_draw(streams_of[11], (TOKENS, D), 1.0, 6.0, ((0, 32),))
    return dict(tokens=tokens, lengths=lengths, variate_ids=variate_ids, time_ids=time_ids, attn_gain=attn_gain, w_qkv=w_qkv, attn_bias=attn_bias, w_out=w_out, ffn_gain=ffn_gain, w_in=w_in, w_down=w_down, cotangent=cotangent)


norm_eps = 1e-06
rope_base = 10000.0
masked_score = -1000000000.0

@jax.custom_vjp
def low(v):
    return lax.optimization_barrier(v.astype(jnp.bfloat16)).astype(jnp.float32)

@jax.custom_vjp
def low_back(v):
    return v

def low_keep(v):
    return (low(v), None)

def low_pass(kept, grad):
    return (grad,)

def back_keep(v):
    return (v, None)

def back_low(kept, grad):
    return (low(grad),)
low.defvjp(low_keep, low_pass)
low_back.defvjp(back_keep, back_low)

def product(first_op, second_op):
    return jnp.dot(first_op, second_op, precision=lax.Precision.HIGHEST, preferred_element_type=jnp.float32)

def rms_scale(values, gain):
    return values * lax.rsqrt(lax.optimization_barrier(jnp.mean(values * values, axis=-1, keepdims=True)) + norm_eps) * gain

def rope_tables(time_row, head_dim):
    half_dim = head_dim // 2
    exponent = jnp.arange(half_dim).astype(jnp.float32) * (2.0 / head_dim)
    inverse = jnp.exp(-jnp.log(rope_base) * exponent)
    angles = time_row.astype(jnp.float32)[:, None] * inverse[None, :]
    angles = jnp.concatenate([angles, angles], axis=1)
    return (jnp.cos(angles)[:, None, :], jnp.sin(angles)[:, None, :])

def rotate(values, cos_table, sin_table):
    half_dim = values.shape[-1] // 2
    turned = jnp.concatenate([-values[..., half_dim:], values[..., :half_dim]], axis=-1)
    return values * cos_table + turned * sin_table

def attention(query, key_rows, values, var_row, key_valid, bias):
    block_rows = min(512, LEN)
    block_count = LEN // block_rows
    score_scale = HEAD_DIM ** (-0.5)

    def one_block(block_items):
        query_rows, var_rows = block_items
        raw_scores = jnp.einsum('qhd,khd->hqk', query_rows, key_rows, precision=lax.Precision.HIGHEST) * score_scale
        same_var = var_rows[:, None] == var_row[None, :]
        raw_scores = raw_scores + jnp.where(same_var[None], bias[0][:, None, None], bias[1][:, None, None])
        scores = jnp.where(key_valid[None, None, :], low_back(raw_scores), masked_score)
        soft_probs = jax.nn.softmax(scores, axis=2)
        return jnp.einsum('hqk,khd->qhd', low(soft_probs), values, precision=lax.Precision.HIGHEST)
    pieces = lax.map(jax.checkpoint(one_block), (query.reshape(block_count, block_rows, HEADS, HEAD_DIM), var_row.reshape(block_count, block_rows)))
    return pieces.reshape(LEN, HEADS, HEAD_DIM)

def sequence_forward(weights, inputs, seq_len, var_row, time_row):
    gain_one, qkv_weight, bias_full, out_weight, gain_two, in_weight, down_weight = weights
    key_valid = jnp.arange(LEN) < seq_len
    cos_table, sin_table = rope_tables(time_row, HEAD_DIM)
    normed_one = low(rms_scale(inputs, gain_one))
    projected = low_back(product(normed_one, qkv_weight)).reshape(LEN, 3, HEADS, HEAD_DIM)
    query = low(rotate(projected[:, 0], cos_table, sin_table))
    key_rows = low(rotate(projected[:, 1], cos_table, sin_table))
    values = low(projected[:, 2])
    attended = attention(query, key_rows, values, var_row, key_valid, bias_full).reshape(LEN, D)
    attended = low_back(low(attended))
    hidden = inputs + low_back(product(attended, out_weight))
    normed_two = low(rms_scale(hidden, gain_two))
    gate_up = low_back(product(normed_two, in_weight))
    activated = low(jax.nn.silu(gate_up[:, :FF]) * gate_up[:, FF:])
    return hidden + low_back(product(activated, down_weight))

def reference(tokens, lengths, variate_ids, time_ids, attn_gain, w_qkv, attn_bias, w_out, ffn_gain, w_in, w_down, cotangent):
    params = (attn_gain.astype(jnp.float32), w_qkv.astype(jnp.float32), attn_bias.astype(jnp.float32), w_out.astype(jnp.float32), ffn_gain.astype(jnp.float32), w_in.astype(jnp.float32), w_down.astype(jnp.float32))
    groups = SEQS // 4
    inputs = tokens.astype(jnp.float32).reshape(groups, 4, LEN, D)
    key_valid = jnp.arange(LEN)[None, :] < lengths[:, None]
    grads_given = jnp.where(key_valid[:, :, None], cotangent.astype(jnp.float32).reshape(SEQS, LEN, D), 0.0)
    grads_given = grads_given.reshape(groups, 4, LEN, D)

    def group_step(totals, group_data):
        group_inputs, group_lengths, group_vars, group_times, group_grads = group_data

        def forward(weights, seq_values):
            return jax.vmap(lambda one_seq, seq_len, var_row, time_row: sequence_forward(weights, one_seq, seq_len, var_row, time_row))(seq_values, group_lengths, group_vars, group_times)
        outputs, pullback = jax.vjp(forward, params, group_inputs)
        d_weights, d_inputs = pullback(group_grads)
        totals = jax.tree.map(lambda summed, addend: summed + addend, totals, d_weights)
        return (totals, (outputs, d_inputs))
    totals = jax.tree.map(jnp.zeros_like, params)
    totals, (outputs, d_inputs) = lax.scan(group_step, totals, (inputs, lengths.reshape(groups, 4), variate_ids.reshape(groups, 4, LEN), time_ids.reshape(groups, 4, LEN), grads_given))
    return (outputs.reshape(SEQS * LEN, D).astype(jnp.bfloat16), d_inputs.reshape(SEQS * LEN, D), totals[0], totals[1], totals[2], totals[3], totals[4], totals[5], totals[6])
```

```python
import functools

import jax
import jax.numpy as jnp
from jax import lax
from jax.experimental import pallas as pl
from jax.experimental.pallas import tpu as pltpu
from jax.sharding import PartitionSpec as P

D = 1024
HEADS = 16
HEAD_DIM = 64
FF = 4096


norm_eps = 1e-06
rope_base = 10000.0
masked_score = -1000000000.0


MESH = pl.DeviceIdType.MESH
ANY = pl.BlockSpec(memory_space=pl.ANY)


class Net:
    def __init__(self, line):
        shard, rep = lax.axis_index("shard"), lax.axis_index("rep")
        self.line = line
        self.z, self.y = shard // 2, shard % 2
        self.x, self.core = rep // 2, rep % 2
        self.own = shard
        self.sibling = (shard, self.x * 2 + 1 - self.core)
        self.across_x = (shard, (1 - self.x) * 2 + self.core)
        self.across_y = (self.z * 2 + 1 - self.y, rep)
        self.above = (jnp.minimum(self.z + 1, line - 1) * 2 + self.y, rep)
        self.below = (jnp.maximum(self.z - 1, 0) * 2 + self.y, rep)
        self.has_above = self.z < line - 1
        self.has_below = self.z > 0

    def greet(self):
        barrier = pltpu.get_barrier_semaphore()

        def hail(partner):
            pl.semaphore_signal(barrier, inc=1, device_id=partner, device_id_type=MESH)

        for partner in (self.sibling, self.across_x, self.across_y):
            hail(partner)
        pl.when(self.has_above)(lambda: hail(self.above))
        pl.when(self.has_below)(lambda: hail(self.below))
        neighbours = jnp.where(self.has_above, 1, 0) + jnp.where(self.has_below, 1, 0)
        pl.semaphore_wait(barrier, 3 + neighbours)


def aligned(value, step):
    return pl.multiple_of(value, step)


def gather_count(line):
    return 2 * line + 3 * 2 * line


def gather_steps(net, source, full, local_sem, send_sem, recv_sem):
    line = net.line
    half, columns = source.shape[0] // 2, source.shape[1]
    split = columns % 1024 == 0
    only = columns * 3 // 8 if split else 0
    shared = columns - 2 * only
    rows = pl.ds(aligned(net.core * half, half), half)
    carried = pl.ds(aligned(net.x * only, 128), only + shared) if split else pl.ds(0, columns)
    lone = pl.ds(aligned(net.x * (only + shared), 128), only) if split else None

    def remote(origin, landing, index, target):
        return pltpu.make_async_remote_copy(
            src_ref=origin,
            dst_ref=landing,
            send_sem=send_sem.at[index],
            recv_sem=recv_sem.at[index],
            device_id=target,
            device_id_type=MESH,
        )

    def piece(z, y):
        return full.at[z * 2 + y, rows, carried]

    def over_z(z, target, base):
        return remote(piece(z, net.y), piece(z, net.y), base + z, target)

    def over_y(z):
        return remote(piece(z, net.y), piece(z, net.y), 2 * line + z, net.across_y)

    def over_x(z, y):
        part = full.at[z * 2 + y, rows, lone]
        return remote(part, part, 3 * line + y * line + z, net.across_x)

    def to_core(z, y):
        part = full.at[z * 2 + y, rows]
        return remote(part, part, 5 * line + y * line + z, net.sibling)

    mine = source.at[rows, carried]
    local = pltpu.make_async_copy(source, full.at[net.own], local_sem)
    first_y = remote(mine, piece(net.z, net.y), 2 * line + net.z, net.across_y)
    first_up = remote(mine, piece(net.z, net.y), net.z, net.above)
    first_down = remote(mine, piece(net.z, net.y), line + net.z, net.below)

    def onward(z, y):
        if split:
            over_x(z, y).start()
        else:
            to_core(z, y).start()

    def start():
        first_y.start()
        pl.when(net.has_above)(first_up.start)
        pl.when(net.has_below)(first_down.start)
        local.start()

    def arrive(hops):
        @pl.when(net.z >= hops)
        def _():
            z = net.z - hops
            over_z(z, net.above, 0).wait_recv()
            pl.when(net.has_above)(over_z(z, net.above, 0).start)
            over_y(z).start()
            onward(z, net.y)

        @pl.when(net.z < line - hops)
        def _():
            z = net.z + hops
            over_z(z, net.below, line).wait_recv()
            pl.when(net.has_below)(over_z(z, net.below, line).start)
            over_y(z).start()
            onward(z, net.y)

    def arrive_y(hops):
        def one(z):
            remote(piece(z, 1 - net.y), piece(z, 1 - net.y), 2 * line + z, net.across_y).wait_recv()
            onward(z, 1 - net.y)

        if hops == 0:
            one(net.z)
        else:
            pl.when(net.z >= hops)(lambda: one(net.z - hops))
            pl.when(net.z < line - hops)(lambda: one(net.z + hops))

    def arrive_x(hops, own_y):
        def one(z):
            y = net.y if own_y else 1 - net.y
            part = full.at[z * 2 + y, rows, pl.ds(aligned((1 - net.x) * (only + shared), 128), only)]
            remote(part, part, 3 * line + y * line + z, net.across_x).wait_recv()
            to_core(z, y).start()

        if not split:
            return
        if hops == 0:
            one(net.z)
        else:
            pl.when(net.z >= hops)(lambda: one(net.z - hops))
            pl.when(net.z < line - hops)(lambda: one(net.z + hops))

    def step(hops):
        def run():
            arrive_y(hops - 1)
            if hops < line:
                arrive(hops)
            if hops >= 2:
                arrive_x(hops - 2, False)
                arrive_x(hops - 1, True)

        return run

    def last():
        arrive_x(line - 1, False)

    def finish():
        local.wait()
        first_y.wait_send()

        @pl.when(net.has_above)
        def _():
            first_up.wait_send()
            for hops in range(1, line - 1):
                pl.when(net.z >= hops)(over_z(net.z - hops, net.above, 0).wait_send)

        @pl.when(net.has_below)
        def _():
            first_down.wait_send()
            for hops in range(1, line - 1):
                pl.when(net.z < line - hops)(over_z(net.z + hops, net.below, line).wait_send)

        for z in range(line):

            def others():
                over_y(z).wait_send()
                if split:
                    over_x(z, net.y).wait_send()
                to_core(z, net.y).wait()

            pl.when(net.z != z)(others)
            if split:
                over_x(z, 1 - net.y).wait_send()
            to_core(z, 1 - net.y).wait()

    return [start] + [step(hops) for hops in range(1, line + 1)] + [last, finish]


def gather_scratch(line, tensors):
    copies = gather_count(line)
    return [
        pltpu.SemaphoreType.DMA((tensors,)),
        pltpu.SemaphoreType.DMA((tensors, copies)),
        pltpu.SemaphoreType.DMA((tensors, copies)),
    ]


REDUCE_BUFFERS = 9


def reduce_split(columns):
    only = columns // 4 if columns % 512 == 0 else 0
    return only, columns - 2 * only


def reduce_scratch(line, shards, half, columns, dtype):
    only, shared = reduce_split(columns)
    carried = only + shared
    return [
        pltpu.VMEM((shards, half, columns), dtype),
        pltpu.VMEM((shards, half, columns), dtype),
        pltpu.VMEM((shards, half, max(only, 128)), dtype),
        pltpu.VMEM((line, half, carried), dtype),
        pltpu.VMEM((line + 1, half, carried), dtype),
        pltpu.VMEM((half, carried), dtype),
        pltpu.VMEM((half, columns), dtype),
        pltpu.VMEM((half, columns), dtype),
        pltpu.VMEM((2 * half, columns), jnp.float32),
    ]


def reduce_count(line):
    return 3 * line + 4


def reduce_steps(net, grad, out, column_start, buffers, local_sem, send_sem, recv_sem):
    kept, got, from_x, from_y, from_z, late_x, final, swapped, wide = buffers
    line = net.line
    shards, half, width = kept.shape
    only, shared = reduce_split(width)
    both = only + shared
    columns = pl.ds(column_start, width)
    mine = pl.ds(aligned(net.core * half, half), half)
    theirs = pl.ds(aligned((1 - net.core) * half, half), half)
    if only:
        carried = pl.ds(aligned(net.x * only, 128), both)
        lone = pl.ds(aligned(net.x * both, 128), only)
        their_lone = pl.ds(aligned((1 - net.x) * both, 128), only)
    else:
        carried = pl.ds(0, width)
    middle = pl.ds(only, shared)

    def remote(origin, landing, index, target):
        return pltpu.make_async_remote_copy(
            src_ref=origin,
            dst_ref=landing,
            send_sem=send_sem.at[index],
            recv_sem=recv_sem.at[index],
            device_id=target,
            device_id_type=MESH,
        )

    local = pltpu.make_async_copy(grad.at[:, mine, columns], kept, local_sem.at[0])
    halves = remote(grad.at[:, theirs, columns], got, 2 * line, net.sibling)
    written = pltpu.make_async_copy(wide, out.at[:, columns], local_sem.at[1])
    to_core = remote(final, swapped, 2 * line + 1, net.sibling)
    end_x = remote(kept.at[net.own, :, carried], late_x, 2 * line + 2, net.across_x)
    if only:
        over_x = remote(kept.at[:, :, their_lone], from_x, 2 * line + 3, net.across_x)

    def over_y(z):
        part = kept.at[z * 2 + 1 - net.y, :, carried]
        return remote(part, from_y.at[z], 2 * line + 4 + z, net.across_y)

    def up(z):
        return remote(kept.at[z * 2 + net.y, :, carried], from_z.at[z + 1], z, net.above)

    def down(z):
        return remote(kept.at[z * 2 + net.y, :, carried], from_z.at[z], line + z, net.below)

    def add(shard, part):
        kept[shard, :, carried] = kept[shard, :, carried] + part

    def first():
        halves.start()
        local.start()

    def second():
        local.wait()
        halves.wait_recv()

        @pl.loop(0, shards)
        def _(shard):
            kept[shard] = kept[shard] + got[shard]

        if only:
            over_x.start()

    def third():
        if only:
            over_x.wait_recv()

            @pl.loop(0, shards)
            def _(shard):
                kept[shard, :, lone] = kept[shard, :, lone] + from_x[shard]

        for z in range(line):
            over_y(z).start()

    def fourth():
        for z in range(line):
            over_y(z).wait_recv()

        @pl.loop(0, line)
        def _(z):
            add(z * 2 + net.y, from_y[z])

    def hop(step):
        def run():
            @pl.when(net.z == step)
            def _():
                for z in range(line - 1, step, -1):
                    if step > 0:
                        up(z).wait_recv()
                        add(z * 2 + net.y, from_z[z + 1])
                    up(z).start()

            @pl.when(net.z == line - 1 - step)
            def _():
                for z in range(line - 1 - step):
                    if step > 0:
                        down(z).wait_recv()
                        add(z * 2 + net.y, from_z[z])
                    down(z).start()

        return run

    def land():
        @pl.when(net.has_below)
        def _():
            up(net.z).wait_recv()
            add(net.own, from_z[net.z + 1])

        @pl.when(net.has_above)
        def _():
            down(net.z).wait_recv()
            add(net.own, from_z[net.z])

        end_x.start()

    def meet():
        end_x.wait_recv()
        if only:
            final[:, lone] = kept[net.own, :, lone]
            for x in range(2):

                @pl.when(net.x == x)
                def _():
                    start = 0 if x == 1 else shared
                    final[:, (1 - x) * both : (1 - x) * both + only] = late_x[:, start : start + only]
                    other = shared * 0 + (only if x == 1 else 0)
                    final[:, only:both] = kept[net.own, :, only:both] + late_x[:, other : other + shared]
        else:
            final[...] = kept[net.own] + late_x[...]
        to_core.start()
        wide[mine, :] = final[...].astype(jnp.float32)

    def swap():
        to_core.wait_recv()
        wide[theirs, :] = swapped[...].astype(jnp.float32)
        written.start()

    def finish():
        written.wait()
        halves.wait_send()
        if only:
            over_x.wait_send()
        for z in range(line):
            over_y(z).wait_send()
            pl.when(net.z < z)(up(z).wait_send)
            pl.when(net.z > z)(down(z).wait_send)
        end_x.wait_send()
        to_core.wait_send()

    hops = [hop(step) for step in range(line - 1)]

    def fourth_and_hop():
        fourth()
        hops[0]()

    return [first, second, third, fourth_and_hop] + hops[1:] + [land, meet, swap, finish]


def staggered(step_lists, gap=1):
    ticks = (len(step_lists) - 1) * gap + max(len(steps) for steps in step_lists)
    out = []
    for tick in range(ticks):
        row = []
        for index, steps in enumerate(step_lists):
            at = tick - index * gap
            if 0 <= at < len(steps):
                row.append(steps[at])
        out.append(row)
    return out


def reduce_chunks(shape):
    shards, rows, columns = shape
    width = columns
    while width % 1024 == 0 and shards * (rows // 2) * width > (1 << 19):
        width //= 2
    return width, columns // width


def gather_kernel(ring, count, *refs):
    sources, fulls = refs[:count], refs[count : 2 * count]
    local_sem, send_sem, recv_sem = refs[2 * count :]
    net = Net(ring)
    net.greet()
    lists = [
        gather_steps(net, sources[i], fulls[i], local_sem.at[i], send_sem.at[i], recv_sem.at[i])
        for i in range(count)
    ]
    for step in range(len(lists[0])):
        for steps in lists:
            steps[step]()


def gather_all(ring, shards, parts):
    return pl.pallas_call(
        functools.partial(gather_kernel, ring, len(parts)),
        out_shape=[jax.ShapeDtypeStruct((shards,) + part.shape, part.dtype) for part in parts],
        in_specs=[ANY] * len(parts),
        out_specs=[ANY] * len(parts),
        scratch_shapes=gather_scratch(ring, len(parts)),
        compiler_params=pltpu.CompilerParams(collective_id=1, has_side_effects=True),
        name="gather_all",
    )(*parts)


def reduce_kernel(ring, plan, *refs):
    count = len(plan)
    grads, outs = refs[:count], refs[count : 2 * count]
    refs = refs[2 * count :]
    local_sem, send_sem, recv_sem = refs[:3]
    refs = refs[3:]
    net = Net(ring)
    net.greet()
    lists = []
    for index, (width, chunks) in enumerate(plan):
        for chunk in range(chunks):
            number = len(lists)
            lists.append(
                reduce_steps(
                    net,
                    grads[index],
                    outs[index],
                    chunk * width,
                    refs[REDUCE_BUFFERS * number : REDUCE_BUFFERS * (number + 1)],
                    local_sem.at[number],
                    send_sem.at[number],
                    recv_sem.at[number],
                )
            )
    for row in staggered(lists):
        for step in row:
            step()


def reduce_all(ring, grads, collective):
    plan = [reduce_chunks(grad.shape) for grad in grads]
    total = sum(chunks for _, chunks in plan)
    scratch = [
        pltpu.SemaphoreType.DMA((total, 2)),
        pltpu.SemaphoreType.DMA((total, reduce_count(ring))),
        pltpu.SemaphoreType.DMA((total, reduce_count(ring))),
    ]
    for grad, (width, chunks) in zip(grads, plan):
        for _ in range(chunks):
            scratch += reduce_scratch(ring, grad.shape[0], grad.shape[1] // 2, width, grad.dtype)
    return pl.pallas_call(
        functools.partial(reduce_kernel, ring, plan),
        out_shape=[jax.ShapeDtypeStruct(grad.shape[1:], jnp.float32) for grad in grads],
        in_specs=[ANY] * len(grads),
        out_specs=[ANY] * len(grads),
        scratch_shapes=scratch,
        compiler_params=pltpu.CompilerParams(
            collective_id=collective, has_side_effects=True, vmem_limit_bytes=60 << 20
        ),
        name="reduce_all",
    )(*grads)


def contract_rows(first_op, second_op):
    return lax.dot_general(
        first_op, second_op, (((0,), (0,)), ((), ())), preferred_element_type=jnp.float32
    )


def times_transpose(first_op, second_op):
    return lax.dot_general(
        first_op, second_op, (((1,), (1,)), ((), ())), preferred_element_type=jnp.float32
    )


def rope_tables(time_rows, head_dim):
    half_dim = head_dim // 2
    exponent = jnp.arange(half_dim).astype(jnp.float32) * (2.0 / head_dim)
    inverse = jnp.exp(-jnp.log(rope_base) * exponent)
    angles = time_rows.astype(jnp.float32)[:, None] * inverse[None, :]
    angles = jnp.concatenate([angles, angles], axis=1)
    return (jnp.cos(angles)[:, None, :], jnp.sin(angles)[:, None, :])


def rotate(values, cos_table, sin_table):
    half_dim = values.shape[-1] // 2
    turned = jnp.concatenate([-values[..., half_dim:], values[..., :half_dim]], axis=-1)
    return values * cos_table + turned * sin_table


def rotate_back(grad_vals, cos_table, sin_table):
    scaled = grad_vals * sin_table
    half_dim = grad_vals.shape[-1] // 2
    turned = jnp.concatenate([scaled[..., half_dim:], -scaled[..., :half_dim]], axis=-1)
    return grad_vals * cos_table + turned


def score_block(query_rows, key_rows, var_rows, var_all, key_valid, bias, score_scale):
    raw_scores = (
        jnp.einsum("qhd,khd->hqk", query_rows, key_rows, preferred_element_type=jnp.float32)
        * score_scale
    )
    same_var = var_rows[:, None] == var_all[None, :]
    raw_scores = raw_scores + jnp.where(
        same_var[None], bias[0][:, None, None], bias[1][:, None, None]
    )
    return (jnp.where(key_valid[None, None, :], raw_scores, masked_score), same_var)


def attend_forward(query, key_rows, values, var_all, key_valid, bias):
    length = query.shape[0]
    block_rows = min(512, length)
    score_scale = query.shape[-1] ** (-0.5)
    pieces = []
    lse_parts = []
    for row_start in range(0, length, block_rows):
        scores, same_var = score_block(
            query[row_start : row_start + block_rows],
            key_rows,
            var_all[row_start : row_start + block_rows],
            var_all,
            key_valid,
            bias,
            score_scale,
        )
        row_peak = jnp.max(scores, axis=2, keepdims=True)
        exp_scores = jnp.exp(scores - row_peak)
        row_total = jnp.sum(exp_scores, axis=2, keepdims=True)
        soft_probs = (exp_scores / row_total).astype(jnp.bfloat16)
        pieces.append(
            jnp.einsum("hqk,khd->qhd", soft_probs, values, preferred_element_type=jnp.float32)
        )
        lse_parts.append((row_peak + jnp.log(row_total))[:, :, 0])
    return (jnp.concatenate(pieces, axis=0), jnp.concatenate(lse_parts, axis=1))


def attend_backward(query, key_rows, values, var_all, key_valid, bias, log_sums, grad_attended):
    length = query.shape[0]
    block_rows = min(512, length)
    score_scale = query.shape[-1] ** (-0.5)
    d_keys = jnp.zeros(key_rows.shape, jnp.float32)
    d_values = jnp.zeros(values.shape, jnp.float32)
    d_bias = jnp.zeros((2, bias.shape[1]), jnp.float32)
    d_query_parts = []
    for row_start in range(0, length, block_rows):
        query_rows = query[row_start : row_start + block_rows]
        scores, same_var = score_block(
            query_rows,
            key_rows,
            var_all[row_start : row_start + block_rows],
            var_all,
            key_valid,
            bias,
            score_scale,
        )
        soft_probs = jnp.exp(scores - log_sums[:, row_start : row_start + block_rows][:, :, None])
        grad_block = grad_attended[row_start : row_start + block_rows]
        d_values = d_values + jnp.einsum(
            "hqk,qhd->khd",
            soft_probs.astype(jnp.bfloat16),
            grad_block,
            preferred_element_type=jnp.float32,
        )
        d_probs = jnp.einsum("qhd,khd->hqk", grad_block, values, preferred_element_type=jnp.float32)
        row_inner = jnp.sum(soft_probs * d_probs, axis=2, keepdims=True)
        d_scores = (soft_probs * (d_probs - row_inner)).astype(jnp.bfloat16)
        same_mask = same_var.astype(jnp.bfloat16)
        in_same = jnp.einsum("hqk,qk->h", d_scores, same_mask, preferred_element_type=jnp.float32)
        in_other = jnp.einsum(
            "hqk,qk->h", d_scores, 1.0 - same_mask, preferred_element_type=jnp.float32
        )
        d_bias = d_bias + jnp.stack([in_same, in_other])
        d_query_parts.append(
            jnp.einsum("hqk,khd->qhd", d_scores, key_rows, preferred_element_type=jnp.float32)
            * score_scale
        )
        d_keys = (
            d_keys
            + jnp.einsum("hqk,qhd->khd", d_scores, query_rows, preferred_element_type=jnp.float32)
            * score_scale
        )
    return (jnp.concatenate(d_query_parts, axis=0), d_keys, d_values, d_bias)


def gathered(line, attn_gain, w_qkv, attn_bias, w_out, ffn_gain, w_in, w_down):
    if not line:
        return tuple(
            lax.all_gather(part, "shard", axis=axis, tiled=True)
            for part, axis in (
                (attn_gain, 0),
                (w_qkv, 0),
                (attn_bias, 1),
                (w_out, 0),
                (ffn_gain, 0),
                (w_in, 0),
                (w_down, 0),
            )
        )
    shards, heads = lax.axis_size("shard"), attn_bias.shape[1]
    small = jnp.zeros((16, 128), jnp.float32)
    small = small.at[0].set(attn_gain.astype(jnp.float32)).at[1].set(ffn_gain.astype(jnp.float32))
    small = small.at[2:4, :heads].set(attn_bias.astype(jnp.float32))
    small, *full = gather_all(line, shards, [small, w_qkv, w_out, w_in, w_down])
    qkv, out, into, down = (part.reshape(-1, part.shape[2]) for part in full)
    low = small.astype(jnp.bfloat16)
    bias = jnp.swapaxes(low[:, 2:4, :heads], 0, 1).reshape(2, -1)
    return (low[:, 0].reshape(-1), qkv, bias, out, low[:, 1].reshape(-1), into, down)


def reduced(line, gain_one, qkv, bias, out, gain_two, into, down):
    if not line:
        grads = ((gain_one, 0), (qkv, 0), (bias, 1), (out, 0), (gain_two, 0), (into, 0), (down, 0))
        owned = [
            lax.psum_scatter(
                grad.astype(jnp.bfloat16), "shard", scatter_dimension=axis, tiled=True
            )
            for grad, axis in grads
        ]
        return tuple(lax.psum(part, "rep").astype(jnp.float32) for part in owned)
    shards = lax.axis_size("shard")
    heads = bias.shape[1] // shards
    small = jnp.zeros((shards, 16, 128), jnp.float32)
    small = small.at[:, 0].set(gain_one.reshape(shards, -1)).at[:, 1].set(gain_two.reshape(shards, -1))
    small = small.at[:, 2:4, :heads].set(jnp.swapaxes(bias.reshape(2, shards, heads), 0, 1))

    def cut(grad):
        return grad.astype(jnp.bfloat16).reshape(shards, -1, grad.shape[1])

    (sum_down,) = reduce_all(line, [cut(down)], 2)
    (sum_in,) = reduce_all(line, [cut(into)], 3)
    sum_out, sum_qkv, small = reduce_all(line, [cut(out), cut(qkv), small], 4)
    return (small[0], sum_qkv, small[2:4, :heads], sum_out, small[1], sum_in, sum_down)


def shards(
    line,
    tokens,
    lengths,
    variate_ids,
    time_ids,
    attn_gain,
    w_qkv,
    attn_bias,
    w_out,
    ffn_gain,
    w_in,
    w_down,
    cotangent,
):
    seq_count, length = variate_ids.shape
    row_count = seq_count * length
    gain_one, qkv_weight, bias_full, out_weight, gain_two, in_weight, down_weight = gathered(
        line, attn_gain, w_qkv, attn_bias, w_out, ffn_gain, w_in, w_down
    )
    positions = jnp.arange(length)
    key_valid = positions[None, :] < lengths[:, None]
    row_valid = key_valid.reshape(row_count, 1)
    cos_table, sin_table = rope_tables(time_ids.reshape(row_count), HEAD_DIM)
    inputs = tokens.astype(jnp.float32)
    inv_one = lax.rsqrt(jnp.mean(inputs * inputs, axis=1, keepdims=True) + norm_eps)
    normed_one = (inputs * inv_one * gain_one).astype(jnp.bfloat16)
    projected = jnp.dot(normed_one, qkv_weight, preferred_element_type=jnp.float32)
    shaped = projected.reshape(row_count, 3, HEADS, HEAD_DIM)
    query = rotate(shaped[:, 0], cos_table, sin_table).astype(jnp.bfloat16)
    key_rows = rotate(shaped[:, 1], cos_table, sin_table).astype(jnp.bfloat16)
    values = shaped[:, 2].astype(jnp.bfloat16)
    seq_shape = (seq_count, length, HEADS, HEAD_DIM)

    def forward_one(seq_items):
        one_query, one_keys, one_values, one_vars, one_valid = seq_items
        return attend_forward(one_query, one_keys, one_values, one_vars, one_valid, bias_full)

    attended, log_sums = lax.map(
        forward_one,
        (
            query.reshape(seq_shape),
            key_rows.reshape(seq_shape),
            values.reshape(seq_shape),
            variate_ids,
            key_valid,
        ),
    )
    attended_low = attended.reshape(row_count, D).astype(jnp.bfloat16)
    hidden = inputs + jnp.dot(attended_low, out_weight, preferred_element_type=jnp.float32)
    inv_two = lax.rsqrt(jnp.mean(hidden * hidden, axis=1, keepdims=True) + norm_eps)
    normed_two = (hidden * inv_two * gain_two).astype(jnp.bfloat16)
    gate_up = jnp.dot(normed_two, in_weight, preferred_element_type=jnp.float32)
    gate_part = gate_up[:, :FF]
    up_part = gate_up[:, FF:]
    sigmoid_gate = jax.nn.sigmoid(gate_part)
    swish_gate = gate_part * sigmoid_gate
    activated = (swish_gate * up_part).astype(jnp.bfloat16)
    result = (hidden + jnp.dot(activated, down_weight, preferred_element_type=jnp.float32)).astype(
        jnp.bfloat16
    )
    grad_rows = jnp.where(row_valid, cotangent, jnp.zeros_like(cotangent))
    grad_down = contract_rows(activated, grad_rows)
    d_act = times_transpose(grad_rows, down_weight)
    d_gate = d_act * up_part * sigmoid_gate * (1.0 + gate_part * (1.0 - sigmoid_gate))
    d_up = d_act * swish_gate
    d_gate_up = jnp.concatenate([d_gate, d_up], axis=1).astype(jnp.bfloat16)
    grad_in = contract_rows(normed_two, d_gate_up)
    d_normed_two = times_transpose(d_gate_up, in_weight)
    unit_two = hidden * inv_two
    grad_gain_two = jnp.sum(d_normed_two * unit_two, axis=0)
    scaled_two = d_normed_two * gain_two
    d_hidden = grad_rows.astype(jnp.float32) + inv_two * (
        scaled_two - unit_two * jnp.mean(scaled_two * unit_two, axis=1, keepdims=True)
    )
    d_branch = d_hidden.astype(jnp.bfloat16)
    grad_out = contract_rows(attended_low, d_branch)
    d_attended = times_transpose(d_branch, out_weight).astype(jnp.bfloat16)

    def backward_one(seq_items):
        one_query, one_keys, one_values, one_vars, one_valid, one_sums, one_grad = seq_items
        return attend_backward(
            one_query, one_keys, one_values, one_vars, one_valid, bias_full, one_sums, one_grad
        )

    d_query, d_keys, d_values, d_bias_seq = lax.map(
        backward_one,
        (
            query.reshape(seq_shape),
            key_rows.reshape(seq_shape),
            values.reshape(seq_shape),
            variate_ids,
            key_valid,
            log_sums,
            d_attended.reshape(seq_shape),
        ),
    )
    grad_bias = jnp.sum(d_bias_seq, axis=0)
    d_query = rotate_back(d_query.reshape(row_count, HEADS, HEAD_DIM), cos_table, sin_table)
    d_keys = rotate_back(d_keys.reshape(row_count, HEADS, HEAD_DIM), cos_table, sin_table)
    d_projected = (
        jnp.stack([d_query, d_keys, d_values.reshape(row_count, HEADS, HEAD_DIM)], axis=1)
        .reshape(row_count, 3 * D)
        .astype(jnp.bfloat16)
    )
    grad_qkv = contract_rows(normed_one, d_projected)
    d_normed_one = times_transpose(d_projected, qkv_weight)
    unit_one = inputs * inv_one
    grad_gain_one = jnp.sum(d_normed_one * unit_one, axis=0)
    scaled_one = d_normed_one * gain_one
    grad_tokens = d_hidden + inv_one * (
        scaled_one - unit_one * jnp.mean(scaled_one * unit_one, axis=1, keepdims=True)
    )
    sum_gain_one, sum_qkv, sum_bias, sum_out, sum_gain_two, sum_in, sum_down = reduced(
        line, grad_gain_one, grad_qkv, grad_bias, grad_out, grad_gain_two, grad_in, grad_down
    )
    return (
        result,
        grad_tokens,
        sum_gain_one,
        sum_qkv,
        sum_bias,
        sum_out,
        sum_gain_two,
        sum_in,
        sum_down,
    )


def solution(mesh):
    placed = (
        P(("shard", "rep"), None),
        P(("shard", "rep")),
        P(("shard", "rep"), None),
        P(("shard", "rep"), None),
        P("shard"),
        P("shard", None),
        P(None, "shard"),
        P("shard", None),
        P("shard"),
        P("shard", None),
        P("shard", None),
        P(("shard", "rep"), None),
    )
    line = mesh.shape["shard"] // 2 if (mesh.shape["shard"], mesh.shape["rep"]) == (8, 4) else 0
    return jax.shard_map(
        functools.partial(shards, line),
        mesh=mesh,
        in_specs=placed,
        out_specs=(
            P(("shard", "rep"), None),
            P(("shard", "rep"), None),
            P("shard"),
            P("shard", None),
            P(None, "shard"),
            P("shard", None),
            P("shard"),
            P("shard", None),
            P("shard", None),
        ),
        check_vma=False,
    )
```

```python
import functools

import jax
import jax.numpy as jnp
from jax import lax
from jax.experimental import pallas as pl
from jax.experimental.pallas import tpu as pltpu
from jax.sharding import PartitionSpec as P

HEADS = 16
HEAD_DIM = 64


norm_eps = 1e-06
rope_base = 10000.0
masked_score = -1000000000.0

MESH = pl.DeviceIdType.MESH
ANY = pl.BlockSpec(memory_space=pl.ANY)


class Net:
    def __init__(self, line):
        shard, rep = lax.axis_index("shard"), lax.axis_index("rep")
        self.line = line
        self.z, self.y = shard // 2, shard % 2
        self.x, self.core = rep // 2, rep % 2
        self.own = shard
        self.sibling = (shard, self.x * 2 + 1 - self.core)
        self.across_x = (shard, (1 - self.x) * 2 + self.core)
        self.across_y = (self.z * 2 + 1 - self.y, rep)
        self.above = (jnp.minimum(self.z + 1, line - 1) * 2 + self.y, rep)
        self.below = (jnp.maximum(self.z - 1, 0) * 2 + self.y, rep)
        self.has_above = self.z < line - 1
        self.has_below = self.z > 0

    def greet(self):
        barrier = pltpu.get_barrier_semaphore()

        def hail(partner):
            pl.semaphore_signal(barrier, inc=1, device_id=partner, device_id_type=MESH)

        for partner in (self.sibling, self.across_x, self.across_y):
            hail(partner)
        pl.when(self.has_above)(lambda: hail(self.above))
        pl.when(self.has_below)(lambda: hail(self.below))
        neighbours = jnp.where(self.has_above, 1, 0) + jnp.where(self.has_below, 1, 0)
        pl.semaphore_wait(barrier, 3 + neighbours)


def aligned(value, step):
    return pl.multiple_of(value, step)


def gather_count(line):
    return 2 * line + 3 * 2 * line


def gather_steps(net, source, full, local_sem, send_sem, recv_sem):
    line = net.line
    half, columns = source.shape[0] // 2, source.shape[1]
    split = columns % 1024 == 0
    only = columns * 3 // 8 if split else 0
    shared = columns - 2 * only
    rows = pl.ds(aligned(net.core * half, half), half)
    carried = pl.ds(aligned(net.x * only, 128), only + shared) if split else pl.ds(0, columns)
    lone = pl.ds(aligned(net.x * (only + shared), 128), only) if split else None

    def remote(origin, landing, index, target):
        return pltpu.make_async_remote_copy(
            src_ref=origin,
            dst_ref=landing,
            send_sem=send_sem.at[index],
            recv_sem=recv_sem.at[index],
            device_id=target,
            device_id_type=MESH,
        )

    def piece(z, y):
        return full.at[z * 2 + y, rows, carried]

    def over_z(z, target, base):
        return remote(piece(z, net.y), piece(z, net.y), base + z, target)

    def over_y(z):
        return remote(piece(z, net.y), piece(z, net.y), 2 * line + z, net.across_y)

    def over_x(z, y):
        part = full.at[z * 2 + y, rows, lone]
        return remote(part, part, 3 * line + y * line + z, net.across_x)

    def to_core(z, y):
        part = full.at[z * 2 + y, rows]
        return remote(part, part, 5 * line + y * line + z, net.sibling)

    mine = source.at[rows, carried]
    local = pltpu.make_async_copy(source, full.at[net.own], local_sem)
    first_y = remote(mine, piece(net.z, net.y), 2 * line + net.z, net.across_y)
    first_up = remote(mine, piece(net.z, net.y), net.z, net.above)
    first_down = remote(mine, piece(net.z, net.y), line + net.z, net.below)

    def onward(z, y):
        if split:
            over_x(z, y).start()
        else:
            to_core(z, y).start()

    def start():
        first_y.start()
        pl.when(net.has_above)(first_up.start)
        pl.when(net.has_below)(first_down.start)
        local.start()

    def arrive(hops):
        @pl.when(net.z >= hops)
        def _():
            z = net.z - hops
            over_z(z, net.above, 0).wait_recv()
            pl.when(net.has_above)(over_z(z, net.above, 0).start)
            over_y(z).start()
            onward(z, net.y)

        @pl.when(net.z < line - hops)
        def _():
            z = net.z + hops
            over_z(z, net.below, line).wait_recv()
            pl.when(net.has_below)(over_z(z, net.below, line).start)
            over_y(z).start()
            onward(z, net.y)

    def arrive_y(hops):
        def one(z):
            remote(piece(z, 1 - net.y), piece(z, 1 - net.y), 2 * line + z, net.across_y).wait_recv()
            onward(z, 1 - net.y)

        if hops == 0:
            one(net.z)
        else:
            pl.when(net.z >= hops)(lambda: one(net.z - hops))
            pl.when(net.z < line - hops)(lambda: one(net.z + hops))

    def arrive_x(hops, own_y):
        def one(z):
            y = net.y if own_y else 1 - net.y
            part = full.at[z * 2 + y, rows, pl.ds(aligned((1 - net.x) * (only + shared), 128), only)]
            remote(part, part, 3 * line + y * line + z, net.across_x).wait_recv()
            to_core(z, y).start()

        if not split:
            return
        if hops == 0:
            one(net.z)
        else:
            pl.when(net.z >= hops)(lambda: one(net.z - hops))
            pl.when(net.z < line - hops)(lambda: one(net.z + hops))

    def step(hops):
        def run():
            arrive_y(hops - 1)
            if hops < line:
                arrive(hops)
            if hops >= 2:
                arrive_x(hops - 2, False)
                arrive_x(hops - 1, True)

        return run

    def last():
        arrive_x(line - 1, False)

    def finish():
        local.wait()
        first_y.wait_send()

        @pl.when(net.has_above)
        def _():
            first_up.wait_send()
            for hops in range(1, line - 1):
                pl.when(net.z >= hops)(over_z(net.z - hops, net.above, 0).wait_send)

        @pl.when(net.has_below)
        def _():
            first_down.wait_send()
            for hops in range(1, line - 1):
                pl.when(net.z < line - hops)(over_z(net.z + hops, net.below, line).wait_send)

        for z in range(line):

            def others():
                over_y(z).wait_send()
                if split:
                    over_x(z, net.y).wait_send()
                to_core(z, net.y).wait()

            pl.when(net.z != z)(others)
            if split:
                over_x(z, 1 - net.y).wait_send()
            to_core(z, 1 - net.y).wait()

    return [start] + [step(hops) for hops in range(1, line + 1)] + [last, finish]


def gather_scratch(line, tensors):
    copies = gather_count(line)
    return [
        pltpu.SemaphoreType.DMA((tensors,)),
        pltpu.SemaphoreType.DMA((tensors, copies)),
        pltpu.SemaphoreType.DMA((tensors, copies)),
    ]


REDUCE_BUFFERS = 9


def reduce_split(columns):
    only = columns // 4 if columns % 512 == 0 else 0
    return only, columns - 2 * only


def reduce_scratch(line, shards, half, columns, dtype):
    only, shared = reduce_split(columns)
    carried = only + shared
    return [
        pltpu.VMEM((shards, half, columns), dtype),
        pltpu.VMEM((shards, half, columns), dtype),
        pltpu.VMEM((shards, half, max(only, 128)), dtype),
        pltpu.VMEM((line, half, carried), dtype),
        pltpu.VMEM((line + 1, half, carried), dtype),
        pltpu.VMEM((half, carried), dtype),
        pltpu.VMEM((half, columns), dtype),
        pltpu.VMEM((half, columns), dtype),
        pltpu.VMEM((2 * half, columns), jnp.float32),
    ]


def reduce_count(line):
    return 3 * line + 4


def reduce_steps(net, grad, out, column_start, out_start, buffers, local_sem, send_sem, recv_sem):
    kept, got, from_x, from_y, from_z, late_x, final, swapped, wide = buffers
    line = net.line
    shards, half, width = kept.shape
    only, shared = reduce_split(width)
    both = only + shared
    columns = pl.ds(column_start, width)
    mine = pl.ds(aligned(net.core * half, half), half)
    theirs = pl.ds(aligned((1 - net.core) * half, half), half)
    if only:
        carried = pl.ds(aligned(net.x * only, 128), both)
        lone = pl.ds(aligned(net.x * both, 128), only)
        their_lone = pl.ds(aligned((1 - net.x) * both, 128), only)
    else:
        carried = pl.ds(0, width)

    def remote(origin, landing, index, target):
        return pltpu.make_async_remote_copy(
            src_ref=origin,
            dst_ref=landing,
            send_sem=send_sem.at[index],
            recv_sem=recv_sem.at[index],
            device_id=target,
            device_id_type=MESH,
        )

    local = pltpu.make_async_copy(grad.at[:, mine, columns], kept, local_sem.at[0])
    halves = remote(grad.at[:, theirs, columns], got, 2 * line, net.sibling)
    written = pltpu.make_async_copy(wide, out.at[:, pl.ds(out_start, width)], local_sem.at[1])
    to_core = remote(final, swapped, 2 * line + 1, net.sibling)
    end_x = remote(kept.at[net.own, :, carried], late_x, 2 * line + 2, net.across_x)
    if only:
        over_x = remote(kept.at[:, :, their_lone], from_x, 2 * line + 3, net.across_x)

    def over_y(z):
        part = kept.at[z * 2 + 1 - net.y, :, carried]
        return remote(part, from_y.at[z], 2 * line + 4 + z, net.across_y)

    def up(z):
        return remote(kept.at[z * 2 + net.y, :, carried], from_z.at[z + 1], z, net.above)

    def down(z):
        return remote(kept.at[z * 2 + net.y, :, carried], from_z.at[z], line + z, net.below)

    def add(shard, part):
        kept[shard, :, carried] = kept[shard, :, carried] + part

    def first():
        halves.start()
        local.start()

    def second():
        local.wait()
        halves.wait_recv()

        @pl.loop(0, shards)
        def _(shard):
            kept[shard] = kept[shard] + got[shard]

        if only:
            over_x.start()

    def third():
        if only:
            over_x.wait_recv()

            @pl.loop(0, shards)
            def _(shard):
                kept[shard, :, lone] = kept[shard, :, lone] + from_x[shard]

        for z in range(line):
            over_y(z).start()

    def fourth():
        for z in range(line):
            over_y(z).wait_recv()

        @pl.loop(0, line)
        def _(z):
            add(z * 2 + net.y, from_y[z])

    def hop(step):
        def run():
            @pl.when(net.z == step)
            def _():
                for z in range(line - 1, step, -1):
                    if step > 0:
                        up(z).wait_recv()
                        add(z * 2 + net.y, from_z[z + 1])
                    up(z).start()

            @pl.when(net.z == line - 1 - step)
            def _():
                for z in range(line - 1 - step):
                    if step > 0:
                        down(z).wait_recv()
                        add(z * 2 + net.y, from_z[z])
                    down(z).start()

        return run

    def land():
        @pl.when(net.has_below)
        def _():
            up(net.z).wait_recv()
            add(net.own, from_z[net.z + 1])

        @pl.when(net.has_above)
        def _():
            down(net.z).wait_recv()
            add(net.own, from_z[net.z])

        end_x.start()

    def meet():
        end_x.wait_recv()
        if only:
            final[:, lone] = kept[net.own, :, lone]
            for x in range(2):

                @pl.when(net.x == x)
                def _():
                    start = 0 if x == 1 else shared
                    final[:, (1 - x) * both : (1 - x) * both + only] = late_x[:, start : start + only]
                    other = shared * 0 + (only if x == 1 else 0)
                    final[:, only:both] = kept[net.own, :, only:both] + late_x[:, other : other + shared]
        else:
            final[...] = kept[net.own] + late_x[...]
        to_core.start()
        wide[mine, :] = final[...].astype(jnp.float32)

    def swap():
        to_core.wait_recv()
        wide[theirs, :] = swapped[...].astype(jnp.float32)
        written.start()

    def finish():
        written.wait()
        halves.wait_send()
        if only:
            over_x.wait_send()
        for z in range(line):
            over_y(z).wait_send()
            pl.when(net.z < z)(up(z).wait_send)
            pl.when(net.z > z)(down(z).wait_send)
        end_x.wait_send()
        to_core.wait_send()

    hops = [hop(step) for step in range(line - 1)]

    def fourth_and_hop():
        fourth()
        hops[0]()

    return [first, second, third, fourth_and_hop] + hops[1:] + [land, meet, swap, finish]


def staggered(step_lists, gap=1):
    ticks = (len(step_lists) - 1) * gap + max(len(steps) for steps in step_lists)
    out = []
    for tick in range(ticks):
        row = []
        for index, steps in enumerate(step_lists):
            at = tick - index * gap
            if 0 <= at < len(steps):
                row.append(steps[at])
        out.append(row)
    return out


def reduce_chunks(shape):
    shards, rows, columns = shape
    width = columns
    while width % 1024 == 0 and shards * (rows // 2) * width > (1 << 19):
        width //= 2
    return width, columns // width


ROWS_BY_ROWS = (((0,), (0,)), ((), ()))
COLUMNS_BY_COLUMNS = (((1,), (1,)), ((), ()))


def product(first_op, second_op, dims=(((1,), (0,)), ((), ()))):
    return lax.dot_general(first_op, second_op, dims, preferred_element_type=jnp.float32)


def inverse_rms(values):
    return lax.rsqrt(jnp.mean(values * values, axis=1, keepdims=True) + norm_eps)


class Carried:
    def __init__(self, line, collective, gathers=(), reduces=()):
        self.line, self.collective = line, collective
        self.gathers, self.reduces = list(gathers), list(reduces)
        self.operands = list(self.gathers)
        self.results = []
        shards = lax.axis_size("shard")
        for part in self.gathers:
            self.results.append(jax.ShapeDtypeStruct((shards,) + part.shape, part.dtype))
        self.scratch = gather_scratch(line, len(self.gathers)) if self.gathers else []
        self.plans = []
        chunks = 0
        for grads in self.reduces:
            plan = [reduce_chunks(grad.shape) for grad in grads]
            self.plans.append(plan)
            chunks += sum(count for _, count in plan)
            self.operands += grads
            columns = sum(grad.shape[2] for grad in grads)
            self.results.append(jax.ShapeDtypeStruct((grads[0].shape[1], columns), jnp.float32))
        if chunks:
            copies = reduce_count(line)
            self.scratch += [
                pltpu.SemaphoreType.DMA((chunks, 2)),
                pltpu.SemaphoreType.DMA((chunks, copies)),
                pltpu.SemaphoreType.DMA((chunks, copies)),
            ]
        for grads, plan in zip(self.reduces, self.plans):
            for grad, (width, count) in zip(grads, plan):
                for _ in range(count):
                    self.scratch += reduce_scratch(line, grad.shape[0], grad.shape[1] // 2, width, grad.dtype)

    def rows(self, net, operands, results, scratch):
        lists = []
        if self.gathers:
            local, send, recv = scratch[:3]
            scratch = scratch[3:]
            for index in range(len(self.gathers)):
                lists.append(
                    gather_steps(
                        net, operands[index], results[index], local.at[index], send.at[index], recv.at[index]
                    )
                )
        operands, results = operands[len(self.gathers) :], results[len(self.gathers) :]
        if self.reduces:
            local, send, recv = scratch[:3]
            scratch = scratch[3:]
        number = 0
        for target, (grads, plan) in enumerate(zip(self.reduces, self.plans)):
            start = 0
            for grad, (width, count) in zip(grads, plan):
                source = operands[0]
                operands = operands[1:]
                for chunk in range(count):
                    lists.append(
                        reduce_steps(
                            net,
                            source,
                            results[target],
                            chunk * width,
                            start + chunk * width,
                            scratch[:REDUCE_BUFFERS],
                            local.at[number],
                            send.at[number],
                            recv.at[number],
                        )
                    )
                    scratch = scratch[REDUCE_BUFFERS:]
                    number += 1
                start += grad.shape[2]
        return staggered(lists)


def carry(body, carried, *, grid, out_shape, in_specs, out_specs, scratch_shapes, name, operands, head=0):
    if carried is None:
        return list(
            pl.pallas_call(
                body,
                grid=(grid,),
                out_shape=out_shape,
                in_specs=in_specs,
                out_specs=out_specs,
                scratch_shapes=scratch_shapes,
                compiler_params=pltpu.CompilerParams(vmem_limit_bytes=60 << 20),
                name=name,
            )(*operands)
        ), []
    counts = [len(in_specs), len(carried.operands), len(out_specs), len(carried.results), len(scratch_shapes)]
    ends = [sum(counts[: i + 1]) for i in range(len(counts))]

    def kernel(*refs):
        own_in, more_in = refs[: ends[0]], refs[ends[0] : ends[1]]
        own_out, more_out = refs[ends[1] : ends[2]], refs[ends[2] : ends[3]]
        own_scratch, more_scratch = refs[ends[3] : ends[4]], refs[ends[4] :]
        step = pl.program_id(0)
        net = Net(carried.line)
        rows = carried.rows(net, more_in, more_out, more_scratch)
        pl.when(step == 0)(net.greet)
        middle = rows[:-1]
        at = [head + (index * (grid - head)) // len(middle) for index in range(len(middle))]
        at[0] = 0
        for place in sorted(set(at)):

            @pl.when(step == place)
            def _():
                for index, row in enumerate(middle):
                    if at[index] == place:
                        for action in row:
                            action()

        body(*own_in, *own_out, *own_scratch)

        @pl.when(step == grid - 1)
        def _():
            for action in rows[-1]:
                action()

    results = pl.pallas_call(
        kernel,
        grid=(grid,),
        out_shape=list(out_shape) + carried.results,
        in_specs=list(in_specs) + [ANY] * len(carried.operands),
        out_specs=list(out_specs) + [ANY] * len(carried.results),
        scratch_shapes=list(scratch_shapes) + carried.scratch,
        compiler_params=pltpu.CompilerParams(
            collective_id=carried.collective, has_side_effects=True, vmem_limit_bytes=63 << 20
        ),
        name=name,
    )(*operands, *carried.operands)
    return list(results[: len(out_shape)]), list(results[len(out_shape) :])


def carry_alone(carried, name):
    return carry(
        lambda: None,
        carried,
        grid=1,
        out_shape=[],
        in_specs=[],
        out_specs=[],
        scratch_shapes=[],
        name=name,
        operands=[],
    )[1]


def whole(*shape):
    return pl.BlockSpec(shape, lambda step: (0,) * len(shape), pipeline_mode=pl.Buffered(1))


def like(shape, dtype):
    return jax.ShapeDtypeStruct(shape, dtype)


def project_kernel(turned, x_ref, gain_ref, w_ref, cos_ref, sin_ref, out_ref, normed_ref):
    step = pl.program_id(0)

    @pl.when(step == 0)
    def _():
        values = x_ref[...].astype(jnp.float32)
        normed = values * inverse_rms(values) * gain_ref[...]
        normed_ref[...] = normed.T.astype(jnp.bfloat16)

    out = product(w_ref[...], normed_ref[...], ROWS_BY_ROWS)

    @pl.when(step < turned)
    def _():
        cos, sin = cos_ref[...], sin_ref[...]
        half = cos.shape[0]
        for start in range(0, out.shape[0], 2 * half):
            first, second = out[start : start + half], out[start + half : start + 2 * half]
            out_ref[start : start + half, :] = (first * cos - second * sin).astype(jnp.bfloat16)
            out_ref[start + half : start + 2 * half, :] = (second * cos + first * sin).astype(jnp.bfloat16)

    @pl.when(step >= turned)
    def _():
        out_ref[...] = out.astype(jnp.bfloat16)


def project(x, gain, weight, cos_t, sin_t, carried):
    rows, width = x.shape
    columns = weight.shape[1]
    block = 512
    return carry(
        functools.partial(project_kernel, 2 * width // block),
        carried,
        grid=columns // block,
        out_shape=[like((columns, rows), jnp.bfloat16), like((width, rows), jnp.bfloat16)],
        in_specs=[
            whole(rows, width),
            whole(1, width),
            pl.BlockSpec((width, block), lambda step: (0, step)),
            whole(*cos_t.shape),
            whole(*sin_t.shape),
        ],
        out_specs=[
            pl.BlockSpec((block, rows), lambda step: (step, 0)),
            pl.BlockSpec((width, rows), lambda step: (0, 0)),
        ],
        scratch_shapes=[],
        name="project",
        operands=[x, gain, weight, cos_t, sin_t],
    )


def branch_kernel(att_ref, w_ref, x_ref, gain_ref, hidden_ref, normed_ref):
    hidden = x_ref[...].astype(jnp.float32) + product(att_ref[...], w_ref[...], ROWS_BY_ROWS)
    hidden_ref[...] = hidden
    normed_ref[...] = (hidden * inverse_rms(hidden) * gain_ref[...]).astype(jnp.bfloat16)


def branch(attended_t, weight, x, gain, carried):
    rows, width = x.shape
    block = 256
    row = pl.BlockSpec((block, width), lambda step: (step, 0))
    return carry(
        branch_kernel,
        carried,
        grid=rows // block,
        out_shape=[like((rows, width), jnp.float32), like((rows, width), jnp.bfloat16)],
        in_specs=[
            pl.BlockSpec((width, block), lambda step: (0, step)),
            whole(*weight.shape),
            row,
            whole(1, width),
        ],
        out_specs=[row, row],
        scratch_shapes=[],
        name="branch",
        operands=[attended_t, weight, x, gain],
    )


def widen_kernel(normed_ref, gate_ref, up_ref, act_ref, to_gate_ref, to_up_ref):
    normed = normed_ref[...]
    gate = product(normed, gate_ref[...])
    up = product(normed, up_ref[...])
    sigmoid = jax.nn.sigmoid(gate)
    swish = gate * sigmoid
    act_ref[...] = (swish * up).astype(jnp.bfloat16)
    to_gate_ref[...] = (up * sigmoid * (1.0 + gate * (1.0 - sigmoid))).astype(jnp.bfloat16)
    to_up_ref[...] = swish.astype(jnp.bfloat16)


def widen(normed, weight, carried):
    rows, width = normed.shape
    inner = weight.shape[1] // 2
    block = 512
    steps = inner // block
    part = pl.BlockSpec((rows, block), lambda step: (0, step))
    return carry(
        widen_kernel,
        carried,
        grid=steps,
        out_shape=[like((rows, inner), jnp.bfloat16)] * 3,
        in_specs=[
            whole(rows, width),
            pl.BlockSpec((width, block), lambda step: (0, step)),
            pl.BlockSpec((width, block), lambda step: (0, steps + step)),
        ],
        out_specs=[part] * 3,
        scratch_shapes=[],
        name="widen",
        operands=[normed, weight, weight],
    )


def narrow_kernel(
    steps, act_ref, to_gate_ref, to_up_ref, w_ref, given_ref, hidden_ref, result_ref, grad_ref, d_gate_ref, d_up_ref, acc_ref
):
    step = pl.program_id(0)
    act, weight, given = act_ref[...], w_ref[...], given_ref[...]
    part = product(act, weight)

    @pl.when(step == 0)
    def _():
        acc_ref[...] = hidden_ref[...] + part

    @pl.when(step > 0)
    def _():
        acc_ref[...] += part

    @pl.when(step == steps - 1)
    def _():
        result_ref[...] = acc_ref[...].astype(jnp.bfloat16)

    grad_ref[...] = product(act, given, ROWS_BY_ROWS).astype(jnp.bfloat16)
    d_act = product(given, weight, COLUMNS_BY_COLUMNS)
    d_gate_ref[...] = (d_act * to_gate_ref[...].astype(jnp.float32)).astype(jnp.bfloat16)
    d_up_ref[...] = (d_act * to_up_ref[...].astype(jnp.float32)).astype(jnp.bfloat16)


def narrow(act, to_gate, to_up, weight, given, hidden, carried):
    rows, inner = act.shape
    width = weight.shape[1]
    block = 512
    steps = inner // block
    part = pl.BlockSpec((rows, block), lambda step: (0, step))
    down = pl.BlockSpec((block, width), lambda step: (step, 0))
    return carry(
        functools.partial(narrow_kernel, steps),
        carried,
        grid=steps,
        out_shape=[
            like((rows, width), jnp.bfloat16),
            like((inner, width), jnp.bfloat16),
            like((rows, inner), jnp.bfloat16),
            like((rows, inner), jnp.bfloat16),
        ],
        in_specs=[part, part, part, down, whole(rows, width), whole(rows, width)],
        out_specs=[pl.BlockSpec((rows, width), lambda step: (0, 0)), down, part, part],
        scratch_shapes=[pltpu.VMEM((rows, width), jnp.float32)],
        name="narrow",
        operands=[act, to_gate, to_up, weight, given, hidden],
    )


def grad_in_kernel(normed_ref, d_gate_ref, d_up_ref, to_gate_ref, to_up_ref, turned_ref):
    @pl.when(pl.program_id(0) == 0)
    def _():
        turned_ref[...] = normed_ref[...].T

    to_gate_ref[...] = product(turned_ref[...], d_gate_ref[...]).astype(jnp.bfloat16)
    to_up_ref[...] = product(turned_ref[...], d_up_ref[...]).astype(jnp.bfloat16)


def grad_into(normed, d_gate, d_up, carried):
    rows, width = normed.shape
    inner = d_gate.shape[1]
    block = 512
    part = pl.BlockSpec((rows, block), lambda step: (0, step))
    out = pl.BlockSpec((width, block), lambda step: (0, step))
    return carry(
        grad_in_kernel,
        carried,
        grid=inner // block,
        out_shape=[like((width, inner), jnp.bfloat16)] * 2,
        in_specs=[whole(rows, width), part, part],
        out_specs=[out, out],
        scratch_shapes=[pltpu.VMEM((width, rows), jnp.bfloat16)],
        name="grad_in",
        operands=[normed, d_gate, d_up],
    )


def norm_back(d_normed, values, gain):
    inverse = inverse_rms(values)
    unit = values * inverse
    scaled = d_normed * gain
    mean = jnp.mean(scaled * unit, axis=1, keepdims=True)
    return inverse * (scaled - unit * mean), jnp.sum(d_normed * unit, axis=0, keepdims=True)


def ffn_back_kernel(
    steps, d_gate_ref, d_up_ref, gate_ref, up_ref, hidden_ref, gain_ref, given_ref, d_hidden_ref, d_branch_ref, grad_gain_ref, acc_ref
):
    step = pl.program_id(0)
    part = product(d_gate_ref[...], gate_ref[...], COLUMNS_BY_COLUMNS)
    part = part + product(d_up_ref[...], up_ref[...], COLUMNS_BY_COLUMNS)

    @pl.when(step == 0)
    def _():
        acc_ref[...] = part

    @pl.when(step > 0)
    def _():
        acc_ref[...] += part

    @pl.when(step == steps - 1)
    def _():
        through, grad_gain = norm_back(acc_ref[...], hidden_ref[...], gain_ref[...])
        d_hidden = given_ref[...].astype(jnp.float32) + through
        d_hidden_ref[...] = d_hidden
        d_branch_ref[...] = d_hidden.astype(jnp.bfloat16)
        grad_gain_ref[...] = grad_gain


def ffn_back(d_gate, d_up, weight, hidden, gain, given, carried):
    rows, width = hidden.shape
    inner = d_gate.shape[1]
    block = 512
    steps = inner // block
    part = pl.BlockSpec((rows, block), lambda step: (0, step))
    full = pl.BlockSpec((rows, width), lambda step: (0, 0))
    return carry(
        functools.partial(ffn_back_kernel, steps),
        carried,
        grid=steps,
        out_shape=[
            like((rows, width), jnp.float32),
            like((rows, width), jnp.bfloat16),
            like((1, width), jnp.float32),
        ],
        in_specs=[
            part,
            part,
            pl.BlockSpec((width, block), lambda step: (0, step)),
            pl.BlockSpec((width, block), lambda step: (0, steps + step)),
            whole(rows, width),
            whole(1, width),
            whole(rows, width),
        ],
        out_specs=[full, full, pl.BlockSpec((1, width), lambda step: (0, 0))],
        scratch_shapes=[pltpu.VMEM((rows, width), jnp.float32)],
        name="ffn_back",
        operands=[d_gate, d_up, weight, weight, hidden, gain, given],
    )


def branch_back_kernel(att_ref, w_ref, d_branch_ref, grad_ref, given_ref):
    d_branch = d_branch_ref[...]
    grad_ref[...] = product(att_ref[...], d_branch).astype(jnp.bfloat16)
    given_ref[...] = product(w_ref[...], d_branch, COLUMNS_BY_COLUMNS).astype(jnp.bfloat16)


def branch_back(attended_t, weight, d_branch, carried):
    rows, width = d_branch.shape
    block = 256
    out = pl.BlockSpec((block, width), lambda step: (step, 0))
    turned = pl.BlockSpec((block, rows), lambda step: (step, 0))
    return carry(
        branch_back_kernel,
        carried,
        grid=attended_t.shape[0] // block,
        out_shape=[like(weight.shape, jnp.bfloat16), like(attended_t.shape, jnp.bfloat16)],
        in_specs=[turned, out, whole(rows, width)],
        out_specs=[out, turned],
        scratch_shapes=[],
        name="branch_back",
        operands=[attended_t, weight, d_branch],
    )


def project_back_kernel(
    steps, normed_ref, dq_ref, dk_ref, dv_ref, w_ref, x_ref, gain_ref, d_hidden_ref, grad_ref, tokens_ref, grad_gain_ref, acc_ref
):
    step = pl.program_id(0)
    third = steps // 3

    def run(d_ref):
        d_part = d_ref[...]
        grad_ref[...] = product(normed_ref[...], d_part, COLUMNS_BY_COLUMNS).astype(jnp.bfloat16)
        part = product(w_ref[...], d_part)

        @pl.when(step == 0)
        def _():
            acc_ref[...] = part

        @pl.when(step > 0)
        def _():
            acc_ref[...] += part

    for index, d_ref in enumerate((dq_ref, dk_ref, dv_ref)):
        pl.when(step // third == index)(functools.partial(run, d_ref))

    @pl.when(step == steps - 1)
    def _():
        values = x_ref[...].astype(jnp.float32)
        through, grad_gain = norm_back(acc_ref[...].T, values, gain_ref[...])
        tokens_ref[...] = d_hidden_ref[...] + through
        grad_gain_ref[...] = grad_gain


def project_back(normed_t, dq, dk, dv, weight, x, gain, d_hidden, carried):
    rows, width = x.shape
    columns = weight.shape[1]
    block = 512
    steps = columns // block
    third = steps // 3
    full = pl.BlockSpec((rows, width), lambda step: (0, 0))

    def part(which):
        return pl.BlockSpec(
            (block, rows), lambda step: (jnp.clip(step - which * third, 0, third - 1), 0)
        )

    return carry(
        functools.partial(project_back_kernel, steps),
        carried,
        grid=steps,
        out_shape=[
            like((width, columns), jnp.bfloat16),
            like((rows, width), jnp.float32),
            like((1, width), jnp.float32),
        ],
        in_specs=[
            whole(*normed_t.shape),
            part(0),
            part(1),
            part(2),
            pl.BlockSpec((width, block), lambda step: (0, step)),
            whole(rows, width),
            whole(1, width),
            whole(rows, width),
        ],
        out_specs=[
            pl.BlockSpec((width, block), lambda step: (0, step)),
            full,
            pl.BlockSpec((1, width), lambda step: (0, 0)),
        ],
        scratch_shapes=[pltpu.VMEM((width, rows), jnp.float32)],
        name="project_back",
        operands=[normed_t, dq, dk, dv, weight, x, gain, d_hidden],
    )


LOG2E = 1.4426950408889634
FEATURES = 16


def two_parts(value):
    high = value.astype(jnp.bfloat16)
    return high, (value - high.astype(jnp.float32)).astype(jnp.bfloat16)


def three_parts(value):
    high, rest = value.astype(jnp.bfloat16), None
    rest = value - high.astype(jnp.float32)
    middle = rest.astype(jnp.bfloat16)
    return high, middle, (rest - middle.astype(jnp.float32)).astype(jnp.bfloat16)


def key_features(variates, valid):
    length = variates.shape[1]
    masks = [(variates == v).astype(jnp.float32) for v in range(4)]
    ones = jnp.ones((1, length), jnp.float32)
    invalid = 1.0 - valid
    rows = masks + masks + [invalid, ones, ones, ones, jnp.zeros((FEATURES - 12, length), jnp.float32)]
    return jnp.concatenate(rows, axis=0).astype(jnp.bfloat16)


def query_features(variates, same, other, log_sums):
    length = variates.shape[1]
    highs, lows = [], []
    for v in range(4):
        bias = jnp.where(variates == v, same, other) * LOG2E
        high, low = two_parts(bias)
        highs.append(high.astype(jnp.float32))
        lows.append(low.astype(jnp.float32))
    if log_sums is None:
        minus = [jnp.zeros((3, length), jnp.float32)]
    else:
        minus = [part.astype(jnp.float32) for part in three_parts(-log_sums)]
    mask = jnp.full((1, length), masked_score, jnp.float32)
    rows = highs + lows + [mask] + minus + [jnp.zeros((FEATURES - 12, length), jnp.float32)]
    return jnp.concatenate(rows, axis=0).astype(jnp.bfloat16)


def contract_depth(first_op, second_op):
    return lax.dot_general(
        first_op, second_op, (((1,), (0,)), ((), ())), preferred_element_type=jnp.float32
    )


def scaled_query(query_t, score_scale):
    return two_parts(query_t.astype(jnp.float32) * (score_scale * LOG2E))


def attend_kernel(blocks, bias_ref, q_ref, k_ref, v_ref, var_ref, valid_ref, o_ref, wide_ref, lse_ref, query_ref):
    head = pl.program_id(0)
    depth, length = q_ref.shape
    width = length // blocks
    same, other = bias_ref[0, head], bias_ref[1, head]
    variates = var_ref[...]
    high, low = scaled_query(q_ref[...], depth ** (-0.5))
    query_ref[...] = jnp.concatenate([high, low, query_features(variates, same, other, None)], axis=0)
    key_t = k_ref[...]
    keys = jnp.concatenate([key_t, key_t, key_features(variates, valid_ref[...])], axis=0).T
    ones = jnp.concatenate(
        [jnp.ones((1, length), jnp.float32), jnp.zeros((FEATURES - 1, length), jnp.float32)], axis=0
    ).astype(jnp.bfloat16)
    values = jnp.concatenate([v_ref[...], ones], axis=0)
    for block in range(blocks):
        at = pl.ds(block * width, width)
        scores = contract_depth(keys, query_ref[:, at])
        peak = jnp.max(scores, axis=0, keepdims=True)
        weights = jnp.exp2(scores - peak).astype(jnp.bfloat16)
        summed = contract_depth(values, weights)
        total = summed[depth : depth + 1]
        attended = summed[:depth] / total
        wide_ref[:, at] = attended
        o_ref[:, at] = attended.astype(jnp.bfloat16)
        lse_ref[0, :, at] = peak + jnp.log2(total)


def attend_forward(qkv_t, variates, valid, bias, heads, carried):
    rows, length = qkv_t.shape
    depth = rows // (3 * heads)

    def part(which):
        return pl.BlockSpec((depth, length), lambda head: (which * heads + head, 0))

    row = pl.BlockSpec((1, length), lambda head: (0, 0))
    return carry(
        functools.partial(attend_kernel, 1),
        carried,
        grid=heads,
        out_shape=[
            jax.ShapeDtypeStruct((heads * depth, length), jnp.bfloat16),
            jax.ShapeDtypeStruct((heads * depth, length), jnp.float32),
            jax.ShapeDtypeStruct((heads, 1, length), jnp.float32),
        ],
        in_specs=[
            pl.BlockSpec(memory_space=pltpu.SMEM),
            part(0),
            part(1),
            part(2),
            row,
            row,
        ],
        out_specs=[
            pl.BlockSpec((depth, length), lambda head: (head, 0)),
            pl.BlockSpec((depth, length), lambda head: (head, 0)),
            pl.BlockSpec((1, 1, length), lambda head: (head, 0, 0)),
        ],
        scratch_shapes=[pltpu.VMEM((2 * depth + FEATURES, length), jnp.bfloat16)],
        name="attend_forward",
        operands=[bias, qkv_t, qkv_t, qkv_t, variates, valid],
    )


def turn_back(grad_t, cos_t, sin_t):
    half = cos_t.shape[0]
    first, second = grad_t[:half], grad_t[half:]
    return jnp.concatenate(
        [first * cos_t + second * sin_t, second * cos_t - first * sin_t], axis=0
    )


def attend_back_kernel(
    blocks, bias_ref, q_ref, k_ref, v_ref, go_ref, wide_ref, lse_ref, var_ref, valid_ref, cos_ref, sin_ref,
    dq_ref, dk_ref, dv_ref, db_ref, query_ref, given_ref, dk_acc, dv_acc,
):
    head = pl.program_id(0)
    depth, length = q_ref.shape
    width = length // blocks
    scale = depth ** (-0.5)
    same, other = bias_ref[0, head], bias_ref[1, head]
    variates = var_ref[...]
    features = key_features(variates, valid_ref[...])
    high, low = scaled_query(q_ref[...], scale)
    query_ref[...] = jnp.concatenate([high, low, query_features(variates, same, other, lse_ref[0])], axis=0)
    key_t = k_ref[...]
    keys = jnp.concatenate([key_t, key_t, features], axis=0).T
    keys_low = jnp.concatenate([key_t, features], axis=0)
    given = go_ref[...]
    inner = jnp.sum(given.astype(jnp.float32) * wide_ref[...], axis=0, keepdims=True)
    minus = [part.astype(jnp.float32) for part in three_parts(-inner)]
    minus = jnp.concatenate(minus + [jnp.zeros((FEATURES - 3, length), jnp.float32)], axis=0)
    given_ref[...] = jnp.concatenate([given, minus.astype(jnp.bfloat16)], axis=0)
    ones = jnp.concatenate(
        [jnp.ones((3, length), jnp.float32), jnp.zeros((FEATURES - 3, length), jnp.float32)], axis=0
    ).astype(jnp.bfloat16)
    values = jnp.concatenate([v_ref[...], ones], axis=0).T
    query_rows = q_ref[...].T
    given_rows = given.T
    in_same = jnp.zeros((1, width), jnp.float32)
    in_other = jnp.zeros((1, width), jnp.float32)
    for block in range(blocks):
        at = pl.ds(block * width, width)
        cut = slice(block * width, (block + 1) * width)
        probs = jnp.exp2(contract_depth(keys, query_ref[:, at]))
        grads = (probs * contract_depth(values, given_ref[:, at])).astype(jnp.bfloat16)
        back = contract_depth(keys_low, grads)
        dq = turn_back(back[:depth] * scale, cos_ref[:, at], sin_ref[:, at])
        dq_ref[:, at] = dq.astype(jnp.bfloat16)
        for v in range(4):
            line = back[depth + v : depth + v + 1]
            hit = variates[:, cut] == v
            in_same = in_same + jnp.where(hit, line, 0.0)
            in_other = in_other + jnp.where(hit, 0.0, line)
        dk = contract_depth(grads, query_rows[cut])
        dv = contract_depth(probs.astype(jnp.bfloat16), given_rows[cut])
        if block == 0:
            dk_acc[...] = dk
            dv_acc[...] = dv
        else:
            dk_acc[...] += dk
            dv_acc[...] += dv
    dk_ref[...] = turn_back((dk_acc[...] * scale).T, cos_ref[...], sin_ref[...]).astype(jnp.bfloat16)
    dv_ref[...] = dv_acc[...].T.astype(jnp.bfloat16)
    db_ref[0, 0:1, :] = in_same
    db_ref[0, 1:2, :] = in_other


def attend_backward(qkv_t, given_t, wide_t, log_sums, variates, valid, bias, cos_t, sin_t, heads, carried):
    rows, length = qkv_t.shape
    depth = rows // (3 * heads)
    blocks = 1

    def part(which):
        return pl.BlockSpec((depth, length), lambda head: (which * heads + head, 0))

    one = pl.BlockSpec((depth, length), lambda head: (head, 0))
    grad = jax.ShapeDtypeStruct((heads * depth, length), jnp.bfloat16)
    return carry(
        functools.partial(attend_back_kernel, blocks),
        carried,
        grid=heads,
        out_shape=[grad, grad, grad, jax.ShapeDtypeStruct((heads, 2, length // blocks), jnp.float32)],
        in_specs=[
            pl.BlockSpec(memory_space=pltpu.SMEM),
            part(0),
            part(1),
            part(2),
            one,
            one,
            pl.BlockSpec((1, 1, length), lambda head: (head, 0, 0)),
            whole(1, length),
            whole(1, length),
            whole(depth // 2, length),
            whole(depth // 2, length),
        ],
        out_specs=[one, one, one, pl.BlockSpec((1, 2, length // blocks), lambda head: (head, 0, 0))],
        scratch_shapes=[
            pltpu.VMEM((2 * depth + FEATURES, length), jnp.bfloat16),
            pltpu.VMEM((depth + FEATURES, length), jnp.bfloat16),
            pltpu.VMEM((length, depth), jnp.float32),
            pltpu.VMEM((length, depth), jnp.float32),
        ],
        name="attend_backward",
        operands=[bias, qkv_t, qkv_t, qkv_t, given_t, wide_t, log_sums, variates, valid, cos_t, sin_t],
    )


def rope_tables(time_ids):
    half = HEAD_DIM // 2
    exponent = jnp.arange(half).astype(jnp.float32) * (2.0 / HEAD_DIM)
    inverse = jnp.exp(-jnp.log(rope_base) * exponent)
    angles = inverse[:, None] * time_ids.astype(jnp.float32)
    return jnp.cos(angles), jnp.sin(angles)


def pack_small(attn_gain, ffn_gain, attn_bias):
    heads = attn_bias.shape[1]
    small = jnp.zeros((16, 128), jnp.float32)
    small = small.at[0].set(attn_gain.astype(jnp.float32)).at[1].set(ffn_gain.astype(jnp.float32))
    return small.at[2:4, :heads].set(attn_bias.astype(jnp.float32))


def pack_grads(shards, gain_one, gain_two, bias):
    heads = bias.shape[1] // shards
    small = jnp.zeros((shards, 16, 128), jnp.float32)
    small = small.at[:, 0].set(gain_one.reshape(shards, -1)).at[:, 1].set(gain_two.reshape(shards, -1))
    return small.at[:, 2:4, :heads].set(jnp.swapaxes(bias.reshape(2, shards, heads), 0, 1))


def shards(
    line,
    tokens,
    lengths,
    variate_ids,
    time_ids,
    attn_gain,
    w_qkv,
    attn_bias,
    w_out,
    ffn_gain,
    w_in,
    w_down,
    cotangent,
):
    parts = lax.axis_size("shard")
    length = variate_ids.shape[1]
    heads = attn_bias.shape[1]
    positions = jnp.arange(length)[None, :]
    key_valid = positions < lengths[:, None]
    valid = key_valid.astype(jnp.float32)
    given = jnp.where(key_valid.reshape(length, 1), cotangent, jnp.zeros_like(cotangent))
    cos_t, sin_t = rope_tables(time_ids)

    def joined(part):
        return part.reshape(-1, part.shape[2])

    def cut(grad):
        return grad.reshape(parts, -1, grad.shape[1])

    def gathering(number, *weights):
        return Carried(line, number, gathers=weights) if line else None

    def reducing(number, *grads):
        return Carried(line, number, reduces=grads) if line else None

    if line:
        small, full_qkv = carry_alone(gathering(1, pack_small(attn_gain, ffn_gain, attn_bias), w_qkv), "gather_qkv")
        qkv_weight = joined(full_qkv)
        gain_one, gain_two = small[:, 0].reshape(1, -1), small[:, 1].reshape(1, -1)
        bias = jnp.swapaxes(small[:, 2:4, :heads], 0, 1).reshape(2, -1)
    else:
        gain_one, gain_two, qkv_weight, out_weight, in_weight, down_weight = (
            lax.all_gather(part, "shard", axis=0, tiled=True)
            for part in (attn_gain, ffn_gain, w_qkv, w_out, w_in, w_down)
        )
        bias = lax.all_gather(attn_bias, "shard", axis=1, tiled=True).astype(jnp.float32)
        gain_one = gain_one.astype(jnp.float32).reshape(1, -1)
        gain_two = gain_two.astype(jnp.float32).reshape(1, -1)

    (qkv_t, normed_t), came = project(tokens, gain_one, qkv_weight, cos_t, sin_t, gathering(2, w_out))
    out_weight = joined(came[0]) if line else out_weight
    (attended_t, wide_t, log_sums), came = attend_forward(
        qkv_t, variate_ids, valid, bias, HEADS, gathering(3, w_in)
    )
    in_weight = joined(came[0]) if line else in_weight
    (hidden, normed_two), _ = branch(attended_t, out_weight, tokens, gain_two, None)
    (act, to_gate, to_up), came = widen(normed_two, in_weight, gathering(4, w_down))
    down_weight = joined(came[0]) if line else down_weight
    (result, grad_down, d_gate, d_up), _ = narrow(act, to_gate, to_up, down_weight, given, hidden, None)
    (grad_gate, grad_up), _ = grad_into(normed_two, d_gate, d_up, None)
    (d_hidden, d_branch, grad_gain_two), came_down = ffn_back(
        d_gate, d_up, in_weight, hidden, gain_two, given, reducing(5, [cut(grad_down)])
    )
    (grad_out, given_t), _ = branch_back(attended_t, out_weight, d_branch, None)
    (dq, dk, dv, bias_parts), came_in = attend_backward(
        qkv_t,
        given_t,
        wide_t,
        log_sums,
        variate_ids,
        valid,
        bias,
        cos_t,
        sin_t,
        HEADS,
        reducing(6, [cut(grad_gate), cut(grad_up)]),
    )
    (grad_qkv, grad_tokens, grad_gain_one), came_out = project_back(
        normed_t, dq, dk, dv, qkv_weight, tokens, gain_one, d_hidden, reducing(7, [cut(grad_out)])
    )
    grad_bias = jnp.sum(bias_parts, axis=2).T
    if line:
        packed = pack_grads(parts, grad_gain_one, grad_gain_two, grad_bias)
        sum_qkv, small = carry_alone(reducing(8, [cut(grad_qkv)], [packed]), "reduce_qkv")
        return (
            result,
            grad_tokens,
            small[0],
            sum_qkv,
            small[2:4, :heads],
            came_out[0],
            small[1],
            came_in[0],
            came_down[0],
        )
    grads = (
        (grad_gain_one.reshape(-1), 0),
        (grad_qkv, 0),
        (grad_bias, 1),
        (grad_out, 0),
        (grad_gain_two.reshape(-1), 0),
        (jnp.concatenate([grad_gate, grad_up], axis=1), 0),
        (grad_down, 0),
    )
    owned = [
        lax.psum_scatter(grad.astype(jnp.bfloat16), "shard", scatter_dimension=axis, tiled=True)
        for grad, axis in grads
    ]
    return (result, grad_tokens) + tuple(lax.psum(part, "rep").astype(jnp.float32) for part in owned)


def solution(mesh):
    placed = (
        P(("shard", "rep"), None),
        P(("shard", "rep")),
        P(("shard", "rep"), None),
        P(("shard", "rep"), None),
        P("shard"),
        P("shard", None),
        P(None, "shard"),
        P("shard", None),
        P("shard"),
        P("shard", None),
        P("shard", None),
        P(("shard", "rep"), None),
    )
    line = mesh.shape["shard"] // 2 if (mesh.shape["shard"], mesh.shape["rep"]) == (8, 4) else 0
    return jax.shard_map(
        functools.partial(shards, line),
        mesh=mesh,
        in_specs=placed,
        out_specs=(
            P(("shard", "rep"), None),
            P(("shard", "rep"), None),
            P("shard"),
            P("shard", None),
            P(None, "shard"),
            P("shard", None),
            P("shard"),
            P("shard", None),
            P("shard", None),
        ),
        check_vma=False,
    )
```

```python
import functools

import jax
import jax.numpy as jnp
from jax import lax
from jax.experimental import pallas as pl
from jax.experimental.pallas import tpu as pltpu
from jax.sharding import PartitionSpec as P

HEADS = 16
HEAD_DIM = 64


norm_eps = 1e-06
rope_base = 10000.0
masked_score = -1000000000.0

MESH = pl.DeviceIdType.MESH
ANY = pl.BlockSpec(memory_space=pl.ANY)


class Net:
    def __init__(self, line):
        shard, rep = lax.axis_index("shard"), lax.axis_index("rep")
        self.line = line
        self.z, self.y = shard // 2, shard % 2
        self.x, self.core = rep // 2, rep % 2
        self.own = shard
        self.sibling = (shard, self.x * 2 + 1 - self.core)
        self.across_x = (shard, (1 - self.x) * 2 + self.core)
        self.across_y = (self.z * 2 + 1 - self.y, rep)
        self.above = (jnp.minimum(self.z + 1, line - 1) * 2 + self.y, rep)
        self.below = (jnp.maximum(self.z - 1, 0) * 2 + self.y, rep)
        self.has_above = self.z < line - 1
        self.has_below = self.z > 0

    def greet(self):
        barrier = pltpu.get_barrier_semaphore()

        def hail(partner):
            pl.semaphore_signal(barrier, inc=1, device_id=partner, device_id_type=MESH)

        for partner in (self.sibling, self.across_x, self.across_y):
            hail(partner)
        pl.when(self.has_above)(lambda: hail(self.above))
        pl.when(self.has_below)(lambda: hail(self.below))
        neighbours = jnp.where(self.has_above, 1, 0) + jnp.where(self.has_below, 1, 0)
        pl.semaphore_wait(barrier, 3 + neighbours)


def aligned(value, step):
    return pl.multiple_of(value, step)


def gather_count(line):
    return 2 * line + 3 * 2 * line


def gather_steps(net, source, full, local_sem, send_sem, recv_sem):
    line = net.line
    height, columns = source.shape
    half = height // 2
    split = columns % 1024 == 0
    only = columns * 3 // 8 if split else 0
    shared = columns - 2 * only
    rows = pl.ds(aligned(net.core * half, half), half)
    carried = pl.ds(aligned(net.x * only, 128), only + shared) if split else pl.ds(0, columns)
    lone = pl.ds(aligned(net.x * (only + shared), 128), only) if split else None

    def remote(origin, landing, index, target):
        return pltpu.make_async_remote_copy(
            src_ref=origin,
            dst_ref=landing,
            send_sem=send_sem.at[index],
            recv_sem=recv_sem.at[index],
            device_id=target,
            device_id_type=MESH,
        )

    def held(z, y, which=None):
        lines = pl.ds(aligned((z * 2 + y) * height + net.core * half, half), half)
        return full.at[lines] if which is None else full.at[lines, which]

    def piece(z, y):
        return held(z, y, carried)

    def over_z(z, target, base):
        return remote(piece(z, net.y), piece(z, net.y), base + z, target)

    def over_y(z):
        return remote(piece(z, net.y), piece(z, net.y), 2 * line + z, net.across_y)

    def over_x(z, y):
        part = held(z, y, lone)
        return remote(part, part, 3 * line + y * line + z, net.across_x)

    def to_core(z, y):
        part = held(z, y)
        return remote(part, part, 5 * line + y * line + z, net.sibling)

    mine = source.at[rows, carried]
    local = pltpu.make_async_copy(source, full.at[pl.ds(aligned(net.own * height, height), height)], local_sem)
    first_y = remote(mine, piece(net.z, net.y), 2 * line + net.z, net.across_y)
    first_up = remote(mine, piece(net.z, net.y), net.z, net.above)
    first_down = remote(mine, piece(net.z, net.y), line + net.z, net.below)

    def onward(z, y):
        if split:
            over_x(z, y).start()
        else:
            to_core(z, y).start()

    def start():
        first_y.start()
        pl.when(net.has_above)(first_up.start)
        pl.when(net.has_below)(first_down.start)
        local.start()

    def arrive(hops):
        @pl.when(net.z >= hops)
        def _():
            z = net.z - hops
            over_z(z, net.above, 0).wait_recv()
            pl.when(net.has_above)(over_z(z, net.above, 0).start)
            over_y(z).start()
            onward(z, net.y)

        @pl.when(net.z < line - hops)
        def _():
            z = net.z + hops
            over_z(z, net.below, line).wait_recv()
            pl.when(net.has_below)(over_z(z, net.below, line).start)
            over_y(z).start()
            onward(z, net.y)

    def arrive_y(hops):
        def one(z):
            remote(piece(z, 1 - net.y), piece(z, 1 - net.y), 2 * line + z, net.across_y).wait_recv()
            onward(z, 1 - net.y)

        if hops == 0:
            one(net.z)
        else:
            pl.when(net.z >= hops)(lambda: one(net.z - hops))
            pl.when(net.z < line - hops)(lambda: one(net.z + hops))

    def arrive_x(hops, own_y):
        def one(z):
            y = net.y if own_y else 1 - net.y
            part = held(z, y, pl.ds(aligned((1 - net.x) * (only + shared), 128), only))
            remote(part, part, 3 * line + y * line + z, net.across_x).wait_recv()
            to_core(z, y).start()

        if not split:
            return
        if hops == 0:
            one(net.z)
        else:
            pl.when(net.z >= hops)(lambda: one(net.z - hops))
            pl.when(net.z < line - hops)(lambda: one(net.z + hops))

    def step(hops):
        def run():
            arrive_y(hops - 1)
            if hops < line:
                arrive(hops)
            if hops >= 2:
                arrive_x(hops - 2, False)
                arrive_x(hops - 1, True)

        return run

    def last():
        arrive_x(line - 1, False)

    def finish():
        local.wait()
        first_y.wait_send()

        @pl.when(net.has_above)
        def _():
            first_up.wait_send()
            for hops in range(1, line - 1):
                pl.when(net.z >= hops)(over_z(net.z - hops, net.above, 0).wait_send)

        @pl.when(net.has_below)
        def _():
            first_down.wait_send()
            for hops in range(1, line - 1):
                pl.when(net.z < line - hops)(over_z(net.z + hops, net.below, line).wait_send)

        for z in range(line):

            def others():
                over_y(z).wait_send()
                if split:
                    over_x(z, net.y).wait_send()
                to_core(z, net.y).wait()

            pl.when(net.z != z)(others)
            if split:
                over_x(z, 1 - net.y).wait_send()
            to_core(z, 1 - net.y).wait()

    return [start] + [step(hops) for hops in range(1, line + 1)] + [last, finish]


def gather_scratch(line, tensors):
    copies = gather_count(line)
    return [
        pltpu.SemaphoreType.DMA((tensors,)),
        pltpu.SemaphoreType.DMA((tensors, copies)),
        pltpu.SemaphoreType.DMA((tensors, copies)),
    ]


REDUCE_BUFFERS = 9


def reduce_split(columns):
    only = columns // 4 if columns % 512 == 0 else 0
    return only, columns - 2 * only


def reduce_scratch(line, shards, half, columns, dtype):
    only, shared = reduce_split(columns)
    carried = only + shared
    return [
        pltpu.VMEM((shards, half, columns), dtype),
        pltpu.VMEM((shards, half, columns), dtype),
        pltpu.VMEM((shards, half, max(only, 128)), dtype),
        pltpu.VMEM((line, half, carried), dtype),
        pltpu.VMEM((line + 1, half, carried), dtype),
        pltpu.VMEM((half, carried), dtype),
        pltpu.VMEM((half, columns), dtype),
        pltpu.VMEM((half, columns), dtype),
        pltpu.VMEM((2 * half, columns), jnp.float32),
    ]


def reduce_count(line):
    return 3 * line + 4


def reduce_steps(net, grad, out, column_start, out_start, buffers, local_sem, send_sem, recv_sem):
    kept, got, from_x, from_y, from_z, late_x, final, swapped, wide = buffers
    line = net.line
    shards, half, width = kept.shape
    only, shared = reduce_split(width)
    both = only + shared
    columns = pl.ds(column_start, width)
    mine = pl.ds(aligned(net.core * half, half), half)
    theirs = pl.ds(aligned((1 - net.core) * half, half), half)
    if only:
        carried = pl.ds(aligned(net.x * only, 128), both)
        lone = pl.ds(aligned(net.x * both, 128), only)
        their_lone = pl.ds(aligned((1 - net.x) * both, 128), only)
    else:
        carried = pl.ds(0, width)

    def remote(origin, landing, index, target):
        return pltpu.make_async_remote_copy(
            src_ref=origin,
            dst_ref=landing,
            send_sem=send_sem.at[index],
            recv_sem=recv_sem.at[index],
            device_id=target,
            device_id_type=MESH,
        )

    local = pltpu.make_async_copy(grad.at[:, mine, columns], kept, local_sem.at[0])
    halves = remote(grad.at[:, theirs, columns], got, 2 * line, net.sibling)
    written = pltpu.make_async_copy(wide, out.at[:, pl.ds(out_start, width)], local_sem.at[1])
    to_core = remote(final, swapped, 2 * line + 1, net.sibling)
    end_x = remote(kept.at[net.own, :, carried], late_x, 2 * line + 2, net.across_x)
    if only:
        over_x = remote(kept.at[:, :, their_lone], from_x, 2 * line + 3, net.across_x)

    def over_y(z):
        part = kept.at[z * 2 + 1 - net.y, :, carried]
        return remote(part, from_y.at[z], 2 * line + 4 + z, net.across_y)

    def up(z):
        return remote(kept.at[z * 2 + net.y, :, carried], from_z.at[z + 1], z, net.above)

    def down(z):
        return remote(kept.at[z * 2 + net.y, :, carried], from_z.at[z], line + z, net.below)

    def add(shard, part):
        kept[shard, :, carried] = kept[shard, :, carried] + part

    def first():
        halves.start()
        local.start()

    def second():
        local.wait()
        halves.wait_recv()

        @pl.loop(0, shards)
        def _(shard):
            kept[shard] = kept[shard] + got[shard]

        if only:
            over_x.start()

    def third():
        if only:
            over_x.wait_recv()

            @pl.loop(0, shards)
            def _(shard):
                kept[shard, :, lone] = kept[shard, :, lone] + from_x[shard]

        for z in range(line):
            over_y(z).start()

    def fourth():
        for z in range(line):
            over_y(z).wait_recv()

        @pl.loop(0, line)
        def _(z):
            add(z * 2 + net.y, from_y[z])

    def hop(step):
        def run():
            @pl.when(net.z == step)
            def _():
                for z in range(line - 1, step, -1):
                    if step > 0:
                        up(z).wait_recv()
                        add(z * 2 + net.y, from_z[z + 1])
                    up(z).start()

            @pl.when(net.z == line - 1 - step)
            def _():
                for z in range(line - 1 - step):
                    if step > 0:
                        down(z).wait_recv()
                        add(z * 2 + net.y, from_z[z])
                    down(z).start()

        return run

    def land():
        @pl.when(net.has_below)
        def _():
            up(net.z).wait_recv()
            add(net.own, from_z[net.z + 1])

        @pl.when(net.has_above)
        def _():
            down(net.z).wait_recv()
            add(net.own, from_z[net.z])

        end_x.start()

    def meet():
        end_x.wait_recv()
        if only:
            final[:, lone] = kept[net.own, :, lone]
            for x in range(2):

                @pl.when(net.x == x)
                def _():
                    start = 0 if x == 1 else shared
                    final[:, (1 - x) * both : (1 - x) * both + only] = late_x[:, start : start + only]
                    other = shared * 0 + (only if x == 1 else 0)
                    final[:, only:both] = kept[net.own, :, only:both] + late_x[:, other : other + shared]
        else:
            final[...] = kept[net.own] + late_x[...]
        to_core.start()
        wide[mine, :] = final[...].astype(jnp.float32)

    def swap():
        to_core.wait_recv()
        wide[theirs, :] = swapped[...].astype(jnp.float32)
        written.start()

    def finish():
        written.wait()
        halves.wait_send()
        if only:
            over_x.wait_send()
        for z in range(line):
            over_y(z).wait_send()
            pl.when(net.z < z)(up(z).wait_send)
            pl.when(net.z > z)(down(z).wait_send)
        end_x.wait_send()
        to_core.wait_send()

    hops = [hop(step) for step in range(line - 1)]

    def fourth_and_hop():
        fourth()
        hops[0]()

    return [first, second, third, fourth_and_hop] + hops[1:] + [land, meet, swap, finish]


def staggered(step_lists, gap=1):
    ticks = (len(step_lists) - 1) * gap + max(len(steps) for steps in step_lists)
    out = []
    for tick in range(ticks):
        row = []
        for index, steps in enumerate(step_lists):
            at = tick - index * gap
            if 0 <= at < len(steps):
                row.append(steps[at])
        out.append(row)
    return out


def reduce_chunks(shape):
    shards, rows, columns = shape
    width = columns
    while width % 1024 == 0 and shards * (rows // 2) * width > (1 << 19):
        width //= 2
    return width, columns // width


ROWS_BY_ROWS = (((0,), (0,)), ((), ()))
COLUMNS_BY_COLUMNS = (((1,), (1,)), ((), ()))


def product(first_op, second_op, dims=(((1,), (0,)), ((), ()))):
    return lax.dot_general(first_op, second_op, dims, preferred_element_type=jnp.float32)


def inverse_rms(values):
    return lax.rsqrt(jnp.mean(values * values, axis=1, keepdims=True) + norm_eps)


class Carried:
    def __init__(self, line, collective, gathers=(), reduces=()):
        self.line, self.collective = line, collective
        self.gathers, self.reduces = list(gathers), list(reduces)
        self.operands = list(self.gathers)
        self.results = []
        shards = lax.axis_size("shard")
        for part in self.gathers:
            self.results.append(jax.ShapeDtypeStruct((shards * part.shape[0], part.shape[1]), part.dtype))
        self.scratch = gather_scratch(line, len(self.gathers)) if self.gathers else []
        self.plans = []
        chunks = 0
        for grads in self.reduces:
            plan = [reduce_chunks(grad.shape) for grad in grads]
            self.plans.append(plan)
            chunks += sum(count for _, count in plan)
            self.operands += grads
            columns = sum(grad.shape[2] for grad in grads)
            self.results.append(jax.ShapeDtypeStruct((grads[0].shape[1], columns), jnp.float32))
        if chunks:
            copies = reduce_count(line)
            self.scratch += [
                pltpu.SemaphoreType.DMA((chunks, 2)),
                pltpu.SemaphoreType.DMA((chunks, copies)),
                pltpu.SemaphoreType.DMA((chunks, copies)),
            ]
        for grads, plan in zip(self.reduces, self.plans):
            for grad, (width, count) in zip(grads, plan):
                for _ in range(count):
                    self.scratch += reduce_scratch(line, grad.shape[0], grad.shape[1] // 2, width, grad.dtype)

    def rows(self, net, operands, results, scratch):
        lists = []
        if self.gathers:
            local, send, recv = scratch[:3]
            scratch = scratch[3:]
            for index in range(len(self.gathers)):
                lists.append(
                    gather_steps(
                        net, operands[index], results[index], local.at[index], send.at[index], recv.at[index]
                    )
                )
        operands, results = operands[len(self.gathers) :], results[len(self.gathers) :]
        if self.reduces:
            local, send, recv = scratch[:3]
            scratch = scratch[3:]
        number = 0
        for target, (grads, plan) in enumerate(zip(self.reduces, self.plans)):
            start = 0
            for grad, (width, count) in zip(grads, plan):
                source = operands[0]
                operands = operands[1:]
                for chunk in range(count):
                    lists.append(
                        reduce_steps(
                            net,
                            source,
                            results[target],
                            chunk * width,
                            start + chunk * width,
                            scratch[:REDUCE_BUFFERS],
                            local.at[number],
                            send.at[number],
                            recv.at[number],
                        )
                    )
                    scratch = scratch[REDUCE_BUFFERS:]
                    number += 1
                start += grad.shape[2]
        return staggered(lists)


def carry(body, carried, *, grid, out_shape, in_specs, out_specs, scratch_shapes, name, operands, head=0):
    if carried is None:
        return list(
            pl.pallas_call(
                body,
                grid=(grid,),
                out_shape=out_shape,
                in_specs=in_specs,
                out_specs=out_specs,
                scratch_shapes=scratch_shapes,
                compiler_params=pltpu.CompilerParams(vmem_limit_bytes=60 << 20),
                name=name,
            )(*operands)
        ), []
    counts = [len(in_specs), len(carried.operands), len(out_specs), len(carried.results), len(scratch_shapes)]
    ends = [sum(counts[: i + 1]) for i in range(len(counts))]

    def kernel(*refs):
        own_in, more_in = refs[: ends[0]], refs[ends[0] : ends[1]]
        own_out, more_out = refs[ends[1] : ends[2]], refs[ends[2] : ends[3]]
        own_scratch, more_scratch = refs[ends[3] : ends[4]], refs[ends[4] :]
        step = pl.program_id(0)
        net = Net(carried.line)
        rows = carried.rows(net, more_in, more_out, more_scratch)
        pl.when(step == 0)(net.greet)
        middle = rows[:-1]
        at = [head + (index * (grid - head)) // len(middle) for index in range(len(middle))]
        at[0] = 0
        for place in sorted(set(at)):

            @pl.when(step == place)
            def _():
                for index, row in enumerate(middle):
                    if at[index] == place:
                        for action in row:
                            action()

        body(*own_in, *own_out, *own_scratch)

        @pl.when(step == grid - 1)
        def _():
            for action in rows[-1]:
                action()

    results = pl.pallas_call(
        kernel,
        grid=(grid,),
        out_shape=list(out_shape) + carried.results,
        in_specs=list(in_specs) + [ANY] * len(carried.operands),
        out_specs=list(out_specs) + [ANY] * len(carried.results),
        scratch_shapes=list(scratch_shapes) + carried.scratch,
        compiler_params=pltpu.CompilerParams(
            collective_id=carried.collective, has_side_effects=True, vmem_limit_bytes=63 << 20
        ),
        name=name,
    )(*operands, *carried.operands)
    return list(results[: len(out_shape)]), list(results[len(out_shape) :])


def carry_alone(carried, name):
    return carry(
        lambda: None,
        carried,
        grid=1,
        out_shape=[],
        in_specs=[],
        out_specs=[],
        scratch_shapes=[],
        name=name,
        operands=[],
    )[1]


def whole(*shape):
    return pl.BlockSpec(shape, lambda step: (0,) * len(shape), pipeline_mode=pl.Buffered(1))


def like(shape, dtype):
    return jax.ShapeDtypeStruct(shape, dtype)


def project_kernel(turned, x_ref, gain_ref, w_ref, cos_ref, sin_ref, out_ref, normed_ref):
    step = pl.program_id(0)

    @pl.when(step == 0)
    def _():
        values = x_ref[...].astype(jnp.float32)
        normed = values * inverse_rms(values) * gain_ref[...]
        normed_ref[...] = normed.T.astype(jnp.bfloat16)

    out = product(w_ref[...], normed_ref[...], ROWS_BY_ROWS)

    @pl.when(step < turned)
    def _():
        cos, sin = cos_ref[...], sin_ref[...]
        half = cos.shape[0]
        for start in range(0, out.shape[0], 2 * half):
            first, second = out[start : start + half], out[start + half : start + 2 * half]
            out_ref[start : start + half, :] = (first * cos - second * sin).astype(jnp.bfloat16)
            out_ref[start + half : start + 2 * half, :] = (second * cos + first * sin).astype(jnp.bfloat16)

    @pl.when(step >= turned)
    def _():
        out_ref[...] = out.astype(jnp.bfloat16)


def project(x, gain, weight, cos_t, sin_t, carried):
    rows, width = x.shape
    columns = weight.shape[1]
    block = 512
    return carry(
        functools.partial(project_kernel, 2 * width // block),
        carried,
        grid=columns // block,
        out_shape=[like((columns, rows), jnp.bfloat16), like((width, rows), jnp.bfloat16)],
        in_specs=[
            whole(rows, width),
            whole(1, width),
            pl.BlockSpec((width, block), lambda step: (0, step)),
            whole(*cos_t.shape),
            whole(*sin_t.shape),
        ],
        out_specs=[
            pl.BlockSpec((block, rows), lambda step: (step, 0)),
            pl.BlockSpec((width, rows), lambda step: (0, 0)),
        ],
        scratch_shapes=[],
        name="project",
        operands=[x, gain, weight, cos_t, sin_t],
    )


def branch_kernel(att_ref, w_ref, x_ref, gain_ref, hidden_ref, normed_ref):
    hidden = x_ref[...].astype(jnp.float32) + product(att_ref[...], w_ref[...], ROWS_BY_ROWS)
    hidden_ref[...] = hidden
    normed_ref[...] = (hidden * inverse_rms(hidden) * gain_ref[...]).astype(jnp.bfloat16)


def branch(attended_t, weight, x, gain, carried):
    rows, width = x.shape
    block = 256
    row = pl.BlockSpec((block, width), lambda step: (step, 0))
    return carry(
        branch_kernel,
        carried,
        grid=rows // block,
        out_shape=[like((rows, width), jnp.float32), like((rows, width), jnp.bfloat16)],
        in_specs=[
            pl.BlockSpec((width, block), lambda step: (0, step)),
            whole(*weight.shape),
            row,
            whole(1, width),
        ],
        out_specs=[row, row],
        scratch_shapes=[],
        name="branch",
        operands=[attended_t, weight, x, gain],
    )


def widen_kernel(normed_ref, gate_ref, up_ref, act_ref, to_gate_ref, to_up_ref):
    normed = normed_ref[...]
    gate = product(normed, gate_ref[...])
    up = product(normed, up_ref[...])
    sigmoid = jax.nn.sigmoid(gate)
    swish = gate * sigmoid
    act_ref[...] = (swish * up).astype(jnp.bfloat16)
    to_gate_ref[...] = (up * sigmoid * (1.0 + gate * (1.0 - sigmoid))).astype(jnp.bfloat16)
    to_up_ref[...] = swish.astype(jnp.bfloat16)


def widen(normed, weight, carried):
    rows, width = normed.shape
    inner = weight.shape[1] // 2
    block = 512
    steps = inner // block
    part = pl.BlockSpec((rows, block), lambda step: (0, step))
    return carry(
        widen_kernel,
        carried,
        grid=steps,
        out_shape=[like((rows, inner), jnp.bfloat16)] * 3,
        in_specs=[
            whole(rows, width),
            pl.BlockSpec((width, block), lambda step: (0, step)),
            pl.BlockSpec((width, block), lambda step: (0, steps + step)),
        ],
        out_specs=[part] * 3,
        scratch_shapes=[],
        name="widen",
        operands=[normed, weight, weight],
    )


def narrow_kernel(
    steps, act_ref, to_gate_ref, to_up_ref, w_ref, given_ref, hidden_ref, result_ref, grad_ref, d_gate_ref, d_up_ref, acc_ref
):
    step = pl.program_id(0)
    act, weight, given = act_ref[...], w_ref[...], given_ref[...]
    part = product(act, weight)

    @pl.when(step == 0)
    def _():
        acc_ref[...] = hidden_ref[...] + part

    @pl.when(step > 0)
    def _():
        acc_ref[...] += part

    @pl.when(step == steps - 1)
    def _():
        result_ref[...] = acc_ref[...].astype(jnp.bfloat16)

    grad_ref[...] = product(act, given, ROWS_BY_ROWS).astype(jnp.bfloat16)
    d_act = product(given, weight, COLUMNS_BY_COLUMNS)
    d_gate_ref[...] = (d_act * to_gate_ref[...].astype(jnp.float32)).astype(jnp.bfloat16)
    d_up_ref[...] = (d_act * to_up_ref[...].astype(jnp.float32)).astype(jnp.bfloat16)


def narrow(act, to_gate, to_up, weight, given, hidden, carried):
    rows, inner = act.shape
    width = weight.shape[1]
    block = 512
    steps = inner // block
    part = pl.BlockSpec((rows, block), lambda step: (0, step))
    down = pl.BlockSpec((block, width), lambda step: (step, 0))
    return carry(
        functools.partial(narrow_kernel, steps),
        carried,
        grid=steps,
        out_shape=[
            like((rows, width), jnp.bfloat16),
            like((inner, width), jnp.bfloat16),
            like((rows, inner), jnp.bfloat16),
            like((rows, inner), jnp.bfloat16),
        ],
        in_specs=[part, part, part, down, whole(rows, width), whole(rows, width)],
        out_specs=[pl.BlockSpec((rows, width), lambda step: (0, 0)), down, part, part],
        scratch_shapes=[pltpu.VMEM((rows, width), jnp.float32)],
        name="narrow",
        operands=[act, to_gate, to_up, weight, given, hidden],
    )


def grad_in_kernel(normed_ref, d_gate_ref, d_up_ref, to_gate_ref, to_up_ref, turned_ref):
    @pl.when(pl.program_id(0) == 0)
    def _():
        turned_ref[...] = normed_ref[...].T

    to_gate_ref[...] = product(turned_ref[...], d_gate_ref[...]).astype(jnp.bfloat16)
    to_up_ref[...] = product(turned_ref[...], d_up_ref[...]).astype(jnp.bfloat16)


def grad_into(normed, d_gate, d_up, carried):
    rows, width = normed.shape
    inner = d_gate.shape[1]
    block = 512
    part = pl.BlockSpec((rows, block), lambda step: (0, step))
    out = pl.BlockSpec((width, block), lambda step: (0, step))
    return carry(
        grad_in_kernel,
        carried,
        grid=inner // block,
        out_shape=[like((width, inner), jnp.bfloat16)] * 2,
        in_specs=[whole(rows, width), part, part],
        out_specs=[out, out],
        scratch_shapes=[pltpu.VMEM((width, rows), jnp.bfloat16)],
        name="grad_in",
        operands=[normed, d_gate, d_up],
    )


def norm_back(d_normed, values, gain):
    inverse = inverse_rms(values)
    unit = values * inverse
    scaled = d_normed * gain
    mean = jnp.mean(scaled * unit, axis=1, keepdims=True)
    return inverse * (scaled - unit * mean), jnp.sum(d_normed * unit, axis=0, keepdims=True)


def ffn_back_kernel(
    steps, d_gate_ref, d_up_ref, gate_ref, up_ref, hidden_ref, gain_ref, given_ref, d_hidden_ref, d_branch_ref, grad_gain_ref, acc_ref
):
    step = pl.program_id(0)
    part = product(d_gate_ref[...], gate_ref[...], COLUMNS_BY_COLUMNS)
    part = part + product(d_up_ref[...], up_ref[...], COLUMNS_BY_COLUMNS)

    @pl.when(step == 0)
    def _():
        acc_ref[...] = part

    @pl.when(step > 0)
    def _():
        acc_ref[...] += part

    @pl.when(step == steps - 1)
    def _():
        through, grad_gain = norm_back(acc_ref[...], hidden_ref[...], gain_ref[...])
        d_hidden = given_ref[...].astype(jnp.float32) + through
        d_hidden_ref[...] = d_hidden
        d_branch_ref[...] = d_hidden.astype(jnp.bfloat16)
        grad_gain_ref[...] = grad_gain


def ffn_back(d_gate, d_up, weight, hidden, gain, given, carried):
    rows, width = hidden.shape
    inner = d_gate.shape[1]
    block = 512
    steps = inner // block
    part = pl.BlockSpec((rows, block), lambda step: (0, step))
    full = pl.BlockSpec((rows, width), lambda step: (0, 0))
    return carry(
        functools.partial(ffn_back_kernel, steps),
        carried,
        grid=steps,
        out_shape=[
            like((rows, width), jnp.float32),
            like((rows, width), jnp.bfloat16),
            like((1, width), jnp.float32),
        ],
        in_specs=[
            part,
            part,
            pl.BlockSpec((width, block), lambda step: (0, step)),
            pl.BlockSpec((width, block), lambda step: (0, steps + step)),
            whole(rows, width),
            whole(1, width),
            whole(rows, width),
        ],
        out_specs=[full, full, pl.BlockSpec((1, width), lambda step: (0, 0))],
        scratch_shapes=[pltpu.VMEM((rows, width), jnp.float32)],
        name="ffn_back",
        operands=[d_gate, d_up, weight, weight, hidden, gain, given],
    )


def branch_back_kernel(att_ref, w_ref, d_branch_ref, grad_ref, given_ref):
    d_branch = d_branch_ref[...]
    grad_ref[...] = product(att_ref[...], d_branch).astype(jnp.bfloat16)
    given_ref[...] = product(w_ref[...], d_branch, COLUMNS_BY_COLUMNS).astype(jnp.bfloat16)


def branch_back(attended_t, weight, d_branch, carried):
    rows, width = d_branch.shape
    block = 256
    out = pl.BlockSpec((block, width), lambda step: (step, 0))
    turned = pl.BlockSpec((block, rows), lambda step: (step, 0))
    return carry(
        branch_back_kernel,
        carried,
        grid=attended_t.shape[0] // block,
        out_shape=[like(weight.shape, jnp.bfloat16), like(attended_t.shape, jnp.bfloat16)],
        in_specs=[turned, out, whole(rows, width)],
        out_specs=[out, turned],
        scratch_shapes=[],
        name="branch_back",
        operands=[attended_t, weight, d_branch],
    )


def project_back_kernel(
    steps, normed_ref, dq_ref, dk_ref, dv_ref, w_ref, x_ref, gain_ref, d_hidden_ref, grad_ref, tokens_ref, grad_gain_ref, acc_ref
):
    step = pl.program_id(0)
    third = steps // 3

    def run(d_ref):
        d_part = d_ref[...]
        grad_ref[...] = product(normed_ref[...], d_part, COLUMNS_BY_COLUMNS).astype(jnp.bfloat16)
        part = product(w_ref[...], d_part)

        @pl.when(step == 0)
        def _():
            acc_ref[...] = part

        @pl.when(step > 0)
        def _():
            acc_ref[...] += part

    for index, d_ref in enumerate((dq_ref, dk_ref, dv_ref)):
        pl.when(step // third == index)(functools.partial(run, d_ref))

    @pl.when(step == steps - 1)
    def _():
        values = x_ref[...].astype(jnp.float32)
        through, grad_gain = norm_back(acc_ref[...].T, values, gain_ref[...])
        tokens_ref[...] = d_hidden_ref[...] + through
        grad_gain_ref[...] = grad_gain


def project_back(normed_t, dq, dk, dv, weight, x, gain, d_hidden, carried):
    rows, width = x.shape
    columns = weight.shape[1]
    block = 512
    steps = columns // block
    third = steps // 3
    full = pl.BlockSpec((rows, width), lambda step: (0, 0))

    def part(which):
        return pl.BlockSpec(
            (block, rows), lambda step: (jnp.clip(step - which * third, 0, third - 1), 0)
        )

    return carry(
        functools.partial(project_back_kernel, steps),
        carried,
        grid=steps,
        out_shape=[
            like((width, columns), jnp.bfloat16),
            like((rows, width), jnp.float32),
            like((1, width), jnp.float32),
        ],
        in_specs=[
            whole(*normed_t.shape),
            part(0),
            part(1),
            part(2),
            pl.BlockSpec((width, block), lambda step: (0, step)),
            whole(rows, width),
            whole(1, width),
            whole(rows, width),
        ],
        out_specs=[
            pl.BlockSpec((width, block), lambda step: (0, step)),
            full,
            pl.BlockSpec((1, width), lambda step: (0, 0)),
        ],
        scratch_shapes=[pltpu.VMEM((width, rows), jnp.float32)],
        name="project_back",
        operands=[normed_t, dq, dk, dv, weight, x, gain, d_hidden],
    )


LOG2E = 1.4426950408889634
FEATURES = 16


def two_parts(value):
    high = value.astype(jnp.bfloat16)
    return high, (value - high.astype(jnp.float32)).astype(jnp.bfloat16)


def three_parts(value):
    high, rest = value.astype(jnp.bfloat16), None
    rest = value - high.astype(jnp.float32)
    middle = rest.astype(jnp.bfloat16)
    return high, middle, (rest - middle.astype(jnp.float32)).astype(jnp.bfloat16)


def key_features(variates, valid):
    length = variates.shape[1]
    masks = [(variates == v).astype(jnp.float32) for v in range(4)]
    ones = jnp.ones((1, length), jnp.float32)
    invalid = 1.0 - valid
    rows = masks + masks + [invalid, ones, ones, ones, jnp.zeros((FEATURES - 12, length), jnp.float32)]
    return jnp.concatenate(rows, axis=0).astype(jnp.bfloat16)


def query_features(variates, same, other, log_sums):
    length = variates.shape[1]
    highs, lows = [], []
    for v in range(4):
        bias = jnp.where(variates == v, same, other) * LOG2E
        high, low = two_parts(bias)
        highs.append(high.astype(jnp.float32))
        lows.append(low.astype(jnp.float32))
    if log_sums is None:
        minus = [jnp.zeros((3, length), jnp.float32)]
    else:
        minus = [part.astype(jnp.float32) for part in three_parts(-log_sums)]
    mask = jnp.full((1, length), masked_score, jnp.float32)
    rows = highs + lows + [mask] + minus + [jnp.zeros((FEATURES - 12, length), jnp.float32)]
    return jnp.concatenate(rows, axis=0).astype(jnp.bfloat16)


def contract_depth(first_op, second_op):
    return lax.dot_general(
        first_op, second_op, (((1,), (0,)), ((), ())), preferred_element_type=jnp.float32
    )


def scaled_query(query_t, score_scale):
    return two_parts(query_t.astype(jnp.float32) * (score_scale * LOG2E))


def attend_kernel(blocks, bias_ref, q_ref, k_ref, v_ref, var_ref, valid_ref, o_ref, wide_ref, lse_ref, query_ref):
    head = pl.program_id(0)
    depth, length = q_ref.shape
    width = length // blocks
    same, other = bias_ref[0, head], bias_ref[1, head]
    variates = var_ref[...]
    high, low = scaled_query(q_ref[...], depth ** (-0.5))
    query_ref[...] = jnp.concatenate([high, low, query_features(variates, same, other, None)], axis=0)
    key_t = k_ref[...]
    keys = jnp.concatenate([key_t, key_t, key_features(variates, valid_ref[...])], axis=0).T
    ones = jnp.concatenate(
        [jnp.ones((1, length), jnp.float32), jnp.zeros((FEATURES - 1, length), jnp.float32)], axis=0
    ).astype(jnp.bfloat16)
    values = jnp.concatenate([v_ref[...], ones], axis=0)
    for block in range(blocks):
        at = pl.ds(block * width, width)
        scores = contract_depth(keys, query_ref[:, at])
        peak = jnp.max(scores, axis=0, keepdims=True)
        weights = jnp.exp2(scores - peak).astype(jnp.bfloat16)
        summed = contract_depth(values, weights)
        total = summed[depth : depth + 1]
        attended = summed[:depth] / total
        wide_ref[:, at] = attended
        o_ref[:, at] = attended.astype(jnp.bfloat16)
        lse_ref[0, :, at] = peak + jnp.log2(total)


def attend_forward(qkv_t, variates, valid, bias, heads, carried):
    rows, length = qkv_t.shape
    depth = rows // (3 * heads)

    def part(which):
        return pl.BlockSpec((depth, length), lambda head: (which * heads + head, 0))

    row = pl.BlockSpec((1, length), lambda head: (0, 0))
    return carry(
        functools.partial(attend_kernel, 1),
        carried,
        grid=heads,
        out_shape=[
            jax.ShapeDtypeStruct((heads * depth, length), jnp.bfloat16),
            jax.ShapeDtypeStruct((heads * depth, length), jnp.float32),
            jax.ShapeDtypeStruct((heads, 1, length), jnp.float32),
        ],
        in_specs=[
            pl.BlockSpec(memory_space=pltpu.SMEM),
            part(0),
            part(1),
            part(2),
            row,
            row,
        ],
        out_specs=[
            pl.BlockSpec((depth, length), lambda head: (head, 0)),
            pl.BlockSpec((depth, length), lambda head: (head, 0)),
            pl.BlockSpec((1, 1, length), lambda head: (head, 0, 0)),
        ],
        scratch_shapes=[pltpu.VMEM((2 * depth + FEATURES, length), jnp.bfloat16)],
        name="attend_forward",
        operands=[bias, qkv_t, qkv_t, qkv_t, variates, valid],
    )


def turn_back(grad_t, cos_t, sin_t):
    half = cos_t.shape[0]
    first, second = grad_t[:half], grad_t[half:]
    return jnp.concatenate(
        [first * cos_t + second * sin_t, second * cos_t - first * sin_t], axis=0
    )


def attend_back_head(
    blocks, head, bias_ref, q_ref, k_ref, v_ref, go_ref, wide_ref, lse_ref, var_ref, valid_ref, cos_ref, sin_ref,
    dq_ref, dk_ref, dv_ref, db_ref, query_ref, given_ref, dk_acc, dv_acc,
):
    depth, length = q_ref.shape
    width = length // blocks
    scale = depth ** (-0.5)
    same, other = bias_ref[0, head], bias_ref[1, head]
    variates = var_ref[...]
    features = key_features(variates, valid_ref[...])
    high, low = scaled_query(q_ref[...], scale)
    query_ref[...] = jnp.concatenate([high, low, query_features(variates, same, other, lse_ref[0])], axis=0)
    key_t = k_ref[...]
    keys = jnp.concatenate([key_t, key_t, features], axis=0).T
    keys_low = jnp.concatenate([key_t, features], axis=0)
    given = go_ref[...]
    inner = jnp.sum(given.astype(jnp.float32) * wide_ref[...], axis=0, keepdims=True)
    minus = [part.astype(jnp.float32) for part in three_parts(-inner)]
    minus = jnp.concatenate(minus + [jnp.zeros((FEATURES - 3, length), jnp.float32)], axis=0)
    given_ref[...] = jnp.concatenate([given, minus.astype(jnp.bfloat16)], axis=0)
    ones = jnp.concatenate(
        [jnp.ones((3, length), jnp.float32), jnp.zeros((FEATURES - 3, length), jnp.float32)], axis=0
    ).astype(jnp.bfloat16)
    values = jnp.concatenate([v_ref[...], ones], axis=0).T
    query_rows = q_ref[...].T
    given_rows = given.T
    in_same = jnp.zeros((1, width), jnp.float32)
    in_other = jnp.zeros((1, width), jnp.float32)
    for block in range(blocks):
        at = pl.ds(block * width, width)
        cut = slice(block * width, (block + 1) * width)
        probs = jnp.exp2(contract_depth(keys, query_ref[:, at]))
        grads = (probs * contract_depth(values, given_ref[:, at])).astype(jnp.bfloat16)
        back = contract_depth(keys_low, grads)
        dq = turn_back(back[:depth] * scale, cos_ref[:, at], sin_ref[:, at])
        dq_ref[:, at] = dq.astype(jnp.bfloat16)
        for v in range(4):
            line = back[depth + v : depth + v + 1]
            hit = variates[:, cut] == v
            in_same = in_same + jnp.where(hit, line, 0.0)
            in_other = in_other + jnp.where(hit, 0.0, line)
        dk = contract_depth(grads, query_rows[cut])
        dv = contract_depth(probs.astype(jnp.bfloat16), given_rows[cut])
        if block == 0:
            dk_acc[...] = dk
            dv_acc[...] = dv
        else:
            dk_acc[...] += dk
            dv_acc[...] += dv
    dk_ref[...] = turn_back((dk_acc[...] * scale).T, cos_ref[...], sin_ref[...]).astype(jnp.bfloat16)
    dv_ref[...] = dv_acc[...].T.astype(jnp.bfloat16)
    db_ref[0, 0:1, :] = in_same
    db_ref[0, 1:2, :] = in_other


def attend_back_kernel(blocks, *refs):
    attend_back_head(blocks, pl.program_id(0), *refs)


def attend_backward(qkv_t, given_t, wide_t, log_sums, variates, valid, bias, cos_t, sin_t, heads, carried):
    rows, length = qkv_t.shape
    depth = rows // (3 * heads)
    blocks = 1

    def part(which):
        return pl.BlockSpec((depth, length), lambda head: (which * heads + head, 0))

    one = pl.BlockSpec((depth, length), lambda head: (head, 0))
    grad = jax.ShapeDtypeStruct((heads * depth, length), jnp.bfloat16)
    return carry(
        functools.partial(attend_back_kernel, blocks),
        carried,
        grid=heads,
        out_shape=[grad, grad, grad, jax.ShapeDtypeStruct((heads, 2, length // blocks), jnp.float32)],
        in_specs=[
            pl.BlockSpec(memory_space=pltpu.SMEM),
            part(0),
            part(1),
            part(2),
            one,
            one,
            pl.BlockSpec((1, 1, length), lambda head: (head, 0, 0)),
            whole(1, length),
            whole(1, length),
            whole(depth // 2, length),
            whole(depth // 2, length),
        ],
        out_specs=[one, one, one, pl.BlockSpec((1, 2, length // blocks), lambda head: (head, 0, 0))],
        scratch_shapes=[
            pltpu.VMEM((2 * depth + FEATURES, length), jnp.bfloat16),
            pltpu.VMEM((depth + FEATURES, length), jnp.bfloat16),
            pltpu.VMEM((length, depth), jnp.float32),
            pltpu.VMEM((length, depth), jnp.float32),
        ],
        name="attend_backward",
        operands=[bias, qkv_t, qkv_t, qkv_t, given_t, wide_t, log_sums, variates, valid, cos_t, sin_t],
    )


TILE = 512
BLOCK = 1024
KEPT, GIVEN, GOT, OVER_X, OVER_Y, OVER_Z, LATE, ENDS, WIDE = 13, 3, 4, 5, 5, 6, 4, 4, 3
STAGES = (0, 1, 3, 5, 7, 8, 9, 10, 11, 12)
SUBSTEPS = 6


def stream_scratch(line, shards, half):
    only, shared = reduce_split(TILE)
    both = only + shared
    low = jnp.bfloat16
    copies = 3 * line + 4
    return [
        pltpu.VMEM((KEPT, shards, half, TILE), low),
        pltpu.VMEM((GIVEN, shards, half, TILE), low),
        pltpu.VMEM((GOT, shards, half, TILE), low),
        pltpu.VMEM((OVER_X, shards, half, only), low),
        pltpu.VMEM((OVER_Y, line, half, both), low),
        pltpu.VMEM((OVER_Z, line + 1, half, both), low),
        pltpu.VMEM((LATE, half, both), low),
        pltpu.VMEM((ENDS, half, TILE), low),
        pltpu.VMEM((ENDS, half, TILE), low),
        pltpu.VMEM((WIDE, 2 * half, TILE), jnp.float32),
        pltpu.SemaphoreType.DMA((KEPT, 4)),
        pltpu.SemaphoreType.DMA((KEPT, copies)),
        pltpu.SemaphoreType.DMA((KEPT, copies)),
    ]


class Stream:
    def __init__(self, net, scratch, writes):
        self.net, self.writes = net, writes
        (
            self.kept,
            self.give,
            self.got,
            self.from_x,
            self.from_y,
            self.from_z,
            self.late,
            self.final,
            self.swapped,
            self.wide,
            self.local_sem,
            self.send_sem,
            self.recv_sem,
        ) = scratch
        self.shards, self.half = self.kept.shape[1], self.kept.shape[2]
        self.only, self.shared = reduce_split(TILE)
        self.both = self.only + self.shared
        self.carried = pl.ds(aligned(net.x * self.only, 128), self.both)
        self.lone = pl.ds(aligned(net.x * self.both, 128), self.only)
        self.their_lone = pl.ds(aligned((1 - net.x) * self.both, 128), self.only)

    def remote(self, tile, origin, landing, index, target):
        slot = tile % KEPT
        return pltpu.make_async_remote_copy(
            src_ref=origin,
            dst_ref=landing,
            send_sem=self.send_sem.at[slot, index],
            recv_sem=self.recv_sem.at[slot, index],
            device_id=target,
            device_id_type=MESH,
        )

    def halves(self, tile):
        line = self.net.line
        return self.remote(tile, self.give.at[tile % GIVEN], self.got.at[tile % GOT], 2 * line, self.net.sibling)

    def over_x(self, tile):
        origin = self.kept.at[tile % KEPT, :, :, self.their_lone]
        return self.remote(tile, origin, self.from_x.at[tile % OVER_X], 2 * self.net.line + 1, self.net.across_x)

    def over_y(self, tile, z):
        net = self.net
        origin = self.kept.at[tile % KEPT, z * 2 + 1 - net.y, :, self.carried]
        return self.remote(tile, origin, self.from_y.at[tile % OVER_Y, z], 2 * net.line + 4 + z, net.across_y)

    def up(self, tile, z):
        net = self.net
        origin = self.kept.at[tile % KEPT, z * 2 + net.y, :, self.carried]
        return self.remote(tile, origin, self.from_z.at[tile % OVER_Z, z + 1], z, net.above)

    def down(self, tile, z):
        net = self.net
        origin = self.kept.at[tile % KEPT, z * 2 + net.y, :, self.carried]
        return self.remote(tile, origin, self.from_z.at[tile % OVER_Z, z], net.line + z, net.below)

    def end_x(self, tile):
        net = self.net
        origin = self.kept.at[tile % KEPT, net.own, :, self.carried]
        return self.remote(tile, origin, self.late.at[tile % LATE], 2 * net.line + 2, net.across_x)

    def to_core(self, tile):
        slot = tile % ENDS
        return self.remote(tile, self.final.at[slot], self.swapped.at[slot], 2 * self.net.line + 3, self.net.sibling)

    def add(self, tile, shard, part):
        slot = tile % KEPT
        self.kept[slot, shard, :, self.carried] = self.kept[slot, shard, :, self.carried] + part

    def born(self, tile):
        self.halves(tile).start()

    def meet_core(self, tile):
        copy = self.halves(tile)
        copy.wait_recv()
        copy.wait_send()
        slot, came = tile % KEPT, tile % GOT

        @pl.loop(0, self.shards)
        def _(shard):
            self.kept[slot, shard] = self.kept[slot, shard] + self.got[came, shard]

        self.over_x(tile).start()

    def meet_x(self, tile):
        self.over_x(tile).wait_recv()
        slot, came = tile % KEPT, tile % OVER_X

        @pl.loop(0, self.shards)
        def _(shard):
            self.kept[slot, shard, :, self.lone] = self.kept[slot, shard, :, self.lone] + self.from_x[came, shard]

        for z in range(self.net.line):
            self.over_y(tile, z).start()

    def meet_y(self, tile):
        for z in range(self.net.line):
            self.over_y(tile, z).wait_recv()
            self.add(tile, z * 2 + self.net.y, self.from_y[tile % OVER_Y, z])
        self.hop(tile, 0)

    def hop(self, tile, step):
        net, came = self.net, tile % OVER_Z

        @pl.when(net.z == step)
        def _():
            for z in range(net.line - 1, step, -1):
                if step > 0:
                    self.up(tile, z).wait_recv()
                    self.add(tile, z * 2 + net.y, self.from_z[came, z + 1])
                self.up(tile, z).start()

        @pl.when(net.z == net.line - 1 - step)
        def _():
            for z in range(net.line - 1 - step):
                if step > 0:
                    self.down(tile, z).wait_recv()
                    self.add(tile, z * 2 + net.y, self.from_z[came, z])
                self.down(tile, z).start()

    def land(self, tile):
        net, came = self.net, tile % OVER_Z

        @pl.when(net.has_below)
        def _():
            self.up(tile, net.z).wait_recv()
            self.add(tile, net.own, self.from_z[came, net.z + 1])

        @pl.when(net.has_above)
        def _():
            self.down(tile, net.z).wait_recv()
            self.add(tile, net.own, self.from_z[came, net.z])

        self.end_x(tile).start()

    def meet(self, tile):
        net, only, both, shared = self.net, self.only, self.both, self.shared
        slot, came, end = tile % KEPT, tile % LATE, tile % ENDS
        self.end_x(tile).wait_recv()
        self.final[end, :, self.lone] = self.kept[slot, net.own, :, self.lone]
        for x in range(2):

            @pl.when(net.x == x)
            def _():
                theirs = 0 if x == 1 else shared
                middle = only if x == 1 else 0
                at = (1 - x) * both
                self.final[end, :, at : at + only] = self.late[came, :, theirs : theirs + only]
                self.final[end, :, only:both] = (
                    self.kept[slot, net.own, :, only:both] + self.late[came, :, middle : middle + shared]
                )

        self.to_core(tile).start()
        mine = pl.ds(aligned(net.core * self.half, self.half), self.half)
        self.wide[tile % WIDE, mine, :] = self.final[end].astype(jnp.float32)

    def swap(self, tile):
        self.to_core(tile).wait_recv()
        theirs = pl.ds(aligned((1 - self.net.core) * self.half, self.half), self.half)
        self.wide[tile % WIDE, theirs, :] = self.swapped[tile % ENDS].astype(jnp.float32)
        self.writes(tile, self.wide.at[tile % WIDE], self.local_sem.at[tile % KEPT], True)

    def finish(self, tile):
        net = self.net
        self.writes(tile, self.wide.at[tile % WIDE], self.local_sem.at[tile % KEPT], False)
        self.over_x(tile).wait_send()
        for z in range(net.line):
            self.over_y(tile, z).wait_send()
            pl.when(net.z < z)(self.up(tile, z).wait_send)
            pl.when(net.z > z)(self.down(tile, z).wait_send)
        self.end_x(tile).wait_send()
        self.to_core(tile).wait_send()

    def stages(self):
        return [
            self.born,
            self.meet_core,
            self.meet_x,
            self.meet_y,
            lambda tile: self.hop(tile, 1),
            lambda tile: self.hop(tile, 2),
            self.land,
            self.meet,
            self.swap,
            self.finish,
        ]


class Plan:
    def __init__(self, blocks, heads):
        self.blocks, self.heads = blocks, heads
        self.ffn = blocks * SUBSTEPS
        self.norm = self.ffn
        self.branch = self.ffn + 1
        self.attend = self.ffn + 2
        self.groups = 4
        self.per_group = heads // self.groups
        self.out = self.ffn + SUBSTEPS
        self.ready = [self.attend + self.per_group * (group + 1) for group in range(self.groups)]
        self.births = list(range(SUBSTEPS, self.out + 2))
        self.ffn_tiles = self.ffn
        self.keys_tiles, self.value_tiles = [], []
        for group in range(self.groups):
            self.keys_tiles.append(len(self.births))
            self.births.append(max(self.ready[group], self.births[-1] + 1))
            if group % 2 == 1:
                self.value_tiles.append(len(self.births))
                self.births.append(self.births[-1] + 1)
        self.last = self.births[-1]
        self.grid = self.last + STAGES[-1] + 1

    def tile_at(self, step):
        regular = self.out + 2 - SUBSTEPS
        tile = step - SUBSTEPS
        known = (step >= SUBSTEPS) & (step < self.out + 2)
        for index in range(regular, len(self.births)):
            hit = step == self.births[index]
            tile = jnp.where(hit, index, tile)
            known = known | hit
        return tile, known


def back_kernel(plan, line, shards, *refs):
    step = pl.program_id(0)
    refs = list(refs)

    def take(count):
        out = refs[:count]
        del refs[:count]
        return out

    normed_hbm, given_hbm, hidden_hbm = take(3)
    early = take(4)
    gather_from = take(4)
    attended_hbm, out_hbm, normed_one_hbm, x_hbm, qkv_hbm = take(5)
    gain_one_ref, gain_two_ref = take(2)
    bias_ref, q_ref, k_ref, v_ref, wide_ref, lse_ref, var_ref, valid_ref, cos_ref, sin_ref = take(10)
    result_hbm, tokens_hbm, sum_in, sum_down, sum_out, sum_qkv = take(6)
    gather_to = take(4)
    grad_gain_one_ref, grad_gain_two_ref, db_ref = take(3)
    normed, turned, given, w_down, w_gate, w_up, act, act_t = take(8)
    d_gate, d_up, acc, through = take(4)
    query_ref, given_aug_ref, dk_acc, dv_acc = take(4)
    load_sem, = take(1)
    gather_local, gather_send, gather_recv = take(3)
    net = Net(line)
    half = BLOCK // shards // 2
    heads_at = step - plan.attend

    def writes(tile, wide, sems, begin):
        rows = 2 * half

        def move(index, origin, landing):
            copy = pltpu.make_async_copy(origin, landing, sems.at[index])
            copy.start() if begin else copy.wait()

        block, kind = tile // SUBSTEPS, tile % SUBSTEPS
        in_ffn = tile < plan.ffn_tiles

        @pl.when(in_ffn & (kind < 2))
        def _():
            lines = pl.ds(aligned(block * rows, rows), rows)
            move(0, wide, sum_down.at[lines, pl.ds(aligned(kind * TILE, TILE), TILE)])

        @pl.when(in_ffn & (kind >= 2))
        def _():
            inner = plan.blocks * BLOCK
            base = ((kind - 2) // 2) * inner
            for piece in range(4):
                shard = (kind % 2) * 4 + piece
                start = base + shard * (inner // shards) + block * (BLOCK // shards)
                columns = pl.ds(aligned(start, 128), 128)
                move(piece, wide.at[:, piece * 128 : (piece + 1) * 128], sum_in.at[:, columns])

        @pl.when((tile >= plan.ffn_tiles) & (tile < plan.ffn_tiles + 2))
        def _():
            start = aligned((tile - plan.ffn_tiles) * TILE, TILE)
            move(0, wide, sum_out.at[:, pl.ds(start, TILE)])

        width = plan.heads * q_ref.shape[0]
        for group, number in enumerate(plan.keys_tiles):

            @pl.when(tile == number)
            def _():
                for part in range(2):
                    start = part * width + group * (TILE // 2)
                    columns = slice(part * (TILE // 2), (part + 1) * (TILE // 2))
                    move(part, wide.at[:, columns], sum_qkv.at[:, pl.ds(start, TILE // 2)])

        for pair, number in enumerate(plan.value_tiles):

            @pl.when(tile == number)
            def _():
                move(0, wide, sum_qkv.at[:, pl.ds(2 * width + pair * TILE, TILE)])

    stream = Stream(net, refs, writes)
    stages = stream.stages()

    def load(index, origin, landing):
        return pltpu.make_async_copy(origin, landing, load_sem.at[index])

    def weight_loads(block):
        if block < 2:
            into, down = early[2 * block], early[2 * block + 1]
        else:
            into, down = gather_to[2 * (block - 2)], gather_to[2 * (block - 2) + 1]
        return [
            load(0, into.at[:, pl.ds(0, BLOCK)], w_gate),
            load(1, into.at[:, pl.ds(BLOCK, BLOCK)], w_up),
            load(2, down, w_down),
        ]

    first_loads = [load(3, normed_hbm, normed), load(4, given_hbm, given), load(5, hidden_hbm, acc)]
    hidden_load = load(5, hidden_hbm, acc)
    result_store = load(6, act, result_hbm)
    attended_load = load(7, attended_hbm, w_down)
    out_load = load(8, out_hbm, d_up.at[0])
    normed_one_load = load(9, normed_one_hbm, turned)
    x_load = load(10, x_hbm, normed)
    tokens_store = load(11, acc, tokens_hbm)

    def qkv_loads(group):
        width = qkv_hbm.shape[1] // 3
        part = width // plan.groups
        page = act_t if group % 2 == 0 else d_up.at[0]
        return [
            load(
                12 + index,
                qkv_hbm.at[:, pl.ds(index * width + group * part, part)],
                page.at[:, pl.ds(index * part, part)],
            )
            for index in range(3)
        ]

    def at(place):
        return pl.when(step == place)

    def start(copies):
        for copy in copies:
            copy.start()

    def wait(copies):
        for copy in copies:
            copy.wait()

    gathers = [
        gather_steps(
            net, gather_from[i], gather_to[i], gather_local.at[i], gather_send.at[i], gather_recv.at[i]
        )
        for i in range(4)
    ]
    gather_places = ((0, 1, 3, 5, 6, 7, 9), (6, 8, 9, 11, 12, 14, 15))

    @at(0)
    def _():
        net.greet()
        start(weight_loads(0) + first_loads)

    for pair, places in enumerate(gather_places):
        for index, place in enumerate(places):

            @at(place)
            def _():
                gathers[2 * pair][index]()
                gathers[2 * pair + 1][index]()

    for stage in range(len(STAGES) - 1, 0, -1):
        tile, known = plan.tile_at(step - STAGES[stage])
        pl.when(known)(functools.partial(stages[stage], tile))

    @at(0)
    def _():
        wait(first_loads)
        turned[...] = normed[...].T

    for block in range(plan.blocks):

        @at(block * SUBSTEPS)
        def _():
            wait(weight_loads(block))

        if block + 1 < plan.blocks:

            @at(block * SUBSTEPS + SUBSTEPS - 1)
            def _():
                start(weight_loads(block + 1))

    block, sub = step // SUBSTEPS, step % SUBSTEPS
    slot = block % 2
    in_ffn = step < plan.ffn

    @pl.when(in_ffn & (sub < 2))
    def _():
        columns = pl.ds(aligned(sub * TILE, TILE), TILE)
        d_act = product(given[...], w_down[columns, :], COLUMNS_BY_COLUMNS)
        gate = product(normed[...], w_gate[:, columns])
        up = product(normed[...], w_up[:, columns])
        sigmoid = jax.nn.sigmoid(gate)
        swish = gate * sigmoid
        act[:, columns] = (swish * up).astype(jnp.bfloat16)
        d_gate[slot, :, columns] = (d_act * up * sigmoid * (1.0 + gate * (1.0 - sigmoid))).astype(jnp.bfloat16)
        d_up[slot, :, columns] = (d_act * swish).astype(jnp.bfloat16)

    @pl.when(in_ffn & (sub == 2))
    def _():
        acc[...] += product(act[...], w_down[...])
        act_t[...] = act[...].T

    @pl.when(in_ffn & (sub == 3))
    def _():
        part = product(d_gate[slot], w_gate[...], COLUMNS_BY_COLUMNS)

        @pl.when(block == 0)
        def _():
            through[...] = part

        @pl.when(block > 0)
        def _():
            through[...] += part

    @pl.when(in_ffn & (sub == 4))
    def _():
        through[...] += product(d_up[slot], w_up[...], COLUMNS_BY_COLUMNS)

    last_sum = plan.ffn - SUBSTEPS + 2

    @at(last_sum)
    def _():
        act[...] = acc[...].astype(jnp.bfloat16)
        result_store.start()

    @at(last_sum + 1)
    def _():
        start([hidden_load, attended_load])

    @at(last_sum + 3)
    def _():
        result_store.wait()

    row_block = 128

    @at(plan.norm)
    def _():
        out_load.start()
        hidden_load.wait()
        grad_gain_two_ref[...] = jnp.zeros_like(grad_gain_two_ref)

        @pl.loop(0, acc.shape[0] // row_block)
        def _(index):
            lines = pl.ds(aligned(index * row_block, row_block), row_block)
            back, grad_gain = norm_back(through[lines, :], acc[lines, :], gain_two_ref[...])
            d_hidden = given[lines, :].astype(jnp.float32) + back
            acc[lines, :] = d_hidden
            d_gate[0, lines, :] = d_hidden.astype(jnp.bfloat16)
            grad_gain_two_ref[...] += grad_gain

    @at(plan.branch)
    def _():
        out_load.wait()
        act[...] = product(d_up[0], d_gate[0], COLUMNS_BY_COLUMNS).astype(jnp.bfloat16)

    for group in range(plan.groups):
        ready = plan.ready[group]

        if group == 0:

            @at(plan.attend)
            def _():
                start(qkv_loads(0))

        @at(ready)
        def _():
            wait(qkv_loads(group))
            if group + 1 < plan.groups:
                start(qkv_loads(group + 1))
            page = act_t if group % 2 == 0 else d_up.at[0]
            quarter = TILE // 2
            base = (group % 2) * TILE
            part = product(page[:, :TILE], w_gate[base : base + TILE, :])
            values = (group // 2) * TILE + (group % 2) * quarter
            part = part + product(page[:, TILE : TILE + quarter], w_up[values : values + quarter, :])
            if group == 0:
                through[...] = part
            else:
                through[...] += part

    @at(plan.out)
    def _():
        attended_load.wait()
        start([normed_one_load, x_load])

    @at(plan.births[plan.keys_tiles[0]])
    def _():
        normed_one_load.wait()

    @pl.when((heads_at >= 0) & (heads_at < plan.heads))
    def _():
        depth = q_ref.shape[0]
        head = heads_at
        group = head // plan.per_group
        q_at = (group % 2) * TILE + (head % plan.per_group) * depth
        k_at = q_at + TILE // 2
        v_at = (group // 2) * TILE + (head % (2 * plan.per_group)) * depth

        def rows(start):
            return pl.ds(aligned(start, depth), depth)

        attend_back_head(
            2,
            head,
            bias_ref,
            q_ref,
            k_ref,
            v_ref,
            act.at[rows(head * depth)],
            wide_ref,
            lse_ref,
            var_ref,
            valid_ref,
            cos_ref,
            sin_ref,
            w_gate.at[rows(q_at)],
            w_gate.at[rows(k_at)],
            w_up.at[rows(v_at)],
            db_ref,
            query_ref,
            given_aug_ref,
            dk_acc,
            dv_acc,
        )

    tile, known = plan.tile_at(step)

    def birth(left, right, dims=(((1,), (0,)), ((), ()))):
        for which, target in ((net.core, stream.kept.at[tile % KEPT]), (1 - net.core, stream.give.at[tile % GIVEN])):
            lines = [
                left[pl.ds(aligned(shard * 2 * half + which * half, half), half), :] for shard in range(shards)
            ]
            out = product(jnp.concatenate(lines, axis=0), right, dims).astype(jnp.bfloat16)
            for shard in range(shards):
                target[shard] = out[shard * half : (shard + 1) * half]

    kind, source = tile % SUBSTEPS, (tile // SUBSTEPS) % 2
    in_tiles = known & (tile < plan.ffn_tiles)
    columns = pl.ds(aligned((kind % 2) * TILE, TILE), TILE)
    pl.when(in_tiles & (kind < 2))(lambda: birth(act_t, given[:, columns]))
    pl.when(in_tiles & (kind >= 2) & (kind < 4))(lambda: birth(turned, d_gate[source, :, columns]))
    pl.when(in_tiles & (kind >= 4))(lambda: birth(turned, d_up[source, :, columns]))
    for number in range(2):
        at(plan.out + number)(
            lambda: birth(w_down, d_gate[0, :, number * TILE : (number + 1) * TILE])
        )
    for group, number in enumerate(plan.keys_tiles):
        base = (group % 2) * TILE
        at(plan.births[number])(lambda: birth(turned, w_gate[base : base + TILE, :], COLUMNS_BY_COLUMNS))
    for pair, number in enumerate(plan.value_tiles):
        base = pair * TILE
        at(plan.births[number])(lambda: birth(turned, w_up[base : base + TILE, :], COLUMNS_BY_COLUMNS))
    pl.when(known)(lambda: stream.born(tile))

    @at(plan.last)
    def _():
        x_load.wait()
        grad_gain_one_ref[...] = jnp.zeros_like(grad_gain_one_ref)

        @pl.loop(0, acc.shape[0] // row_block)
        def _(index):
            lines = pl.ds(aligned(index * row_block, row_block), row_block)
            values = normed[lines, :].astype(jnp.float32)
            back, grad_gain = norm_back(through[:, lines].T, values, gain_one_ref[...])
            acc[lines, :] = acc[lines, :] + back
            grad_gain_one_ref[...] += grad_gain

        tokens_store.start()

    @at(plan.grid - 1)
    def _():
        tokens_store.wait()


def back(line, early, sources, normed_two, given, hidden, attended_t, out_weight, normed_t, x, qkv_weight,
         gain_one, gain_two, bias, qkv_t, wide_t, log_sums, variates, valid, cos_t, sin_t):
    shards = lax.axis_size("shard")
    rows, width = x.shape
    heads = log_sums.shape[0]
    depth = width // heads
    blocks = 4
    plan = Plan(blocks, heads)
    low = jnp.bfloat16
    owned = width // shards
    inner = blocks * BLOCK

    def head_at(step):
        return jnp.clip(step - plan.attend, 0, heads - 1)

    def part(which):
        return pl.BlockSpec((depth, rows), lambda step: (which * heads + head_at(step), 0))

    page = pltpu.VMEM((BLOCK, BLOCK), low)
    copies = gather_count(line)
    row = pl.BlockSpec((1, width), lambda step: (0, 0))
    return pl.pallas_call(
        functools.partial(back_kernel, plan, line, shards),
        grid=(plan.grid,),
        out_shape=[
            like((rows, width), low),
            like((rows, width), jnp.float32),
            like((owned, 2 * inner), jnp.float32),
            like((inner // shards, width), jnp.float32),
            like((owned, width), jnp.float32),
            like((owned, 3 * width), jnp.float32),
        ]
        + [like((shards * source.shape[0], source.shape[1]), low) for source in sources]
        + [
            like((1, width), jnp.float32),
            like((1, width), jnp.float32),
            like((heads, 2, rows // 2), jnp.float32),
        ],
        in_specs=[ANY] * 16
        + [whole(1, width), whole(1, width)]
        + [
            pl.BlockSpec(memory_space=pltpu.SMEM),
            part(0),
            part(1),
            part(2),
            pl.BlockSpec((depth, rows), lambda step: (head_at(step), 0)),
            pl.BlockSpec((1, 1, rows), lambda step: (head_at(step), 0, 0)),
            whole(1, rows),
            whole(1, rows),
            whole(*cos_t.shape),
            whole(*sin_t.shape),
        ],
        out_specs=[ANY] * 10
        + [row, row, pl.BlockSpec((1, 2, rows // 2), lambda step: (head_at(step), 0, 0))],
        scratch_shapes=[page] * 8
        + [
            pltpu.VMEM((2, BLOCK, BLOCK), low),
            pltpu.VMEM((2, BLOCK, BLOCK), low),
            pltpu.VMEM((rows, width), jnp.float32),
            pltpu.VMEM((rows, width), jnp.float32),
            pltpu.VMEM((2 * depth + FEATURES, rows), low),
            pltpu.VMEM((depth + FEATURES, rows), low),
            pltpu.VMEM((rows, depth), jnp.float32),
            pltpu.VMEM((rows, depth), jnp.float32),
            pltpu.SemaphoreType.DMA((15,)),
            pltpu.SemaphoreType.DMA((4,)),
            pltpu.SemaphoreType.DMA((4, copies)),
            pltpu.SemaphoreType.DMA((4, copies)),
        ]
        + stream_scratch(line, shards, owned // 2),
        compiler_params=pltpu.CompilerParams(
            collective_id=9, has_side_effects=True, vmem_limit_bytes=64 << 20
        ),
        name="back",
    )(
        normed_two, given, hidden, *early, *sources, attended_t, out_weight, normed_t, x, qkv_weight,
        gain_one, gain_two, bias, qkv_t, qkv_t, qkv_t, wide_t, log_sums, variates, valid, cos_t, sin_t,
    )


def rope_tables(time_ids):
    half = HEAD_DIM // 2
    exponent = jnp.arange(half).astype(jnp.float32) * (2.0 / HEAD_DIM)
    inverse = jnp.exp(-jnp.log(rope_base) * exponent)
    angles = inverse[:, None] * time_ids.astype(jnp.float32)
    return jnp.cos(angles), jnp.sin(angles)


def pack_small(attn_gain, ffn_gain, attn_bias):
    heads = attn_bias.shape[1]
    small = jnp.zeros((16, 128), jnp.float32)
    small = small.at[0].set(attn_gain.astype(jnp.float32)).at[1].set(ffn_gain.astype(jnp.float32))
    return small.at[2:4, :heads].set(attn_bias.astype(jnp.float32))


def pack_grads(shards, gain_one, gain_two, bias):
    heads = bias.shape[1] // shards
    small = jnp.zeros((shards, 16, 128), jnp.float32)
    small = small.at[:, 0].set(gain_one.reshape(shards, -1)).at[:, 1].set(gain_two.reshape(shards, -1))
    return small.at[:, 2:4, :heads].set(jnp.swapaxes(bias.reshape(2, shards, heads), 0, 1))


def shards(
    line,
    tokens,
    lengths,
    variate_ids,
    time_ids,
    attn_gain,
    w_qkv,
    attn_bias,
    w_out,
    ffn_gain,
    w_in,
    w_down,
    cotangent,
):
    parts = lax.axis_size("shard")
    length = variate_ids.shape[1]
    heads = attn_bias.shape[1]
    positions = jnp.arange(length)[None, :]
    key_valid = positions < lengths[:, None]
    valid = key_valid.astype(jnp.float32)
    given = jnp.where(key_valid.reshape(length, 1), cotangent, jnp.zeros_like(cotangent))
    cos_t, sin_t = rope_tables(time_ids)

    def gathering(number, *weights):
        return Carried(line, number, gathers=weights) if line else None

    def reducing(number, *grads):
        return Carried(line, number, reduces=grads) if line else None

    if line:
        small, full_qkv = carry_alone(gathering(1, pack_small(attn_gain, ffn_gain, attn_bias), w_qkv), "gather_qkv")
        qkv_weight = full_qkv
        small = small.reshape(parts, -1, small.shape[1])
        gain_one, gain_two = small[:, 0].reshape(1, -1), small[:, 1].reshape(1, -1)
        bias = jnp.swapaxes(small[:, 2:4, :heads], 0, 1).reshape(2, -1)
    else:
        gain_one, gain_two, qkv_weight, out_weight, in_weight, down_weight = (
            lax.all_gather(part, "shard", axis=0, tiled=True)
            for part in (attn_gain, ffn_gain, w_qkv, w_out, w_in, w_down)
        )
        bias = lax.all_gather(attn_bias, "shard", axis=1, tiled=True).astype(jnp.float32)
        gain_one = gain_one.astype(jnp.float32).reshape(1, -1)
        gain_two = gain_two.astype(jnp.float32).reshape(1, -1)

    (qkv_t, normed_t), came = project(tokens, gain_one, qkv_weight, cos_t, sin_t, gathering(2, w_out))
    out_weight = came[0] if line else out_weight
    if line:
        owned = w_in.shape[1] // (2 * parts)
        into = [
            jnp.concatenate(
                [w_in[:, piece * owned + block * 128 :][:, :128] for piece in range(2 * parts)], axis=1
            )
            for block in range(4)
        ]
        down = [w_down[block * 128 : (block + 1) * 128] for block in range(4)]
        pairs = [part for pair in zip(into, down) for part in pair]
        (attended_t, wide_t, log_sums), early = attend_forward(
            qkv_t, variate_ids, valid, bias, HEADS, gathering(3, *pairs[:4])
        )
        (hidden, normed_two), _ = branch(attended_t, out_weight, tokens, gain_two, None)
        result, grad_tokens, sum_in, sum_down, sum_out, sum_qkv, *rest = back(
            line, early, pairs[4:], normed_two, given, hidden, attended_t, out_weight, normed_t, tokens, qkv_weight,
            gain_one, gain_two, bias, qkv_t, wide_t, log_sums, variate_ids, valid, cos_t, sin_t,
        )
        grad_gain_one, grad_gain_two, bias_parts = rest[4:]
        packed = pack_grads(parts, grad_gain_one, grad_gain_two, jnp.sum(bias_parts, axis=2).T)
        (small,) = carry_alone(reducing(8, [packed]), "reduce_small")
        return (
            result,
            grad_tokens,
            small[0],
            sum_qkv,
            small[2:4, :heads],
            sum_out,
            small[1],
            sum_in,
            sum_down,
        )
    (attended_t, wide_t, log_sums), came = attend_forward(
        qkv_t, variate_ids, valid, bias, HEADS, None
    )
    (hidden, normed_two), _ = branch(attended_t, out_weight, tokens, gain_two, None)
    (act, to_gate, to_up), _ = widen(normed_two, in_weight, None)
    (result, grad_down, d_gate, d_up), _ = narrow(act, to_gate, to_up, down_weight, given, hidden, None)
    (grad_gate, grad_up), _ = grad_into(normed_two, d_gate, d_up, None)
    (d_hidden, d_branch, grad_gain_two), _ = ffn_back(
        d_gate, d_up, in_weight, hidden, gain_two, given, None
    )
    (grad_out, given_t), _ = branch_back(attended_t, out_weight, d_branch, None)
    (dq, dk, dv, bias_parts), _ = attend_backward(
        qkv_t,
        given_t,
        wide_t,
        log_sums,
        variate_ids,
        valid,
        bias,
        cos_t,
        sin_t,
        HEADS,
        None,
    )
    (grad_qkv, grad_tokens, grad_gain_one), _ = project_back(
        normed_t, dq, dk, dv, qkv_weight, tokens, gain_one, d_hidden, None
    )
    grad_bias = jnp.sum(bias_parts, axis=2).T
    grads = (
        (grad_gain_one.reshape(-1), 0),
        (grad_qkv, 0),
        (grad_bias, 1),
        (grad_out, 0),
        (grad_gain_two.reshape(-1), 0),
        (jnp.concatenate([grad_gate, grad_up], axis=1), 0),
        (grad_down, 0),
    )
    owned = [
        lax.psum_scatter(grad.astype(jnp.bfloat16), "shard", scatter_dimension=axis, tiled=True)
        for grad, axis in grads
    ]
    return (result, grad_tokens) + tuple(lax.psum(part, "rep").astype(jnp.float32) for part in owned)


def solution(mesh):
    placed = (
        P(("shard", "rep"), None),
        P(("shard", "rep")),
        P(("shard", "rep"), None),
        P(("shard", "rep"), None),
        P("shard"),
        P("shard", None),
        P(None, "shard"),
        P("shard", None),
        P("shard"),
        P("shard", None),
        P("shard", None),
        P(("shard", "rep"), None),
    )
    line = mesh.shape["shard"] // 2 if (mesh.shape["shard"], mesh.shape["rep"]) == (8, 4) else 0
    return jax.shard_map(
        functools.partial(shards, line),
        mesh=mesh,
        in_specs=placed,
        out_specs=(
            P(("shard", "rep"), None),
            P(("shard", "rep"), None),
            P("shard"),
            P("shard", None),
            P(None, "shard"),
            P("shard", None),
            P("shard"),
            P("shard", None),
            P("shard", None),
        ),
        check_vma=False,
    )
```

```python
import functools

import jax
import jax.numpy as jnp
from jax import lax
from jax.experimental import pallas as pl
from jax.experimental.pallas import tpu as pltpu
from jax.sharding import PartitionSpec as P

HEADS = 16
HEAD_DIM = 64


norm_eps = 1e-06
rope_base = 10000.0
masked_score = -1000000000.0

MESH = pl.DeviceIdType.MESH
ANY = pl.BlockSpec(memory_space=pl.ANY)


class Net:
    def __init__(self, line):
        shard, rep = lax.axis_index("shard"), lax.axis_index("rep")
        self.line = line
        self.z, self.y = shard // 2, shard % 2
        self.x, self.core = rep // 2, rep % 2
        self.own = shard
        self.sibling = (shard, self.x * 2 + 1 - self.core)
        self.across_x = (shard, (1 - self.x) * 2 + self.core)
        self.across_y = (self.z * 2 + 1 - self.y, rep)
        self.above = (jnp.minimum(self.z + 1, line - 1) * 2 + self.y, rep)
        self.below = (jnp.maximum(self.z - 1, 0) * 2 + self.y, rep)
        self.has_above = self.z < line - 1
        self.has_below = self.z > 0

    def greet(self):
        barrier = pltpu.get_barrier_semaphore()

        def hail(partner):
            pl.semaphore_signal(barrier, inc=1, device_id=partner, device_id_type=MESH)

        for partner in (self.sibling, self.across_x, self.across_y):
            hail(partner)
        pl.when(self.has_above)(lambda: hail(self.above))
        pl.when(self.has_below)(lambda: hail(self.below))
        neighbours = jnp.where(self.has_above, 1, 0) + jnp.where(self.has_below, 1, 0)
        pl.semaphore_wait(barrier, 3 + neighbours)


def aligned(value, step):
    return pl.multiple_of(value, step)


def gather_count(line):
    return 2 * line + 3 * 2 * line


def gather_steps(net, source, full, local_sem, send_sem, recv_sem):
    line = net.line
    height, columns = source.shape
    half = height // 2
    split = columns % 1024 == 0
    only = columns * 3 // 8 if split else 0
    shared = columns - 2 * only
    rows = pl.ds(aligned(net.core * half, half), half)
    carried = pl.ds(aligned(net.x * only, 128), only + shared) if split else pl.ds(0, columns)
    lone = pl.ds(aligned(net.x * (only + shared), 128), only) if split else None

    def remote(origin, landing, index, target):
        return pltpu.make_async_remote_copy(
            src_ref=origin,
            dst_ref=landing,
            send_sem=send_sem.at[index],
            recv_sem=recv_sem.at[index],
            device_id=target,
            device_id_type=MESH,
        )

    def held(z, y, which=None):
        lines = pl.ds(aligned((z * 2 + y) * height + net.core * half, half), half)
        return full.at[lines] if which is None else full.at[lines, which]

    def piece(z, y):
        return held(z, y, carried)

    def over_z(z, target, base):
        return remote(piece(z, net.y), piece(z, net.y), base + z, target)

    def over_y(z):
        return remote(piece(z, net.y), piece(z, net.y), 2 * line + z, net.across_y)

    def over_x(z, y):
        part = held(z, y, lone)
        return remote(part, part, 3 * line + y * line + z, net.across_x)

    def to_core(z, y):
        part = held(z, y)
        return remote(part, part, 5 * line + y * line + z, net.sibling)

    mine = source.at[rows, carried]
    local = pltpu.make_async_copy(source, full.at[pl.ds(aligned(net.own * height, height), height)], local_sem)
    first_y = remote(mine, piece(net.z, net.y), 2 * line + net.z, net.across_y)
    first_up = remote(mine, piece(net.z, net.y), net.z, net.above)
    first_down = remote(mine, piece(net.z, net.y), line + net.z, net.below)

    def onward(z, y):
        if split:
            over_x(z, y).start()
        else:
            to_core(z, y).start()

    def start():
        first_y.start()
        pl.when(net.has_above)(first_up.start)
        pl.when(net.has_below)(first_down.start)
        local.start()

    def arrive(hops):
        @pl.when(net.z >= hops)
        def _():
            z = net.z - hops
            over_z(z, net.above, 0).wait_recv()
            pl.when(net.has_above)(over_z(z, net.above, 0).start)
            over_y(z).start()
            onward(z, net.y)

        @pl.when(net.z < line - hops)
        def _():
            z = net.z + hops
            over_z(z, net.below, line).wait_recv()
            pl.when(net.has_below)(over_z(z, net.below, line).start)
            over_y(z).start()
            onward(z, net.y)

    def arrive_y(hops):
        def one(z):
            remote(piece(z, 1 - net.y), piece(z, 1 - net.y), 2 * line + z, net.across_y).wait_recv()
            onward(z, 1 - net.y)

        if hops == 0:
            one(net.z)
        else:
            pl.when(net.z >= hops)(lambda: one(net.z - hops))
            pl.when(net.z < line - hops)(lambda: one(net.z + hops))

    def arrive_x(hops, own_y):
        def one(z):
            y = net.y if own_y else 1 - net.y
            part = held(z, y, pl.ds(aligned((1 - net.x) * (only + shared), 128), only))
            remote(part, part, 3 * line + y * line + z, net.across_x).wait_recv()
            to_core(z, y).start()

        if not split:
            return
        if hops == 0:
            one(net.z)
        else:
            pl.when(net.z >= hops)(lambda: one(net.z - hops))
            pl.when(net.z < line - hops)(lambda: one(net.z + hops))

    def step(hops):
        def run():
            arrive_y(hops - 1)
            if hops < line:
                arrive(hops)
            if hops >= 2:
                arrive_x(hops - 2, False)
                arrive_x(hops - 1, True)

        return run

    def last():
        arrive_x(line - 1, False)

    def finish():
        local.wait()
        first_y.wait_send()

        @pl.when(net.has_above)
        def _():
            first_up.wait_send()
            for hops in range(1, line - 1):
                pl.when(net.z >= hops)(over_z(net.z - hops, net.above, 0).wait_send)

        @pl.when(net.has_below)
        def _():
            first_down.wait_send()
            for hops in range(1, line - 1):
                pl.when(net.z < line - hops)(over_z(net.z + hops, net.below, line).wait_send)

        for z in range(line):

            def others():
                over_y(z).wait_send()
                if split:
                    over_x(z, net.y).wait_send()
                to_core(z, net.y).wait()

            pl.when(net.z != z)(others)
            if split:
                over_x(z, 1 - net.y).wait_send()
            to_core(z, 1 - net.y).wait()

    return [start] + [step(hops) for hops in range(1, line + 1)] + [last, finish]


REDUCE_BUFFERS = 9


def reduce_split(columns):
    only = columns // 4 if columns % 512 == 0 else 0
    return only, columns - 2 * only


def reduce_scratch(line, shards, half, columns, dtype):
    only, shared = reduce_split(columns)
    carried = only + shared
    return [
        pltpu.VMEM((shards, half, columns), dtype),
        pltpu.VMEM((shards, half, columns), dtype),
        pltpu.VMEM((shards, half, max(only, 128)), dtype),
        pltpu.VMEM((line, half, carried), dtype),
        pltpu.VMEM((line + 1, half, carried), dtype),
        pltpu.VMEM((half, carried), dtype),
        pltpu.VMEM((half, columns), dtype),
        pltpu.VMEM((half, columns), dtype),
        pltpu.VMEM((2 * half, columns), jnp.float32),
    ]


def reduce_count(line):
    return 3 * line + 4


def reduce_steps(net, grad, out, column_start, out_start, buffers, local_sem, send_sem, recv_sem):
    kept, got, from_x, from_y, from_z, late_x, final, swapped, wide = buffers
    line = net.line
    shards, half, width = kept.shape
    only, shared = reduce_split(width)
    both = only + shared
    columns = pl.ds(column_start, width)
    mine = pl.ds(aligned(net.core * half, half), half)
    theirs = pl.ds(aligned((1 - net.core) * half, half), half)
    if only:
        carried = pl.ds(aligned(net.x * only, 128), both)
        lone = pl.ds(aligned(net.x * both, 128), only)
        their_lone = pl.ds(aligned((1 - net.x) * both, 128), only)
    else:
        carried = pl.ds(0, width)

    def remote(origin, landing, index, target):
        return pltpu.make_async_remote_copy(
            src_ref=origin,
            dst_ref=landing,
            send_sem=send_sem.at[index],
            recv_sem=recv_sem.at[index],
            device_id=target,
            device_id_type=MESH,
        )

    local = pltpu.make_async_copy(grad.at[:, mine, columns], kept, local_sem.at[0])
    halves = remote(grad.at[:, theirs, columns], got, 2 * line, net.sibling)
    written = pltpu.make_async_copy(wide, out.at[:, pl.ds(out_start, width)], local_sem.at[1])
    to_core = remote(final, swapped, 2 * line + 1, net.sibling)
    end_x = remote(kept.at[net.own, :, carried], late_x, 2 * line + 2, net.across_x)
    if only:
        over_x = remote(kept.at[:, :, their_lone], from_x, 2 * line + 3, net.across_x)

    def over_y(z):
        part = kept.at[z * 2 + 1 - net.y, :, carried]
        return remote(part, from_y.at[z], 2 * line + 4 + z, net.across_y)

    def up(z):
        return remote(kept.at[z * 2 + net.y, :, carried], from_z.at[z + 1], z, net.above)

    def down(z):
        return remote(kept.at[z * 2 + net.y, :, carried], from_z.at[z], line + z, net.below)

    def add(shard, part):
        kept[shard, :, carried] = kept[shard, :, carried] + part

    def first():
        halves.start()
        local.start()

    def second():
        local.wait()
        halves.wait_recv()

        @pl.loop(0, shards)
        def _(shard):
            kept[shard] = kept[shard] + got[shard]

        if only:
            over_x.start()

    def third():
        if only:
            over_x.wait_recv()

            @pl.loop(0, shards)
            def _(shard):
                kept[shard, :, lone] = kept[shard, :, lone] + from_x[shard]

        for z in range(line):
            over_y(z).start()

    def fourth():
        for z in range(line):
            over_y(z).wait_recv()

        @pl.loop(0, line)
        def _(z):
            add(z * 2 + net.y, from_y[z])

    def hop(step):
        def run():
            @pl.when(net.z == step)
            def _():
                for z in range(line - 1, step, -1):
                    if step > 0:
                        up(z).wait_recv()
                        add(z * 2 + net.y, from_z[z + 1])
                    up(z).start()

            @pl.when(net.z == line - 1 - step)
            def _():
                for z in range(line - 1 - step):
                    if step > 0:
                        down(z).wait_recv()
                        add(z * 2 + net.y, from_z[z])
                    down(z).start()

        return run

    def land():
        @pl.when(net.has_below)
        def _():
            up(net.z).wait_recv()
            add(net.own, from_z[net.z + 1])

        @pl.when(net.has_above)
        def _():
            down(net.z).wait_recv()
            add(net.own, from_z[net.z])

        end_x.start()

    def meet():
        end_x.wait_recv()
        if only:
            final[:, lone] = kept[net.own, :, lone]
            for x in range(2):

                @pl.when(net.x == x)
                def _():
                    start = 0 if x == 1 else shared
                    final[:, (1 - x) * both : (1 - x) * both + only] = late_x[:, start : start + only]
                    other = shared * 0 + (only if x == 1 else 0)
                    final[:, only:both] = kept[net.own, :, only:both] + late_x[:, other : other + shared]
        else:
            final[...] = kept[net.own] + late_x[...]
        to_core.start()
        wide[mine, :] = final[...].astype(jnp.float32)

    def swap():
        to_core.wait_recv()
        wide[theirs, :] = swapped[...].astype(jnp.float32)
        written.start()

    def finish():
        written.wait()
        halves.wait_send()
        if only:
            over_x.wait_send()
        for z in range(line):
            over_y(z).wait_send()
            pl.when(net.z < z)(up(z).wait_send)
            pl.when(net.z > z)(down(z).wait_send)
        end_x.wait_send()
        to_core.wait_send()

    hops = [hop(step) for step in range(line - 1)]

    def fourth_and_hop():
        fourth()
        hops[0]()

    return [first, second, third, fourth_and_hop] + hops[1:] + [land, meet, swap, finish]


ROWS_BY_ROWS = (((0,), (0,)), ((), ()))
COLUMNS_BY_COLUMNS = (((1,), (1,)), ((), ()))


def product(first_op, second_op, dims=(((1,), (0,)), ((), ()))):
    return lax.dot_general(first_op, second_op, dims, preferred_element_type=jnp.float32)


def inverse_rms(values):
    return lax.rsqrt(jnp.mean(values * values, axis=1, keepdims=True) + norm_eps)


def run(body, *, grid, out_shape, in_specs, out_specs, scratch_shapes, name, operands):
    return pl.pallas_call(
        body,
        grid=(grid,),
        out_shape=out_shape,
        in_specs=in_specs,
        out_specs=out_specs,
        scratch_shapes=scratch_shapes,
        compiler_params=pltpu.CompilerParams(vmem_limit_bytes=60 << 20),
        name=name,
    )(*operands)


def whole(*shape):
    return pl.BlockSpec(shape, lambda step: (0,) * len(shape), pipeline_mode=pl.Buffered(1))


def like(shape, dtype):
    return jax.ShapeDtypeStruct(shape, dtype)


def project_kernel(turned, x_ref, gain_ref, w_ref, cos_ref, sin_ref, out_ref, normed_ref):
    step = pl.program_id(0)

    @pl.when(step == 0)
    def _():
        values = x_ref[...].astype(jnp.float32)
        normed = values * inverse_rms(values) * gain_ref[...]
        normed_ref[...] = normed.T.astype(jnp.bfloat16)

    out = product(w_ref[...], normed_ref[...], ROWS_BY_ROWS)

    @pl.when(step < turned)
    def _():
        cos, sin = cos_ref[...], sin_ref[...]
        half = cos.shape[0]
        for start in range(0, out.shape[0], 2 * half):
            first, second = out[start : start + half], out[start + half : start + 2 * half]
            out_ref[start : start + half, :] = (first * cos - second * sin).astype(jnp.bfloat16)
            out_ref[start + half : start + 2 * half, :] = (second * cos + first * sin).astype(jnp.bfloat16)

    @pl.when(step >= turned)
    def _():
        out_ref[...] = out.astype(jnp.bfloat16)


def project(x, gain, weight, cos_t, sin_t):
    rows, width = x.shape
    columns = weight.shape[1]
    block = 512
    return run(
        functools.partial(project_kernel, 2 * width // block),
        grid=columns // block,
        out_shape=[like((columns, rows), jnp.bfloat16), like((width, rows), jnp.bfloat16)],
        in_specs=[
            whole(rows, width),
            whole(1, width),
            pl.BlockSpec((width, block), lambda step: (0, step)),
            whole(*cos_t.shape),
            whole(*sin_t.shape),
        ],
        out_specs=[
            pl.BlockSpec((block, rows), lambda step: (step, 0)),
            pl.BlockSpec((width, rows), lambda step: (0, 0)),
        ],
        scratch_shapes=[],
        name="project",
        operands=[x, gain, weight, cos_t, sin_t],
    )


def branch_kernel(att_ref, w_ref, x_ref, gain_ref, hidden_ref, normed_ref):
    hidden = x_ref[...].astype(jnp.float32) + product(att_ref[...], w_ref[...], ROWS_BY_ROWS)
    hidden_ref[...] = hidden
    normed_ref[...] = (hidden * inverse_rms(hidden) * gain_ref[...]).astype(jnp.bfloat16)


def branch(attended_t, weight, x, gain):
    rows, width = x.shape
    block = 256
    row = pl.BlockSpec((block, width), lambda step: (step, 0))
    return run(
        branch_kernel,
        grid=rows // block,
        out_shape=[like((rows, width), jnp.float32), like((rows, width), jnp.bfloat16)],
        in_specs=[
            pl.BlockSpec((width, block), lambda step: (0, step)),
            whole(*weight.shape),
            row,
            whole(1, width),
        ],
        out_specs=[row, row],
        scratch_shapes=[],
        name="branch",
        operands=[attended_t, weight, x, gain],
    )


def widen_kernel(normed_ref, gate_ref, up_ref, act_ref, to_gate_ref, to_up_ref):
    normed = normed_ref[...]
    gate = product(normed, gate_ref[...])
    up = product(normed, up_ref[...])
    sigmoid = jax.nn.sigmoid(gate)
    swish = gate * sigmoid
    act_ref[...] = (swish * up).astype(jnp.bfloat16)
    to_gate_ref[...] = (up * sigmoid * (1.0 + gate * (1.0 - sigmoid))).astype(jnp.bfloat16)
    to_up_ref[...] = swish.astype(jnp.bfloat16)


def widen(normed, weight):
    rows, width = normed.shape
    inner = weight.shape[1] // 2
    block = 512
    steps = inner // block
    part = pl.BlockSpec((rows, block), lambda step: (0, step))
    return run(
        widen_kernel,
        grid=steps,
        out_shape=[like((rows, inner), jnp.bfloat16)] * 3,
        in_specs=[
            whole(rows, width),
            pl.BlockSpec((width, block), lambda step: (0, step)),
            pl.BlockSpec((width, block), lambda step: (0, steps + step)),
        ],
        out_specs=[part] * 3,
        scratch_shapes=[],
        name="widen",
        operands=[normed, weight, weight],
    )


def narrow_kernel(
    steps, act_ref, to_gate_ref, to_up_ref, w_ref, given_ref, hidden_ref, result_ref, grad_ref, d_gate_ref, d_up_ref, acc_ref
):
    step = pl.program_id(0)
    act, weight, given = act_ref[...], w_ref[...], given_ref[...]
    part = product(act, weight)

    @pl.when(step == 0)
    def _():
        acc_ref[...] = hidden_ref[...] + part

    @pl.when(step > 0)
    def _():
        acc_ref[...] += part

    @pl.when(step == steps - 1)
    def _():
        result_ref[...] = acc_ref[...].astype(jnp.bfloat16)

    grad_ref[...] = product(act, given, ROWS_BY_ROWS).astype(jnp.bfloat16)
    d_act = product(given, weight, COLUMNS_BY_COLUMNS)
    d_gate_ref[...] = (d_act * to_gate_ref[...].astype(jnp.float32)).astype(jnp.bfloat16)
    d_up_ref[...] = (d_act * to_up_ref[...].astype(jnp.float32)).astype(jnp.bfloat16)


def narrow(act, to_gate, to_up, weight, given, hidden):
    rows, inner = act.shape
    width = weight.shape[1]
    block = 512
    steps = inner // block
    part = pl.BlockSpec((rows, block), lambda step: (0, step))
    down = pl.BlockSpec((block, width), lambda step: (step, 0))
    return run(
        functools.partial(narrow_kernel, steps),
        grid=steps,
        out_shape=[
            like((rows, width), jnp.bfloat16),
            like((inner, width), jnp.bfloat16),
            like((rows, inner), jnp.bfloat16),
            like((rows, inner), jnp.bfloat16),
        ],
        in_specs=[part, part, part, down, whole(rows, width), whole(rows, width)],
        out_specs=[pl.BlockSpec((rows, width), lambda step: (0, 0)), down, part, part],
        scratch_shapes=[pltpu.VMEM((rows, width), jnp.float32)],
        name="narrow",
        operands=[act, to_gate, to_up, weight, given, hidden],
    )


def grad_in_kernel(normed_ref, d_gate_ref, d_up_ref, to_gate_ref, to_up_ref, turned_ref):
    @pl.when(pl.program_id(0) == 0)
    def _():
        turned_ref[...] = normed_ref[...].T

    to_gate_ref[...] = product(turned_ref[...], d_gate_ref[...]).astype(jnp.bfloat16)
    to_up_ref[...] = product(turned_ref[...], d_up_ref[...]).astype(jnp.bfloat16)


def grad_into(normed, d_gate, d_up):
    rows, width = normed.shape
    inner = d_gate.shape[1]
    block = 512
    part = pl.BlockSpec((rows, block), lambda step: (0, step))
    out = pl.BlockSpec((width, block), lambda step: (0, step))
    return run(
        grad_in_kernel,
        grid=inner // block,
        out_shape=[like((width, inner), jnp.bfloat16)] * 2,
        in_specs=[whole(rows, width), part, part],
        out_specs=[out, out],
        scratch_shapes=[pltpu.VMEM((width, rows), jnp.bfloat16)],
        name="grad_in",
        operands=[normed, d_gate, d_up],
    )


def norm_back(d_normed, values, gain):
    inverse = inverse_rms(values)
    unit = values * inverse
    scaled = d_normed * gain
    mean = jnp.mean(scaled * unit, axis=1, keepdims=True)
    return inverse * (scaled - unit * mean), jnp.sum(d_normed * unit, axis=0, keepdims=True)


def ffn_back_kernel(
    steps, d_gate_ref, d_up_ref, gate_ref, up_ref, hidden_ref, gain_ref, given_ref, d_hidden_ref, d_branch_ref, grad_gain_ref, acc_ref
):
    step = pl.program_id(0)
    part = product(d_gate_ref[...], gate_ref[...], COLUMNS_BY_COLUMNS)
    part = part + product(d_up_ref[...], up_ref[...], COLUMNS_BY_COLUMNS)

    @pl.when(step == 0)
    def _():
        acc_ref[...] = part

    @pl.when(step > 0)
    def _():
        acc_ref[...] += part

    @pl.when(step == steps - 1)
    def _():
        through, grad_gain = norm_back(acc_ref[...], hidden_ref[...], gain_ref[...])
        d_hidden = given_ref[...].astype(jnp.float32) + through
        d_hidden_ref[...] = d_hidden
        d_branch_ref[...] = d_hidden.astype(jnp.bfloat16)
        grad_gain_ref[...] = grad_gain


def ffn_back(d_gate, d_up, weight, hidden, gain, given):
    rows, width = hidden.shape
    inner = d_gate.shape[1]
    block = 512
    steps = inner // block
    part = pl.BlockSpec((rows, block), lambda step: (0, step))
    full = pl.BlockSpec((rows, width), lambda step: (0, 0))
    return run(
        functools.partial(ffn_back_kernel, steps),
        grid=steps,
        out_shape=[
            like((rows, width), jnp.float32),
            like((rows, width), jnp.bfloat16),
            like((1, width), jnp.float32),
        ],
        in_specs=[
            part,
            part,
            pl.BlockSpec((width, block), lambda step: (0, step)),
            pl.BlockSpec((width, block), lambda step: (0, steps + step)),
            whole(rows, width),
            whole(1, width),
            whole(rows, width),
        ],
        out_specs=[full, full, pl.BlockSpec((1, width), lambda step: (0, 0))],
        scratch_shapes=[pltpu.VMEM((rows, width), jnp.float32)],
        name="ffn_back",
        operands=[d_gate, d_up, weight, weight, hidden, gain, given],
    )


def branch_back_kernel(att_ref, w_ref, d_branch_ref, grad_ref, given_ref):
    d_branch = d_branch_ref[...]
    grad_ref[...] = product(att_ref[...], d_branch).astype(jnp.bfloat16)
    given_ref[...] = product(w_ref[...], d_branch, COLUMNS_BY_COLUMNS).astype(jnp.bfloat16)


def branch_back(attended_t, weight, d_branch):
    rows, width = d_branch.shape
    block = 256
    out = pl.BlockSpec((block, width), lambda step: (step, 0))
    turned = pl.BlockSpec((block, rows), lambda step: (step, 0))
    return run(
        branch_back_kernel,
        grid=attended_t.shape[0] // block,
        out_shape=[like(weight.shape, jnp.bfloat16), like(attended_t.shape, jnp.bfloat16)],
        in_specs=[turned, out, whole(rows, width)],
        out_specs=[out, turned],
        scratch_shapes=[],
        name="branch_back",
        operands=[attended_t, weight, d_branch],
    )


def project_back_kernel(
    steps, normed_ref, dq_ref, dk_ref, dv_ref, w_ref, x_ref, gain_ref, d_hidden_ref, grad_ref, tokens_ref, grad_gain_ref, acc_ref
):
    step = pl.program_id(0)
    third = steps // 3

    def run(d_ref):
        d_part = d_ref[...]
        grad_ref[...] = product(normed_ref[...], d_part, COLUMNS_BY_COLUMNS).astype(jnp.bfloat16)
        part = product(w_ref[...], d_part)

        @pl.when(step == 0)
        def _():
            acc_ref[...] = part

        @pl.when(step > 0)
        def _():
            acc_ref[...] += part

    for index, d_ref in enumerate((dq_ref, dk_ref, dv_ref)):
        pl.when(step // third == index)(functools.partial(run, d_ref))

    @pl.when(step == steps - 1)
    def _():
        values = x_ref[...].astype(jnp.float32)
        through, grad_gain = norm_back(acc_ref[...].T, values, gain_ref[...])
        tokens_ref[...] = d_hidden_ref[...] + through
        grad_gain_ref[...] = grad_gain


def project_back(normed_t, dq, dk, dv, weight, x, gain, d_hidden):
    rows, width = x.shape
    columns = weight.shape[1]
    block = 512
    steps = columns // block
    third = steps // 3
    full = pl.BlockSpec((rows, width), lambda step: (0, 0))

    def part(which):
        return pl.BlockSpec(
            (block, rows), lambda step: (jnp.clip(step - which * third, 0, third - 1), 0)
        )

    return run(
        functools.partial(project_back_kernel, steps),
        grid=steps,
        out_shape=[
            like((width, columns), jnp.bfloat16),
            like((rows, width), jnp.float32),
            like((1, width), jnp.float32),
        ],
        in_specs=[
            whole(*normed_t.shape),
            part(0),
            part(1),
            part(2),
            pl.BlockSpec((width, block), lambda step: (0, step)),
            whole(rows, width),
            whole(1, width),
            whole(rows, width),
        ],
        out_specs=[
            pl.BlockSpec((width, block), lambda step: (0, step)),
            full,
            pl.BlockSpec((1, width), lambda step: (0, 0)),
        ],
        scratch_shapes=[pltpu.VMEM((width, rows), jnp.float32)],
        name="project_back",
        operands=[normed_t, dq, dk, dv, weight, x, gain, d_hidden],
    )


LOG2E = 1.4426950408889634
FEATURES = 16


def two_parts(value):
    high = value.astype(jnp.bfloat16)
    return high, (value - high.astype(jnp.float32)).astype(jnp.bfloat16)


def three_parts(value):
    high, rest = value.astype(jnp.bfloat16), None
    rest = value - high.astype(jnp.float32)
    middle = rest.astype(jnp.bfloat16)
    return high, middle, (rest - middle.astype(jnp.float32)).astype(jnp.bfloat16)


def key_features(variates, valid):
    length = variates.shape[1]
    masks = [(variates == v).astype(jnp.float32) for v in range(4)]
    ones = jnp.ones((1, length), jnp.float32)
    invalid = 1.0 - valid
    rows = masks + masks + [invalid, ones, ones, ones, jnp.zeros((FEATURES - 12, length), jnp.float32)]
    return jnp.concatenate(rows, axis=0).astype(jnp.bfloat16)


def query_features(variates, same, other, log_sums):
    length = variates.shape[1]
    highs, lows = [], []
    for v in range(4):
        bias = jnp.where(variates == v, same, other) * LOG2E
        high, low = two_parts(bias)
        highs.append(high.astype(jnp.float32))
        lows.append(low.astype(jnp.float32))
    if log_sums is None:
        minus = [jnp.zeros((3, length), jnp.float32)]
    else:
        minus = [part.astype(jnp.float32) for part in three_parts(-log_sums)]
    mask = jnp.full((1, length), masked_score, jnp.float32)
    rows = highs + lows + [mask] + minus + [jnp.zeros((FEATURES - 12, length), jnp.float32)]
    return jnp.concatenate(rows, axis=0).astype(jnp.bfloat16)


def contract_depth(first_op, second_op):
    return lax.dot_general(
        first_op, second_op, (((1,), (0,)), ((), ())), preferred_element_type=jnp.float32
    )


def scaled_query(query_t, score_scale):
    return two_parts(query_t.astype(jnp.float32) * (score_scale * LOG2E))


def attend_kernel(blocks, bias_ref, *refs):
    head = pl.program_id(0)
    attend_head(blocks, bias_ref[0, head], bias_ref[1, head], *refs)


def attend_head(blocks, same, other, q_ref, k_ref, v_ref, var_ref, valid_ref, o_ref, wide_ref, lse_ref, query_ref):
    depth, length = q_ref.shape
    width = length // blocks
    variates = var_ref[...]
    high, low = scaled_query(q_ref[...], depth ** (-0.5))
    query_ref[...] = jnp.concatenate([high, low, query_features(variates, same, other, None)], axis=0)
    key_t = k_ref[...]
    keys = jnp.concatenate([key_t, key_t, key_features(variates, valid_ref[...])], axis=0).T
    ones = jnp.concatenate(
        [jnp.ones((1, length), jnp.float32), jnp.zeros((FEATURES - 1, length), jnp.float32)], axis=0
    ).astype(jnp.bfloat16)
    values = jnp.concatenate([v_ref[...], ones], axis=0)
    for block in range(blocks):
        at = pl.ds(block * width, width)
        scores = contract_depth(keys, query_ref[:, at])
        peak = jnp.max(scores, axis=0, keepdims=True)
        weights = jnp.exp2(scores - peak).astype(jnp.bfloat16)
        summed = contract_depth(values, weights)
        total = summed[depth : depth + 1]
        attended = summed[:depth] / total
        wide_ref[:, at] = attended
        o_ref[:, at] = attended.astype(jnp.bfloat16)
        lse_ref[0, :, at] = peak + jnp.log2(total)


def attend_forward(qkv_t, variates, valid, bias, heads):
    rows, length = qkv_t.shape
    depth = rows // (3 * heads)

    def part(which):
        return pl.BlockSpec((depth, length), lambda head: (which * heads + head, 0))

    row = pl.BlockSpec((1, length), lambda head: (0, 0))
    return run(
        functools.partial(attend_kernel, 1),
        grid=heads,
        out_shape=[
            jax.ShapeDtypeStruct((heads * depth, length), jnp.bfloat16),
            jax.ShapeDtypeStruct((heads * depth, length), jnp.float32),
            jax.ShapeDtypeStruct((heads, 1, length), jnp.float32),
        ],
        in_specs=[
            pl.BlockSpec(memory_space=pltpu.SMEM),
            part(0),
            part(1),
            part(2),
            row,
            row,
        ],
        out_specs=[
            pl.BlockSpec((depth, length), lambda head: (head, 0)),
            pl.BlockSpec((depth, length), lambda head: (head, 0)),
            pl.BlockSpec((1, 1, length), lambda head: (head, 0, 0)),
        ],
        scratch_shapes=[pltpu.VMEM((2 * depth + FEATURES, length), jnp.bfloat16)],
        name="attend_forward",
        operands=[bias, qkv_t, qkv_t, qkv_t, variates, valid],
    )


def turn_back(grad_t, cos_t, sin_t):
    half = cos_t.shape[0]
    first, second = grad_t[:half], grad_t[half:]
    return jnp.concatenate(
        [first * cos_t + second * sin_t, second * cos_t - first * sin_t], axis=0
    )


def attend_back_head(
    blocks, same, other, q_ref, k_ref, v_ref, go_ref, wide_ref, lse_ref, var_ref, valid_ref, cos_ref, sin_ref,
    dq_ref, dk_ref, dv_ref, query_ref, given_ref, dk_acc, dv_acc,
):
    depth, length = q_ref.shape
    width = length // blocks
    scale = depth ** (-0.5)
    variates = var_ref[...]
    features = key_features(variates, valid_ref[...])
    high, low = scaled_query(q_ref[...], scale)
    query_ref[...] = jnp.concatenate([high, low, query_features(variates, same, other, lse_ref[0])], axis=0)
    key_t = k_ref[...]
    keys = jnp.concatenate([key_t, key_t, features], axis=0).T
    keys_low = jnp.concatenate([key_t, features], axis=0)
    given = go_ref[...]
    inner = jnp.sum(given.astype(jnp.float32) * wide_ref[...], axis=0, keepdims=True)
    minus = [part.astype(jnp.float32) for part in three_parts(-inner)]
    minus = jnp.concatenate(minus + [jnp.zeros((FEATURES - 3, length), jnp.float32)], axis=0)
    given_ref[...] = jnp.concatenate([given, minus.astype(jnp.bfloat16)], axis=0)
    ones = jnp.concatenate(
        [jnp.ones((3, length), jnp.float32), jnp.zeros((FEATURES - 3, length), jnp.float32)], axis=0
    ).astype(jnp.bfloat16)
    values = jnp.concatenate([v_ref[...], ones], axis=0).T
    query_rows = q_ref[...].T
    given_rows = given.T
    in_same = jnp.zeros((1, width), jnp.float32)
    in_other = jnp.zeros((1, width), jnp.float32)
    for block in range(blocks):
        at = pl.ds(block * width, width)
        cut = slice(block * width, (block + 1) * width)
        probs = jnp.exp2(contract_depth(keys, query_ref[:, at]))
        grads = (probs * contract_depth(values, given_ref[:, at])).astype(jnp.bfloat16)
        back = contract_depth(keys_low, grads)
        dq = turn_back(back[:depth] * scale, cos_ref[:, at], sin_ref[:, at])
        dq_ref[:, at] = dq.astype(jnp.bfloat16)
        for v in range(4):
            line = back[depth + v : depth + v + 1]
            hit = variates[:, cut] == v
            in_same = in_same + jnp.where(hit, line, 0.0)
            in_other = in_other + jnp.where(hit, 0.0, line)
        dk = contract_depth(grads, query_rows[cut])
        dv = contract_depth(probs.astype(jnp.bfloat16), given_rows[cut])
        if block == 0:
            dk_acc[...] = dk
            dv_acc[...] = dv
        else:
            dk_acc[...] += dk
            dv_acc[...] += dv
    dk_ref[...] = turn_back((dk_acc[...] * scale).T, cos_ref[...], sin_ref[...]).astype(jnp.bfloat16)
    dv_ref[...] = dv_acc[...].T.astype(jnp.bfloat16)
    return in_same, in_other


def attend_back_kernel(blocks, bias_ref, *refs):
    head = pl.program_id(0)
    *refs, db_ref, query_ref, given_ref, dk_acc, dv_acc = refs
    in_same, in_other = attend_back_head(
        blocks, bias_ref[0, head], bias_ref[1, head], *refs, query_ref, given_ref, dk_acc, dv_acc
    )
    db_ref[0, 0:1, :] = in_same
    db_ref[0, 1:2, :] = in_other


def attend_backward(qkv_t, given_t, wide_t, log_sums, variates, valid, bias, cos_t, sin_t, heads):
    rows, length = qkv_t.shape
    depth = rows // (3 * heads)
    blocks = 1

    def part(which):
        return pl.BlockSpec((depth, length), lambda head: (which * heads + head, 0))

    one = pl.BlockSpec((depth, length), lambda head: (head, 0))
    grad = jax.ShapeDtypeStruct((heads * depth, length), jnp.bfloat16)
    return run(
        functools.partial(attend_back_kernel, blocks),
        grid=heads,
        out_shape=[grad, grad, grad, jax.ShapeDtypeStruct((heads, 2, length // blocks), jnp.float32)],
        in_specs=[
            pl.BlockSpec(memory_space=pltpu.SMEM),
            part(0),
            part(1),
            part(2),
            one,
            one,
            pl.BlockSpec((1, 1, length), lambda head: (head, 0, 0)),
            whole(1, length),
            whole(1, length),
            whole(depth // 2, length),
            whole(depth // 2, length),
        ],
        out_specs=[one, one, one, pl.BlockSpec((1, 2, length // blocks), lambda head: (head, 0, 0))],
        scratch_shapes=[
            pltpu.VMEM((2 * depth + FEATURES, length), jnp.bfloat16),
            pltpu.VMEM((depth + FEATURES, length), jnp.bfloat16),
            pltpu.VMEM((length, depth), jnp.float32),
            pltpu.VMEM((length, depth), jnp.float32),
        ],
        name="attend_backward",
        operands=[bias, qkv_t, qkv_t, qkv_t, given_t, wide_t, log_sums, variates, valid, cos_t, sin_t],
    )


PRELUDE = 7
FRONT_PLACES = (
    (0, 1, 2, 3, 4, 5, 6),
    (1, 3, 4, 5, 7, 8, 9),
    (3, 6, 8, 10, 13, 16, 18),
    (8, 12, 15, 18, 21, 24, 28),
)


def bias_of(small_ref, head, per_shard):
    row = 16 * (head // per_shard) + 2
    return small_ref[row, head % per_shard], small_ref[row + 1, head % per_shard]


def gain_of(small_ref, shards, which):
    rows = [small_ref[16 * shard + which : 16 * shard + which + 1, :] for shard in range(shards)]
    return jnp.concatenate(rows, axis=1)


def front_kernel(line, shards, heads, *refs):
    step = pl.program_id(0)
    refs = list(refs)

    def take(count):
        out = refs[:count]
        del refs[:count]
        return out

    small, w_qkv, w_out, w_in, w_down, x_hbm = take(6)
    var_ref, valid_ref, cos_ref, sin_ref = take(4)
    small_all, qkv_all, out_all, into_0, down_0, into_1, down_1 = take(7)
    intos = take(4)
    qkv_hbm, normed_hbm, attended_hbm, hidden_hbm, normed_two_hbm = take(5)
    wide_ref, lse_ref = take(2)
    x, weight, normed_t, qkv, attended, hidden, normed_two, small_ref, query_ref, bias_ref, wide_rows, cut_rows = take(12)
    load_sem, cut_sem, local_sem, send_sem, recv_sem = refs
    net = Net(line)
    rows, width = x.shape
    block = 512
    projected = 3 * width // block
    attend = PRELUDE + projected
    last = attend + heads
    depth = width // heads

    def load(index, origin, landing):
        return pltpu.make_async_copy(origin, landing, load_sem.at[index])

    def at(place):
        return pl.when(step == place)

    inner = w_in.shape[1] // 2
    owned = inner // shards
    piece_width = BLOCK // shards

    w_in_load = pltpu.make_async_copy(w_in, wide_rows, cut_sem.at[4])

    def cut_store(number):
        return pltpu.make_async_copy(cut_rows.at[number], intos[number], cut_sem.at[number])

    def down_part(number):
        return w_down.at[pl.ds(number * piece_width, piece_width)]

    tensors = (
        ((small, small_all), (w_qkv, qkv_all)),
        ((w_out, out_all),),
        ((intos[0], into_0), (down_part(0), down_0)),
        ((intos[1], into_1), (down_part(1), down_1)),
    )
    number = 0
    groups = []
    for group in tensors:
        lists = []
        for source, full in group:
            lists.append(
                gather_steps(
                    net, source, full, local_sem.at[number], send_sem.at[number], recv_sem.at[number]
                )
            )
            number += 1
        groups.append(lists)

    x_load = load(0, x_hbm, x)
    small_load = load(1, small_all, small_ref)
    weight_load = load(2, qkv_all, weight)
    bias_load = load(9, small_all, bias_ref)
    normed_store = load(3, normed_t, normed_hbm)
    qkv_store = load(4, qkv, qkv_hbm)
    attended_store = load(5, attended, attended_hbm)
    out_load = load(6, out_all, weight.at[:, pl.ds(0, width)])
    hidden_store = load(7, hidden, hidden_hbm)
    normed_two_store = load(8, normed_two, normed_two_hbm)

    @at(0)
    def _():
        net.greet()
        x_load.start()
        w_in_load.start()

    for lists, places in zip(groups, FRONT_PLACES):
        for index, place in enumerate(places):

            @at(place)
            def _():
                if place == FRONT_PLACES[2][0] and lists is groups[2]:
                    cut_store(0).wait()
                if place == FRONT_PLACES[3][0] and lists is groups[3]:
                    cut_store(1).wait()
                for steps in lists:
                    steps[index]()

    @at(0)
    def _():
        w_in_load.wait()
        for index in range(4):
            for piece in range(2 * shards):
                start = piece * owned + index * piece_width
                cut_rows[index, :, piece * piece_width : (piece + 1) * piece_width] = wide_rows[
                    :, start : start + piece_width
                ]
            cut_store(index).start()

    @at(PRELUDE - 1)
    def _():
        cut_store(2).wait()
        cut_store(3).wait()
        weight_load.start()
        small_load.start()
        bias_load.start()
        x_load.wait()
        small_load.wait()
        bias_load.wait()
        gain = gain_of(small_ref, shards, 0)
        values = x[...].astype(jnp.float32)
        normed = values * inverse_rms(values) * gain
        normed_t[...] = normed.T.astype(jnp.bfloat16)
        normed_store.start()
        weight_load.wait()

    @pl.when((step >= PRELUDE) & (step < attend))
    def _():
        index = step - PRELUDE
        columns = pl.ds(aligned(index * block, block), block)
        out = product(weight[:, columns], normed_t[...], ROWS_BY_ROWS)
        lines = qkv.at[columns]

        @pl.when(index < 2 * width // block)
        def _():
            cos, sin = cos_ref[...], sin_ref[...]
            half = depth // 2
            for start in range(0, block, depth):
                first, second = out[start : start + half], out[start + half : start + depth]
                lines[start : start + half, :] = (first * cos - second * sin).astype(jnp.bfloat16)
                lines[start + half : start + depth, :] = (second * cos + first * sin).astype(jnp.bfloat16)

        @pl.when(index >= 2 * width // block)
        def _():
            lines[...] = out.astype(jnp.bfloat16)

    @at(attend)
    def _():
        qkv_store.start()

    @pl.when((step >= attend) & (step < last))
    def _():
        head = step - attend

        def part(which):
            return qkv.at[pl.ds(aligned(which * width + head * depth, depth), depth)]

        same, other = bias_of(bias_ref, head, heads // shards)
        attend_head(
            1,
            same,
            other,
            part(0),
            part(1),
            part(2),
            var_ref,
            valid_ref,
            attended.at[pl.ds(aligned(head * depth, depth), depth)],
            wide_ref,
            lse_ref,
            query_ref,
        )

    @at(last - 1)
    def _():
        out_load.start()
        attended_store.start()

    @at(last)
    def _():
        out_load.wait()
        gain = gain_of(small_ref, shards, 1)
        part = 256
        for index in range(rows // part):
            lines = slice(index * part, (index + 1) * part)
            sums = product(attended[:, lines], weight[:, :width], ROWS_BY_ROWS)
            values = x[lines, :].astype(jnp.float32) + sums
            hidden[lines, :] = values
            normed_two[lines, :] = (values * inverse_rms(values) * gain).astype(jnp.bfloat16)
        hidden_store.start()
        normed_two_store.start()
        for store in (normed_store, qkv_store, attended_store, hidden_store, normed_two_store):
            store.wait()


def front(line, small, w_qkv, w_out, w_in, w_down, x, variates, valid, cos_t, sin_t, heads):
    shards = lax.axis_size("shard")
    rows, width = x.shape
    depth = width // heads
    low = jnp.bfloat16
    piece = BLOCK // shards
    grid = PRELUDE + 3 * width // 512 + heads + 1
    copies = gather_count(line)

    def head_at(step):
        return jnp.clip(step - (PRELUDE + 3 * width // 512), 0, heads - 1)

    def gathered(rows, columns, dtype=low):
        return like((shards * rows, columns), dtype)

    owned = w_qkv.shape[0]
    return pl.pallas_call(
        functools.partial(front_kernel, line, shards, heads),
        grid=(grid,),
        out_shape=[
            gathered(16, 128, jnp.float32),
            gathered(*w_qkv.shape),
            gathered(*w_out.shape),
            gathered(owned, 2 * BLOCK),
            gathered(piece, width),
            gathered(owned, 2 * BLOCK),
            gathered(piece, width),
        ]
        + [like((owned, 2 * BLOCK), low)] * 4
        + [
            like((3 * width, rows), low),
            like((width, rows), low),
            like((width, rows), low),
            like((rows, width), jnp.float32),
            like((rows, width), low),
            like((width, rows), jnp.float32),
            like((heads, 1, rows), jnp.float32),
        ],
        in_specs=[ANY] * 6
        + [
            whole(1, rows),
            whole(1, rows),
            whole(*cos_t.shape),
            whole(*sin_t.shape),
        ],
        out_specs=[ANY] * 16
        + [
            pl.BlockSpec((depth, rows), lambda step: (head_at(step), 0)),
            pl.BlockSpec((1, 1, rows), lambda step: (head_at(step), 0, 0)),
        ],
        scratch_shapes=[
            pltpu.VMEM((rows, width), low),
            pltpu.VMEM((width, 3 * width), low),
            pltpu.VMEM((width, rows), low),
            pltpu.VMEM((3 * width, rows), low),
            pltpu.VMEM((width, rows), low),
            pltpu.VMEM((rows, width), jnp.float32),
            pltpu.VMEM((rows, width), low),
            pltpu.VMEM((16 * shards, 128), jnp.float32),
            pltpu.VMEM((2 * depth + FEATURES, rows), low),
            pltpu.SMEM((16 * shards, 128), jnp.float32),
            pltpu.VMEM(w_in.shape, low),
            pltpu.VMEM((4, owned, 2 * BLOCK), low),
            pltpu.SemaphoreType.DMA((10,)),
            pltpu.SemaphoreType.DMA((5,)),
            pltpu.SemaphoreType.DMA((7,)),
            pltpu.SemaphoreType.DMA((7, copies)),
            pltpu.SemaphoreType.DMA((7, copies)),
        ],
        compiler_params=pltpu.CompilerParams(
            collective_id=1, has_side_effects=True, vmem_limit_bytes=62 << 20
        ),
        name="front",
    )(small, w_qkv, w_out, w_in, w_down, x, variates, valid, cos_t, sin_t)


TILE = 512
BLOCK = 1024
KEPT, GIVEN, GOT, OVER_X, OVER_Y, OVER_Z, LATE, ENDS, WIDE = 13, 3, 4, 5, 5, 6, 4, 4, 3
STAGES = (0, 1, 3, 5, 7, 8, 9, 10, 11, 12)
SUBSTEPS = 6


def stream_scratch(line, shards, half):
    only, shared = reduce_split(TILE)
    both = only + shared
    low = jnp.bfloat16
    copies = 3 * line + 4
    return [
        pltpu.VMEM((KEPT, shards, half, TILE), low),
        pltpu.VMEM((GIVEN, shards, half, TILE), low),
        pltpu.VMEM((GOT, shards, half, TILE), low),
        pltpu.VMEM((OVER_X, shards, half, only), low),
        pltpu.VMEM((OVER_Y, line, half, both), low),
        pltpu.VMEM((OVER_Z, line + 1, half, both), low),
        pltpu.VMEM((LATE, half, both), low),
        pltpu.VMEM((ENDS, half, TILE), low),
        pltpu.VMEM((ENDS, half, TILE), low),
        pltpu.VMEM((WIDE, 2 * half, TILE), jnp.float32),
        pltpu.SemaphoreType.DMA((KEPT, 4)),
        pltpu.SemaphoreType.DMA((KEPT, copies)),
        pltpu.SemaphoreType.DMA((KEPT, copies)),
    ]


class Stream:
    def __init__(self, net, scratch, writes):
        self.net, self.writes = net, writes
        (
            self.kept,
            self.give,
            self.got,
            self.from_x,
            self.from_y,
            self.from_z,
            self.late,
            self.final,
            self.swapped,
            self.wide,
            self.local_sem,
            self.send_sem,
            self.recv_sem,
        ) = scratch
        self.shards, self.half = self.kept.shape[1], self.kept.shape[2]
        self.only, self.shared = reduce_split(TILE)
        self.both = self.only + self.shared
        self.carried = pl.ds(aligned(net.x * self.only, 128), self.both)
        self.lone = pl.ds(aligned(net.x * self.both, 128), self.only)
        self.their_lone = pl.ds(aligned((1 - net.x) * self.both, 128), self.only)

    def remote(self, tile, origin, landing, index, target):
        slot = tile % KEPT
        return pltpu.make_async_remote_copy(
            src_ref=origin,
            dst_ref=landing,
            send_sem=self.send_sem.at[slot, index],
            recv_sem=self.recv_sem.at[slot, index],
            device_id=target,
            device_id_type=MESH,
        )

    def halves(self, tile):
        line = self.net.line
        return self.remote(tile, self.give.at[tile % GIVEN], self.got.at[tile % GOT], 2 * line, self.net.sibling)

    def over_x(self, tile):
        origin = self.kept.at[tile % KEPT, :, :, self.their_lone]
        return self.remote(tile, origin, self.from_x.at[tile % OVER_X], 2 * self.net.line + 1, self.net.across_x)

    def over_y(self, tile, z):
        net = self.net
        origin = self.kept.at[tile % KEPT, z * 2 + 1 - net.y, :, self.carried]
        return self.remote(tile, origin, self.from_y.at[tile % OVER_Y, z], 2 * net.line + 4 + z, net.across_y)

    def up(self, tile, z):
        net = self.net
        origin = self.kept.at[tile % KEPT, z * 2 + net.y, :, self.carried]
        return self.remote(tile, origin, self.from_z.at[tile % OVER_Z, z + 1], z, net.above)

    def down(self, tile, z):
        net = self.net
        origin = self.kept.at[tile % KEPT, z * 2 + net.y, :, self.carried]
        return self.remote(tile, origin, self.from_z.at[tile % OVER_Z, z], net.line + z, net.below)

    def end_x(self, tile):
        net = self.net
        origin = self.kept.at[tile % KEPT, net.own, :, self.carried]
        return self.remote(tile, origin, self.late.at[tile % LATE], 2 * net.line + 2, net.across_x)

    def to_core(self, tile):
        slot = tile % ENDS
        return self.remote(tile, self.final.at[slot], self.swapped.at[slot], 2 * self.net.line + 3, self.net.sibling)

    def add(self, tile, shard, part):
        slot = tile % KEPT
        self.kept[slot, shard, :, self.carried] = self.kept[slot, shard, :, self.carried] + part

    def born(self, tile):
        self.halves(tile).start()

    def meet_core(self, tile):
        copy = self.halves(tile)
        copy.wait_recv()
        copy.wait_send()
        slot, came = tile % KEPT, tile % GOT

        @pl.loop(0, self.shards)
        def _(shard):
            self.kept[slot, shard] = self.kept[slot, shard] + self.got[came, shard]

        self.over_x(tile).start()

    def meet_x(self, tile):
        self.over_x(tile).wait_recv()
        slot, came = tile % KEPT, tile % OVER_X

        @pl.loop(0, self.shards)
        def _(shard):
            self.kept[slot, shard, :, self.lone] = self.kept[slot, shard, :, self.lone] + self.from_x[came, shard]

        for z in range(self.net.line):
            self.over_y(tile, z).start()

    def meet_y(self, tile):
        for z in range(self.net.line):
            self.over_y(tile, z).wait_recv()
            self.add(tile, z * 2 + self.net.y, self.from_y[tile % OVER_Y, z])
        self.hop(tile, 0)

    def hop(self, tile, step):
        net, came = self.net, tile % OVER_Z

        @pl.when(net.z == step)
        def _():
            for z in range(net.line - 1, step, -1):
                if step > 0:
                    self.up(tile, z).wait_recv()
                    self.add(tile, z * 2 + net.y, self.from_z[came, z + 1])
                self.up(tile, z).start()

        @pl.when(net.z == net.line - 1 - step)
        def _():
            for z in range(net.line - 1 - step):
                if step > 0:
                    self.down(tile, z).wait_recv()
                    self.add(tile, z * 2 + net.y, self.from_z[came, z])
                self.down(tile, z).start()

    def land(self, tile):
        net, came = self.net, tile % OVER_Z

        @pl.when(net.has_below)
        def _():
            self.up(tile, net.z).wait_recv()
            self.add(tile, net.own, self.from_z[came, net.z + 1])

        @pl.when(net.has_above)
        def _():
            self.down(tile, net.z).wait_recv()
            self.add(tile, net.own, self.from_z[came, net.z])

        self.end_x(tile).start()

    def meet(self, tile):
        net, only, both, shared = self.net, self.only, self.both, self.shared
        slot, came, end = tile % KEPT, tile % LATE, tile % ENDS
        self.end_x(tile).wait_recv()
        self.final[end, :, self.lone] = self.kept[slot, net.own, :, self.lone]
        for x in range(2):

            @pl.when(net.x == x)
            def _():
                theirs = 0 if x == 1 else shared
                middle = only if x == 1 else 0
                at = (1 - x) * both
                self.final[end, :, at : at + only] = self.late[came, :, theirs : theirs + only]
                self.final[end, :, only:both] = (
                    self.kept[slot, net.own, :, only:both] + self.late[came, :, middle : middle + shared]
                )

        self.to_core(tile).start()
        mine = pl.ds(aligned(net.core * self.half, self.half), self.half)
        self.wide[tile % WIDE, mine, :] = self.final[end].astype(jnp.float32)

    def swap(self, tile):
        self.to_core(tile).wait_recv()
        theirs = pl.ds(aligned((1 - self.net.core) * self.half, self.half), self.half)
        self.wide[tile % WIDE, theirs, :] = self.swapped[tile % ENDS].astype(jnp.float32)
        self.writes(tile, self.wide.at[tile % WIDE], self.local_sem.at[tile % KEPT], True)

    def finish(self, tile):
        net = self.net
        self.writes(tile, self.wide.at[tile % WIDE], self.local_sem.at[tile % KEPT], False)
        self.over_x(tile).wait_send()
        for z in range(net.line):
            self.over_y(tile, z).wait_send()
            pl.when(net.z < z)(self.up(tile, z).wait_send)
            pl.when(net.z > z)(self.down(tile, z).wait_send)
        self.end_x(tile).wait_send()
        self.to_core(tile).wait_send()

    def stages(self):
        return [
            self.born,
            self.meet_core,
            self.meet_x,
            self.meet_y,
            lambda tile: self.hop(tile, 1),
            lambda tile: self.hop(tile, 2),
            self.land,
            self.meet,
            self.swap,
            self.finish,
        ]


class Plan:
    def __init__(self, blocks, heads):
        self.blocks, self.heads = blocks, heads
        self.ffn = blocks * SUBSTEPS
        self.norm = self.ffn
        self.branch = self.ffn + 1
        self.attend = self.ffn + 2
        self.groups = 4
        self.per_group = heads // self.groups
        self.out = self.ffn + SUBSTEPS
        self.ready = [self.attend + self.per_group * (group + 1) for group in range(self.groups)]
        self.births = list(range(SUBSTEPS, self.out + 2))
        self.ffn_tiles = self.ffn
        self.keys_tiles, self.value_tiles = [], []
        for group in range(self.groups):
            self.keys_tiles.append(len(self.births))
            self.births.append(max(self.ready[group], self.births[-1] + 1))
            if group % 2 == 1:
                self.value_tiles.append(len(self.births))
                self.births.append(self.births[-1] + 1)
        self.last = self.births[-1]
        self.grid = self.last + STAGES[-1] + 1

    def tile_at(self, step):
        regular = self.out + 2 - SUBSTEPS
        tile = step - SUBSTEPS
        known = (step >= SUBSTEPS) & (step < self.out + 2)
        for index in range(regular, len(self.births)):
            hit = step == self.births[index]
            tile = jnp.where(hit, index, tile)
            known = known | hit
        return tile, known


def back_kernel(plan, line, shards, *refs):
    step = pl.program_id(0)
    refs = list(refs)

    def take(count):
        out = refs[:count]
        del refs[:count]
        return out

    normed_hbm, given_hbm, hidden_hbm = take(3)
    early = take(4)
    into_2, into_3, down_hbm = take(3)
    attended_hbm, out_hbm, normed_one_hbm, x_hbm, qkv_hbm = take(5)
    small_hbm, = take(1)
    q_ref, k_ref, v_ref, wide_ref, lse_ref, var_ref, valid_ref, cos_ref, sin_ref = take(9)
    result_hbm, tokens_hbm, sum_in, sum_down, sum_out, sum_qkv, sum_small = take(7)
    gather_to = take(4)
    normed, turned, given, w_down, w_gate, w_up, act, act_t = take(8)
    d_gate, d_up, acc, through = take(4)
    query_ref, given_aug_ref, dk_acc, dv_acc = take(4)
    load_sem, = take(1)
    gather_local, gather_send, gather_recv = take(3)
    small_ref, bias_ref, grad_gain_one_ref, grad_gain_two_ref, grad_small = take(5)
    small_buffers = take(REDUCE_BUFFERS)
    small_local, small_send, small_recv = take(3)
    net = Net(line)
    piece = BLOCK // shards
    gather_from = [
        into_2,
        down_hbm.at[pl.ds(2 * piece, piece)],
        into_3,
        down_hbm.at[pl.ds(3 * piece, piece)],
    ]
    half = BLOCK // shards // 2
    heads_at = step - plan.attend

    def writes(tile, wide, sems, begin):
        rows = 2 * half

        def move(index, origin, landing):
            copy = pltpu.make_async_copy(origin, landing, sems.at[index])
            copy.start() if begin else copy.wait()

        block, kind = tile // SUBSTEPS, tile % SUBSTEPS
        in_ffn = tile < plan.ffn_tiles

        @pl.when(in_ffn & (kind < 2))
        def _():
            lines = pl.ds(aligned(block * rows, rows), rows)
            move(0, wide, sum_down.at[lines, pl.ds(aligned(kind * TILE, TILE), TILE)])

        @pl.when(in_ffn & (kind >= 2))
        def _():
            inner = plan.blocks * BLOCK
            base = ((kind - 2) // 2) * inner
            for piece in range(4):
                shard = (kind % 2) * 4 + piece
                start = base + shard * (inner // shards) + block * (BLOCK // shards)
                columns = pl.ds(aligned(start, 128), 128)
                move(piece, wide.at[:, piece * 128 : (piece + 1) * 128], sum_in.at[:, columns])

        @pl.when((tile >= plan.ffn_tiles) & (tile < plan.ffn_tiles + 2))
        def _():
            start = aligned((tile - plan.ffn_tiles) * TILE, TILE)
            move(0, wide, sum_out.at[:, pl.ds(start, TILE)])

        width = plan.heads * q_ref.shape[0]
        for group, number in enumerate(plan.keys_tiles):

            @pl.when(tile == number)
            def _():
                for part in range(2):
                    start = part * width + group * (TILE // 2)
                    columns = slice(part * (TILE // 2), (part + 1) * (TILE // 2))
                    move(part, wide.at[:, columns], sum_qkv.at[:, pl.ds(start, TILE // 2)])

        for pair, number in enumerate(plan.value_tiles):

            @pl.when(tile == number)
            def _():
                move(0, wide, sum_qkv.at[:, pl.ds(2 * width + pair * TILE, TILE)])

    stream = Stream(net, refs, writes)
    stages = stream.stages()

    def load(index, origin, landing):
        return pltpu.make_async_copy(origin, landing, load_sem.at[index])

    def weight_loads(block):
        if block < 2:
            into, down = early[2 * block], early[2 * block + 1]
        else:
            into, down = gather_to[2 * (block - 2)], gather_to[2 * (block - 2) + 1]
        return [
            load(0, into.at[:, pl.ds(0, BLOCK)], w_gate),
            load(1, into.at[:, pl.ds(BLOCK, BLOCK)], w_up),
            load(2, down, w_down),
        ]

    first_loads = [
        load(3, normed_hbm, normed),
        load(4, given_hbm, given),
        load(5, hidden_hbm, acc),
        load(15, small_hbm, small_ref),
        load(16, small_hbm, bias_ref),
    ]
    hidden_load = load(5, hidden_hbm, acc)
    result_store = load(6, act, result_hbm)
    attended_load = load(7, attended_hbm, w_down)
    out_load = load(8, out_hbm, d_up.at[0])
    normed_one_load = load(9, normed_one_hbm, turned)
    x_load = load(10, x_hbm, normed)
    tokens_store = load(11, acc, tokens_hbm)

    def qkv_loads(group):
        width = qkv_hbm.shape[1] // 3
        part = width // plan.groups
        page = act_t if group % 2 == 0 else d_up.at[0]
        return [
            load(
                12 + index,
                qkv_hbm.at[:, pl.ds(index * width + group * part, part)],
                page.at[:, pl.ds(index * part, part)],
            )
            for index in range(3)
        ]

    def at(place):
        return pl.when(step == place)

    def start(copies):
        for copy in copies:
            copy.start()

    def wait(copies):
        for copy in copies:
            copy.wait()

    gathers = [
        gather_steps(
            net, gather_from[i], gather_to[i], gather_local.at[i], gather_send.at[i], gather_recv.at[i]
        )
        for i in range(4)
    ]
    gather_places = ((0, 1, 3, 5, 6, 7, 9), (6, 8, 9, 11, 12, 14, 15))

    @at(0)
    def _():
        net.greet()
        start(weight_loads(0) + first_loads)

    for pair, places in enumerate(gather_places):
        for index, place in enumerate(places):

            @at(place)
            def _():
                gathers[2 * pair][index]()
                gathers[2 * pair + 1][index]()

    for stage in range(len(STAGES) - 1, 0, -1):
        tile, known = plan.tile_at(step - STAGES[stage])
        pl.when(known)(functools.partial(stages[stage], tile))

    @at(0)
    def _():
        wait(first_loads)
        grad_small[...] = jnp.zeros_like(grad_small)
        turned[...] = normed[...].T

    for block in range(plan.blocks):

        @at(block * SUBSTEPS)
        def _():
            wait(weight_loads(block))

        if block + 1 < plan.blocks:

            @at(block * SUBSTEPS + SUBSTEPS - 1)
            def _():
                start(weight_loads(block + 1))

    block, sub = step // SUBSTEPS, step % SUBSTEPS
    slot = block % 2
    in_ffn = step < plan.ffn

    @pl.when(in_ffn & (sub < 2))
    def _():
        columns = pl.ds(aligned(sub * TILE, TILE), TILE)
        d_act = product(given[...], w_down[columns, :], COLUMNS_BY_COLUMNS)
        gate = product(normed[...], w_gate[:, columns])
        up = product(normed[...], w_up[:, columns])
        sigmoid = jax.nn.sigmoid(gate)
        swish = gate * sigmoid
        act[:, columns] = (swish * up).astype(jnp.bfloat16)
        d_gate[slot, :, columns] = (d_act * up * sigmoid * (1.0 + gate * (1.0 - sigmoid))).astype(jnp.bfloat16)
        d_up[slot, :, columns] = (d_act * swish).astype(jnp.bfloat16)

    @pl.when(in_ffn & (sub == 2))
    def _():
        acc[...] += product(act[...], w_down[...])
        act_t[...] = act[...].T

    @pl.when(in_ffn & (sub == 3))
    def _():
        part = product(d_gate[slot], w_gate[...], COLUMNS_BY_COLUMNS)

        @pl.when(block == 0)
        def _():
            through[...] = part

        @pl.when(block > 0)
        def _():
            through[...] += part

    @pl.when(in_ffn & (sub == 4))
    def _():
        through[...] += product(d_up[slot], w_up[...], COLUMNS_BY_COLUMNS)

    last_sum = plan.ffn - SUBSTEPS + 2

    @at(last_sum)
    def _():
        act[...] = acc[...].astype(jnp.bfloat16)
        result_store.start()

    @at(last_sum + 1)
    def _():
        start([hidden_load, attended_load])

    @at(last_sum + 3)
    def _():
        result_store.wait()

    row_block = 128

    @at(plan.norm)
    def _():
        out_load.start()
        hidden_load.wait()
        grad_gain_two_ref[...] = jnp.zeros_like(grad_gain_two_ref)
        gain_two = gain_of(small_ref, shards, 1)

        @pl.loop(0, acc.shape[0] // row_block)
        def _(index):
            lines = pl.ds(aligned(index * row_block, row_block), row_block)
            back, grad_gain = norm_back(through[lines, :], acc[lines, :], gain_two)
            d_hidden = given[lines, :].astype(jnp.float32) + back
            acc[lines, :] = d_hidden
            d_gate[0, lines, :] = d_hidden.astype(jnp.bfloat16)
            grad_gain_two_ref[...] += grad_gain

    @at(plan.branch)
    def _():
        out_load.wait()
        act[...] = product(d_up[0], d_gate[0], COLUMNS_BY_COLUMNS).astype(jnp.bfloat16)

    for group in range(plan.groups):
        ready = plan.ready[group]

        if group == 0:

            @at(plan.attend)
            def _():
                start(qkv_loads(0))

        @at(ready)
        def _():
            wait(qkv_loads(group))
            if group + 1 < plan.groups:
                start(qkv_loads(group + 1))
            page = act_t if group % 2 == 0 else d_up.at[0]
            quarter = TILE // 2
            base = (group % 2) * TILE
            part = product(page[:, :TILE], w_gate[base : base + TILE, :])
            values = (group // 2) * TILE + (group % 2) * quarter
            part = part + product(page[:, TILE : TILE + quarter], w_up[values : values + quarter, :])
            if group == 0:
                through[...] = part
            else:
                through[...] += part

    @at(plan.out)
    def _():
        attended_load.wait()
        start([normed_one_load, x_load])

    @at(plan.births[plan.keys_tiles[0]])
    def _():
        normed_one_load.wait()

    @pl.when((heads_at >= 0) & (heads_at < plan.heads))
    def _():
        depth = q_ref.shape[0]
        head = heads_at
        group = head // plan.per_group
        q_at = (group % 2) * TILE + (head % plan.per_group) * depth
        k_at = q_at + TILE // 2
        v_at = (group // 2) * TILE + (head % (2 * plan.per_group)) * depth

        def rows(start):
            return pl.ds(aligned(start, depth), depth)

        per_shard = plan.heads // shards
        same, other = bias_of(bias_ref, head, per_shard)
        sums = attend_back_head(
            2,
            same,
            other,
            q_ref,
            k_ref,
            v_ref,
            act.at[rows(head * depth)],
            wide_ref,
            lse_ref,
            var_ref,
            valid_ref,
            cos_ref,
            sin_ref,
            w_gate.at[rows(q_at)],
            w_gate.at[rows(k_at)],
            w_up.at[rows(v_at)],
            query_ref,
            given_aug_ref,
            dk_acc,
            dv_acc,
        )
        for which, lanes in enumerate(sums):
            folded = sum(lanes[:, start : start + 128] for start in range(0, lanes.shape[1], 128))
            grad_small[head // per_shard, pl.ds(2 + 2 * (head % per_shard) + which, 1), :] = folded

    tile, known = plan.tile_at(step)

    def birth(left, right, dims=(((1,), (0,)), ((), ()))):
        for which, target in ((net.core, stream.kept.at[tile % KEPT]), (1 - net.core, stream.give.at[tile % GIVEN])):
            lines = [
                left[pl.ds(aligned(shard * 2 * half + which * half, half), half), :] for shard in range(shards)
            ]
            out = product(jnp.concatenate(lines, axis=0), right, dims).astype(jnp.bfloat16)
            for shard in range(shards):
                target[shard] = out[shard * half : (shard + 1) * half]

    kind, source = tile % SUBSTEPS, (tile // SUBSTEPS) % 2
    in_tiles = known & (tile < plan.ffn_tiles)
    columns = pl.ds(aligned((kind % 2) * TILE, TILE), TILE)
    pl.when(in_tiles & (kind < 2))(lambda: birth(act_t, given[:, columns]))
    pl.when(in_tiles & (kind >= 2) & (kind < 4))(lambda: birth(turned, d_gate[source, :, columns]))
    pl.when(in_tiles & (kind >= 4))(lambda: birth(turned, d_up[source, :, columns]))
    for number in range(2):
        at(plan.out + number)(
            lambda: birth(w_down, d_gate[0, :, number * TILE : (number + 1) * TILE])
        )
    for group, number in enumerate(plan.keys_tiles):
        base = (group % 2) * TILE
        at(plan.births[number])(lambda: birth(turned, w_gate[base : base + TILE, :], COLUMNS_BY_COLUMNS))
    for pair, number in enumerate(plan.value_tiles):
        base = pair * TILE
        at(plan.births[number])(lambda: birth(turned, w_up[base : base + TILE, :], COLUMNS_BY_COLUMNS))
    pl.when(known)(lambda: stream.born(tile))

    @at(plan.last)
    def _():
        x_load.wait()
        grad_gain_one_ref[...] = jnp.zeros_like(grad_gain_one_ref)
        gain_one = gain_of(small_ref, shards, 0)

        @pl.loop(0, acc.shape[0] // row_block)
        def _(index):
            lines = pl.ds(aligned(index * row_block, row_block), row_block)
            values = normed[lines, :].astype(jnp.float32)
            back, grad_gain = norm_back(through[:, lines].T, values, gain_one)
            acc[lines, :] = acc[lines, :] + back
            grad_gain_one_ref[...] += grad_gain

        tokens_store.start()
        for shard in range(shards):
            columns = slice(shard * 128, (shard + 1) * 128)
            grad_small[shard, 0:1, :] = grad_gain_one_ref[:, columns]
            grad_small[shard, 1:2, :] = grad_gain_two_ref[:, columns]

    small_steps = reduce_steps(
        net, grad_small, sum_small, 0, 0, small_buffers, small_local, small_send, small_recv
    )
    for index, action in enumerate(small_steps):
        at(plan.last + 1 + index)(action)

    @at(plan.grid - 1)
    def _():
        tokens_store.wait()


def back(line, early, sources, own_down, normed_two, given, hidden, attended_t, out_weight, normed_t, x, qkv_weight,
         small, qkv_t, wide_t, log_sums, variates, valid, cos_t, sin_t):
    shards = lax.axis_size("shard")
    rows, width = x.shape
    heads = log_sums.shape[0]
    depth = width // heads
    blocks = 4
    plan = Plan(blocks, heads)
    low = jnp.bfloat16
    owned = width // shards
    inner = blocks * BLOCK

    def head_at(step):
        return jnp.clip(step - plan.attend, 0, heads - 1)

    def part(which):
        return pl.BlockSpec((depth, rows), lambda step: (which * heads + head_at(step), 0))

    page = pltpu.VMEM((BLOCK, BLOCK), low)
    copies = gather_count(line)
    return pl.pallas_call(
        functools.partial(back_kernel, plan, line, shards),
        grid=(plan.grid,),
        out_shape=[
            like((rows, width), low),
            like((rows, width), jnp.float32),
            like((owned, 2 * inner), jnp.float32),
            like((inner // shards, width), jnp.float32),
            like((owned, width), jnp.float32),
            like((owned, 3 * width), jnp.float32),
            like((16, 128), jnp.float32),
        ]
        + [like((width, 2 * BLOCK), low), like((BLOCK, width), low)] * 2
,
        in_specs=[ANY] * 16
        + [
            part(0),
            part(1),
            part(2),
            pl.BlockSpec((depth, rows), lambda step: (head_at(step), 0)),
            pl.BlockSpec((1, 1, rows), lambda step: (head_at(step), 0, 0)),
            whole(1, rows),
            whole(1, rows),
            whole(*cos_t.shape),
            whole(*sin_t.shape),
        ],
        out_specs=[ANY] * 11,
        scratch_shapes=[page] * 8
        + [
            pltpu.VMEM((2, BLOCK, BLOCK), low),
            pltpu.VMEM((2, BLOCK, BLOCK), low),
            pltpu.VMEM((rows, width), jnp.float32),
            pltpu.VMEM((rows, width), jnp.float32),
            pltpu.VMEM((2 * depth + FEATURES, rows), low),
            pltpu.VMEM((depth + FEATURES, rows), low),
            pltpu.VMEM((rows, depth), jnp.float32),
            pltpu.VMEM((rows, depth), jnp.float32),
            pltpu.SemaphoreType.DMA((17,)),
            pltpu.SemaphoreType.DMA((4,)),
            pltpu.SemaphoreType.DMA((4, copies)),
            pltpu.SemaphoreType.DMA((4, copies)),
            pltpu.VMEM((16 * shards, 128), jnp.float32),
            pltpu.SMEM((16 * shards, 128), jnp.float32),
            pltpu.VMEM((1, width), jnp.float32),
            pltpu.VMEM((1, width), jnp.float32),
            pltpu.VMEM((shards, 16, 128), jnp.float32),
        ]
        + reduce_scratch(line, shards, 8, 128, jnp.float32)
        + [
            pltpu.SemaphoreType.DMA((2,)),
            pltpu.SemaphoreType.DMA((reduce_count(line),)),
            pltpu.SemaphoreType.DMA((reduce_count(line),)),
        ]
        + stream_scratch(line, shards, owned // 2),
        compiler_params=pltpu.CompilerParams(
            collective_id=9, has_side_effects=True, vmem_limit_bytes=64 << 20
        ),
        name="back",
    )(
        normed_two, given, hidden, *early, *sources, own_down, attended_t, out_weight, normed_t, x, qkv_weight,
        small, qkv_t, qkv_t, qkv_t, wide_t, log_sums, variates, valid, cos_t, sin_t,
    )


def rope_tables(time_ids):
    half = HEAD_DIM // 2
    exponent = jnp.arange(half).astype(jnp.float32) * (2.0 / HEAD_DIM)
    inverse = jnp.exp(-jnp.log(rope_base) * exponent)
    angles = inverse[:, None] * time_ids.astype(jnp.float32)
    return jnp.cos(angles), jnp.sin(angles)


def pack_small(attn_gain, ffn_gain, attn_bias):
    heads = attn_bias.shape[1]
    small = jnp.zeros((16, 128), jnp.float32)
    small = small.at[0].set(attn_gain.astype(jnp.float32)).at[1].set(ffn_gain.astype(jnp.float32))
    return small.at[2:4, :heads].set(attn_bias.astype(jnp.float32))


def shards(
    line,
    tokens,
    lengths,
    variate_ids,
    time_ids,
    attn_gain,
    w_qkv,
    attn_bias,
    w_out,
    ffn_gain,
    w_in,
    w_down,
    cotangent,
):
    length = variate_ids.shape[1]
    heads = attn_bias.shape[1]
    key_valid = jnp.arange(length)[None, :] < lengths[:, None]
    valid = key_valid.astype(jnp.float32)
    given = jnp.where(key_valid.reshape(length, 1), cotangent, jnp.zeros_like(cotangent))
    cos_t, sin_t = rope_tables(time_ids)
    if line:
        small, qkv_weight, out_weight, into_0, down_0, into_1, down_1, *rest = front(
            line,
            pack_small(attn_gain, ffn_gain, attn_bias),
            w_qkv,
            w_out,
            w_in,
            w_down,
            tokens,
            variate_ids,
            valid,
            cos_t,
            sin_t,
            HEADS,
        )
        intos, (qkv_t, normed_t, attended_t, hidden, normed_two, wide_t, log_sums) = rest[:4], rest[4:]
        result, grad_tokens, sum_in, sum_down, sum_out, sum_qkv, small = back(
            line,
            [into_0, down_0, into_1, down_1],
            [intos[2], intos[3]],
            w_down,
            normed_two,
            given,
            hidden,
            attended_t,
            out_weight,
            normed_t,
            tokens,
            qkv_weight,
            small,
            qkv_t,
            wide_t,
            log_sums,
            variate_ids,
            valid,
            cos_t,
            sin_t,
        )[:7]
        return (
            result,
            grad_tokens,
            small[0],
            sum_qkv,
            jnp.sum(small[2 : 2 + 2 * heads], axis=1).reshape(heads, 2).T,
            sum_out,
            small[1],
            sum_in,
            sum_down,
        )
    gain_one, gain_two, qkv_weight, out_weight, in_weight, down_weight = (
        lax.all_gather(part, "shard", axis=0, tiled=True)
        for part in (attn_gain, ffn_gain, w_qkv, w_out, w_in, w_down)
    )
    bias = lax.all_gather(attn_bias, "shard", axis=1, tiled=True).astype(jnp.float32)
    gain_one = gain_one.astype(jnp.float32).reshape(1, -1)
    gain_two = gain_two.astype(jnp.float32).reshape(1, -1)
    qkv_t, normed_t = project(tokens, gain_one, qkv_weight, cos_t, sin_t)
    attended_t, wide_t, log_sums = attend_forward(qkv_t, variate_ids, valid, bias, HEADS)
    hidden, normed_two = branch(attended_t, out_weight, tokens, gain_two)
    act, to_gate, to_up = widen(normed_two, in_weight)
    result, grad_down, d_gate, d_up = narrow(act, to_gate, to_up, down_weight, given, hidden)
    grad_gate, grad_up = grad_into(normed_two, d_gate, d_up)
    d_hidden, d_branch, grad_gain_two = ffn_back(d_gate, d_up, in_weight, hidden, gain_two, given)
    grad_out, given_t = branch_back(attended_t, out_weight, d_branch)
    dq, dk, dv, bias_parts = attend_backward(
        qkv_t, given_t, wide_t, log_sums, variate_ids, valid, bias, cos_t, sin_t, HEADS
    )
    grad_qkv, grad_tokens, grad_gain_one = project_back(
        normed_t, dq, dk, dv, qkv_weight, tokens, gain_one, d_hidden
    )
    grads = (
        (grad_gain_one.reshape(-1), 0),
        (grad_qkv, 0),
        (jnp.sum(bias_parts, axis=2).T, 1),
        (grad_out, 0),
        (grad_gain_two.reshape(-1), 0),
        (jnp.concatenate([grad_gate, grad_up], axis=1), 0),
        (grad_down, 0),
    )
    owned = [
        lax.psum_scatter(grad.astype(jnp.bfloat16), "shard", scatter_dimension=axis, tiled=True)
        for grad, axis in grads
    ]
    return (result, grad_tokens) + tuple(lax.psum(part, "rep").astype(jnp.float32) for part in owned)


def solution(mesh):
    placed = (
        P(("shard", "rep"), None),
        P(("shard", "rep")),
        P(("shard", "rep"), None),
        P(("shard", "rep"), None),
        P("shard"),
        P("shard", None),
        P(None, "shard"),
        P("shard", None),
        P("shard"),
        P("shard", None),
        P("shard", None),
        P(("shard", "rep"), None),
    )
    line = mesh.shape["shard"] // 2 if (mesh.shape["shard"], mesh.shape["rep"]) == (8, 4) else 0
    return jax.shard_map(
        functools.partial(shards, line),
        mesh=mesh,
        in_specs=placed,
        out_specs=(
            P(("shard", "rep"), None),
            P(("shard", "rep"), None),
            P("shard"),
            P("shard", None),
            P(None, "shard"),
            P("shard", None),
            P("shard"),
            P("shard", None),
            P("shard", None),
        ),
        check_vma=False,
    )
```

```python
import functools

import jax
import jax.numpy as jnp
from jax import lax
from jax.experimental import pallas as pl
from jax.experimental.pallas import tpu as pltpu
from jax.sharding import PartitionSpec as P

HEADS = 16
HEAD_DIM = 64


norm_eps = 1e-06
rope_base = 10000.0
masked_score = -1000000000.0

MESH = pl.DeviceIdType.MESH
ANY = pl.BlockSpec(memory_space=pl.ANY)


class Net:
    def __init__(self, line):
        shard, rep = lax.axis_index("shard"), lax.axis_index("rep")
        self.line = line
        self.z, self.y = shard // 2, shard % 2
        self.x, self.core = rep // 2, rep % 2
        self.own = shard
        self.sibling = (shard, self.x * 2 + 1 - self.core)
        self.across_x = (shard, (1 - self.x) * 2 + self.core)
        self.across_y = (self.z * 2 + 1 - self.y, rep)
        self.above = (jnp.minimum(self.z + 1, line - 1) * 2 + self.y, rep)
        self.below = (jnp.maximum(self.z - 1, 0) * 2 + self.y, rep)
        self.has_above = self.z < line - 1
        self.has_below = self.z > 0

    def greet(self):
        barrier = pltpu.get_barrier_semaphore()

        def hail(partner):
            pl.semaphore_signal(barrier, inc=1, device_id=partner, device_id_type=MESH)

        for partner in (self.sibling, self.across_x, self.across_y):
            hail(partner)
        pl.when(self.has_above)(lambda: hail(self.above))
        pl.when(self.has_below)(lambda: hail(self.below))
        neighbours = jnp.where(self.has_above, 1, 0) + jnp.where(self.has_below, 1, 0)
        pl.semaphore_wait(barrier, 3 + neighbours)


def aligned(value, step):
    return pl.multiple_of(value, step)


def gather_count(line):
    return 2 * line + 3 * 2 * line


def gather_steps(net, source, full, local_sem, send_sem, recv_sem):
    line = net.line
    height, columns = source.shape
    half = height // 2
    split = columns % 1024 == 0
    only = columns * 3 // 8 if split else 0
    shared = columns - 2 * only
    rows = pl.ds(aligned(net.core * half, half), half)
    carried = pl.ds(aligned(net.x * only, 128), only + shared) if split else pl.ds(0, columns)
    lone = pl.ds(aligned(net.x * (only + shared), 128), only) if split else None

    def remote(origin, landing, index, target):
        return pltpu.make_async_remote_copy(
            src_ref=origin,
            dst_ref=landing,
            send_sem=send_sem.at[index],
            recv_sem=recv_sem.at[index],
            device_id=target,
            device_id_type=MESH,
        )

    def held(z, y, which=None):
        lines = pl.ds(aligned((z * 2 + y) * height + net.core * half, half), half)
        return full.at[lines] if which is None else full.at[lines, which]

    def piece(z, y):
        return held(z, y, carried)

    def over_z(z, target, base):
        return remote(piece(z, net.y), piece(z, net.y), base + z, target)

    def over_y(z):
        return remote(piece(z, net.y), piece(z, net.y), 2 * line + z, net.across_y)

    def over_x(z, y):
        part = held(z, y, lone)
        return remote(part, part, 3 * line + y * line + z, net.across_x)

    def to_core(z, y):
        part = held(z, y)
        return remote(part, part, 5 * line + y * line + z, net.sibling)

    mine = source.at[rows, carried]
    local = pltpu.make_async_copy(source, full.at[pl.ds(aligned(net.own * height, height), height)], local_sem)
    first_y = remote(mine, piece(net.z, net.y), 2 * line + net.z, net.across_y)
    first_up = remote(mine, piece(net.z, net.y), net.z, net.above)
    first_down = remote(mine, piece(net.z, net.y), line + net.z, net.below)

    def onward(z, y):
        if split:
            over_x(z, y).start()
        else:
            to_core(z, y).start()

    def start():
        first_y.start()
        pl.when(net.has_above)(first_up.start)
        pl.when(net.has_below)(first_down.start)
        local.start()

    def arrive(hops):
        @pl.when(net.z >= hops)
        def _():
            z = net.z - hops
            over_z(z, net.above, 0).wait_recv()
            pl.when(net.has_above)(over_z(z, net.above, 0).start)
            over_y(z).start()
            onward(z, net.y)

        @pl.when(net.z < line - hops)
        def _():
            z = net.z + hops
            over_z(z, net.below, line).wait_recv()
            pl.when(net.has_below)(over_z(z, net.below, line).start)
            over_y(z).start()
            onward(z, net.y)

    def arrive_y(hops):
        def one(z):
            remote(piece(z, 1 - net.y), piece(z, 1 - net.y), 2 * line + z, net.across_y).wait_recv()
            onward(z, 1 - net.y)

        if hops == 0:
            one(net.z)
        else:
            pl.when(net.z >= hops)(lambda: one(net.z - hops))
            pl.when(net.z < line - hops)(lambda: one(net.z + hops))

    def arrive_x(hops, own_y):
        def one(z):
            y = net.y if own_y else 1 - net.y
            part = held(z, y, pl.ds(aligned((1 - net.x) * (only + shared), 128), only))
            remote(part, part, 3 * line + y * line + z, net.across_x).wait_recv()
            to_core(z, y).start()

        if not split:
            return
        if hops == 0:
            one(net.z)
        else:
            pl.when(net.z >= hops)(lambda: one(net.z - hops))
            pl.when(net.z < line - hops)(lambda: one(net.z + hops))

    def step(hops):
        def run():
            arrive_y(hops - 1)
            if hops < line:
                arrive(hops)
            if hops >= 2:
                arrive_x(hops - 2, False)
                arrive_x(hops - 1, True)

        return run

    def last():
        arrive_x(line - 1, False)

    def finish():
        local.wait()
        first_y.wait_send()

        @pl.when(net.has_above)
        def _():
            first_up.wait_send()
            for hops in range(1, line - 1):
                pl.when(net.z >= hops)(over_z(net.z - hops, net.above, 0).wait_send)

        @pl.when(net.has_below)
        def _():
            first_down.wait_send()
            for hops in range(1, line - 1):
                pl.when(net.z < line - hops)(over_z(net.z + hops, net.below, line).wait_send)

        for z in range(line):

            def others():
                over_y(z).wait_send()
                if split:
                    over_x(z, net.y).wait_send()
                to_core(z, net.y).wait()

            pl.when(net.z != z)(others)
            if split:
                over_x(z, 1 - net.y).wait_send()
            to_core(z, 1 - net.y).wait()

    return [start] + [step(hops) for hops in range(1, line + 1)] + [last, finish]


REDUCE_BUFFERS = 9


def reduce_split(columns):
    only = columns // 4 if columns % 512 == 0 else 0
    return only, columns - 2 * only


def reduce_scratch(line, shards, half, columns, dtype):
    only, shared = reduce_split(columns)
    carried = only + shared
    return [
        pltpu.VMEM((shards, half, columns), dtype),
        pltpu.VMEM((shards, half, columns), dtype),
        pltpu.VMEM((shards, half, max(only, 128)), dtype),
        pltpu.VMEM((line, half, carried), dtype),
        pltpu.VMEM((line + 1, half, carried), dtype),
        pltpu.VMEM((half, carried), dtype),
        pltpu.VMEM((half, columns), dtype),
        pltpu.VMEM((half, columns), dtype),
        pltpu.VMEM((2 * half, columns), jnp.float32),
    ]


def reduce_count(line):
    return 3 * line + 4


def reduce_steps(net, grad, out, column_start, out_start, buffers, local_sem, send_sem, recv_sem):
    kept, got, from_x, from_y, from_z, late_x, final, swapped, wide = buffers
    line = net.line
    shards, half, width = kept.shape
    only, shared = reduce_split(width)
    both = only + shared
    columns = pl.ds(column_start, width)
    mine = pl.ds(aligned(net.core * half, half), half)
    theirs = pl.ds(aligned((1 - net.core) * half, half), half)
    if only:
        carried = pl.ds(aligned(net.x * only, 128), both)
        lone = pl.ds(aligned(net.x * both, 128), only)
        their_lone = pl.ds(aligned((1 - net.x) * both, 128), only)
    else:
        carried = pl.ds(0, width)

    def remote(origin, landing, index, target):
        return pltpu.make_async_remote_copy(
            src_ref=origin,
            dst_ref=landing,
            send_sem=send_sem.at[index],
            recv_sem=recv_sem.at[index],
            device_id=target,
            device_id_type=MESH,
        )

    local = pltpu.make_async_copy(grad.at[:, mine, columns], kept, local_sem.at[0])
    halves = remote(grad.at[:, theirs, columns], got, 2 * line, net.sibling)
    written = pltpu.make_async_copy(wide, out.at[:, pl.ds(out_start, width)], local_sem.at[1])
    to_core = remote(final, swapped, 2 * line + 1, net.sibling)
    end_x = remote(kept.at[net.own, :, carried], late_x, 2 * line + 2, net.across_x)
    if only:
        over_x = remote(kept.at[:, :, their_lone], from_x, 2 * line + 3, net.across_x)

    def over_y(z):
        part = kept.at[z * 2 + 1 - net.y, :, carried]
        return remote(part, from_y.at[z], 2 * line + 4 + z, net.across_y)

    def up(z):
        return remote(kept.at[z * 2 + net.y, :, carried], from_z.at[z + 1], z, net.above)

    def down(z):
        return remote(kept.at[z * 2 + net.y, :, carried], from_z.at[z], line + z, net.below)

    def add(shard, part):
        kept[shard, :, carried] = kept[shard, :, carried] + part

    def first():
        halves.start()
        local.start()

    def second():
        local.wait()
        halves.wait_recv()

        @pl.loop(0, shards)
        def _(shard):
            kept[shard] = kept[shard] + got[shard]

        if only:
            over_x.start()

    def third():
        if only:
            over_x.wait_recv()

            @pl.loop(0, shards)
            def _(shard):
                kept[shard, :, lone] = kept[shard, :, lone] + from_x[shard]

        for z in range(line):
            over_y(z).start()

    def fourth():
        for z in range(line):
            over_y(z).wait_recv()

        @pl.loop(0, line)
        def _(z):
            add(z * 2 + net.y, from_y[z])

    def hop(step):
        def run():
            @pl.when(net.z == step)
            def _():
                for z in range(line - 1, step, -1):
                    if step > 0:
                        up(z).wait_recv()
                        add(z * 2 + net.y, from_z[z + 1])
                    up(z).start()

            @pl.when(net.z == line - 1 - step)
            def _():
                for z in range(line - 1 - step):
                    if step > 0:
                        down(z).wait_recv()
                        add(z * 2 + net.y, from_z[z])
                    down(z).start()

        return run

    def land():
        @pl.when(net.has_below)
        def _():
            up(net.z).wait_recv()
            add(net.own, from_z[net.z + 1])

        @pl.when(net.has_above)
        def _():
            down(net.z).wait_recv()
            add(net.own, from_z[net.z])

        end_x.start()

    def meet():
        end_x.wait_recv()
        if only:
            final[:, lone] = kept[net.own, :, lone]
            for x in range(2):

                @pl.when(net.x == x)
                def _():
                    start = 0 if x == 1 else shared
                    final[:, (1 - x) * both : (1 - x) * both + only] = late_x[:, start : start + only]
                    other = shared * 0 + (only if x == 1 else 0)
                    final[:, only:both] = kept[net.own, :, only:both] + late_x[:, other : other + shared]
        else:
            final[...] = kept[net.own] + late_x[...]
        to_core.start()
        wide[mine, :] = final[...].astype(jnp.float32)

    def swap():
        to_core.wait_recv()
        wide[theirs, :] = swapped[...].astype(jnp.float32)
        written.start()

    def finish():
        written.wait()
        halves.wait_send()
        if only:
            over_x.wait_send()
        for z in range(line):
            over_y(z).wait_send()
            pl.when(net.z < z)(up(z).wait_send)
            pl.when(net.z > z)(down(z).wait_send)
        end_x.wait_send()
        to_core.wait_send()

    hops = [hop(step) for step in range(line - 1)]

    def fourth_and_hop():
        fourth()
        hops[0]()

    return [first, second, third, fourth_and_hop] + hops[1:] + [land, meet, swap, finish]


ROWS_BY_ROWS = (((0,), (0,)), ((), ()))
COLUMNS_BY_COLUMNS = (((1,), (1,)), ((), ()))


def product(first_op, second_op, dims=(((1,), (0,)), ((), ()))):
    return lax.dot_general(first_op, second_op, dims, preferred_element_type=jnp.float32)


def inverse_rms(values):
    return lax.rsqrt(jnp.mean(values * values, axis=1, keepdims=True) + norm_eps)


def run(body, *, grid, out_shape, in_specs, out_specs, scratch_shapes, name, operands):
    return pl.pallas_call(
        body,
        grid=(grid,),
        out_shape=out_shape,
        in_specs=in_specs,
        out_specs=out_specs,
        scratch_shapes=scratch_shapes,
        compiler_params=pltpu.CompilerParams(vmem_limit_bytes=60 << 20),
        name=name,
    )(*operands)


def whole(*shape):
    return pl.BlockSpec(shape, lambda step: (0,) * len(shape), pipeline_mode=pl.Buffered(1))


def like(shape, dtype):
    return jax.ShapeDtypeStruct(shape, dtype)


def project_kernel(turned, x_ref, gain_ref, w_ref, cos_ref, sin_ref, out_ref, normed_ref):
    step = pl.program_id(0)

    @pl.when(step == 0)
    def _():
        values = x_ref[...].astype(jnp.float32)
        normed = values * inverse_rms(values) * gain_ref[...]
        normed_ref[...] = normed.T.astype(jnp.bfloat16)

    out = product(w_ref[...], normed_ref[...], ROWS_BY_ROWS)

    @pl.when(step < turned)
    def _():
        cos, sin = cos_ref[...], sin_ref[...]
        half = cos.shape[0]
        for start in range(0, out.shape[0], 2 * half):
            first, second = out[start : start + half], out[start + half : start + 2 * half]
            out_ref[start : start + half, :] = (first * cos - second * sin).astype(jnp.bfloat16)
            out_ref[start + half : start + 2 * half, :] = (second * cos + first * sin).astype(jnp.bfloat16)

    @pl.when(step >= turned)
    def _():
        out_ref[...] = out.astype(jnp.bfloat16)


def project(x, gain, weight, cos_t, sin_t):
    rows, width = x.shape
    columns = weight.shape[1]
    block = 512
    return run(
        functools.partial(project_kernel, 2 * width // block),
        grid=columns // block,
        out_shape=[like((columns, rows), jnp.bfloat16), like((width, rows), jnp.bfloat16)],
        in_specs=[
            whole(rows, width),
            whole(1, width),
            pl.BlockSpec((width, block), lambda step: (0, step)),
            whole(*cos_t.shape),
            whole(*sin_t.shape),
        ],
        out_specs=[
            pl.BlockSpec((block, rows), lambda step: (step, 0)),
            pl.BlockSpec((width, rows), lambda step: (0, 0)),
        ],
        scratch_shapes=[],
        name="project",
        operands=[x, gain, weight, cos_t, sin_t],
    )


def branch_kernel(att_ref, w_ref, x_ref, gain_ref, hidden_ref, normed_ref):
    hidden = x_ref[...].astype(jnp.float32) + product(att_ref[...], w_ref[...], ROWS_BY_ROWS)
    hidden_ref[...] = hidden
    normed_ref[...] = (hidden * inverse_rms(hidden) * gain_ref[...]).astype(jnp.bfloat16)


def branch(attended_t, weight, x, gain):
    rows, width = x.shape
    block = 256
    row = pl.BlockSpec((block, width), lambda step: (step, 0))
    return run(
        branch_kernel,
        grid=rows // block,
        out_shape=[like((rows, width), jnp.float32), like((rows, width), jnp.bfloat16)],
        in_specs=[
            pl.BlockSpec((width, block), lambda step: (0, step)),
            whole(*weight.shape),
            row,
            whole(1, width),
        ],
        out_specs=[row, row],
        scratch_shapes=[],
        name="branch",
        operands=[attended_t, weight, x, gain],
    )


def widen_kernel(normed_ref, gate_ref, up_ref, act_ref, to_gate_ref, to_up_ref):
    normed = normed_ref[...]
    gate = product(normed, gate_ref[...])
    up = product(normed, up_ref[...])
    sigmoid = jax.nn.sigmoid(gate)
    swish = gate * sigmoid
    act_ref[...] = (swish * up).astype(jnp.bfloat16)
    to_gate_ref[...] = (up * sigmoid * (1.0 + gate * (1.0 - sigmoid))).astype(jnp.bfloat16)
    to_up_ref[...] = swish.astype(jnp.bfloat16)


def widen(normed, weight):
    rows, width = normed.shape
    inner = weight.shape[1] // 2
    block = 512
    steps = inner // block
    part = pl.BlockSpec((rows, block), lambda step: (0, step))
    return run(
        widen_kernel,
        grid=steps,
        out_shape=[like((rows, inner), jnp.bfloat16)] * 3,
        in_specs=[
            whole(rows, width),
            pl.BlockSpec((width, block), lambda step: (0, step)),
            pl.BlockSpec((width, block), lambda step: (0, steps + step)),
        ],
        out_specs=[part] * 3,
        scratch_shapes=[],
        name="widen",
        operands=[normed, weight, weight],
    )


def narrow_kernel(
    steps, act_ref, to_gate_ref, to_up_ref, w_ref, given_ref, hidden_ref, result_ref, grad_ref, d_gate_ref, d_up_ref, acc_ref
):
    step = pl.program_id(0)
    act, weight, given = act_ref[...], w_ref[...], given_ref[...]
    part = product(act, weight)

    @pl.when(step == 0)
    def _():
        acc_ref[...] = hidden_ref[...] + part

    @pl.when(step > 0)
    def _():
        acc_ref[...] += part

    @pl.when(step == steps - 1)
    def _():
        result_ref[...] = acc_ref[...].astype(jnp.bfloat16)

    grad_ref[...] = product(act, given, ROWS_BY_ROWS).astype(jnp.bfloat16)
    d_act = product(given, weight, COLUMNS_BY_COLUMNS)
    d_gate_ref[...] = (d_act * to_gate_ref[...].astype(jnp.float32)).astype(jnp.bfloat16)
    d_up_ref[...] = (d_act * to_up_ref[...].astype(jnp.float32)).astype(jnp.bfloat16)


def narrow(act, to_gate, to_up, weight, given, hidden):
    rows, inner = act.shape
    width = weight.shape[1]
    block = 512
    steps = inner // block
    part = pl.BlockSpec((rows, block), lambda step: (0, step))
    down = pl.BlockSpec((block, width), lambda step: (step, 0))
    return run(
        functools.partial(narrow_kernel, steps),
        grid=steps,
        out_shape=[
            like((rows, width), jnp.bfloat16),
            like((inner, width), jnp.bfloat16),
            like((rows, inner), jnp.bfloat16),
            like((rows, inner), jnp.bfloat16),
        ],
        in_specs=[part, part, part, down, whole(rows, width), whole(rows, width)],
        out_specs=[pl.BlockSpec((rows, width), lambda step: (0, 0)), down, part, part],
        scratch_shapes=[pltpu.VMEM((rows, width), jnp.float32)],
        name="narrow",
        operands=[act, to_gate, to_up, weight, given, hidden],
    )


def grad_in_kernel(normed_ref, d_gate_ref, d_up_ref, to_gate_ref, to_up_ref, turned_ref):
    @pl.when(pl.program_id(0) == 0)
    def _():
        turned_ref[...] = normed_ref[...].T

    to_gate_ref[...] = product(turned_ref[...], d_gate_ref[...]).astype(jnp.bfloat16)
    to_up_ref[...] = product(turned_ref[...], d_up_ref[...]).astype(jnp.bfloat16)


def grad_into(normed, d_gate, d_up):
    rows, width = normed.shape
    inner = d_gate.shape[1]
    block = 512
    part = pl.BlockSpec((rows, block), lambda step: (0, step))
    out = pl.BlockSpec((width, block), lambda step: (0, step))
    return run(
        grad_in_kernel,
        grid=inner // block,
        out_shape=[like((width, inner), jnp.bfloat16)] * 2,
        in_specs=[whole(rows, width), part, part],
        out_specs=[out, out],
        scratch_shapes=[pltpu.VMEM((width, rows), jnp.bfloat16)],
        name="grad_in",
        operands=[normed, d_gate, d_up],
    )


def norm_back(d_normed, values, gain):
    inverse = inverse_rms(values)
    unit = values * inverse
    scaled = d_normed * gain
    mean = jnp.mean(scaled * unit, axis=1, keepdims=True)
    return inverse * (scaled - unit * mean), jnp.sum(d_normed * unit, axis=0, keepdims=True)


def ffn_back_kernel(
    steps, d_gate_ref, d_up_ref, gate_ref, up_ref, hidden_ref, gain_ref, given_ref, d_hidden_ref, d_branch_ref, grad_gain_ref, acc_ref
):
    step = pl.program_id(0)
    part = product(d_gate_ref[...], gate_ref[...], COLUMNS_BY_COLUMNS)
    part = part + product(d_up_ref[...], up_ref[...], COLUMNS_BY_COLUMNS)

    @pl.when(step == 0)
    def _():
        acc_ref[...] = part

    @pl.when(step > 0)
    def _():
        acc_ref[...] += part

    @pl.when(step == steps - 1)
    def _():
        through, grad_gain = norm_back(acc_ref[...], hidden_ref[...], gain_ref[...])
        d_hidden = given_ref[...].astype(jnp.float32) + through
        d_hidden_ref[...] = d_hidden
        d_branch_ref[...] = d_hidden.astype(jnp.bfloat16)
        grad_gain_ref[...] = grad_gain


def ffn_back(d_gate, d_up, weight, hidden, gain, given):
    rows, width = hidden.shape
    inner = d_gate.shape[1]
    block = 512
    steps = inner // block
    part = pl.BlockSpec((rows, block), lambda step: (0, step))
    full = pl.BlockSpec((rows, width), lambda step: (0, 0))
    return run(
        functools.partial(ffn_back_kernel, steps),
        grid=steps,
        out_shape=[
            like((rows, width), jnp.float32),
            like((rows, width), jnp.bfloat16),
            like((1, width), jnp.float32),
        ],
        in_specs=[
            part,
            part,
            pl.BlockSpec((width, block), lambda step: (0, step)),
            pl.BlockSpec((width, block), lambda step: (0, steps + step)),
            whole(rows, width),
            whole(1, width),
            whole(rows, width),
        ],
        out_specs=[full, full, pl.BlockSpec((1, width), lambda step: (0, 0))],
        scratch_shapes=[pltpu.VMEM((rows, width), jnp.float32)],
        name="ffn_back",
        operands=[d_gate, d_up, weight, weight, hidden, gain, given],
    )


def branch_back_kernel(att_ref, w_ref, d_branch_ref, grad_ref, given_ref):
    d_branch = d_branch_ref[...]
    grad_ref[...] = product(att_ref[...], d_branch).astype(jnp.bfloat16)
    given_ref[...] = product(w_ref[...], d_branch, COLUMNS_BY_COLUMNS).astype(jnp.bfloat16)


def branch_back(attended_t, weight, d_branch):
    rows, width = d_branch.shape
    block = 256
    out = pl.BlockSpec((block, width), lambda step: (step, 0))
    turned = pl.BlockSpec((block, rows), lambda step: (step, 0))
    return run(
        branch_back_kernel,
        grid=attended_t.shape[0] // block,
        out_shape=[like(weight.shape, jnp.bfloat16), like(attended_t.shape, jnp.bfloat16)],
        in_specs=[turned, out, whole(rows, width)],
        out_specs=[out, turned],
        scratch_shapes=[],
        name="branch_back",
        operands=[attended_t, weight, d_branch],
    )


def project_back_kernel(
    steps, normed_ref, dq_ref, dk_ref, dv_ref, w_ref, x_ref, gain_ref, d_hidden_ref, grad_ref, tokens_ref, grad_gain_ref, acc_ref
):
    step = pl.program_id(0)
    third = steps // 3

    def run(d_ref):
        d_part = d_ref[...]
        grad_ref[...] = product(normed_ref[...], d_part, COLUMNS_BY_COLUMNS).astype(jnp.bfloat16)
        part = product(w_ref[...], d_part)

        @pl.when(step == 0)
        def _():
            acc_ref[...] = part

        @pl.when(step > 0)
        def _():
            acc_ref[...] += part

    for index, d_ref in enumerate((dq_ref, dk_ref, dv_ref)):
        pl.when(step // third == index)(functools.partial(run, d_ref))

    @pl.when(step == steps - 1)
    def _():
        values = x_ref[...].astype(jnp.float32)
        through, grad_gain = norm_back(acc_ref[...].T, values, gain_ref[...])
        tokens_ref[...] = d_hidden_ref[...] + through
        grad_gain_ref[...] = grad_gain


def project_back(normed_t, dq, dk, dv, weight, x, gain, d_hidden):
    rows, width = x.shape
    columns = weight.shape[1]
    block = 512
    steps = columns // block
    third = steps // 3
    full = pl.BlockSpec((rows, width), lambda step: (0, 0))

    def part(which):
        return pl.BlockSpec(
            (block, rows), lambda step: (jnp.clip(step - which * third, 0, third - 1), 0)
        )

    return run(
        functools.partial(project_back_kernel, steps),
        grid=steps,
        out_shape=[
            like((width, columns), jnp.bfloat16),
            like((rows, width), jnp.float32),
            like((1, width), jnp.float32),
        ],
        in_specs=[
            whole(*normed_t.shape),
            part(0),
            part(1),
            part(2),
            pl.BlockSpec((width, block), lambda step: (0, step)),
            whole(rows, width),
            whole(1, width),
            whole(rows, width),
        ],
        out_specs=[
            pl.BlockSpec((width, block), lambda step: (0, step)),
            full,
            pl.BlockSpec((1, width), lambda step: (0, 0)),
        ],
        scratch_shapes=[pltpu.VMEM((width, rows), jnp.float32)],
        name="project_back",
        operands=[normed_t, dq, dk, dv, weight, x, gain, d_hidden],
    )


LOG2E = 1.4426950408889634
FEATURES = 16


def two_parts(value):
    high = value.astype(jnp.bfloat16)
    return high, (value - high.astype(jnp.float32)).astype(jnp.bfloat16)


def three_parts(value):
    high, rest = value.astype(jnp.bfloat16), None
    rest = value - high.astype(jnp.float32)
    middle = rest.astype(jnp.bfloat16)
    return high, middle, (rest - middle.astype(jnp.float32)).astype(jnp.bfloat16)


def key_features(variates, valid):
    length = variates.shape[1]
    masks = [(variates == v).astype(jnp.float32) for v in range(4)]
    ones = jnp.ones((1, length), jnp.float32)
    invalid = 1.0 - valid
    rows = masks + masks + [invalid, ones, ones, ones, jnp.zeros((FEATURES - 12, length), jnp.float32)]
    return jnp.concatenate(rows, axis=0).astype(jnp.bfloat16)


def query_features(variates, same, other, log_sums):
    length = variates.shape[1]
    highs, lows = [], []
    for v in range(4):
        bias = jnp.where(variates == v, same, other) * LOG2E
        high, low = two_parts(bias)
        highs.append(high.astype(jnp.float32))
        lows.append(low.astype(jnp.float32))
    if log_sums is None:
        minus = [jnp.zeros((3, length), jnp.float32)]
    else:
        minus = [part.astype(jnp.float32) for part in three_parts(-log_sums)]
    mask = jnp.full((1, length), masked_score, jnp.float32)
    rows = highs + lows + [mask] + minus + [jnp.zeros((FEATURES - 12, length), jnp.float32)]
    return jnp.concatenate(rows, axis=0).astype(jnp.bfloat16)


def contract_depth(first_op, second_op):
    return lax.dot_general(
        first_op, second_op, (((1,), (0,)), ((), ())), preferred_element_type=jnp.float32
    )


def scaled_query(query_t, score_scale):
    return two_parts(query_t.astype(jnp.float32) * (score_scale * LOG2E))


def attend_kernel(blocks, bias_ref, *refs):
    head = pl.program_id(0)
    attend_head(blocks, bias_ref[0, head], bias_ref[1, head], *refs)


def attend_head(blocks, same, other, q_ref, k_ref, v_ref, var_ref, valid_ref, o_ref, wide_ref, lse_ref, query_ref):
    depth, length = q_ref.shape
    width = length // blocks
    variates = var_ref[...]
    high, low = scaled_query(q_ref[...], depth ** (-0.5))
    query_ref[...] = jnp.concatenate([high, low, query_features(variates, same, other, None)], axis=0)
    key_t = k_ref[...]
    keys = jnp.concatenate([key_t, key_t, key_features(variates, valid_ref[...])], axis=0).T
    ones = jnp.concatenate(
        [jnp.ones((1, length), jnp.float32), jnp.zeros((FEATURES - 1, length), jnp.float32)], axis=0
    ).astype(jnp.bfloat16)
    values = jnp.concatenate([v_ref[...], ones], axis=0)
    for block in range(blocks):
        at = pl.ds(block * width, width)
        scores = contract_depth(keys, query_ref[:, at])
        peak = jnp.max(scores, axis=0, keepdims=True)
        weights = jnp.exp2(scores - peak).astype(jnp.bfloat16)
        summed = contract_depth(values, weights)
        total = summed[depth : depth + 1]
        attended = summed[:depth] / total
        wide_ref[:, at] = attended
        o_ref[:, at] = attended.astype(jnp.bfloat16)
        lse_ref[0, :, at] = peak + jnp.log2(total)


def attend_forward(qkv_t, variates, valid, bias, heads):
    rows, length = qkv_t.shape
    depth = rows // (3 * heads)

    def part(which):
        return pl.BlockSpec((depth, length), lambda head: (which * heads + head, 0))

    row = pl.BlockSpec((1, length), lambda head: (0, 0))
    return run(
        functools.partial(attend_kernel, 1),
        grid=heads,
        out_shape=[
            jax.ShapeDtypeStruct((heads * depth, length), jnp.bfloat16),
            jax.ShapeDtypeStruct((heads * depth, length), jnp.float32),
            jax.ShapeDtypeStruct((heads, 1, length), jnp.float32),
        ],
        in_specs=[
            pl.BlockSpec(memory_space=pltpu.SMEM),
            part(0),
            part(1),
            part(2),
            row,
            row,
        ],
        out_specs=[
            pl.BlockSpec((depth, length), lambda head: (head, 0)),
            pl.BlockSpec((depth, length), lambda head: (head, 0)),
            pl.BlockSpec((1, 1, length), lambda head: (head, 0, 0)),
        ],
        scratch_shapes=[pltpu.VMEM((2 * depth + FEATURES, length), jnp.bfloat16)],
        name="attend_forward",
        operands=[bias, qkv_t, qkv_t, qkv_t, variates, valid],
    )


def turn_back(grad_t, cos_t, sin_t):
    half = cos_t.shape[0]
    first, second = grad_t[:half], grad_t[half:]
    return jnp.concatenate(
        [first * cos_t + second * sin_t, second * cos_t - first * sin_t], axis=0
    )


def attend_back_head(
    blocks, same, other, q_ref, k_ref, v_ref, go_ref, wide_ref, lse_ref, var_ref, valid_ref, cos_ref, sin_ref,
    dq_ref, dk_ref, dv_ref, query_ref, given_ref, dk_acc, dv_acc,
):
    depth, length = q_ref.shape
    width = length // blocks
    scale = depth ** (-0.5)
    variates = var_ref[...]
    features = key_features(variates, valid_ref[...])
    high, low = scaled_query(q_ref[...], scale)
    query_ref[...] = jnp.concatenate([high, low, query_features(variates, same, other, lse_ref[0])], axis=0)
    key_t = k_ref[...]
    keys = jnp.concatenate([key_t, key_t, features], axis=0).T
    keys_low = jnp.concatenate([key_t, features], axis=0)
    given = go_ref[...]
    inner = jnp.sum(given.astype(jnp.float32) * wide_ref[...], axis=0, keepdims=True)
    minus = [part.astype(jnp.float32) for part in three_parts(-inner)]
    minus = jnp.concatenate(minus + [jnp.zeros((FEATURES - 3, length), jnp.float32)], axis=0)
    given_ref[...] = jnp.concatenate([given, minus.astype(jnp.bfloat16)], axis=0)
    ones = jnp.concatenate(
        [jnp.ones((3, length), jnp.float32), jnp.zeros((FEATURES - 3, length), jnp.float32)], axis=0
    ).astype(jnp.bfloat16)
    values = jnp.concatenate([v_ref[...], ones], axis=0).T
    query_rows = q_ref[...].T
    given_rows = given.T
    in_same = jnp.zeros((1, width), jnp.float32)
    in_other = jnp.zeros((1, width), jnp.float32)
    for block in range(blocks):
        at = pl.ds(block * width, width)
        cut = slice(block * width, (block + 1) * width)
        probs = jnp.exp2(contract_depth(keys, query_ref[:, at]))
        grads = (probs * contract_depth(values, given_ref[:, at])).astype(jnp.bfloat16)
        back = contract_depth(keys_low, grads)
        dq = turn_back(back[:depth] * scale, cos_ref[:, at], sin_ref[:, at])
        dq_ref[:, at] = dq.astype(jnp.bfloat16)
        for v in range(4):
            line = back[depth + v : depth + v + 1]
            hit = variates[:, cut] == v
            in_same = in_same + jnp.where(hit, line, 0.0)
            in_other = in_other + jnp.where(hit, 0.0, line)
        dk = contract_depth(grads, query_rows[cut])
        dv = contract_depth(probs.astype(jnp.bfloat16), given_rows[cut])
        if block == 0:
            dk_acc[...] = dk
            dv_acc[...] = dv
        else:
            dk_acc[...] += dk
            dv_acc[...] += dv
    dk_ref[...] = turn_back((dk_acc[...] * scale).T, cos_ref[...], sin_ref[...]).astype(jnp.bfloat16)
    dv_ref[...] = dv_acc[...].T.astype(jnp.bfloat16)
    return in_same, in_other


def attend_back_kernel(blocks, bias_ref, *refs):
    head = pl.program_id(0)
    *refs, db_ref, query_ref, given_ref, dk_acc, dv_acc = refs
    in_same, in_other = attend_back_head(
        blocks, bias_ref[0, head], bias_ref[1, head], *refs, query_ref, given_ref, dk_acc, dv_acc
    )
    db_ref[0, 0:1, :] = in_same
    db_ref[0, 1:2, :] = in_other


def attend_backward(qkv_t, given_t, wide_t, log_sums, variates, valid, bias, cos_t, sin_t, heads):
    rows, length = qkv_t.shape
    depth = rows // (3 * heads)
    blocks = 1

    def part(which):
        return pl.BlockSpec((depth, length), lambda head: (which * heads + head, 0))

    one = pl.BlockSpec((depth, length), lambda head: (head, 0))
    grad = jax.ShapeDtypeStruct((heads * depth, length), jnp.bfloat16)
    return run(
        functools.partial(attend_back_kernel, blocks),
        grid=heads,
        out_shape=[grad, grad, grad, jax.ShapeDtypeStruct((heads, 2, length // blocks), jnp.float32)],
        in_specs=[
            pl.BlockSpec(memory_space=pltpu.SMEM),
            part(0),
            part(1),
            part(2),
            one,
            one,
            pl.BlockSpec((1, 1, length), lambda head: (head, 0, 0)),
            whole(1, length),
            whole(1, length),
            whole(depth // 2, length),
            whole(depth // 2, length),
        ],
        out_specs=[one, one, one, pl.BlockSpec((1, 2, length // blocks), lambda head: (head, 0, 0))],
        scratch_shapes=[
            pltpu.VMEM((2 * depth + FEATURES, length), jnp.bfloat16),
            pltpu.VMEM((depth + FEATURES, length), jnp.bfloat16),
            pltpu.VMEM((length, depth), jnp.float32),
            pltpu.VMEM((length, depth), jnp.float32),
        ],
        name="attend_backward",
        operands=[bias, qkv_t, qkv_t, qkv_t, given_t, wide_t, log_sums, variates, valid, cos_t, sin_t],
    )


PRELUDE = 7
FRONT_PLACES = (
    (0, 1, 2, 3, 4, 5, 6),
    (1, 3, 4, 5, 7, 8, 9),
    (3, 6, 8, 10, 13, 16, 18),
    (8, 12, 15, 18, 21, 24, 28),
)


def bias_of(small_ref, head, per_shard):
    row = 16 * (head // per_shard) + 2
    return small_ref[row, head % per_shard], small_ref[row + 1, head % per_shard]


def gain_of(small_ref, shards, which):
    rows = [small_ref[16 * shard + which : 16 * shard + which + 1, :] for shard in range(shards)]
    return jnp.concatenate(rows, axis=1)


def front_kernel(line, shards, heads, *refs):
    step = pl.program_id(0)
    refs = list(refs)

    def take(count):
        out = refs[:count]
        del refs[:count]
        return out

    small, w_qkv, w_out, w_in, w_down, x_hbm = take(6)
    var_ref, valid_ref, cos_ref, sin_ref = take(4)
    small_all, qkv_all, out_all, into_0, down_0, into_1, down_1 = take(7)
    intos = take(4)
    qkv_hbm, normed_hbm, attended_hbm, hidden_hbm, normed_two_hbm = take(5)
    wide_ref, lse_ref = take(2)
    x, weight, normed_t, qkv, attended, hidden, normed_two, small_ref, query_ref, bias_ref, wide_rows, cut_rows = take(12)
    load_sem, cut_sem, local_sem, send_sem, recv_sem = refs
    net = Net(line)
    rows, width = x.shape
    block = 512
    projected = 3 * width // block
    attend = PRELUDE + projected
    last = attend + heads
    depth = width // heads

    def load(index, origin, landing):
        return pltpu.make_async_copy(origin, landing, load_sem.at[index])

    def at(place):
        return pl.when(step == place)

    inner = w_in.shape[1] // 2
    owned = inner // shards
    piece_width = BLOCK // shards

    w_in_load = pltpu.make_async_copy(w_in, wide_rows, cut_sem.at[4])

    def cut_store(number):
        return pltpu.make_async_copy(cut_rows.at[number], intos[number], cut_sem.at[number])

    def down_part(number):
        return w_down.at[pl.ds(number * piece_width, piece_width)]

    tensors = (
        ((small, small_all), (w_qkv, qkv_all)),
        ((w_out, out_all),),
        ((intos[0], into_0), (down_part(0), down_0)),
        ((intos[1], into_1), (down_part(1), down_1)),
    )
    number = 0
    groups = []
    for group in tensors:
        lists = []
        for source, full in group:
            lists.append(
                gather_steps(
                    net, source, full, local_sem.at[number], send_sem.at[number], recv_sem.at[number]
                )
            )
            number += 1
        groups.append(lists)

    x_load = load(0, x_hbm, x)
    small_load = load(1, small_all, small_ref)
    weight_load = load(2, qkv_all, weight)
    bias_load = load(9, small_all, bias_ref)
    normed_store = load(3, normed_t, normed_hbm)
    qkv_store = load(4, qkv, qkv_hbm)
    attended_store = load(5, attended, attended_hbm)
    out_load = load(6, out_all, weight.at[:, pl.ds(0, width)])
    hidden_store = load(7, hidden, hidden_hbm)
    normed_two_store = load(8, normed_two, normed_two_hbm)

    @at(0)
    def _():
        net.greet()
        x_load.start()
        w_in_load.start()

    for lists, places in zip(groups, FRONT_PLACES):
        for index, place in enumerate(places):

            @at(place)
            def _():
                if place == FRONT_PLACES[2][0] and lists is groups[2]:
                    cut_store(0).wait()
                if place == FRONT_PLACES[3][0] and lists is groups[3]:
                    cut_store(1).wait()
                for steps in lists:
                    steps[index]()

    @at(0)
    def _():
        w_in_load.wait()
        for index in range(4):
            for piece in range(2 * shards):
                start = piece * owned + index * piece_width
                cut_rows[index, :, piece * piece_width : (piece + 1) * piece_width] = wide_rows[
                    :, start : start + piece_width
                ]
            cut_store(index).start()

    @at(PRELUDE - 1)
    def _():
        cut_store(2).wait()
        cut_store(3).wait()
        weight_load.start()
        small_load.start()
        bias_load.start()
        x_load.wait()
        small_load.wait()
        bias_load.wait()
        gain = gain_of(small_ref, shards, 0)
        values = x[...].astype(jnp.float32)
        normed = values * inverse_rms(values) * gain
        normed_t[...] = normed.T.astype(jnp.bfloat16)
        normed_store.start()
        weight_load.wait()

    @pl.when((step >= PRELUDE) & (step < attend))
    def _():
        index = step - PRELUDE
        columns = pl.ds(aligned(index * block, block), block)
        out = product(weight[:, columns], normed_t[...], ROWS_BY_ROWS)
        lines = qkv.at[columns]

        @pl.when(index < 2 * width // block)
        def _():
            cos, sin = cos_ref[...], sin_ref[...]
            half = depth // 2
            for start in range(0, block, depth):
                first, second = out[start : start + half], out[start + half : start + depth]
                lines[start : start + half, :] = (first * cos - second * sin).astype(jnp.bfloat16)
                lines[start + half : start + depth, :] = (second * cos + first * sin).astype(jnp.bfloat16)

        @pl.when(index >= 2 * width // block)
        def _():
            lines[...] = out.astype(jnp.bfloat16)

    @at(attend)
    def _():
        qkv_store.start()

    @pl.when((step >= attend) & (step < last))
    def _():
        head = step - attend

        def part(which):
            return qkv.at[pl.ds(aligned(which * width + head * depth, depth), depth)]

        same, other = bias_of(bias_ref, head, heads // shards)
        attend_head(
            1,
            same,
            other,
            part(0),
            part(1),
            part(2),
            var_ref,
            valid_ref,
            attended.at[pl.ds(aligned(head * depth, depth), depth)],
            wide_ref,
            lse_ref,
            query_ref,
        )

    @at(last - 1)
    def _():
        out_load.start()
        attended_store.start()

    @at(last)
    def _():
        out_load.wait()
        gain = gain_of(small_ref, shards, 1)
        part = 256
        for index in range(rows // part):
            lines = slice(index * part, (index + 1) * part)
            sums = product(attended[:, lines], weight[:, :width], ROWS_BY_ROWS)
            values = x[lines, :].astype(jnp.float32) + sums
            hidden[lines, :] = values
            normed_two[lines, :] = (values * inverse_rms(values) * gain).astype(jnp.bfloat16)
        hidden_store.start()
        normed_two_store.start()
        for store in (normed_store, qkv_store, attended_store, hidden_store, normed_two_store):
            store.wait()


def front(line, small, w_qkv, w_out, w_in, w_down, x, variates, valid, cos_t, sin_t, heads):
    shards = lax.axis_size("shard")
    rows, width = x.shape
    depth = width // heads
    low = jnp.bfloat16
    piece = BLOCK // shards
    grid = PRELUDE + 3 * width // 512 + heads + 1
    copies = gather_count(line)

    def head_at(step):
        return jnp.clip(step - (PRELUDE + 3 * width // 512), 0, heads - 1)

    def gathered(rows, columns, dtype=low):
        return like((shards * rows, columns), dtype)

    owned = w_qkv.shape[0]
    return pl.pallas_call(
        functools.partial(front_kernel, line, shards, heads),
        grid=(grid,),
        out_shape=[
            gathered(16, 128, jnp.float32),
            gathered(*w_qkv.shape),
            gathered(*w_out.shape),
            gathered(owned, 2 * BLOCK),
            gathered(piece, width),
            gathered(owned, 2 * BLOCK),
            gathered(piece, width),
        ]
        + [like((owned, 2 * BLOCK), low)] * 4
        + [
            like((3 * width, rows), low),
            like((width, rows), low),
            like((width, rows), low),
            like((rows, width), jnp.float32),
            like((rows, width), low),
            like((width, rows), jnp.float32),
            like((heads, 1, rows), jnp.float32),
        ],
        in_specs=[ANY] * 6
        + [
            whole(1, rows),
            whole(1, rows),
            whole(*cos_t.shape),
            whole(*sin_t.shape),
        ],
        out_specs=[ANY] * 16
        + [
            pl.BlockSpec((depth, rows), lambda step: (head_at(step), 0)),
            pl.BlockSpec((1, 1, rows), lambda step: (head_at(step), 0, 0)),
        ],
        scratch_shapes=[
            pltpu.VMEM((rows, width), low),
            pltpu.VMEM((width, 3 * width), low),
            pltpu.VMEM((width, rows), low),
            pltpu.VMEM((3 * width, rows), low),
            pltpu.VMEM((width, rows), low),
            pltpu.VMEM((rows, width), jnp.float32),
            pltpu.VMEM((rows, width), low),
            pltpu.VMEM((16 * shards, 128), jnp.float32),
            pltpu.VMEM((2 * depth + FEATURES, rows), low),
            pltpu.SMEM((16 * shards, 128), jnp.float32),
            pltpu.VMEM(w_in.shape, low),
            pltpu.VMEM((4, owned, 2 * BLOCK), low),
            pltpu.SemaphoreType.DMA((10,)),
            pltpu.SemaphoreType.DMA((5,)),
            pltpu.SemaphoreType.DMA((7,)),
            pltpu.SemaphoreType.DMA((7, copies)),
            pltpu.SemaphoreType.DMA((7, copies)),
        ],
        compiler_params=pltpu.CompilerParams(
            collective_id=1, has_side_effects=True, vmem_limit_bytes=62 << 20
        ),
        name="front",
    )(small, w_qkv, w_out, w_in, w_down, x, variates, valid, cos_t, sin_t)


TILE = 512
BLOCK = 1024
KEPT, GIVEN, GOT, OVER_X, OVER_Y, OVER_Z, LATE, ENDS, WIDE = 13, 3, 4, 5, 5, 6, 4, 4, 3
STAGES = (0, 1, 3, 5, 7, 8, 9, 10, 11, 12)
SUBSTEPS = 6


def stream_scratch(line, shards, half):
    only, shared = reduce_split(TILE)
    both = only + shared
    low = jnp.bfloat16
    copies = 7
    return [
        pltpu.VMEM((KEPT, shards, half, TILE), low),
        pltpu.VMEM((GIVEN, shards, half, TILE), low),
        pltpu.VMEM((GOT, shards, half, TILE), low),
        pltpu.VMEM((OVER_X, shards, half, only), low),
        pltpu.VMEM((OVER_Y, line, half, both), low),
        pltpu.VMEM((OVER_Z, line + 1, half, both), low),
        pltpu.VMEM((LATE, half, both), low),
        pltpu.VMEM((ENDS, half, TILE), low),
        pltpu.VMEM((ENDS, half, TILE), low),
        pltpu.VMEM((WIDE, 2 * half, TILE), jnp.float32),
        pltpu.SemaphoreType.DMA((KEPT, 4)),
        pltpu.SemaphoreType.DMA((KEPT, copies)),
        pltpu.SemaphoreType.DMA((KEPT, copies)),
    ]


class Stream:
    def __init__(self, net, scratch, writes):
        self.net, self.writes = net, writes
        (
            self.kept,
            self.give,
            self.got,
            self.from_x,
            self.from_y,
            self.from_z,
            self.late,
            self.final,
            self.swapped,
            self.wide,
            self.local_sem,
            self.send_sem,
            self.recv_sem,
        ) = scratch
        self.shards, self.half = self.kept.shape[1], self.kept.shape[2]
        self.own = net.y * net.line + net.z
        self.only, self.shared = reduce_split(TILE)
        self.both = self.only + self.shared
        self.carried = pl.ds(aligned(net.x * self.only, 128), self.both)
        self.lone = pl.ds(aligned(net.x * self.both, 128), self.only)
        self.their_lone = pl.ds(aligned((1 - net.x) * self.both, 128), self.only)

    def remote(self, tile, origin, landing, index, target):
        slot = tile % KEPT
        return pltpu.make_async_remote_copy(
            src_ref=origin,
            dst_ref=landing,
            send_sem=self.send_sem.at[slot, index],
            recv_sem=self.recv_sem.at[slot, index],
            device_id=target,
            device_id_type=MESH,
        )

    def halves(self, tile):
        return self.remote(tile, self.give.at[tile % GIVEN], self.got.at[tile % GOT], 3, self.net.sibling)

    def over_x(self, tile):
        origin = self.kept.at[tile % KEPT, :, :, self.their_lone]
        return self.remote(tile, origin, self.from_x.at[tile % OVER_X], 4, self.net.across_x)

    def over_y(self, tile):
        net = self.net
        origin = self.kept.at[tile % KEPT, pl.ds((1 - net.y) * net.line, net.line), :, self.carried]
        return self.remote(tile, origin, self.from_y.at[tile % OVER_Y], 2, net.across_y)

    def up(self, tile, z):
        net, count = self.net, self.net.line - 1 - z
        origin = self.kept.at[tile % KEPT, pl.ds(net.y * net.line + z + 1, count), :, self.carried]
        return self.remote(tile, origin, self.from_z.at[tile % OVER_Z, pl.ds(z + 2, count)], 0, net.above)

    def down(self, tile, z):
        net = self.net
        origin = self.kept.at[tile % KEPT, pl.ds(net.y * net.line, z), :, self.carried]
        return self.remote(tile, origin, self.from_z.at[tile % OVER_Z, pl.ds(0, z)], 1, net.below)

    def end_x(self, tile):
        net = self.net
        origin = self.kept.at[tile % KEPT, self.own, :, self.carried]
        return self.remote(tile, origin, self.late.at[tile % LATE], 5, net.across_x)

    def to_core(self, tile):
        slot = tile % ENDS
        return self.remote(tile, self.final.at[slot], self.swapped.at[slot], 6, self.net.sibling)

    def add(self, tile, shard, part):
        slot = tile % KEPT
        self.kept[slot, shard, :, self.carried] = self.kept[slot, shard, :, self.carried] + part

    def born(self, tile):
        self.halves(tile).start()

    def meet_core(self, tile):
        copy = self.halves(tile)
        copy.wait_recv()
        copy.wait_send()
        slot, came = tile % KEPT, tile % GOT

        @pl.loop(0, self.shards)
        def _(shard):
            self.kept[slot, shard] = self.kept[slot, shard] + self.got[came, shard]

        self.over_x(tile).start()

    def meet_x(self, tile):
        self.over_x(tile).wait_recv()
        slot, came = tile % KEPT, tile % OVER_X

        @pl.loop(0, self.shards)
        def _(shard):
            self.kept[slot, shard, :, self.lone] = self.kept[slot, shard, :, self.lone] + self.from_x[came, shard]

        self.over_y(tile).start()

    def meet_y(self, tile):
        self.over_y(tile).wait_recv()
        came, base = tile % OVER_Y, self.net.y * self.net.line

        @pl.loop(0, self.net.line)
        def _(z):
            self.add(tile, base + z, self.from_y[came, z])

        self.hop(tile, 0)

    def hop(self, tile, step):
        net, came = self.net, tile % OVER_Z
        base, end = net.y * net.line, net.line - 1

        @pl.when(net.z == step)
        def _():
            if step > 0:
                self.up(tile, step - 1).wait_recv()
                for z in range(step + 1, net.line):
                    self.add(tile, base + z, self.from_z[came, z + 1])
            self.up(tile, step).start()

        @pl.when(net.z == end - step)
        def _():
            if step > 0:
                self.down(tile, end - step + 1).wait_recv()
                for z in range(end - step):
                    self.add(tile, base + z, self.from_z[came, z])
            self.down(tile, end - step).start()

    def land(self, tile):
        net, came, end = self.net, tile % OVER_Z, self.net.line - 1
        pl.when(net.z == end)(self.up(tile, end - 1).wait_recv)
        pl.when(net.z == 0)(self.down(tile, 1).wait_recv)

        @pl.when(net.has_below)
        def _():
            self.add(tile, self.own, self.from_z[came, net.z + 1])

        @pl.when(net.has_above)
        def _():
            self.add(tile, self.own, self.from_z[came, net.z])

        self.end_x(tile).start()

    def meet(self, tile):
        net, only, both, shared = self.net, self.only, self.both, self.shared
        slot, came, end = tile % KEPT, tile % LATE, tile % ENDS
        self.end_x(tile).wait_recv()
        self.final[end, :, self.lone] = self.kept[slot, self.own, :, self.lone]
        for x in range(2):

            @pl.when(net.x == x)
            def _():
                theirs = 0 if x == 1 else shared
                middle = only if x == 1 else 0
                at = (1 - x) * both
                self.final[end, :, at : at + only] = self.late[came, :, theirs : theirs + only]
                self.final[end, :, only:both] = (
                    self.kept[slot, self.own, :, only:both] + self.late[came, :, middle : middle + shared]
                )

        self.to_core(tile).start()
        mine = pl.ds(aligned(net.core * self.half, self.half), self.half)
        self.wide[tile % WIDE, mine, :] = self.final[end].astype(jnp.float32)

    def swap(self, tile):
        self.to_core(tile).wait_recv()
        theirs = pl.ds(aligned((1 - self.net.core) * self.half, self.half), self.half)
        self.wide[tile % WIDE, theirs, :] = self.swapped[tile % ENDS].astype(jnp.float32)
        self.writes(tile, self.wide.at[tile % WIDE], self.local_sem.at[tile % KEPT], True)

    def finish(self, tile):
        net = self.net
        self.writes(tile, self.wide.at[tile % WIDE], self.local_sem.at[tile % KEPT], False)
        self.over_x(tile).wait_send()
        self.over_y(tile).wait_send()
        for z in range(net.line - 1):
            pl.when(net.z == z)(self.up(tile, z).wait_send)
            pl.when(net.z == z + 1)(self.down(tile, z + 1).wait_send)
        self.end_x(tile).wait_send()
        self.to_core(tile).wait_send()

    def stages(self):
        return [
            self.born,
            self.meet_core,
            self.meet_x,
            self.meet_y,
            lambda tile: self.hop(tile, 1),
            lambda tile: self.hop(tile, 2),
            self.land,
            self.meet,
            self.swap,
            self.finish,
        ]


class Plan:
    def __init__(self, blocks, heads):
        self.blocks, self.heads = blocks, heads
        self.ffn = blocks * SUBSTEPS
        self.norm = self.ffn
        self.branch = self.ffn + 1
        self.attend = self.ffn + 2
        self.groups = 4
        self.per_group = heads // self.groups
        self.out = self.ffn + SUBSTEPS
        self.ready = [self.attend + self.per_group * (group + 1) for group in range(self.groups)]
        self.births = list(range(SUBSTEPS, self.out + 2))
        self.ffn_tiles = self.ffn
        self.keys_tiles, self.value_tiles = [], []
        for group in range(self.groups):
            self.keys_tiles.append(len(self.births))
            self.births.append(max(self.ready[group], self.births[-1] + 1))
            if group % 2 == 1:
                self.value_tiles.append(len(self.births))
                self.births.append(self.births[-1] + 1)
        self.last = self.births[-1]
        self.grid = self.last + STAGES[-1] + 1

    def tile_at(self, step):
        regular = self.out + 2 - SUBSTEPS
        tile = step - SUBSTEPS
        known = (step >= SUBSTEPS) & (step < self.out + 2)
        for index in range(regular, len(self.births)):
            hit = step == self.births[index]
            tile = jnp.where(hit, index, tile)
            known = known | hit
        return tile, known


def back_kernel(plan, line, shards, *refs):
    step = pl.program_id(0)
    refs = list(refs)

    def take(count):
        out = refs[:count]
        del refs[:count]
        return out

    normed_hbm, given_hbm, hidden_hbm = take(3)
    early = take(4)
    into_2, into_3, down_hbm = take(3)
    attended_hbm, out_hbm, normed_one_hbm, x_hbm, qkv_hbm = take(5)
    small_hbm, = take(1)
    q_ref, k_ref, v_ref, wide_ref, lse_ref, var_ref, valid_ref, cos_ref, sin_ref = take(9)
    result_hbm, tokens_hbm, sum_in, sum_down, sum_out, sum_qkv, sum_small = take(7)
    gather_to = take(4)
    normed, turned, given, w_down, w_gate, w_up, act, act_t = take(8)
    d_gate, d_up, acc, through = take(4)
    query_ref, given_aug_ref, dk_acc, dv_acc = take(4)
    load_sem, = take(1)
    gather_local, gather_send, gather_recv = take(3)
    small_ref, bias_ref, grad_gain_one_ref, grad_gain_two_ref, grad_small = take(5)
    small_buffers = take(REDUCE_BUFFERS)
    small_local, small_send, small_recv = take(3)
    net = Net(line)
    piece = BLOCK // shards
    gather_from = [
        into_2,
        down_hbm.at[pl.ds(2 * piece, piece)],
        into_3,
        down_hbm.at[pl.ds(3 * piece, piece)],
    ]
    half = BLOCK // shards // 2
    heads_at = step - plan.attend

    def writes(tile, wide, sems, begin):
        rows = 2 * half

        def move(index, origin, landing):
            copy = pltpu.make_async_copy(origin, landing, sems.at[index])
            copy.start() if begin else copy.wait()

        block, kind = tile // SUBSTEPS, tile % SUBSTEPS
        in_ffn = tile < plan.ffn_tiles

        @pl.when(in_ffn & (kind < 2))
        def _():
            lines = pl.ds(aligned(block * rows, rows), rows)
            move(0, wide, sum_down.at[lines, pl.ds(aligned(kind * TILE, TILE), TILE)])

        @pl.when(in_ffn & (kind >= 2))
        def _():
            inner = plan.blocks * BLOCK
            base = ((kind - 2) // 2) * inner
            for piece in range(4):
                shard = (kind % 2) * 4 + piece
                start = base + shard * (inner // shards) + block * (BLOCK // shards)
                columns = pl.ds(aligned(start, 128), 128)
                move(piece, wide.at[:, piece * 128 : (piece + 1) * 128], sum_in.at[:, columns])

        @pl.when((tile >= plan.ffn_tiles) & (tile < plan.ffn_tiles + 2))
        def _():
            start = aligned((tile - plan.ffn_tiles) * TILE, TILE)
            move(0, wide, sum_out.at[:, pl.ds(start, TILE)])

        width = plan.heads * q_ref.shape[0]
        for group, number in enumerate(plan.keys_tiles):

            @pl.when(tile == number)
            def _():
                for part in range(2):
                    start = part * width + group * (TILE // 2)
                    columns = slice(part * (TILE // 2), (part + 1) * (TILE // 2))
                    move(part, wide.at[:, columns], sum_qkv.at[:, pl.ds(start, TILE // 2)])

        for pair, number in enumerate(plan.value_tiles):

            @pl.when(tile == number)
            def _():
                move(0, wide, sum_qkv.at[:, pl.ds(2 * width + pair * TILE, TILE)])

    stream = Stream(net, refs, writes)
    stages = stream.stages()

    def load(index, origin, landing):
        return pltpu.make_async_copy(origin, landing, load_sem.at[index])

    def weight_loads(block):
        if block < 2:
            into, down = early[2 * block], early[2 * block + 1]
        else:
            into, down = gather_to[2 * (block - 2)], gather_to[2 * (block - 2) + 1]
        return [
            load(0, into.at[:, pl.ds(0, BLOCK)], w_gate),
            load(1, into.at[:, pl.ds(BLOCK, BLOCK)], w_up),
            load(2, down, w_down),
        ]

    first_loads = [
        load(3, normed_hbm, normed),
        load(4, given_hbm, given),
        load(5, hidden_hbm, acc),
        load(15, small_hbm, small_ref),
        load(16, small_hbm, bias_ref),
    ]
    hidden_load = load(5, hidden_hbm, acc)
    result_store = load(6, act, result_hbm)
    attended_wait = load(7, attended_hbm, w_down)
    out_load = load(8, out_hbm, d_up.at[0])
    normed_one_wait = load(9, normed_one_hbm, turned)
    x_load = load(10, x_hbm, normed)
    tokens_store = load(11, acc, tokens_hbm)

    def placed():
        for shard in range(shards):
            order = (shard % 2) * line + shard // 2
            for part in range(2):
                which = net.core if part == 0 else 1 - net.core
                start = (shard * 2 + part) * half
                yield start, aligned((which * shards + order) * half, half)

    def in_order(index, origin, landing):
        return [load(index, origin.at[pl.ds(start, half)], landing.at[pl.ds(to, half)]) for start, to in placed()]

    def turn_into(page, value):
        flipped = value.T
        for start, to in placed():
            page[pl.ds(to, half), :] = flipped[start : start + half]

    def qkv_loads(group):
        width = qkv_hbm.shape[1] // 3
        part = width // plan.groups
        page = act_t if group % 2 == 0 else d_up.at[0]
        return [
            load(
                12 + index,
                qkv_hbm.at[:, pl.ds(index * width + group * part, part)],
                page.at[:, pl.ds(index * part, part)],
            )
            for index in range(3)
        ]

    def at(place):
        return pl.when(step == place)

    def start(copies):
        for copy in copies:
            copy.start()

    def wait(copies):
        for copy in copies:
            copy.wait()

    gathers = [
        gather_steps(
            net, gather_from[i], gather_to[i], gather_local.at[i], gather_send.at[i], gather_recv.at[i]
        )
        for i in range(4)
    ]
    gather_places = ((0, 2, 4, 6, 8, 9, 10), (7, 9, 11, 12, 14, 15, 16))

    @at(0)
    def _():
        net.greet()
        start(weight_loads(0) + first_loads)

    for pair, places in enumerate(gather_places):
        for index, place in enumerate(places):

            @at(place)
            def _():
                gathers[2 * pair][index]()
                gathers[2 * pair + 1][index]()

    for stage in range(len(STAGES) - 1, 0, -1):
        tile, known = plan.tile_at(step - STAGES[stage])
        pl.when(known)(functools.partial(stages[stage], tile))

    @at(0)
    def _():
        wait(first_loads)
        grad_small[...] = jnp.zeros_like(grad_small)
        turn_into(turned, normed[...])

    for block in range(plan.blocks):

        @at(block * SUBSTEPS)
        def _():
            wait(weight_loads(block))

        if block + 1 < plan.blocks:

            @at(block * SUBSTEPS + SUBSTEPS - 1)
            def _():
                start(weight_loads(block + 1))

    block, sub = step // SUBSTEPS, step % SUBSTEPS
    slot = block % 2
    in_ffn = step < plan.ffn

    @pl.when(in_ffn & (sub < 2))
    def _():
        columns = pl.ds(aligned(sub * TILE, TILE), TILE)
        d_act = product(given[...], w_down[columns, :], COLUMNS_BY_COLUMNS)
        gate = product(normed[...], w_gate[:, columns])
        up = product(normed[...], w_up[:, columns])
        sigmoid = jax.nn.sigmoid(gate)
        swish = gate * sigmoid
        act[:, columns] = (swish * up).astype(jnp.bfloat16)
        d_gate[slot, :, columns] = (d_act * up * sigmoid * (1.0 + gate * (1.0 - sigmoid))).astype(jnp.bfloat16)
        d_up[slot, :, columns] = (d_act * swish).astype(jnp.bfloat16)

    @pl.when(in_ffn & (sub == 2))
    def _():
        acc[...] += product(act[...], w_down[...])
        turn_into(act_t, act[...])

    @pl.when(in_ffn & (sub == 3))
    def _():
        part = product(d_gate[slot], w_gate[...], COLUMNS_BY_COLUMNS)

        @pl.when(block == 0)
        def _():
            through[...] = part

        @pl.when(block > 0)
        def _():
            through[...] += part

    @pl.when(in_ffn & (sub == 4))
    def _():
        through[...] += product(d_up[slot], w_up[...], COLUMNS_BY_COLUMNS)

    last_sum = plan.ffn - SUBSTEPS + 2

    @at(last_sum)
    def _():
        act[...] = acc[...].astype(jnp.bfloat16)
        result_store.start()

    @at(last_sum + 1)
    def _():
        start([hidden_load] + in_order(7, attended_hbm, w_down))

    @at(last_sum + 3)
    def _():
        result_store.wait()

    row_block = 128

    @at(plan.norm)
    def _():
        out_load.start()
        hidden_load.wait()
        grad_gain_two_ref[...] = jnp.zeros_like(grad_gain_two_ref)
        gain_two = gain_of(small_ref, shards, 1)

        @pl.loop(0, acc.shape[0] // row_block)
        def _(index):
            lines = pl.ds(aligned(index * row_block, row_block), row_block)
            back, grad_gain = norm_back(through[lines, :], acc[lines, :], gain_two)
            d_hidden = given[lines, :].astype(jnp.float32) + back
            acc[lines, :] = d_hidden
            d_gate[0, lines, :] = d_hidden.astype(jnp.bfloat16)
            grad_gain_two_ref[...] += grad_gain

    @at(plan.branch)
    def _():
        out_load.wait()
        act[...] = product(d_up[0], d_gate[0], COLUMNS_BY_COLUMNS).astype(jnp.bfloat16)
        through[...] = jnp.zeros_like(through)

    for group in range(plan.groups):
        ready = plan.ready[group]

        if group == 0:

            @at(plan.attend)
            def _():
                start(qkv_loads(0))

        @at(ready)
        def _():
            wait(qkv_loads(group))
            if group + 1 < plan.groups:
                start(qkv_loads(group + 1))

    quarter = TILE // 2
    for parity, page in enumerate((act_t, d_up.at[0])):
        base = parity * TILE
        now = (step == plan.ready[parity]) | (step == plan.ready[parity + 2])
        pair = jnp.where(step == plan.ready[parity + 2], 1, 0)
        value_at = pl.ds(aligned(pair * TILE + parity * quarter, quarter), quarter)

        @pl.when(now)
        def _():
            through[...] += product(page[:, :TILE], w_gate[base : base + TILE, :])
            through[...] += product(page[:, TILE : TILE + quarter], w_up[value_at, :])

    @at(plan.out)
    def _():
        attended_wait.wait()
        start(in_order(9, normed_one_hbm, turned) + [x_load])

    @at(plan.births[plan.keys_tiles[0]])
    def _():
        normed_one_wait.wait()

    @pl.when((heads_at >= 0) & (heads_at < plan.heads))
    def _():
        depth = q_ref.shape[0]
        head = heads_at
        group = head // plan.per_group
        q_at = (group % 2) * TILE + (head % plan.per_group) * depth
        k_at = q_at + TILE // 2
        v_at = (group // 2) * TILE + (head % (2 * plan.per_group)) * depth

        def rows(start):
            return pl.ds(aligned(start, depth), depth)

        per_shard = plan.heads // shards
        same, other = bias_of(bias_ref, head, per_shard)
        sums = attend_back_head(
            2,
            same,
            other,
            q_ref,
            k_ref,
            v_ref,
            act.at[rows(head * depth)],
            wide_ref,
            lse_ref,
            var_ref,
            valid_ref,
            cos_ref,
            sin_ref,
            w_gate.at[rows(q_at)],
            w_gate.at[rows(k_at)],
            w_up.at[rows(v_at)],
            query_ref,
            given_aug_ref,
            dk_acc,
            dv_acc,
        )
        for which, lanes in enumerate(sums):
            folded = sum(lanes[:, start : start + 128] for start in range(0, lanes.shape[1], 128))
            grad_small[head // per_shard, pl.ds(2 + 2 * (head % per_shard) + which, 1), :] = folded

    tile, known = plan.tile_at(step)

    def birth(left, right, dims=(((1,), (0,)), ((), ()))):
        out = product(left[...], right, dims).astype(jnp.bfloat16)
        kept, give = stream.kept.at[tile % KEPT], stream.give.at[tile % GIVEN]
        for order in range(shards):
            kept[order] = out[order * half : (order + 1) * half]
            give[order] = out[(shards + order) * half : (shards + order + 1) * half]

    def chosen(numbers, bases):
        base, hit = 0, False
        for number, start in zip(numbers, bases):
            now = step == plan.births[number]
            base, hit = jnp.where(now, start, base), now | hit
        return pl.ds(aligned(base, TILE), TILE), hit

    kind, source = tile % SUBSTEPS, (tile // SUBSTEPS) % 2
    in_tiles = known & (tile < plan.ffn_tiles)
    columns = pl.ds(aligned((kind % 2) * TILE, TILE), TILE)
    pl.when(in_tiles & (kind < 2))(lambda: birth(act_t, given[:, columns]))
    pl.when(in_tiles & (kind >= 2) & (kind < 4))(lambda: birth(turned, d_gate[source, :, columns]))
    pl.when(in_tiles & (kind >= 4))(lambda: birth(turned, d_up[source, :, columns]))
    out_columns = pl.ds(aligned(jnp.clip(step - plan.out, 0, 1) * TILE, TILE), TILE)
    pl.when((step == plan.out) | (step == plan.out + 1))(lambda: birth(w_down, d_gate[0, :, out_columns]))
    lines, hit = chosen(plan.keys_tiles, [(group % 2) * TILE for group in range(plan.groups)])
    pl.when(hit)(lambda: birth(turned, w_gate[lines, :], COLUMNS_BY_COLUMNS))
    value_lines, value_hit = chosen(plan.value_tiles, [pair * TILE for pair in range(plan.groups // 2)])
    pl.when(value_hit)(lambda: birth(turned, w_up[value_lines, :], COLUMNS_BY_COLUMNS))
    pl.when(known)(lambda: stream.born(tile))

    @at(plan.last + 1)
    def _():
        x_load.wait()
        grad_gain_one_ref[...] = jnp.zeros_like(grad_gain_one_ref)
        gain_one = gain_of(small_ref, shards, 0)

        @pl.loop(0, acc.shape[0] // row_block)
        def _(index):
            lines = pl.ds(aligned(index * row_block, row_block), row_block)
            values = normed[lines, :].astype(jnp.float32)
            back, grad_gain = norm_back(through[:, lines].T, values, gain_one)
            acc[lines, :] = acc[lines, :] + back
            grad_gain_one_ref[...] += grad_gain

        tokens_store.start()
        for shard in range(shards):
            columns = slice(shard * 128, (shard + 1) * 128)
            grad_small[shard, 0:1, :] = grad_gain_one_ref[:, columns]
            grad_small[shard, 1:2, :] = grad_gain_two_ref[:, columns]

    small_steps = reduce_steps(
        net, grad_small, sum_small, 0, 0, small_buffers, small_local, small_send, small_recv
    )
    for index, action in enumerate(small_steps):
        at(plan.last + 2 + index)(action)

    @at(plan.grid - 1)
    def _():
        tokens_store.wait()


def back(line, early, sources, own_down, normed_two, given, hidden, attended_t, out_weight, normed_t, x, qkv_weight,
         small, qkv_t, wide_t, log_sums, variates, valid, cos_t, sin_t):
    shards = lax.axis_size("shard")
    rows, width = x.shape
    heads = log_sums.shape[0]
    depth = width // heads
    blocks = 4
    plan = Plan(blocks, heads)
    low = jnp.bfloat16
    owned = width // shards
    inner = blocks * BLOCK

    def head_at(step):
        return jnp.clip(step - plan.attend, 0, heads - 1)

    def part(which):
        return pl.BlockSpec((depth, rows), lambda step: (which * heads + head_at(step), 0))

    page = pltpu.VMEM((BLOCK, BLOCK), low)
    copies = gather_count(line)
    return pl.pallas_call(
        functools.partial(back_kernel, plan, line, shards),
        grid=(plan.grid,),
        out_shape=[
            like((rows, width), low),
            like((rows, width), jnp.float32),
            like((owned, 2 * inner), jnp.float32),
            like((inner // shards, width), jnp.float32),
            like((owned, width), jnp.float32),
            like((owned, 3 * width), jnp.float32),
            like((16, 128), jnp.float32),
        ]
        + [like((width, 2 * BLOCK), low), like((BLOCK, width), low)] * 2
,
        in_specs=[ANY] * 16
        + [
            part(0),
            part(1),
            part(2),
            pl.BlockSpec((depth, rows), lambda step: (head_at(step), 0)),
            pl.BlockSpec((1, 1, rows), lambda step: (head_at(step), 0, 0)),
            whole(1, rows),
            whole(1, rows),
            whole(*cos_t.shape),
            whole(*sin_t.shape),
        ],
        out_specs=[ANY] * 11,
        scratch_shapes=[page] * 8
        + [
            pltpu.VMEM((2, BLOCK, BLOCK), low),
            pltpu.VMEM((2, BLOCK, BLOCK), low),
            pltpu.VMEM((rows, width), jnp.float32),
            pltpu.VMEM((rows, width), jnp.float32),
            pltpu.VMEM((2 * depth + FEATURES, rows), low),
            pltpu.VMEM((depth + FEATURES, rows), low),
            pltpu.VMEM((rows, depth), jnp.float32),
            pltpu.VMEM((rows, depth), jnp.float32),
            pltpu.SemaphoreType.DMA((17,)),
            pltpu.SemaphoreType.DMA((4,)),
            pltpu.SemaphoreType.DMA((4, copies)),
            pltpu.SemaphoreType.DMA((4, copies)),
            pltpu.VMEM((16 * shards, 128), jnp.float32),
            pltpu.SMEM((16 * shards, 128), jnp.float32),
            pltpu.VMEM((1, width), jnp.float32),
            pltpu.VMEM((1, width), jnp.float32),
            pltpu.VMEM((shards, 16, 128), jnp.float32),
        ]
        + reduce_scratch(line, shards, 8, 128, jnp.float32)
        + [
            pltpu.SemaphoreType.DMA((2,)),
            pltpu.SemaphoreType.DMA((reduce_count(line),)),
            pltpu.SemaphoreType.DMA((reduce_count(line),)),
        ]
        + stream_scratch(line, shards, owned // 2),
        compiler_params=pltpu.CompilerParams(
            collective_id=9, has_side_effects=True, vmem_limit_bytes=64 << 20
        ),
        name="back",
    )(
        normed_two, given, hidden, *early, *sources, own_down, attended_t, out_weight, normed_t, x, qkv_weight,
        small, qkv_t, qkv_t, qkv_t, wide_t, log_sums, variates, valid, cos_t, sin_t,
    )


def rope_tables(time_ids):
    half = HEAD_DIM // 2
    exponent = jnp.arange(half).astype(jnp.float32) * (2.0 / HEAD_DIM)
    inverse = jnp.exp(-jnp.log(rope_base) * exponent)
    angles = inverse[:, None] * time_ids.astype(jnp.float32)
    return jnp.cos(angles), jnp.sin(angles)


def pack_small(attn_gain, ffn_gain, attn_bias):
    heads = attn_bias.shape[1]
    small = jnp.zeros((16, 128), jnp.float32)
    small = small.at[0].set(attn_gain.astype(jnp.float32)).at[1].set(ffn_gain.astype(jnp.float32))
    return small.at[2:4, :heads].set(attn_bias.astype(jnp.float32))


def shards(
    line,
    tokens,
    lengths,
    variate_ids,
    time_ids,
    attn_gain,
    w_qkv,
    attn_bias,
    w_out,
    ffn_gain,
    w_in,
    w_down,
    cotangent,
):
    length = variate_ids.shape[1]
    heads = attn_bias.shape[1]
    key_valid = jnp.arange(length)[None, :] < lengths[:, None]
    valid = key_valid.astype(jnp.float32)
    given = jnp.where(key_valid.reshape(length, 1), cotangent, jnp.zeros_like(cotangent))
    cos_t, sin_t = rope_tables(time_ids)
    if line:
        small, qkv_weight, out_weight, into_0, down_0, into_1, down_1, *rest = front(
            line,
            pack_small(attn_gain, ffn_gain, attn_bias),
            w_qkv,
            w_out,
            w_in,
            w_down,
            tokens,
            variate_ids,
            valid,
            cos_t,
            sin_t,
            HEADS,
        )
        intos, (qkv_t, normed_t, attended_t, hidden, normed_two, wide_t, log_sums) = rest[:4], rest[4:]
        result, grad_tokens, sum_in, sum_down, sum_out, sum_qkv, small = back(
            line,
            [into_0, down_0, into_1, down_1],
            [intos[2], intos[3]],
            w_down,
            normed_two,
            given,
            hidden,
            attended_t,
            out_weight,
            normed_t,
            tokens,
            qkv_weight,
            small,
            qkv_t,
            wide_t,
            log_sums,
            variate_ids,
            valid,
            cos_t,
            sin_t,
        )[:7]
        return (
            result,
            grad_tokens,
            small[0],
            sum_qkv,
            jnp.sum(small[2 : 2 + 2 * heads], axis=1).reshape(heads, 2).T,
            sum_out,
            small[1],
            sum_in,
            sum_down,
        )
    gain_one, gain_two, qkv_weight, out_weight, in_weight, down_weight = (
        lax.all_gather(part, "shard", axis=0, tiled=True)
        for part in (attn_gain, ffn_gain, w_qkv, w_out, w_in, w_down)
    )
    bias = lax.all_gather(attn_bias, "shard", axis=1, tiled=True).astype(jnp.float32)
    gain_one = gain_one.astype(jnp.float32).reshape(1, -1)
    gain_two = gain_two.astype(jnp.float32).reshape(1, -1)
    qkv_t, normed_t = project(tokens, gain_one, qkv_weight, cos_t, sin_t)
    attended_t, wide_t, log_sums = attend_forward(qkv_t, variate_ids, valid, bias, HEADS)
    hidden, normed_two = branch(attended_t, out_weight, tokens, gain_two)
    act, to_gate, to_up = widen(normed_two, in_weight)
    result, grad_down, d_gate, d_up = narrow(act, to_gate, to_up, down_weight, given, hidden)
    grad_gate, grad_up = grad_into(normed_two, d_gate, d_up)
    d_hidden, d_branch, grad_gain_two = ffn_back(d_gate, d_up, in_weight, hidden, gain_two, given)
    grad_out, given_t = branch_back(attended_t, out_weight, d_branch)
    dq, dk, dv, bias_parts = attend_backward(
        qkv_t, given_t, wide_t, log_sums, variate_ids, valid, bias, cos_t, sin_t, HEADS
    )
    grad_qkv, grad_tokens, grad_gain_one = project_back(
        normed_t, dq, dk, dv, qkv_weight, tokens, gain_one, d_hidden
    )
    grads = (
        (grad_gain_one.reshape(-1), 0),
        (grad_qkv, 0),
        (jnp.sum(bias_parts, axis=2).T, 1),
        (grad_out, 0),
        (grad_gain_two.reshape(-1), 0),
        (jnp.concatenate([grad_gate, grad_up], axis=1), 0),
        (grad_down, 0),
    )
    owned = [
        lax.psum_scatter(grad.astype(jnp.bfloat16), "shard", scatter_dimension=axis, tiled=True)
        for grad, axis in grads
    ]
    return (result, grad_tokens) + tuple(lax.psum(part, "rep").astype(jnp.float32) for part in owned)


def solution(mesh):
    placed = (
        P(("shard", "rep"), None),
        P(("shard", "rep")),
        P(("shard", "rep"), None),
        P(("shard", "rep"), None),
        P("shard"),
        P("shard", None),
        P(None, "shard"),
        P("shard", None),
        P("shard"),
        P("shard", None),
        P("shard", None),
        P(("shard", "rep"), None),
    )
    line = mesh.shape["shard"] // 2 if (mesh.shape["shard"], mesh.shape["rep"]) == (8, 4) else 0
    return jax.shard_map(
        functools.partial(shards, line),
        mesh=mesh,
        in_specs=placed,
        out_specs=(
            P(("shard", "rep"), None),
            P(("shard", "rep"), None),
            P("shard"),
            P("shard", None),
            P(None, "shard"),
            P("shard", None),
            P("shard"),
            P("shard", None),
            P("shard", None),
        ),
        check_vma=False,
    )
```

```python
import functools

import jax
import jax.numpy as jnp
from jax import lax
from jax.experimental import pallas as pl
from jax.experimental.pallas import tpu as pltpu
from jax.sharding import PartitionSpec as P

HEADS = 16
HEAD_DIM = 64


norm_eps = 1e-06
rope_base = 10000.0
masked_score = -1000000000.0

MESH = pl.DeviceIdType.MESH
ANY = pl.BlockSpec(memory_space=pl.ANY)


class Net:
    def __init__(self, line):
        shard, rep = lax.axis_index("shard"), lax.axis_index("rep")
        self.line = line
        self.z, self.y = shard // 2, shard % 2
        self.x, self.core = rep // 2, rep % 2
        self.own = shard
        self.sibling = (shard, self.x * 2 + 1 - self.core)
        self.across_x = (shard, (1 - self.x) * 2 + self.core)
        self.across_y = (self.z * 2 + 1 - self.y, rep)
        self.above = (jnp.minimum(self.z + 1, line - 1) * 2 + self.y, rep)
        self.below = (jnp.maximum(self.z - 1, 0) * 2 + self.y, rep)
        self.has_above = self.z < line - 1
        self.has_below = self.z > 0

    def greet(self):
        barrier = pltpu.get_barrier_semaphore()

        def hail(partner):
            pl.semaphore_signal(barrier, inc=1, device_id=partner, device_id_type=MESH)

        for partner in (self.sibling, self.across_x, self.across_y):
            hail(partner)
        pl.when(self.has_above)(lambda: hail(self.above))
        pl.when(self.has_below)(lambda: hail(self.below))
        neighbours = jnp.where(self.has_above, 1, 0) + jnp.where(self.has_below, 1, 0)
        pl.semaphore_wait(barrier, 3 + neighbours)


def aligned(value, step):
    return pl.multiple_of(value, step)


def gather_count(line):
    return 2 * line + 3 * 2 * line


def gather_steps(net, source, full, local_sem, send_sem, recv_sem):
    line = net.line
    height, columns = source.shape
    half = height // 2
    split = columns % 1024 == 0
    only = columns * 3 // 8 if split else 0
    shared = columns - 2 * only
    rows = pl.ds(aligned(net.core * half, half), half)
    carried = pl.ds(aligned(net.x * only, 128), only + shared) if split else pl.ds(0, columns)
    lone = pl.ds(aligned(net.x * (only + shared), 128), only) if split else None

    def remote(origin, landing, index, target):
        return pltpu.make_async_remote_copy(
            src_ref=origin,
            dst_ref=landing,
            send_sem=send_sem.at[index],
            recv_sem=recv_sem.at[index],
            device_id=target,
            device_id_type=MESH,
        )

    def held(z, y, which=None):
        lines = pl.ds(aligned((z * 2 + y) * height + net.core * half, half), half)
        return full.at[lines] if which is None else full.at[lines, which]

    def piece(z, y):
        return held(z, y, carried)

    def over_z(z, target, base):
        return remote(piece(z, net.y), piece(z, net.y), base + z, target)

    def over_y(z):
        return remote(piece(z, net.y), piece(z, net.y), 2 * line + z, net.across_y)

    def over_x(z, y):
        part = held(z, y, lone)
        return remote(part, part, 3 * line + y * line + z, net.across_x)

    def to_core(z, y):
        part = held(z, y)
        return remote(part, part, 5 * line + y * line + z, net.sibling)

    mine = source.at[rows, carried]
    local = pltpu.make_async_copy(source, full.at[pl.ds(aligned(net.own * height, height), height)], local_sem)
    first_y = remote(mine, piece(net.z, net.y), 2 * line + net.z, net.across_y)
    first_up = remote(mine, piece(net.z, net.y), net.z, net.above)
    first_down = remote(mine, piece(net.z, net.y), line + net.z, net.below)

    def onward(z, y):
        if split:
            over_x(z, y).start()
        else:
            to_core(z, y).start()

    def start():
        first_y.start()
        pl.when(net.has_above)(first_up.start)
        pl.when(net.has_below)(first_down.start)
        local.start()

    def arrive(hops):
        @pl.when(net.z >= hops)
        def _():
            z = net.z - hops
            over_z(z, net.above, 0).wait_recv()
            pl.when(net.has_above)(over_z(z, net.above, 0).start)
            over_y(z).start()
            onward(z, net.y)

        @pl.when(net.z < line - hops)
        def _():
            z = net.z + hops
            over_z(z, net.below, line).wait_recv()
            pl.when(net.has_below)(over_z(z, net.below, line).start)
            over_y(z).start()
            onward(z, net.y)

    def arrive_y(hops):
        def one(z):
            remote(piece(z, 1 - net.y), piece(z, 1 - net.y), 2 * line + z, net.across_y).wait_recv()
            onward(z, 1 - net.y)

        if hops == 0:
            one(net.z)
        else:
            pl.when(net.z >= hops)(lambda: one(net.z - hops))
            pl.when(net.z < line - hops)(lambda: one(net.z + hops))

    def arrive_x(hops, own_y):
        def one(z):
            y = net.y if own_y else 1 - net.y
            part = held(z, y, pl.ds(aligned((1 - net.x) * (only + shared), 128), only))
            remote(part, part, 3 * line + y * line + z, net.across_x).wait_recv()
            to_core(z, y).start()

        if not split:
            return
        if hops == 0:
            one(net.z)
        else:
            pl.when(net.z >= hops)(lambda: one(net.z - hops))
            pl.when(net.z < line - hops)(lambda: one(net.z + hops))

    def step(hops):
        def run():
            arrive_y(hops - 1)
            if hops < line:
                arrive(hops)
            if hops >= 2:
                arrive_x(hops - 2, False)
                arrive_x(hops - 1, True)

        return run

    def last():
        arrive_x(line - 1, False)

    def finish():
        local.wait()
        first_y.wait_send()

        @pl.when(net.has_above)
        def _():
            first_up.wait_send()
            for hops in range(1, line - 1):
                pl.when(net.z >= hops)(over_z(net.z - hops, net.above, 0).wait_send)

        @pl.when(net.has_below)
        def _():
            first_down.wait_send()
            for hops in range(1, line - 1):
                pl.when(net.z < line - hops)(over_z(net.z + hops, net.below, line).wait_send)

        for z in range(line):

            def others():
                over_y(z).wait_send()
                if split:
                    over_x(z, net.y).wait_send()
                to_core(z, net.y).wait()

            pl.when(net.z != z)(others)
            if split:
                over_x(z, 1 - net.y).wait_send()
            to_core(z, 1 - net.y).wait()

    return [start] + [step(hops) for hops in range(1, line + 1)] + [last, finish]


REDUCE_BUFFERS = 9


def reduce_split(columns):
    only = columns // 4 if columns % 512 == 0 else 0
    return only, columns - 2 * only


def reduce_scratch(line, shards, half, columns, dtype):
    only, shared = reduce_split(columns)
    carried = only + shared
    return [
        pltpu.VMEM((shards, half, columns), dtype),
        pltpu.VMEM((shards, half, columns), dtype),
        pltpu.VMEM((shards, half, max(only, 128)), dtype),
        pltpu.VMEM((line, half, carried), dtype),
        pltpu.VMEM((line + 1, half, carried), dtype),
        pltpu.VMEM((half, carried), dtype),
        pltpu.VMEM((half, columns), dtype),
        pltpu.VMEM((half, columns), dtype),
        pltpu.VMEM((2 * half, columns), jnp.float32),
    ]


def reduce_count(line):
    return 3 * line + 4


def reduce_steps(net, grad, out, column_start, out_start, buffers, local_sem, send_sem, recv_sem):
    kept, got, from_x, from_y, from_z, late_x, final, swapped, wide = buffers
    line = net.line
    shards, half, width = kept.shape
    only, shared = reduce_split(width)
    both = only + shared
    columns = pl.ds(column_start, width)
    mine = pl.ds(aligned(net.core * half, half), half)
    theirs = pl.ds(aligned((1 - net.core) * half, half), half)
    if only:
        carried = pl.ds(aligned(net.x * only, 128), both)
        lone = pl.ds(aligned(net.x * both, 128), only)
        their_lone = pl.ds(aligned((1 - net.x) * both, 128), only)
    else:
        carried = pl.ds(0, width)

    def remote(origin, landing, index, target):
        return pltpu.make_async_remote_copy(
            src_ref=origin,
            dst_ref=landing,
            send_sem=send_sem.at[index],
            recv_sem=recv_sem.at[index],
            device_id=target,
            device_id_type=MESH,
        )

    local = pltpu.make_async_copy(grad.at[:, mine, columns], kept, local_sem.at[0])
    halves = remote(grad.at[:, theirs, columns], got, 2 * line, net.sibling)
    written = pltpu.make_async_copy(wide, out.at[:, pl.ds(out_start, width)], local_sem.at[1])
    to_core = remote(final, swapped, 2 * line + 1, net.sibling)
    end_x = remote(kept.at[net.own, :, carried], late_x, 2 * line + 2, net.across_x)
    if only:
        over_x = remote(kept.at[:, :, their_lone], from_x, 2 * line + 3, net.across_x)

    def over_y(z):
        part = kept.at[z * 2 + 1 - net.y, :, carried]
        return remote(part, from_y.at[z], 2 * line + 4 + z, net.across_y)

    def up(z):
        return remote(kept.at[z * 2 + net.y, :, carried], from_z.at[z + 1], z, net.above)

    def down(z):
        return remote(kept.at[z * 2 + net.y, :, carried], from_z.at[z], line + z, net.below)

    def add(shard, part):
        kept[shard, :, carried] = kept[shard, :, carried] + part

    def first():
        halves.start()
        local.start()

    def second():
        local.wait()
        halves.wait_recv()

        @pl.loop(0, shards)
        def _(shard):
            kept[shard] = kept[shard] + got[shard]

        if only:
            over_x.start()

    def third():
        if only:
            over_x.wait_recv()

            @pl.loop(0, shards)
            def _(shard):
                kept[shard, :, lone] = kept[shard, :, lone] + from_x[shard]

        for z in range(line):
            over_y(z).start()

    def fourth():
        for z in range(line):
            over_y(z).wait_recv()

        @pl.loop(0, line)
        def _(z):
            add(z * 2 + net.y, from_y[z])

    def hop(step):
        def run():
            @pl.when(net.z == step)
            def _():
                for z in range(line - 1, step, -1):
                    if step > 0:
                        up(z).wait_recv()
                        add(z * 2 + net.y, from_z[z + 1])
                    up(z).start()

            @pl.when(net.z == line - 1 - step)
            def _():
                for z in range(line - 1 - step):
                    if step > 0:
                        down(z).wait_recv()
                        add(z * 2 + net.y, from_z[z])
                    down(z).start()

        return run

    def land():
        @pl.when(net.has_below)
        def _():
            up(net.z).wait_recv()
            add(net.own, from_z[net.z + 1])

        @pl.when(net.has_above)
        def _():
            down(net.z).wait_recv()
            add(net.own, from_z[net.z])

        end_x.start()

    def meet():
        end_x.wait_recv()
        if only:
            final[:, lone] = kept[net.own, :, lone]
            for x in range(2):

                @pl.when(net.x == x)
                def _():
                    start = 0 if x == 1 else shared
                    final[:, (1 - x) * both : (1 - x) * both + only] = late_x[:, start : start + only]
                    other = shared * 0 + (only if x == 1 else 0)
                    final[:, only:both] = kept[net.own, :, only:both] + late_x[:, other : other + shared]
        else:
            final[...] = kept[net.own] + late_x[...]
        to_core.start()
        wide[mine, :] = final[...].astype(jnp.float32)

    def swap():
        to_core.wait_recv()
        wide[theirs, :] = swapped[...].astype(jnp.float32)
        written.start()

    def finish():
        written.wait()
        halves.wait_send()
        if only:
            over_x.wait_send()
        for z in range(line):
            over_y(z).wait_send()
            pl.when(net.z < z)(up(z).wait_send)
            pl.when(net.z > z)(down(z).wait_send)
        end_x.wait_send()
        to_core.wait_send()

    hops = [hop(step) for step in range(line - 1)]

    def fourth_and_hop():
        fourth()
        hops[0]()

    return [first, second, third, fourth_and_hop] + hops[1:] + [land, meet, swap, finish]


ROWS_BY_ROWS = (((0,), (0,)), ((), ()))
COLUMNS_BY_COLUMNS = (((1,), (1,)), ((), ()))


def product(first_op, second_op, dims=(((1,), (0,)), ((), ()))):
    return lax.dot_general(first_op, second_op, dims, preferred_element_type=jnp.float32)


def inverse_rms(values):
    return lax.rsqrt(jnp.mean(values * values, axis=1, keepdims=True) + norm_eps)


def run(body, *, grid, out_shape, in_specs, out_specs, scratch_shapes, name, operands):
    return pl.pallas_call(
        body,
        grid=(grid,),
        out_shape=out_shape,
        in_specs=in_specs,
        out_specs=out_specs,
        scratch_shapes=scratch_shapes,
        compiler_params=pltpu.CompilerParams(vmem_limit_bytes=60 << 20),
        name=name,
    )(*operands)


def whole(*shape):
    return pl.BlockSpec(shape, lambda step: (0,) * len(shape), pipeline_mode=pl.Buffered(1))


def like(shape, dtype):
    return jax.ShapeDtypeStruct(shape, dtype)


def project_kernel(turned, x_ref, gain_ref, w_ref, cos_ref, sin_ref, out_ref, normed_ref):
    step = pl.program_id(0)

    @pl.when(step == 0)
    def _():
        values = x_ref[...].astype(jnp.float32)
        normed = values * inverse_rms(values) * gain_ref[...]
        normed_ref[...] = normed.T.astype(jnp.bfloat16)

    out = product(w_ref[...], normed_ref[...], ROWS_BY_ROWS)

    @pl.when(step < turned)
    def _():
        cos, sin = cos_ref[...], sin_ref[...]
        half = cos.shape[0]
        for start in range(0, out.shape[0], 2 * half):
            first, second = out[start : start + half], out[start + half : start + 2 * half]
            out_ref[start : start + half, :] = (first * cos - second * sin).astype(jnp.bfloat16)
            out_ref[start + half : start + 2 * half, :] = (second * cos + first * sin).astype(jnp.bfloat16)

    @pl.when(step >= turned)
    def _():
        out_ref[...] = out.astype(jnp.bfloat16)


def project(x, gain, weight, cos_t, sin_t):
    rows, width = x.shape
    columns = weight.shape[1]
    block = 512
    return run(
        functools.partial(project_kernel, 2 * width // block),
        grid=columns // block,
        out_shape=[like((columns, rows), jnp.bfloat16), like((width, rows), jnp.bfloat16)],
        in_specs=[
            whole(rows, width),
            whole(1, width),
            pl.BlockSpec((width, block), lambda step: (0, step)),
            whole(*cos_t.shape),
            whole(*sin_t.shape),
        ],
        out_specs=[
            pl.BlockSpec((block, rows), lambda step: (step, 0)),
            pl.BlockSpec((width, rows), lambda step: (0, 0)),
        ],
        scratch_shapes=[],
        name="project",
        operands=[x, gain, weight, cos_t, sin_t],
    )


def branch_kernel(att_ref, w_ref, x_ref, gain_ref, hidden_ref, normed_ref):
    hidden = x_ref[...].astype(jnp.float32) + product(att_ref[...], w_ref[...], ROWS_BY_ROWS)
    hidden_ref[...] = hidden
    normed_ref[...] = (hidden * inverse_rms(hidden) * gain_ref[...]).astype(jnp.bfloat16)


def branch(attended_t, weight, x, gain):
    rows, width = x.shape
    block = 256
    row = pl.BlockSpec((block, width), lambda step: (step, 0))
    return run(
        branch_kernel,
        grid=rows // block,
        out_shape=[like((rows, width), jnp.float32), like((rows, width), jnp.bfloat16)],
        in_specs=[
            pl.BlockSpec((width, block), lambda step: (0, step)),
            whole(*weight.shape),
            row,
            whole(1, width),
        ],
        out_specs=[row, row],
        scratch_shapes=[],
        name="branch",
        operands=[attended_t, weight, x, gain],
    )


def widen_kernel(normed_ref, gate_ref, up_ref, act_ref, to_gate_ref, to_up_ref):
    normed = normed_ref[...]
    gate = product(normed, gate_ref[...])
    up = product(normed, up_ref[...])
    sigmoid = jax.nn.sigmoid(gate)
    swish = gate * sigmoid
    act_ref[...] = (swish * up).astype(jnp.bfloat16)
    to_gate_ref[...] = (up * sigmoid * (1.0 + gate * (1.0 - sigmoid))).astype(jnp.bfloat16)
    to_up_ref[...] = swish.astype(jnp.bfloat16)


def widen(normed, weight):
    rows, width = normed.shape
    inner = weight.shape[1] // 2
    block = 512
    steps = inner // block
    part = pl.BlockSpec((rows, block), lambda step: (0, step))
    return run(
        widen_kernel,
        grid=steps,
        out_shape=[like((rows, inner), jnp.bfloat16)] * 3,
        in_specs=[
            whole(rows, width),
            pl.BlockSpec((width, block), lambda step: (0, step)),
            pl.BlockSpec((width, block), lambda step: (0, steps + step)),
        ],
        out_specs=[part] * 3,
        scratch_shapes=[],
        name="widen",
        operands=[normed, weight, weight],
    )


def narrow_kernel(
    steps, act_ref, to_gate_ref, to_up_ref, w_ref, given_ref, hidden_ref, result_ref, grad_ref, d_gate_ref, d_up_ref, acc_ref
):
    step = pl.program_id(0)
    act, weight, given = act_ref[...], w_ref[...], given_ref[...]
    part = product(act, weight)

    @pl.when(step == 0)
    def _():
        acc_ref[...] = hidden_ref[...] + part

    @pl.when(step > 0)
    def _():
        acc_ref[...] += part

    @pl.when(step == steps - 1)
    def _():
        result_ref[...] = acc_ref[...].astype(jnp.bfloat16)

    grad_ref[...] = product(act, given, ROWS_BY_ROWS).astype(jnp.bfloat16)
    d_act = product(given, weight, COLUMNS_BY_COLUMNS)
    d_gate_ref[...] = (d_act * to_gate_ref[...].astype(jnp.float32)).astype(jnp.bfloat16)
    d_up_ref[...] = (d_act * to_up_ref[...].astype(jnp.float32)).astype(jnp.bfloat16)


def narrow(act, to_gate, to_up, weight, given, hidden):
    rows, inner = act.shape
    width = weight.shape[1]
    block = 512
    steps = inner // block
    part = pl.BlockSpec((rows, block), lambda step: (0, step))
    down = pl.BlockSpec((block, width), lambda step: (step, 0))
    return run(
        functools.partial(narrow_kernel, steps),
        grid=steps,
        out_shape=[
            like((rows, width), jnp.bfloat16),
            like((inner, width), jnp.bfloat16),
            like((rows, inner), jnp.bfloat16),
            like((rows, inner), jnp.bfloat16),
        ],
        in_specs=[part, part, part, down, whole(rows, width), whole(rows, width)],
        out_specs=[pl.BlockSpec((rows, width), lambda step: (0, 0)), down, part, part],
        scratch_shapes=[pltpu.VMEM((rows, width), jnp.float32)],
        name="narrow",
        operands=[act, to_gate, to_up, weight, given, hidden],
    )


def grad_in_kernel(normed_ref, d_gate_ref, d_up_ref, to_gate_ref, to_up_ref, turned_ref):
    @pl.when(pl.program_id(0) == 0)
    def _():
        turned_ref[...] = normed_ref[...].T

    to_gate_ref[...] = product(turned_ref[...], d_gate_ref[...]).astype(jnp.bfloat16)
    to_up_ref[...] = product(turned_ref[...], d_up_ref[...]).astype(jnp.bfloat16)


def grad_into(normed, d_gate, d_up):
    rows, width = normed.shape
    inner = d_gate.shape[1]
    block = 512
    part = pl.BlockSpec((rows, block), lambda step: (0, step))
    out = pl.BlockSpec((width, block), lambda step: (0, step))
    return run(
        grad_in_kernel,
        grid=inner // block,
        out_shape=[like((width, inner), jnp.bfloat16)] * 2,
        in_specs=[whole(rows, width), part, part],
        out_specs=[out, out],
        scratch_shapes=[pltpu.VMEM((width, rows), jnp.bfloat16)],
        name="grad_in",
        operands=[normed, d_gate, d_up],
    )


def norm_back(d_normed, values, gain):
    inverse = inverse_rms(values)
    unit = values * inverse
    scaled = d_normed * gain
    mean = jnp.mean(scaled * unit, axis=1, keepdims=True)
    return inverse * (scaled - unit * mean), jnp.sum(d_normed * unit, axis=0, keepdims=True)


def ffn_back_kernel(
    steps, d_gate_ref, d_up_ref, gate_ref, up_ref, hidden_ref, gain_ref, given_ref, d_hidden_ref, d_branch_ref, grad_gain_ref, acc_ref
):
    step = pl.program_id(0)
    part = product(d_gate_ref[...], gate_ref[...], COLUMNS_BY_COLUMNS)
    part = part + product(d_up_ref[...], up_ref[...], COLUMNS_BY_COLUMNS)

    @pl.when(step == 0)
    def _():
        acc_ref[...] = part

    @pl.when(step > 0)
    def _():
        acc_ref[...] += part

    @pl.when(step == steps - 1)
    def _():
        through, grad_gain = norm_back(acc_ref[...], hidden_ref[...], gain_ref[...])
        d_hidden = given_ref[...].astype(jnp.float32) + through
        d_hidden_ref[...] = d_hidden
        d_branch_ref[...] = d_hidden.astype(jnp.bfloat16)
        grad_gain_ref[...] = grad_gain


def ffn_back(d_gate, d_up, weight, hidden, gain, given):
    rows, width = hidden.shape
    inner = d_gate.shape[1]
    block = 512
    steps = inner // block
    part = pl.BlockSpec((rows, block), lambda step: (0, step))
    full = pl.BlockSpec((rows, width), lambda step: (0, 0))
    return run(
        functools.partial(ffn_back_kernel, steps),
        grid=steps,
        out_shape=[
            like((rows, width), jnp.float32),
            like((rows, width), jnp.bfloat16),
            like((1, width), jnp.float32),
        ],
        in_specs=[
            part,
            part,
            pl.BlockSpec((width, block), lambda step: (0, step)),
            pl.BlockSpec((width, block), lambda step: (0, steps + step)),
            whole(rows, width),
            whole(1, width),
            whole(rows, width),
        ],
        out_specs=[full, full, pl.BlockSpec((1, width), lambda step: (0, 0))],
        scratch_shapes=[pltpu.VMEM((rows, width), jnp.float32)],
        name="ffn_back",
        operands=[d_gate, d_up, weight, weight, hidden, gain, given],
    )


def branch_back_kernel(att_ref, w_ref, d_branch_ref, grad_ref, given_ref):
    d_branch = d_branch_ref[...]
    grad_ref[...] = product(att_ref[...], d_branch).astype(jnp.bfloat16)
    given_ref[...] = product(w_ref[...], d_branch, COLUMNS_BY_COLUMNS).astype(jnp.bfloat16)


def branch_back(attended_t, weight, d_branch):
    rows, width = d_branch.shape
    block = 256
    out = pl.BlockSpec((block, width), lambda step: (step, 0))
    turned = pl.BlockSpec((block, rows), lambda step: (step, 0))
    return run(
        branch_back_kernel,
        grid=attended_t.shape[0] // block,
        out_shape=[like(weight.shape, jnp.bfloat16), like(attended_t.shape, jnp.bfloat16)],
        in_specs=[turned, out, whole(rows, width)],
        out_specs=[out, turned],
        scratch_shapes=[],
        name="branch_back",
        operands=[attended_t, weight, d_branch],
    )


def project_back_kernel(
    steps, normed_ref, dq_ref, dk_ref, dv_ref, w_ref, x_ref, gain_ref, d_hidden_ref, grad_ref, tokens_ref, grad_gain_ref, acc_ref
):
    step = pl.program_id(0)
    third = steps // 3

    def run(d_ref):
        d_part = d_ref[...]
        grad_ref[...] = product(normed_ref[...], d_part, COLUMNS_BY_COLUMNS).astype(jnp.bfloat16)
        part = product(w_ref[...], d_part)

        @pl.when(step == 0)
        def _():
            acc_ref[...] = part

        @pl.when(step > 0)
        def _():
            acc_ref[...] += part

    for index, d_ref in enumerate((dq_ref, dk_ref, dv_ref)):
        pl.when(step // third == index)(functools.partial(run, d_ref))

    @pl.when(step == steps - 1)
    def _():
        values = x_ref[...].astype(jnp.float32)
        through, grad_gain = norm_back(acc_ref[...].T, values, gain_ref[...])
        tokens_ref[...] = d_hidden_ref[...] + through
        grad_gain_ref[...] = grad_gain


def project_back(normed_t, dq, dk, dv, weight, x, gain, d_hidden):
    rows, width = x.shape
    columns = weight.shape[1]
    block = 512
    steps = columns // block
    third = steps // 3
    full = pl.BlockSpec((rows, width), lambda step: (0, 0))

    def part(which):
        return pl.BlockSpec(
            (block, rows), lambda step: (jnp.clip(step - which * third, 0, third - 1), 0)
        )

    return run(
        functools.partial(project_back_kernel, steps),
        grid=steps,
        out_shape=[
            like((width, columns), jnp.bfloat16),
            like((rows, width), jnp.float32),
            like((1, width), jnp.float32),
        ],
        in_specs=[
            whole(*normed_t.shape),
            part(0),
            part(1),
            part(2),
            pl.BlockSpec((width, block), lambda step: (0, step)),
            whole(rows, width),
            whole(1, width),
            whole(rows, width),
        ],
        out_specs=[
            pl.BlockSpec((width, block), lambda step: (0, step)),
            full,
            pl.BlockSpec((1, width), lambda step: (0, 0)),
        ],
        scratch_shapes=[pltpu.VMEM((width, rows), jnp.float32)],
        name="project_back",
        operands=[normed_t, dq, dk, dv, weight, x, gain, d_hidden],
    )


LOG2E = 1.4426950408889634
FEATURES = 16


def two_parts(value):
    high = value.astype(jnp.bfloat16)
    return high, (value - high.astype(jnp.float32)).astype(jnp.bfloat16)


def three_parts(value):
    high, rest = value.astype(jnp.bfloat16), None
    rest = value - high.astype(jnp.float32)
    middle = rest.astype(jnp.bfloat16)
    return high, middle, (rest - middle.astype(jnp.float32)).astype(jnp.bfloat16)


def key_features(variates, valid):
    length = variates.shape[1]
    masks = [(variates == v).astype(jnp.float32) for v in range(4)]
    ones = jnp.ones((1, length), jnp.float32)
    invalid = 1.0 - valid
    rows = masks + masks + [invalid, ones, ones, ones, jnp.zeros((FEATURES - 12, length), jnp.float32)]
    return jnp.concatenate(rows, axis=0).astype(jnp.bfloat16)


def query_features(variates, same, other, log_sums):
    length = variates.shape[1]
    highs, lows = [], []
    for v in range(4):
        bias = jnp.where(variates == v, same, other) * LOG2E
        high, low = two_parts(bias)
        highs.append(high.astype(jnp.float32))
        lows.append(low.astype(jnp.float32))
    if log_sums is None:
        minus = [jnp.zeros((3, length), jnp.float32)]
    else:
        minus = [part.astype(jnp.float32) for part in three_parts(-log_sums)]
    mask = jnp.full((1, length), masked_score, jnp.float32)
    rows = highs + lows + [mask] + minus + [jnp.zeros((FEATURES - 12, length), jnp.float32)]
    return jnp.concatenate(rows, axis=0).astype(jnp.bfloat16)


def contract_depth(first_op, second_op):
    return lax.dot_general(
        first_op, second_op, (((1,), (0,)), ((), ())), preferred_element_type=jnp.float32
    )


def scaled_query(query_t, score_scale):
    return two_parts(query_t.astype(jnp.float32) * (score_scale * LOG2E))


def attend_kernel(blocks, bias_ref, *refs):
    head = pl.program_id(0)
    attend_head(blocks, bias_ref[0, head], bias_ref[1, head], *refs)


def attend_head(blocks, same, other, q_ref, k_ref, v_ref, var_ref, valid_ref, o_ref, wide_ref, lse_ref, query_ref):
    depth, length = q_ref.shape
    width = length // blocks
    variates = var_ref[...]
    high, low = scaled_query(q_ref[...], depth ** (-0.5))
    query_ref[...] = jnp.concatenate([high, low, query_features(variates, same, other, None)], axis=0)
    key_t = k_ref[...]
    keys = jnp.concatenate([key_t, key_t, key_features(variates, valid_ref[...])], axis=0).T
    ones = jnp.concatenate(
        [jnp.ones((1, length), jnp.float32), jnp.zeros((FEATURES - 1, length), jnp.float32)], axis=0
    ).astype(jnp.bfloat16)
    values = jnp.concatenate([v_ref[...], ones], axis=0)
    for block in range(blocks):
        at = pl.ds(block * width, width)
        scores = contract_depth(keys, query_ref[:, at])
        peak = jnp.max(scores, axis=0, keepdims=True)
        weights = jnp.exp2(scores - peak).astype(jnp.bfloat16)
        summed = contract_depth(values, weights)
        total = summed[depth : depth + 1]
        attended = summed[:depth] / total
        wide_ref[:, at] = attended
        o_ref[:, at] = attended.astype(jnp.bfloat16)
        lse_ref[0, :, at] = peak + jnp.log2(total)


def attend_forward(qkv_t, variates, valid, bias, heads):
    rows, length = qkv_t.shape
    depth = rows // (3 * heads)

    def part(which):
        return pl.BlockSpec((depth, length), lambda head: (which * heads + head, 0))

    row = pl.BlockSpec((1, length), lambda head: (0, 0))
    return run(
        functools.partial(attend_kernel, 1),
        grid=heads,
        out_shape=[
            jax.ShapeDtypeStruct((heads * depth, length), jnp.bfloat16),
            jax.ShapeDtypeStruct((heads * depth, length), jnp.float32),
            jax.ShapeDtypeStruct((heads, 1, length), jnp.float32),
        ],
        in_specs=[
            pl.BlockSpec(memory_space=pltpu.SMEM),
            part(0),
            part(1),
            part(2),
            row,
            row,
        ],
        out_specs=[
            pl.BlockSpec((depth, length), lambda head: (head, 0)),
            pl.BlockSpec((depth, length), lambda head: (head, 0)),
            pl.BlockSpec((1, 1, length), lambda head: (head, 0, 0)),
        ],
        scratch_shapes=[pltpu.VMEM((2 * depth + FEATURES, length), jnp.bfloat16)],
        name="attend_forward",
        operands=[bias, qkv_t, qkv_t, qkv_t, variates, valid],
    )


def turn_back(grad_t, cos_t, sin_t):
    half = cos_t.shape[0]
    first, second = grad_t[:half], grad_t[half:]
    return jnp.concatenate(
        [first * cos_t + second * sin_t, second * cos_t - first * sin_t], axis=0
    )


def attend_back_head(
    blocks, same, other, q_ref, k_ref, v_ref, go_ref, wide_ref, lse_ref, var_ref, valid_ref, cos_ref, sin_ref,
    dq_ref, dk_ref, dv_ref, query_ref, given_ref, dk_acc, dv_acc,
):
    depth, length = q_ref.shape
    width = length // blocks
    scale = depth ** (-0.5)
    variates = var_ref[...]
    features = key_features(variates, valid_ref[...])
    high, low = scaled_query(q_ref[...], scale)
    query_ref[...] = jnp.concatenate([high, low, query_features(variates, same, other, lse_ref[0])], axis=0)
    key_t = k_ref[...]
    keys = jnp.concatenate([key_t, key_t, features], axis=0).T
    keys_low = jnp.concatenate([key_t, features], axis=0)
    given = go_ref[...]
    inner = jnp.sum(given.astype(jnp.float32) * wide_ref[...], axis=0, keepdims=True)
    minus = [part.astype(jnp.float32) for part in three_parts(-inner)]
    minus = jnp.concatenate(minus + [jnp.zeros((FEATURES - 3, length), jnp.float32)], axis=0)
    given_ref[...] = jnp.concatenate([given, minus.astype(jnp.bfloat16)], axis=0)
    ones = jnp.concatenate(
        [jnp.ones((3, length), jnp.float32), jnp.zeros((FEATURES - 3, length), jnp.float32)], axis=0
    ).astype(jnp.bfloat16)
    values = jnp.concatenate([v_ref[...], ones], axis=0).T
    query_rows = q_ref[...].T
    given_rows = given.T
    in_same = jnp.zeros((1, width), jnp.float32)
    in_other = jnp.zeros((1, width), jnp.float32)
    for block in range(blocks):
        at = pl.ds(block * width, width)
        cut = slice(block * width, (block + 1) * width)
        probs = jnp.exp2(contract_depth(keys, query_ref[:, at]))
        grads = (probs * contract_depth(values, given_ref[:, at])).astype(jnp.bfloat16)
        back = contract_depth(keys_low, grads)
        dq = turn_back(back[:depth] * scale, cos_ref[:, at], sin_ref[:, at])
        dq_ref[:, at] = dq.astype(jnp.bfloat16)
        for v in range(4):
            line = back[depth + v : depth + v + 1]
            hit = variates[:, cut] == v
            in_same = in_same + jnp.where(hit, line, 0.0)
            in_other = in_other + jnp.where(hit, 0.0, line)
        dk = contract_depth(grads, query_rows[cut])
        dv = contract_depth(probs.astype(jnp.bfloat16), given_rows[cut])
        if block == 0:
            dk_acc[...] = dk
            dv_acc[...] = dv
        else:
            dk_acc[...] += dk
            dv_acc[...] += dv
    dk_ref[...] = turn_back((dk_acc[...] * scale).T, cos_ref[...], sin_ref[...]).astype(jnp.bfloat16)
    dv_ref[...] = dv_acc[...].T.astype(jnp.bfloat16)
    return in_same, in_other


def attend_back_kernel(blocks, bias_ref, *refs):
    head = pl.program_id(0)
    *refs, db_ref, query_ref, given_ref, dk_acc, dv_acc = refs
    in_same, in_other = attend_back_head(
        blocks, bias_ref[0, head], bias_ref[1, head], *refs, query_ref, given_ref, dk_acc, dv_acc
    )
    db_ref[0, 0:1, :] = in_same
    db_ref[0, 1:2, :] = in_other


def attend_backward(qkv_t, given_t, wide_t, log_sums, variates, valid, bias, cos_t, sin_t, heads):
    rows, length = qkv_t.shape
    depth = rows // (3 * heads)
    blocks = 1

    def part(which):
        return pl.BlockSpec((depth, length), lambda head: (which * heads + head, 0))

    one = pl.BlockSpec((depth, length), lambda head: (head, 0))
    grad = jax.ShapeDtypeStruct((heads * depth, length), jnp.bfloat16)
    return run(
        functools.partial(attend_back_kernel, blocks),
        grid=heads,
        out_shape=[grad, grad, grad, jax.ShapeDtypeStruct((heads, 2, length // blocks), jnp.float32)],
        in_specs=[
            pl.BlockSpec(memory_space=pltpu.SMEM),
            part(0),
            part(1),
            part(2),
            one,
            one,
            pl.BlockSpec((1, 1, length), lambda head: (head, 0, 0)),
            whole(1, length),
            whole(1, length),
            whole(depth // 2, length),
            whole(depth // 2, length),
        ],
        out_specs=[one, one, one, pl.BlockSpec((1, 2, length // blocks), lambda head: (head, 0, 0))],
        scratch_shapes=[
            pltpu.VMEM((2 * depth + FEATURES, length), jnp.bfloat16),
            pltpu.VMEM((depth + FEATURES, length), jnp.bfloat16),
            pltpu.VMEM((length, depth), jnp.float32),
            pltpu.VMEM((length, depth), jnp.float32),
        ],
        name="attend_backward",
        operands=[bias, qkv_t, qkv_t, qkv_t, given_t, wide_t, log_sums, variates, valid, cos_t, sin_t],
    )


PRELUDE = 7
FRONT_PLACES = (
    (0, 1, 2, 3, 4, 5, 6),
    (1, 3, 4, 5, 7, 8, 9),
    (3, 6, 8, 10, 13, 16, 18),
    (8, 12, 15, 18, 21, 24, 28),
)


def bias_of(small_ref, head, per_shard):
    row = 16 * (head // per_shard) + 2
    return small_ref[row, head % per_shard], small_ref[row + 1, head % per_shard]


def gain_of(small_ref, shards, which):
    rows = [small_ref[16 * shard + which : 16 * shard + which + 1, :] for shard in range(shards)]
    return jnp.concatenate(rows, axis=1)


def front_kernel(line, shards, heads, *refs):
    step = pl.program_id(0)
    refs = list(refs)

    def take(count):
        out = refs[:count]
        del refs[:count]
        return out

    small, w_qkv, w_out, w_in, w_down, x_hbm = take(6)
    var_ref, valid_ref, cos_ref, sin_ref = take(4)
    small_all, qkv_all, out_all, into_0, down_0, into_1, down_1 = take(7)
    intos = take(4)
    qkv_hbm, normed_hbm, attended_hbm, hidden_hbm, normed_two_hbm = take(5)
    wide_ref, lse_ref = take(2)
    x, weight, normed_t, qkv, attended, hidden, normed_two, small_ref, query_ref, bias_ref, wide_rows, cut_rows = take(12)
    load_sem, cut_sem, local_sem, send_sem, recv_sem = refs
    net = Net(line)
    rows, width = x.shape
    block = 512
    projected = 3 * width // block
    attend = PRELUDE + projected
    last = attend + heads
    depth = width // heads

    def load(index, origin, landing):
        return pltpu.make_async_copy(origin, landing, load_sem.at[index])

    def at(place):
        return pl.when(step == place)

    inner = w_in.shape[1] // 2
    owned = inner // shards
    piece_width = BLOCK // shards

    w_in_load = pltpu.make_async_copy(w_in, wide_rows, cut_sem.at[4])

    def cut_store(number):
        return pltpu.make_async_copy(cut_rows.at[number], intos[number], cut_sem.at[number])

    def down_part(number):
        return w_down.at[pl.ds(number * piece_width, piece_width)]

    tensors = (
        ((small, small_all), (w_qkv, qkv_all)),
        ((w_out, out_all),),
        ((intos[0], into_0), (down_part(0), down_0)),
        ((intos[1], into_1), (down_part(1), down_1)),
    )
    number = 0
    groups = []
    for group in tensors:
        lists = []
        for source, full in group:
            lists.append(
                gather_steps(
                    net, source, full, local_sem.at[number], send_sem.at[number], recv_sem.at[number]
                )
            )
            number += 1
        groups.append(lists)

    x_load = load(0, x_hbm, x)
    small_load = load(1, small_all, small_ref)
    weight_load = load(2, qkv_all, weight)
    bias_load = load(9, small_all, bias_ref)
    normed_store = load(3, normed_t, normed_hbm)
    qkv_store = load(4, qkv, qkv_hbm)
    attended_store = load(5, attended, attended_hbm)
    out_load = load(6, out_all, weight.at[:, pl.ds(0, width)])
    hidden_store = load(7, hidden, hidden_hbm)
    normed_two_store = load(8, normed_two, normed_two_hbm)

    @at(0)
    def _():
        net.greet()
        x_load.start()
        w_in_load.start()

    for lists, places in zip(groups, FRONT_PLACES):
        for index, place in enumerate(places):

            @at(place)
            def _():
                if place == FRONT_PLACES[2][0] and lists is groups[2]:
                    cut_store(0).wait()
                if place == FRONT_PLACES[3][0] and lists is groups[3]:
                    cut_store(1).wait()
                for steps in lists:
                    steps[index]()

    @at(0)
    def _():
        w_in_load.wait()
        for index in range(4):
            for piece in range(2 * shards):
                start = piece * owned + index * piece_width
                cut_rows[index, :, piece * piece_width : (piece + 1) * piece_width] = wide_rows[
                    :, start : start + piece_width
                ]
            cut_store(index).start()

    @at(PRELUDE - 1)
    def _():
        cut_store(2).wait()
        cut_store(3).wait()
        weight_load.start()
        small_load.start()
        bias_load.start()
        x_load.wait()
        small_load.wait()
        bias_load.wait()
        gain = gain_of(small_ref, shards, 0)
        values = x[...].astype(jnp.float32)
        normed = values * inverse_rms(values) * gain
        normed_t[...] = normed.T.astype(jnp.bfloat16)
        normed_store.start()
        weight_load.wait()

    @pl.when((step >= PRELUDE) & (step < attend))
    def _():
        index = step - PRELUDE
        columns = pl.ds(aligned(index * block, block), block)
        out = product(weight[:, columns], normed_t[...], ROWS_BY_ROWS)
        lines = qkv.at[columns]

        @pl.when(index < 2 * width // block)
        def _():
            cos, sin = cos_ref[...], sin_ref[...]
            half = depth // 2
            for start in range(0, block, depth):
                first, second = out[start : start + half], out[start + half : start + depth]
                lines[start : start + half, :] = (first * cos - second * sin).astype(jnp.bfloat16)
                lines[start + half : start + depth, :] = (second * cos + first * sin).astype(jnp.bfloat16)

        @pl.when(index >= 2 * width // block)
        def _():
            lines[...] = out.astype(jnp.bfloat16)

    @at(attend)
    def _():
        qkv_store.start()

    @pl.when((step >= attend) & (step < last))
    def _():
        head = step - attend

        def part(which):
            return qkv.at[pl.ds(aligned(which * width + head * depth, depth), depth)]

        same, other = bias_of(bias_ref, head, heads // shards)
        attend_head(
            1,
            same,
            other,
            part(0),
            part(1),
            part(2),
            var_ref,
            valid_ref,
            attended.at[pl.ds(aligned(head * depth, depth), depth)],
            wide_ref,
            lse_ref,
            query_ref,
        )

    @at(last - 1)
    def _():
        out_load.start()
        attended_store.start()

    @at(last)
    def _():
        out_load.wait()
        gain = gain_of(small_ref, shards, 1)
        part = 256
        for index in range(rows // part):
            lines = slice(index * part, (index + 1) * part)
            sums = product(attended[:, lines], weight[:, :width], ROWS_BY_ROWS)
            values = x[lines, :].astype(jnp.float32) + sums
            hidden[lines, :] = values
            normed_two[lines, :] = (values * inverse_rms(values) * gain).astype(jnp.bfloat16)
        hidden_store.start()
        normed_two_store.start()
        for store in (normed_store, qkv_store, attended_store, hidden_store, normed_two_store):
            store.wait()


def front(line, small, w_qkv, w_out, w_in, w_down, x, variates, valid, cos_t, sin_t, heads):
    shards = lax.axis_size("shard")
    rows, width = x.shape
    depth = width // heads
    low = jnp.bfloat16
    piece = BLOCK // shards
    grid = PRELUDE + 3 * width // 512 + heads + 1
    copies = gather_count(line)

    def head_at(step):
        return jnp.clip(step - (PRELUDE + 3 * width // 512), 0, heads - 1)

    def gathered(rows, columns, dtype=low):
        return like((shards * rows, columns), dtype)

    owned = w_qkv.shape[0]
    return pl.pallas_call(
        functools.partial(front_kernel, line, shards, heads),
        grid=(grid,),
        out_shape=[
            gathered(16, 128, jnp.float32),
            gathered(*w_qkv.shape),
            gathered(*w_out.shape),
            gathered(owned, 2 * BLOCK),
            gathered(piece, width),
            gathered(owned, 2 * BLOCK),
            gathered(piece, width),
        ]
        + [like((owned, 2 * BLOCK), low)] * 4
        + [
            like((3 * width, rows), low),
            like((width, rows), low),
            like((width, rows), low),
            like((rows, width), jnp.float32),
            like((rows, width), low),
            like((width, rows), jnp.float32),
            like((heads, 1, rows), jnp.float32),
        ],
        in_specs=[ANY] * 6
        + [
            whole(1, rows),
            whole(1, rows),
            whole(*cos_t.shape),
            whole(*sin_t.shape),
        ],
        out_specs=[ANY] * 16
        + [
            pl.BlockSpec((depth, rows), lambda step: (head_at(step), 0)),
            pl.BlockSpec((1, 1, rows), lambda step: (head_at(step), 0, 0)),
        ],
        scratch_shapes=[
            pltpu.VMEM((rows, width), low),
            pltpu.VMEM((width, 3 * width), low),
            pltpu.VMEM((width, rows), low),
            pltpu.VMEM((3 * width, rows), low),
            pltpu.VMEM((width, rows), low),
            pltpu.VMEM((rows, width), jnp.float32),
            pltpu.VMEM((rows, width), low),
            pltpu.VMEM((16 * shards, 128), jnp.float32),
            pltpu.VMEM((2 * depth + FEATURES, rows), low),
            pltpu.SMEM((16 * shards, 128), jnp.float32),
            pltpu.VMEM(w_in.shape, low),
            pltpu.VMEM((4, owned, 2 * BLOCK), low),
            pltpu.SemaphoreType.DMA((10,)),
            pltpu.SemaphoreType.DMA((5,)),
            pltpu.SemaphoreType.DMA((7,)),
            pltpu.SemaphoreType.DMA((7, copies)),
            pltpu.SemaphoreType.DMA((7, copies)),
        ],
        compiler_params=pltpu.CompilerParams(
            collective_id=1, has_side_effects=True, vmem_limit_bytes=62 << 20
        ),
        name="front",
    )(small, w_qkv, w_out, w_in, w_down, x, variates, valid, cos_t, sin_t)


TILE = 512
BLOCK = 1024
KEPT, GIVEN, GOT, OVER_X, OVER_Y, OVER_Z, LATE, ENDS, WIDE = 13, 3, 4, 5, 5, 6, 4, 4, 3
STAGES = (0, 1, 3, 5, 7, 8, 9, 10, 11, 12)
SUBSTEPS = 6


def stream_scratch(line, shards, half):
    only, shared = reduce_split(TILE)
    both = only + shared
    low = jnp.bfloat16
    copies = 7
    return [
        pltpu.VMEM((KEPT, shards, half, TILE), low),
        pltpu.VMEM((GIVEN, shards, half, TILE), low),
        pltpu.VMEM((GOT, shards, half, TILE), low),
        pltpu.VMEM((OVER_X, shards, half, only), low),
        pltpu.VMEM((OVER_Y, line, half, both), low),
        pltpu.VMEM((OVER_Z, line + 1, half, both), low),
        pltpu.VMEM((LATE, half, both), low),
        pltpu.VMEM((ENDS, half, TILE), low),
        pltpu.VMEM((ENDS, half, TILE), low),
        pltpu.VMEM((WIDE, 2 * half, TILE), jnp.float32),
        pltpu.SemaphoreType.DMA((KEPT, 4)),
        pltpu.SemaphoreType.DMA((KEPT, copies)),
        pltpu.SemaphoreType.DMA((KEPT, copies)),
    ]


class Stream:
    def __init__(self, net, scratch, writes):
        self.net, self.writes = net, writes
        (
            self.kept,
            self.give,
            self.got,
            self.from_x,
            self.from_y,
            self.from_z,
            self.late,
            self.final,
            self.swapped,
            self.wide,
            self.local_sem,
            self.send_sem,
            self.recv_sem,
        ) = scratch
        self.shards, self.half = self.kept.shape[1], self.kept.shape[2]
        self.own = net.y * net.line + net.z
        self.only, self.shared = reduce_split(TILE)
        self.both = self.only + self.shared
        self.carried = pl.ds(aligned(net.x * self.only, 128), self.both)
        self.lone = pl.ds(aligned(net.x * self.both, 128), self.only)
        self.their_lone = pl.ds(aligned((1 - net.x) * self.both, 128), self.only)

    def remote(self, tile, origin, landing, index, target):
        slot = tile % KEPT
        return pltpu.make_async_remote_copy(
            src_ref=origin,
            dst_ref=landing,
            send_sem=self.send_sem.at[slot, index],
            recv_sem=self.recv_sem.at[slot, index],
            device_id=target,
            device_id_type=MESH,
        )

    def halves(self, tile):
        return self.remote(tile, self.give.at[tile % GIVEN], self.got.at[tile % GOT], 3, self.net.sibling)

    def over_x(self, tile):
        origin = self.kept.at[tile % KEPT, :, :, self.their_lone]
        return self.remote(tile, origin, self.from_x.at[tile % OVER_X], 4, self.net.across_x)

    def over_y(self, tile):
        net = self.net
        origin = self.kept.at[tile % KEPT, pl.ds((1 - net.y) * net.line, net.line), :, self.carried]
        return self.remote(tile, origin, self.from_y.at[tile % OVER_Y], 2, net.across_y)

    def up(self, tile, z):
        net, count = self.net, self.net.line - 1 - z
        origin = self.kept.at[tile % KEPT, pl.ds(net.y * net.line + z + 1, count), :, self.carried]
        return self.remote(tile, origin, self.from_z.at[tile % OVER_Z, pl.ds(z + 2, count)], 0, net.above)

    def down(self, tile, z):
        net = self.net
        origin = self.kept.at[tile % KEPT, pl.ds(net.y * net.line, z), :, self.carried]
        return self.remote(tile, origin, self.from_z.at[tile % OVER_Z, pl.ds(0, z)], 1, net.below)

    def end_x(self, tile):
        net = self.net
        origin = self.kept.at[tile % KEPT, self.own, :, self.carried]
        return self.remote(tile, origin, self.late.at[tile % LATE], 5, net.across_x)

    def to_core(self, tile):
        slot = tile % ENDS
        return self.remote(tile, self.final.at[slot], self.swapped.at[slot], 6, self.net.sibling)

    def add(self, tile, shard, part):
        slot = tile % KEPT
        self.kept[slot, shard, :, self.carried] = self.kept[slot, shard, :, self.carried] + part

    def born(self, tile):
        self.halves(tile).start()

    def meet_core(self, tile):
        copy = self.halves(tile)
        copy.wait_recv()
        copy.wait_send()
        slot, came = tile % KEPT, tile % GOT

        @pl.loop(0, self.shards)
        def _(shard):
            self.kept[slot, shard] = self.kept[slot, shard] + self.got[came, shard]

        self.over_x(tile).start()

    def meet_x(self, tile):
        self.over_x(tile).wait_recv()
        slot, came = tile % KEPT, tile % OVER_X

        @pl.loop(0, self.shards)
        def _(shard):
            self.kept[slot, shard, :, self.lone] = self.kept[slot, shard, :, self.lone] + self.from_x[came, shard]

        self.over_y(tile).start()

    def meet_y(self, tile):
        self.over_y(tile).wait_recv()
        came, base = tile % OVER_Y, self.net.y * self.net.line

        @pl.loop(0, self.net.line)
        def _(z):
            self.add(tile, base + z, self.from_y[came, z])

        self.hop(tile, 0)

    def hop(self, tile, step):
        net, came = self.net, tile % OVER_Z
        base, end = net.y * net.line, net.line - 1

        @pl.when(net.z == step)
        def _():
            if step > 0:
                self.up(tile, step - 1).wait_recv()
                for z in range(step + 1, net.line):
                    self.add(tile, base + z, self.from_z[came, z + 1])
            self.up(tile, step).start()

        @pl.when(net.z == end - step)
        def _():
            if step > 0:
                self.down(tile, end - step + 1).wait_recv()
                for z in range(end - step):
                    self.add(tile, base + z, self.from_z[came, z])
            self.down(tile, end - step).start()

    def land(self, tile):
        net, came, end = self.net, tile % OVER_Z, self.net.line - 1
        pl.when(net.z == end)(self.up(tile, end - 1).wait_recv)
        pl.when(net.z == 0)(self.down(tile, 1).wait_recv)

        @pl.when(net.has_below)
        def _():
            self.add(tile, self.own, self.from_z[came, net.z + 1])

        @pl.when(net.has_above)
        def _():
            self.add(tile, self.own, self.from_z[came, net.z])

        self.end_x(tile).start()

    def meet(self, tile):
        net, only, both, shared = self.net, self.only, self.both, self.shared
        slot, came, end = tile % KEPT, tile % LATE, tile % ENDS
        self.end_x(tile).wait_recv()
        self.final[end, :, self.lone] = self.kept[slot, self.own, :, self.lone]
        for x in range(2):

            @pl.when(net.x == x)
            def _():
                theirs = 0 if x == 1 else shared
                middle = only if x == 1 else 0
                at = (1 - x) * both
                self.final[end, :, at : at + only] = self.late[came, :, theirs : theirs + only]
                self.final[end, :, only:both] = (
                    self.kept[slot, self.own, :, only:both] + self.late[came, :, middle : middle + shared]
                )

        self.to_core(tile).start()
        mine = pl.ds(aligned(net.core * self.half, self.half), self.half)
        self.wide[tile % WIDE, mine, :] = self.final[end].astype(jnp.float32)

    def swap(self, tile):
        self.to_core(tile).wait_recv()
        theirs = pl.ds(aligned((1 - self.net.core) * self.half, self.half), self.half)
        self.wide[tile % WIDE, theirs, :] = self.swapped[tile % ENDS].astype(jnp.float32)
        self.writes(tile, self.wide.at[tile % WIDE], self.local_sem.at[tile % KEPT], True)

    def finish(self, tile):
        net = self.net
        self.writes(tile, self.wide.at[tile % WIDE], self.local_sem.at[tile % KEPT], False)
        self.over_x(tile).wait_send()
        self.over_y(tile).wait_send()
        for z in range(net.line - 1):
            pl.when(net.z == z)(self.up(tile, z).wait_send)
            pl.when(net.z == z + 1)(self.down(tile, z + 1).wait_send)
        self.end_x(tile).wait_send()
        self.to_core(tile).wait_send()

    def stages(self):
        return [
            self.born,
            self.meet_core,
            self.meet_x,
            self.meet_y,
            lambda tile: self.hop(tile, 1),
            lambda tile: self.hop(tile, 2),
            self.land,
            self.meet,
            self.swap,
            self.finish,
        ]


class Plan:
    def __init__(self, blocks, heads):
        self.blocks, self.heads = blocks, heads
        self.ffn = blocks * SUBSTEPS
        self.norm = self.ffn
        self.branch = self.ffn + 1
        self.attend = self.ffn + 2
        self.groups = 4
        self.per_group = heads // self.groups
        self.out = self.ffn + SUBSTEPS
        self.ready = [self.attend + self.per_group * (group + 1) for group in range(self.groups)]
        self.births = list(range(SUBSTEPS, self.out + 2))
        self.ffn_tiles = self.ffn
        self.keys_tiles, self.value_tiles = [], []
        for group in range(self.groups):
            self.keys_tiles.append(len(self.births))
            self.births.append(max(self.ready[group], self.births[-1] + 1))
            if group % 2 == 1:
                self.value_tiles.append(len(self.births))
                self.births.append(self.births[-1] + 1)
        self.last = self.births[-1]
        self.grid = self.last + STAGES[-1] + 1

    def tile_at(self, step):
        regular = self.out + 2 - SUBSTEPS
        tile = step - SUBSTEPS
        known = (step >= SUBSTEPS) & (step < self.out + 2)
        for index in range(regular, len(self.births)):
            hit = step == self.births[index]
            tile = jnp.where(hit, index, tile)
            known = known | hit
        return tile, known


def back_kernel(plan, line, shards, *refs):
    step = pl.program_id(0)
    refs = list(refs)

    def take(count):
        out = refs[:count]
        del refs[:count]
        return out

    normed_hbm, given_hbm, hidden_hbm = take(3)
    early = take(4)
    into_2, into_3, down_hbm = take(3)
    attended_hbm, out_hbm, normed_one_hbm, x_hbm, qkv_hbm = take(5)
    small_hbm, = take(1)
    length_ref, q_ref, k_ref, v_ref, wide_ref, lse_ref, var_ref, valid_ref, cos_ref, sin_ref = take(10)
    result_hbm, tokens_hbm, sum_in, sum_down, sum_out, sum_qkv, sum_small = take(7)
    gather_to = take(4)
    normed, turned, given, w_down, w_gate, w_up, act, act_t = take(8)
    d_gate, d_up, acc, through = take(4)
    query_ref, given_aug_ref, dk_acc, dv_acc = take(4)
    load_sem, = take(1)
    gather_local, gather_send, gather_recv = take(3)
    small_ref, bias_ref, grad_gain_one_ref, grad_gain_two_ref, grad_small = take(5)
    small_buffers = take(REDUCE_BUFFERS)
    small_local, small_send, small_recv = take(3)
    net = Net(line)
    piece = BLOCK // shards
    gather_from = [
        into_2,
        down_hbm.at[pl.ds(2 * piece, piece)],
        into_3,
        down_hbm.at[pl.ds(3 * piece, piece)],
    ]
    half = BLOCK // shards // 2
    heads_at = step - plan.attend

    def writes(tile, wide, sems, begin):
        rows = 2 * half

        def move(index, origin, landing):
            copy = pltpu.make_async_copy(origin, landing, sems.at[index])
            copy.start() if begin else copy.wait()

        block, kind = tile // SUBSTEPS, tile % SUBSTEPS
        in_ffn = tile < plan.ffn_tiles

        @pl.when(in_ffn & (kind < 2))
        def _():
            lines = pl.ds(aligned(block * rows, rows), rows)
            move(0, wide, sum_down.at[lines, pl.ds(aligned(kind * TILE, TILE), TILE)])

        @pl.when(in_ffn & (kind >= 2))
        def _():
            inner = plan.blocks * BLOCK
            base = ((kind - 2) // 2) * inner
            for piece in range(4):
                shard = (kind % 2) * 4 + piece
                start = base + shard * (inner // shards) + block * (BLOCK // shards)
                columns = pl.ds(aligned(start, 128), 128)
                move(piece, wide.at[:, piece * 128 : (piece + 1) * 128], sum_in.at[:, columns])

        @pl.when((tile >= plan.ffn_tiles) & (tile < plan.ffn_tiles + 2))
        def _():
            start = aligned((tile - plan.ffn_tiles) * TILE, TILE)
            move(0, wide, sum_out.at[:, pl.ds(start, TILE)])

        width = plan.heads * q_ref.shape[0]
        for group, number in enumerate(plan.keys_tiles):

            @pl.when(tile == number)
            def _():
                for part in range(2):
                    start = part * width + group * (TILE // 2)
                    columns = slice(part * (TILE // 2), (part + 1) * (TILE // 2))
                    move(part, wide.at[:, columns], sum_qkv.at[:, pl.ds(start, TILE // 2)])

        for pair, number in enumerate(plan.value_tiles):

            @pl.when(tile == number)
            def _():
                move(0, wide, sum_qkv.at[:, pl.ds(2 * width + pair * TILE, TILE)])

    stream = Stream(net, refs, writes)
    stages = stream.stages()

    def load(index, origin, landing):
        return pltpu.make_async_copy(origin, landing, load_sem.at[index])

    def weight_loads(block):
        if block < 2:
            into, down = early[2 * block], early[2 * block + 1]
        else:
            into, down = gather_to[2 * (block - 2)], gather_to[2 * (block - 2) + 1]
        return [
            load(0, into.at[:, pl.ds(0, BLOCK)], w_gate),
            load(1, into.at[:, pl.ds(BLOCK, BLOCK)], w_up),
            load(2, down, w_down),
        ]

    first_loads = [
        load(3, normed_hbm, normed),
        load(4, given_hbm, given),
        load(5, hidden_hbm, acc),
        load(15, small_hbm, small_ref),
        load(16, small_hbm, bias_ref),
    ]
    hidden_load = load(5, hidden_hbm, acc)
    result_store = load(6, act, result_hbm)
    attended_wait = load(7, attended_hbm, w_down)
    out_load = load(8, out_hbm, d_up.at[0])
    normed_one_wait = load(9, normed_one_hbm, turned)
    x_load = load(10, x_hbm, normed)
    tokens_store = load(11, acc, tokens_hbm)

    def placed():
        for shard in range(shards):
            order = (shard % 2) * line + shard // 2
            for part in range(2):
                which = net.core if part == 0 else 1 - net.core
                start = (shard * 2 + part) * half
                yield start, aligned((which * shards + order) * half, half)

    def in_order(index, origin, landing):
        return [load(index, origin.at[pl.ds(start, half)], landing.at[pl.ds(to, half)]) for start, to in placed()]

    def turn_into(page, value):
        flipped = value.T
        for start, to in placed():
            page[pl.ds(to, half), :] = flipped[start : start + half]

    def qkv_loads(group):
        width = qkv_hbm.shape[1] // 3
        part = width // plan.groups
        page = act_t if group % 2 == 0 else d_up.at[0]
        return [
            load(
                12 + index,
                qkv_hbm.at[:, pl.ds(index * width + group * part, part)],
                page.at[:, pl.ds(index * part, part)],
            )
            for index in range(3)
        ]

    def at(place):
        return pl.when(step == place)

    def start(copies):
        for copy in copies:
            copy.start()

    def wait(copies):
        for copy in copies:
            copy.wait()

    gathers = [
        gather_steps(
            net, gather_from[i], gather_to[i], gather_local.at[i], gather_send.at[i], gather_recv.at[i]
        )
        for i in range(4)
    ]
    gather_places = ((0, 2, 4, 6, 8, 9, 10), (7, 9, 11, 12, 14, 15, 16))

    @at(0)
    def _():
        net.greet()
        start(weight_loads(0) + first_loads)

    for pair, places in enumerate(gather_places):
        for index, place in enumerate(places):

            @at(place)
            def _():
                gathers[2 * pair][index]()
                gathers[2 * pair + 1][index]()

    for stage in range(len(STAGES) - 1, 0, -1):
        tile, known = plan.tile_at(step - STAGES[stage])
        pl.when(known)(functools.partial(stages[stage], tile))

    @at(0)
    def _():
        wait(first_loads)
        position = lax.broadcasted_iota(jnp.int32, (given.shape[0], 1), 0)
        counted = jnp.where(position < length_ref[0], 1.0, 0.0).astype(jnp.bfloat16)
        given[...] = given[...] * counted
        grad_small[...] = jnp.zeros_like(grad_small)
        turn_into(turned, normed[...])

    for block in range(plan.blocks):

        @at(block * SUBSTEPS)
        def _():
            wait(weight_loads(block))

        if block + 1 < plan.blocks:

            @at(block * SUBSTEPS + SUBSTEPS - 1)
            def _():
                start(weight_loads(block + 1))

    block, sub = step // SUBSTEPS, step % SUBSTEPS
    slot = block % 2
    in_ffn = step < plan.ffn

    @pl.when(in_ffn & (sub < 2))
    def _():
        columns = pl.ds(aligned(sub * TILE, TILE), TILE)
        d_act = product(given[...], w_down[columns, :], COLUMNS_BY_COLUMNS)
        gate = product(normed[...], w_gate[:, columns])
        up = product(normed[...], w_up[:, columns])
        sigmoid = jax.nn.sigmoid(gate)
        swish = gate * sigmoid
        act[:, columns] = (swish * up).astype(jnp.bfloat16)
        d_gate[slot, :, columns] = (d_act * up * sigmoid * (1.0 + gate * (1.0 - sigmoid))).astype(jnp.bfloat16)
        d_up[slot, :, columns] = (d_act * swish).astype(jnp.bfloat16)

    @pl.when(in_ffn & (sub == 2))
    def _():
        acc[...] += product(act[...], w_down[...])
        turn_into(act_t, act[...])

    @pl.when(in_ffn & (sub == 3))
    def _():
        part = product(d_gate[slot], w_gate[...], COLUMNS_BY_COLUMNS)

        @pl.when(block == 0)
        def _():
            through[...] = part

        @pl.when(block > 0)
        def _():
            through[...] += part

    @pl.when(in_ffn & (sub == 4))
    def _():
        through[...] += product(d_up[slot], w_up[...], COLUMNS_BY_COLUMNS)

    last_sum = plan.ffn - SUBSTEPS + 2

    @at(last_sum)
    def _():
        act[...] = acc[...].astype(jnp.bfloat16)
        result_store.start()

    @at(last_sum + 1)
    def _():
        start([hidden_load] + in_order(7, attended_hbm, w_down))

    @at(last_sum + 3)
    def _():
        result_store.wait()

    row_block = 128

    @at(plan.norm)
    def _():
        out_load.start()
        hidden_load.wait()
        grad_gain_two_ref[...] = jnp.zeros_like(grad_gain_two_ref)
        gain_two = gain_of(small_ref, shards, 1)

        @pl.loop(0, acc.shape[0] // row_block)
        def _(index):
            lines = pl.ds(aligned(index * row_block, row_block), row_block)
            back, grad_gain = norm_back(through[lines, :], acc[lines, :], gain_two)
            d_hidden = given[lines, :].astype(jnp.float32) + back
            acc[lines, :] = d_hidden
            d_gate[0, lines, :] = d_hidden.astype(jnp.bfloat16)
            grad_gain_two_ref[...] += grad_gain

    @at(plan.branch)
    def _():
        out_load.wait()
        act[...] = product(d_up[0], d_gate[0], COLUMNS_BY_COLUMNS).astype(jnp.bfloat16)
        through[...] = jnp.zeros_like(through)

    for group in range(plan.groups):
        ready = plan.ready[group]

        if group == 0:

            @at(plan.attend)
            def _():
                start(qkv_loads(0))

        @at(ready)
        def _():
            wait(qkv_loads(group))
            if group + 1 < plan.groups:
                start(qkv_loads(group + 1))

    quarter = TILE // 2
    for parity, page in enumerate((act_t, d_up.at[0])):
        base = parity * TILE
        now = (step == plan.ready[parity]) | (step == plan.ready[parity + 2])
        pair = jnp.where(step == plan.ready[parity + 2], 1, 0)
        value_at = pl.ds(aligned(pair * TILE + parity * quarter, quarter), quarter)

        @pl.when(now)
        def _():
            part = product(page[:, :TILE], w_gate[base : base + TILE, :])
            through[...] += part + product(page[:, TILE : TILE + quarter], w_up[value_at, :])

    @at(plan.out)
    def _():
        attended_wait.wait()
        start(in_order(9, normed_one_hbm, turned) + [x_load])

    @at(plan.births[plan.keys_tiles[0]])
    def _():
        normed_one_wait.wait()

    @pl.when((heads_at >= 0) & (heads_at < plan.heads))
    def _():
        depth = q_ref.shape[0]
        head = heads_at
        group = head // plan.per_group
        q_at = (group % 2) * TILE + (head % plan.per_group) * depth
        k_at = q_at + TILE // 2
        v_at = (group // 2) * TILE + (head % (2 * plan.per_group)) * depth

        def rows(start):
            return pl.ds(aligned(start, depth), depth)

        per_shard = plan.heads // shards
        same, other = bias_of(bias_ref, head, per_shard)
        sums = attend_back_head(
            2,
            same,
            other,
            q_ref,
            k_ref,
            v_ref,
            act.at[rows(head * depth)],
            wide_ref,
            lse_ref,
            var_ref,
            valid_ref,
            cos_ref,
            sin_ref,
            w_gate.at[rows(q_at)],
            w_gate.at[rows(k_at)],
            w_up.at[rows(v_at)],
            query_ref,
            given_aug_ref,
            dk_acc,
            dv_acc,
        )
        for which, lanes in enumerate(sums):
            folded = sum(lanes[:, start : start + 128] for start in range(0, lanes.shape[1], 128))
            grad_small[head // per_shard, pl.ds(2 + 2 * (head % per_shard) + which, 1), :] = folded

    tile, known = plan.tile_at(step)

    def birth(left, right, dims=(((1,), (0,)), ((), ()))):
        out = product(left[...], right, dims).astype(jnp.bfloat16)
        kept, give = stream.kept.at[tile % KEPT], stream.give.at[tile % GIVEN]
        for order in range(shards):
            kept[order] = out[order * half : (order + 1) * half]
            give[order] = out[(shards + order) * half : (shards + order + 1) * half]

    def chosen(numbers, bases):
        base, hit = 0, False
        for number, start in zip(numbers, bases):
            now = step == plan.births[number]
            base, hit = jnp.where(now, start, base), now | hit
        return pl.ds(aligned(base, TILE), TILE), hit

    kind, source = tile % SUBSTEPS, (tile // SUBSTEPS) % 2
    in_tiles = known & (tile < plan.ffn_tiles)
    columns = pl.ds(aligned((kind % 2) * TILE, TILE), TILE)
    pl.when(in_tiles & (kind < 2))(lambda: birth(act_t, given[:, columns]))
    pl.when(in_tiles & (kind >= 2) & (kind < 4))(lambda: birth(turned, d_gate[source, :, columns]))
    pl.when(in_tiles & (kind >= 4))(lambda: birth(turned, d_up[source, :, columns]))
    out_columns = pl.ds(aligned(jnp.clip(step - plan.out, 0, 1) * TILE, TILE), TILE)
    pl.when((step == plan.out) | (step == plan.out + 1))(lambda: birth(w_down, d_gate[0, :, out_columns]))
    lines, hit = chosen(plan.keys_tiles, [(group % 2) * TILE for group in range(plan.groups)])
    pl.when(hit)(lambda: birth(turned, w_gate[lines, :], COLUMNS_BY_COLUMNS))
    value_lines, value_hit = chosen(plan.value_tiles, [pair * TILE for pair in range(plan.groups // 2)])
    pl.when(value_hit)(lambda: birth(turned, w_up[value_lines, :], COLUMNS_BY_COLUMNS))
    pl.when(known)(lambda: stream.born(tile))

    @at(plan.last + 1)
    def _():
        x_load.wait()
        grad_gain_one_ref[...] = jnp.zeros_like(grad_gain_one_ref)
        gain_one = gain_of(small_ref, shards, 0)

        @pl.loop(0, acc.shape[0] // row_block)
        def _(index):
            lines = pl.ds(aligned(index * row_block, row_block), row_block)
            values = normed[lines, :].astype(jnp.float32)
            back, grad_gain = norm_back(through[:, lines].T, values, gain_one)
            acc[lines, :] = acc[lines, :] + back
            grad_gain_one_ref[...] += grad_gain

        tokens_store.start()
        for shard in range(shards):
            columns = slice(shard * 128, (shard + 1) * 128)
            grad_small[shard, 0:1, :] = grad_gain_one_ref[:, columns]
            grad_small[shard, 1:2, :] = grad_gain_two_ref[:, columns]

    small_steps = reduce_steps(
        net, grad_small, sum_small, 0, 0, small_buffers, small_local, small_send, small_recv
    )
    for index, action in enumerate(small_steps):
        at(plan.last + 2 + index)(action)

    @at(plan.grid - 1)
    def _():
        tokens_store.wait()


def back(line, early, sources, own_down, normed_two, given, hidden, attended_t, out_weight, normed_t, x, qkv_weight,
         small, lengths, qkv_t, wide_t, log_sums, variates, valid, cos_t, sin_t):
    shards = lax.axis_size("shard")
    rows, width = x.shape
    heads = log_sums.shape[0]
    depth = width // heads
    blocks = 4
    plan = Plan(blocks, heads)
    low = jnp.bfloat16
    owned = width // shards
    inner = blocks * BLOCK

    def head_at(step):
        return jnp.clip(step - plan.attend, 0, heads - 1)

    def part(which):
        return pl.BlockSpec((depth, rows), lambda step: (which * heads + head_at(step), 0))

    page = pltpu.VMEM((BLOCK, BLOCK), low)
    copies = gather_count(line)
    return pl.pallas_call(
        functools.partial(back_kernel, plan, line, shards),
        grid=(plan.grid,),
        out_shape=[
            like((rows, width), low),
            like((rows, width), jnp.float32),
            like((owned, 2 * inner), jnp.float32),
            like((inner // shards, width), jnp.float32),
            like((owned, width), jnp.float32),
            like((owned, 3 * width), jnp.float32),
            like((16, 128), jnp.float32),
        ]
        + [like((width, 2 * BLOCK), low), like((BLOCK, width), low)] * 2
,
        in_specs=[ANY] * 16
        + [
            pl.BlockSpec(memory_space=pltpu.SMEM),
            part(0),
            part(1),
            part(2),
            pl.BlockSpec((depth, rows), lambda step: (head_at(step), 0)),
            pl.BlockSpec((1, 1, rows), lambda step: (head_at(step), 0, 0)),
            whole(1, rows),
            whole(1, rows),
            whole(*cos_t.shape),
            whole(*sin_t.shape),
        ],
        out_specs=[ANY] * 11,
        scratch_shapes=[page] * 8
        + [
            pltpu.VMEM((2, BLOCK, BLOCK), low),
            pltpu.VMEM((2, BLOCK, BLOCK), low),
            pltpu.VMEM((rows, width), jnp.float32),
            pltpu.VMEM((rows, width), jnp.float32),
            pltpu.VMEM((2 * depth + FEATURES, rows), low),
            pltpu.VMEM((depth + FEATURES, rows), low),
            pltpu.VMEM((rows, depth), jnp.float32),
            pltpu.VMEM((rows, depth), jnp.float32),
            pltpu.SemaphoreType.DMA((17,)),
            pltpu.SemaphoreType.DMA((4,)),
            pltpu.SemaphoreType.DMA((4, copies)),
            pltpu.SemaphoreType.DMA((4, copies)),
            pltpu.VMEM((16 * shards, 128), jnp.float32),
            pltpu.SMEM((16 * shards, 128), jnp.float32),
            pltpu.VMEM((1, width), jnp.float32),
            pltpu.VMEM((1, width), jnp.float32),
            pltpu.VMEM((shards, 16, 128), jnp.float32),
        ]
        + reduce_scratch(line, shards, 8, 128, jnp.float32)
        + [
            pltpu.SemaphoreType.DMA((2,)),
            pltpu.SemaphoreType.DMA((reduce_count(line),)),
            pltpu.SemaphoreType.DMA((reduce_count(line),)),
        ]
        + stream_scratch(line, shards, owned // 2),
        compiler_params=pltpu.CompilerParams(
            collective_id=9, has_side_effects=True, vmem_limit_bytes=64 << 20
        ),
        name="back",
    )(
        normed_two, given, hidden, *early, *sources, own_down, attended_t, out_weight, normed_t, x, qkv_weight,
        small, lengths, qkv_t, qkv_t, qkv_t, wide_t, log_sums, variates, valid, cos_t, sin_t,
    )


def rope_tables(time_ids):
    half = HEAD_DIM // 2
    exponent = jnp.arange(half).astype(jnp.float32) * (2.0 / HEAD_DIM)
    inverse = jnp.exp(-jnp.log(rope_base) * exponent)
    angles = inverse[:, None] * time_ids.astype(jnp.float32)
    return jnp.cos(angles), jnp.sin(angles)


def pack_small(attn_gain, ffn_gain, attn_bias):
    heads = attn_bias.shape[1]
    small = jnp.zeros((16, 128), jnp.float32)
    small = small.at[0].set(attn_gain.astype(jnp.float32)).at[1].set(ffn_gain.astype(jnp.float32))
    return small.at[2:4, :heads].set(attn_bias.astype(jnp.float32))


def shards(
    line,
    tokens,
    lengths,
    variate_ids,
    time_ids,
    attn_gain,
    w_qkv,
    attn_bias,
    w_out,
    ffn_gain,
    w_in,
    w_down,
    cotangent,
):
    length = variate_ids.shape[1]
    heads = attn_bias.shape[1]
    key_valid = jnp.arange(length)[None, :] < lengths[:, None]
    valid = key_valid.astype(jnp.float32)
    cos_t, sin_t = rope_tables(time_ids)
    if line:
        small, qkv_weight, out_weight, into_0, down_0, into_1, down_1, *rest = front(
            line,
            pack_small(attn_gain, ffn_gain, attn_bias),
            w_qkv,
            w_out,
            w_in,
            w_down,
            tokens,
            variate_ids,
            valid,
            cos_t,
            sin_t,
            HEADS,
        )
        intos, (qkv_t, normed_t, attended_t, hidden, normed_two, wide_t, log_sums) = rest[:4], rest[4:]
        result, grad_tokens, sum_in, sum_down, sum_out, sum_qkv, small = back(
            line,
            [into_0, down_0, into_1, down_1],
            [intos[2], intos[3]],
            w_down,
            normed_two,
            cotangent,
            hidden,
            attended_t,
            out_weight,
            normed_t,
            tokens,
            qkv_weight,
            small,
            lengths,
            qkv_t,
            wide_t,
            log_sums,
            variate_ids,
            valid,
            cos_t,
            sin_t,
        )[:7]
        return (
            result,
            grad_tokens,
            small[0],
            sum_qkv,
            jnp.sum(small[2 : 2 + 2 * heads], axis=1).reshape(heads, 2).T,
            sum_out,
            small[1],
            sum_in,
            sum_down,
        )
    given = jnp.where(key_valid.reshape(length, 1), cotangent, jnp.zeros_like(cotangent))
    gain_one, gain_two, qkv_weight, out_weight, in_weight, down_weight = (
        lax.all_gather(part, "shard", axis=0, tiled=True)
        for part in (attn_gain, ffn_gain, w_qkv, w_out, w_in, w_down)
    )
    bias = lax.all_gather(attn_bias, "shard", axis=1, tiled=True).astype(jnp.float32)
    gain_one = gain_one.astype(jnp.float32).reshape(1, -1)
    gain_two = gain_two.astype(jnp.float32).reshape(1, -1)
    qkv_t, normed_t = project(tokens, gain_one, qkv_weight, cos_t, sin_t)
    attended_t, wide_t, log_sums = attend_forward(qkv_t, variate_ids, valid, bias, HEADS)
    hidden, normed_two = branch(attended_t, out_weight, tokens, gain_two)
    act, to_gate, to_up = widen(normed_two, in_weight)
    result, grad_down, d_gate, d_up = narrow(act, to_gate, to_up, down_weight, given, hidden)
    grad_gate, grad_up = grad_into(normed_two, d_gate, d_up)
    d_hidden, d_branch, grad_gain_two = ffn_back(d_gate, d_up, in_weight, hidden, gain_two, given)
    grad_out, given_t = branch_back(attended_t, out_weight, d_branch)
    dq, dk, dv, bias_parts = attend_backward(
        qkv_t, given_t, wide_t, log_sums, variate_ids, valid, bias, cos_t, sin_t, HEADS
    )
    grad_qkv, grad_tokens, grad_gain_one = project_back(
        normed_t, dq, dk, dv, qkv_weight, tokens, gain_one, d_hidden
    )
    grads = (
        (grad_gain_one.reshape(-1), 0),
        (grad_qkv, 0),
        (jnp.sum(bias_parts, axis=2).T, 1),
        (grad_out, 0),
        (grad_gain_two.reshape(-1), 0),
        (jnp.concatenate([grad_gate, grad_up], axis=1), 0),
        (grad_down, 0),
    )
    owned = [
        lax.psum_scatter(grad.astype(jnp.bfloat16), "shard", scatter_dimension=axis, tiled=True)
        for grad, axis in grads
    ]
    return (result, grad_tokens) + tuple(lax.psum(part, "rep").astype(jnp.float32) for part in owned)


def solution(mesh):
    placed = (
        P(("shard", "rep"), None),
        P(("shard", "rep")),
        P(("shard", "rep"), None),
        P(("shard", "rep"), None),
        P("shard"),
        P("shard", None),
        P(None, "shard"),
        P("shard", None),
        P("shard"),
        P("shard", None),
        P("shard", None),
        P(("shard", "rep"), None),
    )
    line = mesh.shape["shard"] // 2 if (mesh.shape["shard"], mesh.shape["rep"]) == (8, 4) else 0
    return jax.shard_map(
        functools.partial(shards, line),
        mesh=mesh,
        in_specs=placed,
        out_specs=(
            P(("shard", "rep"), None),
            P(("shard", "rep"), None),
            P("shard"),
            P("shard", None),
            P(None, "shard"),
            P("shard", None),
            P("shard"),
            P("shard", None),
            P("shard", None),
        ),
        check_vma=False,
    )
```

```python
import functools

import jax
import jax.numpy as jnp
from jax import lax
from jax.experimental import pallas as pl
from jax.experimental.pallas import tpu as pltpu
from jax.sharding import PartitionSpec as P

HEADS = 16
HEAD_DIM = 64


norm_eps = 1e-06
rope_base = 10000.0
masked_score = -1000000000.0

MESH = pl.DeviceIdType.MESH
ANY = pl.BlockSpec(memory_space=pl.ANY)


class Net:
    def __init__(self, line):
        shard, rep = lax.axis_index("shard"), lax.axis_index("rep")
        self.line = line
        self.z, self.y = shard // 2, shard % 2
        self.x, self.core = rep // 2, rep % 2
        self.own = shard
        self.sibling = (shard, self.x * 2 + 1 - self.core)
        self.across_x = (shard, (1 - self.x) * 2 + self.core)
        self.across_y = (self.z * 2 + 1 - self.y, rep)
        self.above = (jnp.minimum(self.z + 1, line - 1) * 2 + self.y, rep)
        self.below = (jnp.maximum(self.z - 1, 0) * 2 + self.y, rep)
        self.has_above = self.z < line - 1
        self.has_below = self.z > 0

    def greet(self):
        barrier = pltpu.get_barrier_semaphore()

        def hail(partner):
            pl.semaphore_signal(barrier, inc=1, device_id=partner, device_id_type=MESH)

        for partner in (self.sibling, self.across_x, self.across_y):
            hail(partner)
        pl.when(self.has_above)(lambda: hail(self.above))
        pl.when(self.has_below)(lambda: hail(self.below))
        neighbours = jnp.where(self.has_above, 1, 0) + jnp.where(self.has_below, 1, 0)
        pl.semaphore_wait(barrier, 3 + neighbours)


def aligned(value, step):
    return pl.multiple_of(value, step)


def gather_count(line):
    return 2 * line + 3 * 2 * line


def gather_steps(net, source, full, local_sem, send_sem, recv_sem):
    line = net.line
    height, columns = source.shape
    half = height // 2
    split = columns % 1024 == 0
    only = columns * 3 // 8 if split else 0
    shared = columns - 2 * only
    rows = pl.ds(aligned(net.core * half, half), half)
    carried = pl.ds(aligned(net.x * only, 128), only + shared) if split else pl.ds(0, columns)
    lone = pl.ds(aligned(net.x * (only + shared), 128), only) if split else None

    def remote(origin, landing, index, target):
        return pltpu.make_async_remote_copy(
            src_ref=origin,
            dst_ref=landing,
            send_sem=send_sem.at[index],
            recv_sem=recv_sem.at[index],
            device_id=target,
            device_id_type=MESH,
        )

    def held(z, y, which=None):
        lines = pl.ds(aligned((z * 2 + y) * height + net.core * half, half), half)
        return full.at[lines] if which is None else full.at[lines, which]

    def piece(z, y):
        return held(z, y, carried)

    def over_z(z, target, base):
        return remote(piece(z, net.y), piece(z, net.y), base + z, target)

    def over_y(z):
        return remote(piece(z, net.y), piece(z, net.y), 2 * line + z, net.across_y)

    def over_x(z, y):
        part = held(z, y, lone)
        return remote(part, part, 3 * line + y * line + z, net.across_x)

    def to_core(z, y):
        part = held(z, y)
        return remote(part, part, 5 * line + y * line + z, net.sibling)

    mine = source.at[rows, carried]
    local = pltpu.make_async_copy(source, full.at[pl.ds(aligned(net.own * height, height), height)], local_sem)
    first_y = remote(mine, piece(net.z, net.y), 2 * line + net.z, net.across_y)
    first_up = remote(mine, piece(net.z, net.y), net.z, net.above)
    first_down = remote(mine, piece(net.z, net.y), line + net.z, net.below)

    def onward(z, y):
        if split:
            over_x(z, y).start()
        else:
            to_core(z, y).start()

    def start():
        first_y.start()
        pl.when(net.has_above)(first_up.start)
        pl.when(net.has_below)(first_down.start)
        local.start()

    def arrive(hops):
        @pl.when(net.z >= hops)
        def _():
            z = net.z - hops
            over_z(z, net.above, 0).wait_recv()
            pl.when(net.has_above)(over_z(z, net.above, 0).start)
            over_y(z).start()
            onward(z, net.y)

        @pl.when(net.z < line - hops)
        def _():
            z = net.z + hops
            over_z(z, net.below, line).wait_recv()
            pl.when(net.has_below)(over_z(z, net.below, line).start)
            over_y(z).start()
            onward(z, net.y)

    def arrive_y(hops):
        def one(z):
            remote(piece(z, 1 - net.y), piece(z, 1 - net.y), 2 * line + z, net.across_y).wait_recv()
            onward(z, 1 - net.y)

        if hops == 0:
            one(net.z)
        else:
            pl.when(net.z >= hops)(lambda: one(net.z - hops))
            pl.when(net.z < line - hops)(lambda: one(net.z + hops))

    def arrive_x(hops, own_y):
        def one(z):
            y = net.y if own_y else 1 - net.y
            part = held(z, y, pl.ds(aligned((1 - net.x) * (only + shared), 128), only))
            remote(part, part, 3 * line + y * line + z, net.across_x).wait_recv()
            to_core(z, y).start()

        if not split:
            return
        if hops == 0:
            one(net.z)
        else:
            pl.when(net.z >= hops)(lambda: one(net.z - hops))
            pl.when(net.z < line - hops)(lambda: one(net.z + hops))

    def step(hops):
        def run():
            arrive_y(hops - 1)
            if hops < line:
                arrive(hops)
            if hops >= 2:
                arrive_x(hops - 2, False)
                arrive_x(hops - 1, True)

        return run

    def last():
        arrive_x(line - 1, False)

    def finish():
        local.wait()
        first_y.wait_send()

        @pl.when(net.has_above)
        def _():
            first_up.wait_send()
            for hops in range(1, line - 1):
                pl.when(net.z >= hops)(over_z(net.z - hops, net.above, 0).wait_send)

        @pl.when(net.has_below)
        def _():
            first_down.wait_send()
            for hops in range(1, line - 1):
                pl.when(net.z < line - hops)(over_z(net.z + hops, net.below, line).wait_send)

        for z in range(line):

            def others():
                over_y(z).wait_send()
                if split:
                    over_x(z, net.y).wait_send()
                to_core(z, net.y).wait()

            pl.when(net.z != z)(others)
            if split:
                over_x(z, 1 - net.y).wait_send()
            to_core(z, 1 - net.y).wait()

    return [start] + [step(hops) for hops in range(1, line + 1)] + [last, finish]


REDUCE_BUFFERS = 9


def reduce_split(columns):
    only = columns // 4 if columns % 512 == 0 else 0
    return only, columns - 2 * only


def reduce_scratch(line, shards, half, columns, dtype):
    only, shared = reduce_split(columns)
    carried = only + shared
    return [
        pltpu.VMEM((shards, half, columns), dtype),
        pltpu.VMEM((shards, half, columns), dtype),
        pltpu.VMEM((shards, half, max(only, 128)), dtype),
        pltpu.VMEM((line, half, carried), dtype),
        pltpu.VMEM((line + 1, half, carried), dtype),
        pltpu.VMEM((half, carried), dtype),
        pltpu.VMEM((half, columns), dtype),
        pltpu.VMEM((half, columns), dtype),
        pltpu.VMEM((2 * half, columns), jnp.float32),
    ]


def reduce_count(line):
    return 3 * line + 4


def reduce_steps(net, grad, out, column_start, out_start, buffers, local_sem, send_sem, recv_sem):
    kept, got, from_x, from_y, from_z, late_x, final, swapped, wide = buffers
    line = net.line
    shards, half, width = kept.shape
    only, shared = reduce_split(width)
    both = only + shared
    columns = pl.ds(column_start, width)
    mine = pl.ds(aligned(net.core * half, half), half)
    theirs = pl.ds(aligned((1 - net.core) * half, half), half)
    if only:
        carried = pl.ds(aligned(net.x * only, 128), both)
        lone = pl.ds(aligned(net.x * both, 128), only)
        their_lone = pl.ds(aligned((1 - net.x) * both, 128), only)
    else:
        carried = pl.ds(0, width)

    def remote(origin, landing, index, target):
        return pltpu.make_async_remote_copy(
            src_ref=origin,
            dst_ref=landing,
            send_sem=send_sem.at[index],
            recv_sem=recv_sem.at[index],
            device_id=target,
            device_id_type=MESH,
        )

    local = pltpu.make_async_copy(grad.at[:, mine, columns], kept, local_sem.at[0])
    halves = remote(grad.at[:, theirs, columns], got, 2 * line, net.sibling)
    written = pltpu.make_async_copy(wide, out.at[:, pl.ds(out_start, width)], local_sem.at[1])
    to_core = remote(final, swapped, 2 * line + 1, net.sibling)
    end_x = remote(kept.at[net.own, :, carried], late_x, 2 * line + 2, net.across_x)
    if only:
        over_x = remote(kept.at[:, :, their_lone], from_x, 2 * line + 3, net.across_x)

    def over_y(z):
        part = kept.at[z * 2 + 1 - net.y, :, carried]
        return remote(part, from_y.at[z], 2 * line + 4 + z, net.across_y)

    def up(z):
        return remote(kept.at[z * 2 + net.y, :, carried], from_z.at[z + 1], z, net.above)

    def down(z):
        return remote(kept.at[z * 2 + net.y, :, carried], from_z.at[z], line + z, net.below)

    def add(shard, part):
        kept[shard, :, carried] = kept[shard, :, carried] + part

    def first():
        halves.start()
        local.start()

    def second():
        local.wait()
        halves.wait_recv()

        @pl.loop(0, shards)
        def _(shard):
            kept[shard] = kept[shard] + got[shard]

        if only:
            over_x.start()

    def third():
        if only:
            over_x.wait_recv()

            @pl.loop(0, shards)
            def _(shard):
                kept[shard, :, lone] = kept[shard, :, lone] + from_x[shard]

        for z in range(line):
            over_y(z).start()

    def fourth():
        for z in range(line):
            over_y(z).wait_recv()

        @pl.loop(0, line)
        def _(z):
            add(z * 2 + net.y, from_y[z])

    def hop(step):
        def run():
            @pl.when(net.z == step)
            def _():
                for z in range(line - 1, step, -1):
                    if step > 0:
                        up(z).wait_recv()
                        add(z * 2 + net.y, from_z[z + 1])
                    up(z).start()

            @pl.when(net.z == line - 1 - step)
            def _():
                for z in range(line - 1 - step):
                    if step > 0:
                        down(z).wait_recv()
                        add(z * 2 + net.y, from_z[z])
                    down(z).start()

        return run

    def land():
        @pl.when(net.has_below)
        def _():
            up(net.z).wait_recv()
            add(net.own, from_z[net.z + 1])

        @pl.when(net.has_above)
        def _():
            down(net.z).wait_recv()
            add(net.own, from_z[net.z])

        end_x.start()

    def meet():
        end_x.wait_recv()
        if only:
            final[:, lone] = kept[net.own, :, lone]
            for x in range(2):

                @pl.when(net.x == x)
                def _():
                    start = 0 if x == 1 else shared
                    final[:, (1 - x) * both : (1 - x) * both + only] = late_x[:, start : start + only]
                    other = shared * 0 + (only if x == 1 else 0)
                    final[:, only:both] = kept[net.own, :, only:both] + late_x[:, other : other + shared]
        else:
            final[...] = kept[net.own] + late_x[...]
        to_core.start()
        wide[mine, :] = final[...].astype(jnp.float32)

    def swap():
        to_core.wait_recv()
        wide[theirs, :] = swapped[...].astype(jnp.float32)
        written.start()

    def finish():
        written.wait()
        halves.wait_send()
        if only:
            over_x.wait_send()
        for z in range(line):
            over_y(z).wait_send()
            pl.when(net.z < z)(up(z).wait_send)
            pl.when(net.z > z)(down(z).wait_send)
        end_x.wait_send()
        to_core.wait_send()

    hops = [hop(step) for step in range(line - 1)]

    def fourth_and_hop():
        fourth()
        hops[0]()

    return [first, second, third, fourth_and_hop] + hops[1:] + [land, meet, swap, finish]


ROWS_BY_ROWS = (((0,), (0,)), ((), ()))
COLUMNS_BY_COLUMNS = (((1,), (1,)), ((), ()))


def product(first_op, second_op, dims=(((1,), (0,)), ((), ()))):
    return lax.dot_general(first_op, second_op, dims, preferred_element_type=jnp.float32)


def inverse_rms(values):
    return lax.rsqrt(jnp.mean(values * values, axis=1, keepdims=True) + norm_eps)


def run(body, *, grid, out_shape, in_specs, out_specs, scratch_shapes, name, operands):
    return pl.pallas_call(
        body,
        grid=(grid,),
        out_shape=out_shape,
        in_specs=in_specs,
        out_specs=out_specs,
        scratch_shapes=scratch_shapes,
        compiler_params=pltpu.CompilerParams(vmem_limit_bytes=60 << 20),
        name=name,
    )(*operands)


def whole(*shape):
    return pl.BlockSpec(shape, lambda step: (0,) * len(shape), pipeline_mode=pl.Buffered(1))


def like(shape, dtype):
    return jax.ShapeDtypeStruct(shape, dtype)


def project_kernel(turned, x_ref, gain_ref, w_ref, cos_ref, sin_ref, out_ref, normed_ref):
    step = pl.program_id(0)

    @pl.when(step == 0)
    def _():
        values = x_ref[...].astype(jnp.float32)
        normed = values * inverse_rms(values) * gain_ref[...]
        normed_ref[...] = normed.T.astype(jnp.bfloat16)

    out = product(w_ref[...], normed_ref[...], ROWS_BY_ROWS)

    @pl.when(step < turned)
    def _():
        cos, sin = cos_ref[...], sin_ref[...]
        half = cos.shape[0]
        for start in range(0, out.shape[0], 2 * half):
            first, second = out[start : start + half], out[start + half : start + 2 * half]
            out_ref[start : start + half, :] = (first * cos - second * sin).astype(jnp.bfloat16)
            out_ref[start + half : start + 2 * half, :] = (second * cos + first * sin).astype(jnp.bfloat16)

    @pl.when(step >= turned)
    def _():
        out_ref[...] = out.astype(jnp.bfloat16)


def project(x, gain, weight, cos_t, sin_t):
    rows, width = x.shape
    columns = weight.shape[1]
    block = 512
    return run(
        functools.partial(project_kernel, 2 * width // block),
        grid=columns // block,
        out_shape=[like((columns, rows), jnp.bfloat16), like((width, rows), jnp.bfloat16)],
        in_specs=[
            whole(rows, width),
            whole(1, width),
            pl.BlockSpec((width, block), lambda step: (0, step)),
            whole(*cos_t.shape),
            whole(*sin_t.shape),
        ],
        out_specs=[
            pl.BlockSpec((block, rows), lambda step: (step, 0)),
            pl.BlockSpec((width, rows), lambda step: (0, 0)),
        ],
        scratch_shapes=[],
        name="project",
        operands=[x, gain, weight, cos_t, sin_t],
    )


def branch_kernel(att_ref, w_ref, x_ref, gain_ref, hidden_ref, normed_ref):
    hidden = x_ref[...].astype(jnp.float32) + product(att_ref[...], w_ref[...], ROWS_BY_ROWS)
    hidden_ref[...] = hidden
    normed_ref[...] = (hidden * inverse_rms(hidden) * gain_ref[...]).astype(jnp.bfloat16)


def branch(attended_t, weight, x, gain):
    rows, width = x.shape
    block = 256
    row = pl.BlockSpec((block, width), lambda step: (step, 0))
    return run(
        branch_kernel,
        grid=rows // block,
        out_shape=[like((rows, width), jnp.float32), like((rows, width), jnp.bfloat16)],
        in_specs=[
            pl.BlockSpec((width, block), lambda step: (0, step)),
            whole(*weight.shape),
            row,
            whole(1, width),
        ],
        out_specs=[row, row],
        scratch_shapes=[],
        name="branch",
        operands=[attended_t, weight, x, gain],
    )


def widen_kernel(normed_ref, gate_ref, up_ref, act_ref, to_gate_ref, to_up_ref):
    normed = normed_ref[...]
    gate = product(normed, gate_ref[...])
    up = product(normed, up_ref[...])
    sigmoid = jax.nn.sigmoid(gate)
    swish = gate * sigmoid
    act_ref[...] = (swish * up).astype(jnp.bfloat16)
    to_gate_ref[...] = (up * sigmoid * (1.0 + gate * (1.0 - sigmoid))).astype(jnp.bfloat16)
    to_up_ref[...] = swish.astype(jnp.bfloat16)


def widen(normed, weight):
    rows, width = normed.shape
    inner = weight.shape[1] // 2
    block = 512
    steps = inner // block
    part = pl.BlockSpec((rows, block), lambda step: (0, step))
    return run(
        widen_kernel,
        grid=steps,
        out_shape=[like((rows, inner), jnp.bfloat16)] * 3,
        in_specs=[
            whole(rows, width),
            pl.BlockSpec((width, block), lambda step: (0, step)),
            pl.BlockSpec((width, block), lambda step: (0, steps + step)),
        ],
        out_specs=[part] * 3,
        scratch_shapes=[],
        name="widen",
        operands=[normed, weight, weight],
    )


def narrow_kernel(
    steps, act_ref, to_gate_ref, to_up_ref, w_ref, given_ref, hidden_ref, result_ref, grad_ref, d_gate_ref, d_up_ref, acc_ref
):
    step = pl.program_id(0)
    act, weight, given = act_ref[...], w_ref[...], given_ref[...]
    part = product(act, weight)

    @pl.when(step == 0)
    def _():
        acc_ref[...] = hidden_ref[...] + part

    @pl.when(step > 0)
    def _():
        acc_ref[...] += part

    @pl.when(step == steps - 1)
    def _():
        result_ref[...] = acc_ref[...].astype(jnp.bfloat16)

    grad_ref[...] = product(act, given, ROWS_BY_ROWS).astype(jnp.bfloat16)
    d_act = product(given, weight, COLUMNS_BY_COLUMNS)
    d_gate_ref[...] = (d_act * to_gate_ref[...].astype(jnp.float32)).astype(jnp.bfloat16)
    d_up_ref[...] = (d_act * to_up_ref[...].astype(jnp.float32)).astype(jnp.bfloat16)


def narrow(act, to_gate, to_up, weight, given, hidden):
    rows, inner = act.shape
    width = weight.shape[1]
    block = 512
    steps = inner // block
    part = pl.BlockSpec((rows, block), lambda step: (0, step))
    down = pl.BlockSpec((block, width), lambda step: (step, 0))
    return run(
        functools.partial(narrow_kernel, steps),
        grid=steps,
        out_shape=[
            like((rows, width), jnp.bfloat16),
            like((inner, width), jnp.bfloat16),
            like((rows, inner), jnp.bfloat16),
            like((rows, inner), jnp.bfloat16),
        ],
        in_specs=[part, part, part, down, whole(rows, width), whole(rows, width)],
        out_specs=[pl.BlockSpec((rows, width), lambda step: (0, 0)), down, part, part],
        scratch_shapes=[pltpu.VMEM((rows, width), jnp.float32)],
        name="narrow",
        operands=[act, to_gate, to_up, weight, given, hidden],
    )


def grad_in_kernel(normed_ref, d_gate_ref, d_up_ref, to_gate_ref, to_up_ref, turned_ref):
    @pl.when(pl.program_id(0) == 0)
    def _():
        turned_ref[...] = normed_ref[...].T

    to_gate_ref[...] = product(turned_ref[...], d_gate_ref[...]).astype(jnp.bfloat16)
    to_up_ref[...] = product(turned_ref[...], d_up_ref[...]).astype(jnp.bfloat16)


def grad_into(normed, d_gate, d_up):
    rows, width = normed.shape
    inner = d_gate.shape[1]
    block = 512
    part = pl.BlockSpec((rows, block), lambda step: (0, step))
    out = pl.BlockSpec((width, block), lambda step: (0, step))
    return run(
        grad_in_kernel,
        grid=inner // block,
        out_shape=[like((width, inner), jnp.bfloat16)] * 2,
        in_specs=[whole(rows, width), part, part],
        out_specs=[out, out],
        scratch_shapes=[pltpu.VMEM((width, rows), jnp.bfloat16)],
        name="grad_in",
        operands=[normed, d_gate, d_up],
    )


def norm_back(d_normed, values, gain):
    inverse = inverse_rms(values)
    unit = values * inverse
    scaled = d_normed * gain
    mean = jnp.mean(scaled * unit, axis=1, keepdims=True)
    return inverse * (scaled - unit * mean), jnp.sum(d_normed * unit, axis=0, keepdims=True)


def ffn_back_kernel(
    steps, d_gate_ref, d_up_ref, gate_ref, up_ref, hidden_ref, gain_ref, given_ref, d_hidden_ref, d_branch_ref, grad_gain_ref, acc_ref
):
    step = pl.program_id(0)
    part = product(d_gate_ref[...], gate_ref[...], COLUMNS_BY_COLUMNS)
    part = part + product(d_up_ref[...], up_ref[...], COLUMNS_BY_COLUMNS)

    @pl.when(step == 0)
    def _():
        acc_ref[...] = part

    @pl.when(step > 0)
    def _():
        acc_ref[...] += part

    @pl.when(step == steps - 1)
    def _():
        through, grad_gain = norm_back(acc_ref[...], hidden_ref[...], gain_ref[...])
        d_hidden = given_ref[...].astype(jnp.float32) + through
        d_hidden_ref[...] = d_hidden
        d_branch_ref[...] = d_hidden.astype(jnp.bfloat16)
        grad_gain_ref[...] = grad_gain


def ffn_back(d_gate, d_up, weight, hidden, gain, given):
    rows, width = hidden.shape
    inner = d_gate.shape[1]
    block = 512
    steps = inner // block
    part = pl.BlockSpec((rows, block), lambda step: (0, step))
    full = pl.BlockSpec((rows, width), lambda step: (0, 0))
    return run(
        functools.partial(ffn_back_kernel, steps),
        grid=steps,
        out_shape=[
            like((rows, width), jnp.float32),
            like((rows, width), jnp.bfloat16),
            like((1, width), jnp.float32),
        ],
        in_specs=[
            part,
            part,
            pl.BlockSpec((width, block), lambda step: (0, step)),
            pl.BlockSpec((width, block), lambda step: (0, steps + step)),
            whole(rows, width),
            whole(1, width),
            whole(rows, width),
        ],
        out_specs=[full, full, pl.BlockSpec((1, width), lambda step: (0, 0))],
        scratch_shapes=[pltpu.VMEM((rows, width), jnp.float32)],
        name="ffn_back",
        operands=[d_gate, d_up, weight, weight, hidden, gain, given],
    )


def branch_back_kernel(att_ref, w_ref, d_branch_ref, grad_ref, given_ref):
    d_branch = d_branch_ref[...]
    grad_ref[...] = product(att_ref[...], d_branch).astype(jnp.bfloat16)
    given_ref[...] = product(w_ref[...], d_branch, COLUMNS_BY_COLUMNS).astype(jnp.bfloat16)


def branch_back(attended_t, weight, d_branch):
    rows, width = d_branch.shape
    block = 256
    out = pl.BlockSpec((block, width), lambda step: (step, 0))
    turned = pl.BlockSpec((block, rows), lambda step: (step, 0))
    return run(
        branch_back_kernel,
        grid=attended_t.shape[0] // block,
        out_shape=[like(weight.shape, jnp.bfloat16), like(attended_t.shape, jnp.bfloat16)],
        in_specs=[turned, out, whole(rows, width)],
        out_specs=[out, turned],
        scratch_shapes=[],
        name="branch_back",
        operands=[attended_t, weight, d_branch],
    )


def project_back_kernel(
    steps, normed_ref, dq_ref, dk_ref, dv_ref, w_ref, x_ref, gain_ref, d_hidden_ref, grad_ref, tokens_ref, grad_gain_ref, acc_ref
):
    step = pl.program_id(0)
    third = steps // 3

    def run(d_ref):
        d_part = d_ref[...]
        grad_ref[...] = product(normed_ref[...], d_part, COLUMNS_BY_COLUMNS).astype(jnp.bfloat16)
        part = product(w_ref[...], d_part)

        @pl.when(step == 0)
        def _():
            acc_ref[...] = part

        @pl.when(step > 0)
        def _():
            acc_ref[...] += part

    for index, d_ref in enumerate((dq_ref, dk_ref, dv_ref)):
        pl.when(step // third == index)(functools.partial(run, d_ref))

    @pl.when(step == steps - 1)
    def _():
        values = x_ref[...].astype(jnp.float32)
        through, grad_gain = norm_back(acc_ref[...].T, values, gain_ref[...])
        tokens_ref[...] = d_hidden_ref[...] + through
        grad_gain_ref[...] = grad_gain


def project_back(normed_t, dq, dk, dv, weight, x, gain, d_hidden):
    rows, width = x.shape
    columns = weight.shape[1]
    block = 512
    steps = columns // block
    third = steps // 3
    full = pl.BlockSpec((rows, width), lambda step: (0, 0))

    def part(which):
        return pl.BlockSpec(
            (block, rows), lambda step: (jnp.clip(step - which * third, 0, third - 1), 0)
        )

    return run(
        functools.partial(project_back_kernel, steps),
        grid=steps,
        out_shape=[
            like((width, columns), jnp.bfloat16),
            like((rows, width), jnp.float32),
            like((1, width), jnp.float32),
        ],
        in_specs=[
            whole(*normed_t.shape),
            part(0),
            part(1),
            part(2),
            pl.BlockSpec((width, block), lambda step: (0, step)),
            whole(rows, width),
            whole(1, width),
            whole(rows, width),
        ],
        out_specs=[
            pl.BlockSpec((width, block), lambda step: (0, step)),
            full,
            pl.BlockSpec((1, width), lambda step: (0, 0)),
        ],
        scratch_shapes=[pltpu.VMEM((width, rows), jnp.float32)],
        name="project_back",
        operands=[normed_t, dq, dk, dv, weight, x, gain, d_hidden],
    )


LOG2E = 1.4426950408889634
FEATURES = 16


def two_parts(value):
    high = value.astype(jnp.bfloat16)
    return high, (value - high.astype(jnp.float32)).astype(jnp.bfloat16)


def three_parts(value):
    high, rest = value.astype(jnp.bfloat16), None
    rest = value - high.astype(jnp.float32)
    middle = rest.astype(jnp.bfloat16)
    return high, middle, (rest - middle.astype(jnp.float32)).astype(jnp.bfloat16)


def key_features(variates, valid):
    length = variates.shape[1]
    masks = [(variates == v).astype(jnp.float32) for v in range(4)]
    ones = jnp.ones((1, length), jnp.float32)
    invalid = 1.0 - valid
    rows = masks + masks + [invalid, ones, ones, ones, jnp.zeros((FEATURES - 12, length), jnp.float32)]
    return jnp.concatenate(rows, axis=0).astype(jnp.bfloat16)


def query_features(variates, same, other, log_sums):
    length = variates.shape[1]
    highs, lows = [], []
    for v in range(4):
        bias = jnp.where(variates == v, same, other) * LOG2E
        high, low = two_parts(bias)
        highs.append(high.astype(jnp.float32))
        lows.append(low.astype(jnp.float32))
    if log_sums is None:
        minus = [jnp.zeros((3, length), jnp.float32)]
    else:
        minus = [part.astype(jnp.float32) for part in three_parts(-log_sums)]
    mask = jnp.full((1, length), masked_score, jnp.float32)
    rows = highs + lows + [mask] + minus + [jnp.zeros((FEATURES - 12, length), jnp.float32)]
    return jnp.concatenate(rows, axis=0).astype(jnp.bfloat16)


def contract_depth(first_op, second_op):
    return lax.dot_general(
        first_op, second_op, (((1,), (0,)), ((), ())), preferred_element_type=jnp.float32
    )


def scaled_query(query_t, score_scale):
    return two_parts(query_t.astype(jnp.float32) * (score_scale * LOG2E))


def attend_kernel(blocks, bias_ref, *refs):
    head = pl.program_id(0)
    attend_head(blocks, bias_ref[0, head], bias_ref[1, head], *refs)


def attend_head(blocks, same, other, q_ref, k_ref, v_ref, var_ref, valid_ref, o_ref, wide_ref, lse_ref, query_ref):
    depth, length = q_ref.shape
    width = length // blocks
    variates = var_ref[...]
    high, low = scaled_query(q_ref[...], depth ** (-0.5))
    query_ref[...] = jnp.concatenate([high, low, query_features(variates, same, other, None)], axis=0)
    key_t = k_ref[...]
    keys = jnp.concatenate([key_t, key_t, key_features(variates, valid_ref[...])], axis=0).T
    ones = jnp.concatenate(
        [jnp.ones((1, length), jnp.float32), jnp.zeros((FEATURES - 1, length), jnp.float32)], axis=0
    ).astype(jnp.bfloat16)
    values = jnp.concatenate([v_ref[...], ones], axis=0)
    for block in range(blocks):
        at = pl.ds(block * width, width)
        scores = contract_depth(keys, query_ref[:, at])
        peak = jnp.max(scores, axis=0, keepdims=True)
        weights = jnp.exp2(scores - peak).astype(jnp.bfloat16)
        summed = contract_depth(values, weights)
        total = summed[depth : depth + 1]
        attended = summed[:depth] / total
        wide_ref[:, at] = attended
        o_ref[:, at] = attended.astype(jnp.bfloat16)
        lse_ref[0, :, at] = peak + jnp.log2(total)


def attend_forward(qkv_t, variates, valid, bias, heads):
    rows, length = qkv_t.shape
    depth = rows // (3 * heads)

    def part(which):
        return pl.BlockSpec((depth, length), lambda head: (which * heads + head, 0))

    row = pl.BlockSpec((1, length), lambda head: (0, 0))
    return run(
        functools.partial(attend_kernel, 1),
        grid=heads,
        out_shape=[
            jax.ShapeDtypeStruct((heads * depth, length), jnp.bfloat16),
            jax.ShapeDtypeStruct((heads * depth, length), jnp.float32),
            jax.ShapeDtypeStruct((heads, 1, length), jnp.float32),
        ],
        in_specs=[
            pl.BlockSpec(memory_space=pltpu.SMEM),
            part(0),
            part(1),
            part(2),
            row,
            row,
        ],
        out_specs=[
            pl.BlockSpec((depth, length), lambda head: (head, 0)),
            pl.BlockSpec((depth, length), lambda head: (head, 0)),
            pl.BlockSpec((1, 1, length), lambda head: (head, 0, 0)),
        ],
        scratch_shapes=[pltpu.VMEM((2 * depth + FEATURES, length), jnp.bfloat16)],
        name="attend_forward",
        operands=[bias, qkv_t, qkv_t, qkv_t, variates, valid],
    )


def turn_back(grad_t, cos_t, sin_t):
    half = cos_t.shape[0]
    first, second = grad_t[:half], grad_t[half:]
    return jnp.concatenate(
        [first * cos_t + second * sin_t, second * cos_t - first * sin_t], axis=0
    )


def attend_back_head(
    blocks, same, other, q_ref, k_ref, v_ref, go_ref, wide_ref, lse_ref, var_ref, valid_ref, cos_ref, sin_ref,
    dq_ref, dk_ref, dv_ref, query_ref, given_ref, dk_acc, dv_acc,
):
    depth, length = q_ref.shape
    width = length // blocks
    scale = depth ** (-0.5)
    variates = var_ref[...]
    features = key_features(variates, valid_ref[...])
    high, low = scaled_query(q_ref[...], scale)
    query_ref[...] = jnp.concatenate([high, low, query_features(variates, same, other, lse_ref[0])], axis=0)
    key_t = k_ref[...]
    keys = jnp.concatenate([key_t, key_t, features], axis=0).T
    keys_low = jnp.concatenate([key_t, features], axis=0)
    given = go_ref[...]
    inner = jnp.sum(given.astype(jnp.float32) * wide_ref[...], axis=0, keepdims=True)
    minus = [part.astype(jnp.float32) for part in three_parts(-inner)]
    minus = jnp.concatenate(minus + [jnp.zeros((FEATURES - 3, length), jnp.float32)], axis=0)
    given_ref[...] = jnp.concatenate([given, minus.astype(jnp.bfloat16)], axis=0)
    ones = jnp.concatenate(
        [jnp.ones((3, length), jnp.float32), jnp.zeros((FEATURES - 3, length), jnp.float32)], axis=0
    ).astype(jnp.bfloat16)
    values = jnp.concatenate([v_ref[...], ones], axis=0).T
    query_rows = q_ref[...].T
    given_rows = given.T
    in_same = jnp.zeros((1, width), jnp.float32)
    in_other = jnp.zeros((1, width), jnp.float32)
    for block in range(blocks):
        at = pl.ds(block * width, width)
        cut = slice(block * width, (block + 1) * width)
        probs = jnp.exp2(contract_depth(keys, query_ref[:, at]))
        grads = (probs * contract_depth(values, given_ref[:, at])).astype(jnp.bfloat16)
        back = contract_depth(keys_low, grads)
        dq = turn_back(back[:depth] * scale, cos_ref[:, at], sin_ref[:, at])
        dq_ref[:, at] = dq.astype(jnp.bfloat16)
        for v in range(4):
            line = back[depth + v : depth + v + 1]
            hit = variates[:, cut] == v
            in_same = in_same + jnp.where(hit, line, 0.0)
            in_other = in_other + jnp.where(hit, 0.0, line)
        dk = contract_depth(grads, query_rows[cut])
        dv = contract_depth(probs.astype(jnp.bfloat16), given_rows[cut])
        if block == 0:
            dk_acc[...] = dk
            dv_acc[...] = dv
        else:
            dk_acc[...] += dk
            dv_acc[...] += dv
    dk_ref[...] = turn_back((dk_acc[...] * scale).T, cos_ref[...], sin_ref[...]).astype(jnp.bfloat16)
    dv_ref[...] = dv_acc[...].T.astype(jnp.bfloat16)
    return in_same, in_other


def attend_back_kernel(blocks, bias_ref, *refs):
    head = pl.program_id(0)
    *refs, db_ref, query_ref, given_ref, dk_acc, dv_acc = refs
    in_same, in_other = attend_back_head(
        blocks, bias_ref[0, head], bias_ref[1, head], *refs, query_ref, given_ref, dk_acc, dv_acc
    )
    db_ref[0, 0:1, :] = in_same
    db_ref[0, 1:2, :] = in_other


def attend_backward(qkv_t, given_t, wide_t, log_sums, variates, valid, bias, cos_t, sin_t, heads):
    rows, length = qkv_t.shape
    depth = rows // (3 * heads)
    blocks = 1

    def part(which):
        return pl.BlockSpec((depth, length), lambda head: (which * heads + head, 0))

    one = pl.BlockSpec((depth, length), lambda head: (head, 0))
    grad = jax.ShapeDtypeStruct((heads * depth, length), jnp.bfloat16)
    return run(
        functools.partial(attend_back_kernel, blocks),
        grid=heads,
        out_shape=[grad, grad, grad, jax.ShapeDtypeStruct((heads, 2, length // blocks), jnp.float32)],
        in_specs=[
            pl.BlockSpec(memory_space=pltpu.SMEM),
            part(0),
            part(1),
            part(2),
            one,
            one,
            pl.BlockSpec((1, 1, length), lambda head: (head, 0, 0)),
            whole(1, length),
            whole(1, length),
            whole(depth // 2, length),
            whole(depth // 2, length),
        ],
        out_specs=[one, one, one, pl.BlockSpec((1, 2, length // blocks), lambda head: (head, 0, 0))],
        scratch_shapes=[
            pltpu.VMEM((2 * depth + FEATURES, length), jnp.bfloat16),
            pltpu.VMEM((depth + FEATURES, length), jnp.bfloat16),
            pltpu.VMEM((length, depth), jnp.float32),
            pltpu.VMEM((length, depth), jnp.float32),
        ],
        name="attend_backward",
        operands=[bias, qkv_t, qkv_t, qkv_t, given_t, wide_t, log_sums, variates, valid, cos_t, sin_t],
    )


PRELUDE = 7
FRONT_PLACES = (
    (0, 1, 2, 3, 4, 5, 6),
    (1, 3, 4, 5, 7, 8, 9),
    (3, 6, 8, 10, 13, 16, 18),
    (8, 12, 15, 18, 21, 24, 28),
)


def bias_of(small_ref, head, per_shard):
    row = 16 * (head // per_shard) + 2
    return small_ref[row, head % per_shard], small_ref[row + 1, head % per_shard]


def gain_of(small_ref, shards, which):
    rows = [small_ref[16 * shard + which : 16 * shard + which + 1, :] for shard in range(shards)]
    return jnp.concatenate(rows, axis=1)


def front_kernel(line, shards, heads, *refs):
    step = pl.program_id(0)
    refs = list(refs)

    def take(count):
        out = refs[:count]
        del refs[:count]
        return out

    small, w_qkv, w_out, w_in, w_down, x_hbm = take(6)
    var_ref, valid_ref, cos_ref, sin_ref = take(4)
    small_all, qkv_all, out_all, into_0, down_0, into_1, down_1 = take(7)
    intos = take(4)
    qkv_hbm, normed_hbm, attended_hbm, hidden_hbm, normed_two_hbm = take(5)
    wide_ref, lse_ref = take(2)
    x, weight, normed_t, qkv, attended, hidden, normed_two, small_ref, query_ref, bias_ref, wide_rows, cut_rows = take(12)
    load_sem, cut_sem, local_sem, send_sem, recv_sem = refs
    net = Net(line)
    rows, width = x.shape
    block = 512
    projected = 3 * width // block
    attend = PRELUDE + projected
    last = attend + heads
    depth = width // heads

    def load(index, origin, landing):
        return pltpu.make_async_copy(origin, landing, load_sem.at[index])

    def at(place):
        return pl.when(step == place)

    inner = w_in.shape[1] // 2
    owned = inner // shards
    piece_width = BLOCK // shards

    w_in_load = pltpu.make_async_copy(w_in, wide_rows, cut_sem.at[4])

    def cut_store(number):
        return pltpu.make_async_copy(cut_rows.at[number], intos[number], cut_sem.at[number])

    def down_part(number):
        return w_down.at[pl.ds(number * piece_width, piece_width)]

    tensors = (
        ((small, small_all), (w_qkv, qkv_all)),
        ((w_out, out_all),),
        ((intos[0], into_0), (down_part(0), down_0)),
        ((intos[1], into_1), (down_part(1), down_1)),
    )
    number = 0
    groups = []
    for group in tensors:
        lists = []
        for source, full in group:
            lists.append(
                gather_steps(
                    net, source, full, local_sem.at[number], send_sem.at[number], recv_sem.at[number]
                )
            )
            number += 1
        groups.append(lists)

    x_load = load(0, x_hbm, x)
    small_load = load(1, small_all, small_ref)
    weight_load = load(2, qkv_all, weight)
    bias_load = load(9, small_all, bias_ref)
    normed_store = load(3, normed_t, normed_hbm)
    qkv_store = load(4, qkv, qkv_hbm)
    attended_store = load(5, attended, attended_hbm)
    out_load = load(6, out_all, weight.at[:, pl.ds(0, width)])
    hidden_store = load(7, hidden, hidden_hbm)
    normed_two_store = load(8, normed_two, normed_two_hbm)

    @at(0)
    def _():
        net.greet()
        x_load.start()
        w_in_load.start()

    for lists, places in zip(groups, FRONT_PLACES):
        for index, place in enumerate(places):

            @at(place)
            def _():
                if place == FRONT_PLACES[2][0] and lists is groups[2]:
                    cut_store(0).wait()
                if place == FRONT_PLACES[3][0] and lists is groups[3]:
                    cut_store(1).wait()
                for steps in lists:
                    steps[index]()

    @at(0)
    def _():
        w_in_load.wait()
        for index in range(4):
            for piece in range(2 * shards):
                start = piece * owned + index * piece_width
                cut_rows[index, :, piece * piece_width : (piece + 1) * piece_width] = wide_rows[
                    :, start : start + piece_width
                ]
            cut_store(index).start()

    @at(PRELUDE - 1)
    def _():
        cut_store(2).wait()
        cut_store(3).wait()
        weight_load.start()
        small_load.start()
        bias_load.start()
        x_load.wait()
        small_load.wait()
        bias_load.wait()
        gain = gain_of(small_ref, shards, 0)
        values = x[...].astype(jnp.float32)
        normed = values * inverse_rms(values) * gain
        normed_t[...] = normed.T.astype(jnp.bfloat16)
        normed_store.start()
        weight_load.wait()

    @pl.when((step >= PRELUDE) & (step < attend))
    def _():
        index = step - PRELUDE
        columns = pl.ds(aligned(index * block, block), block)
        out = product(weight[:, columns], normed_t[...], ROWS_BY_ROWS)
        lines = qkv.at[columns]

        @pl.when(index < 2 * width // block)
        def _():
            cos, sin = cos_ref[...], sin_ref[...]
            half = depth // 2
            for start in range(0, block, depth):
                first, second = out[start : start + half], out[start + half : start + depth]
                lines[start : start + half, :] = (first * cos - second * sin).astype(jnp.bfloat16)
                lines[start + half : start + depth, :] = (second * cos + first * sin).astype(jnp.bfloat16)

        @pl.when(index >= 2 * width // block)
        def _():
            lines[...] = out.astype(jnp.bfloat16)

    @at(attend)
    def _():
        qkv_store.start()

    @pl.when((step >= attend) & (step < last))
    def _():
        head = step - attend

        def part(which):
            return qkv.at[pl.ds(aligned(which * width + head * depth, depth), depth)]

        same, other = bias_of(bias_ref, head, heads // shards)
        attend_head(
            1,
            same,
            other,
            part(0),
            part(1),
            part(2),
            var_ref,
            valid_ref,
            attended.at[pl.ds(aligned(head * depth, depth), depth)],
            wide_ref,
            lse_ref,
            query_ref,
        )

    @at(last - 1)
    def _():
        out_load.start()
        attended_store.start()

    @at(last)
    def _():
        out_load.wait()
        gain = gain_of(small_ref, shards, 1)
        part = 256
        for index in range(rows // part):
            lines = slice(index * part, (index + 1) * part)
            sums = product(attended[:, lines], weight[:, :width], ROWS_BY_ROWS)
            values = x[lines, :].astype(jnp.float32) + sums
            hidden[lines, :] = values
            normed_two[lines, :] = (values * inverse_rms(values) * gain).astype(jnp.bfloat16)
        hidden_store.start()
        normed_two_store.start()
        for store in (normed_store, qkv_store, attended_store, hidden_store, normed_two_store):
            store.wait()


def front(line, small, w_qkv, w_out, w_in, w_down, x, variates, valid, cos_t, sin_t, heads):
    shards = lax.axis_size("shard")
    rows, width = x.shape
    depth = width // heads
    low = jnp.bfloat16
    piece = BLOCK // shards
    grid = PRELUDE + 3 * width // 512 + heads + 1
    copies = gather_count(line)

    def head_at(step):
        return jnp.clip(step - (PRELUDE + 3 * width // 512), 0, heads - 1)

    def gathered(rows, columns, dtype=low):
        return like((shards * rows, columns), dtype)

    owned = w_qkv.shape[0]
    return pl.pallas_call(
        functools.partial(front_kernel, line, shards, heads),
        grid=(grid,),
        out_shape=[
            gathered(16, 128, jnp.float32),
            gathered(*w_qkv.shape),
            gathered(*w_out.shape),
            gathered(owned, 2 * BLOCK),
            gathered(piece, width),
            gathered(owned, 2 * BLOCK),
            gathered(piece, width),
        ]
        + [like((owned, 2 * BLOCK), low)] * 4
        + [
            like((3 * width, rows), low),
            like((width, rows), low),
            like((width, rows), low),
            like((rows, width), jnp.float32),
            like((rows, width), low),
            like((width, rows), jnp.float32),
            like((heads, 1, rows), jnp.float32),
        ],
        in_specs=[ANY] * 6
        + [
            whole(1, rows),
            whole(1, rows),
            whole(*cos_t.shape),
            whole(*sin_t.shape),
        ],
        out_specs=[ANY] * 16
        + [
            pl.BlockSpec((depth, rows), lambda step: (head_at(step), 0)),
            pl.BlockSpec((1, 1, rows), lambda step: (head_at(step), 0, 0)),
        ],
        scratch_shapes=[
            pltpu.VMEM((rows, width), low),
            pltpu.VMEM((width, 3 * width), low),
            pltpu.VMEM((width, rows), low),
            pltpu.VMEM((3 * width, rows), low),
            pltpu.VMEM((width, rows), low),
            pltpu.VMEM((rows, width), jnp.float32),
            pltpu.VMEM((rows, width), low),
            pltpu.VMEM((16 * shards, 128), jnp.float32),
            pltpu.VMEM((2 * depth + FEATURES, rows), low),
            pltpu.SMEM((16 * shards, 128), jnp.float32),
            pltpu.VMEM(w_in.shape, low),
            pltpu.VMEM((4, owned, 2 * BLOCK), low),
            pltpu.SemaphoreType.DMA((10,)),
            pltpu.SemaphoreType.DMA((5,)),
            pltpu.SemaphoreType.DMA((7,)),
            pltpu.SemaphoreType.DMA((7, copies)),
            pltpu.SemaphoreType.DMA((7, copies)),
        ],
        compiler_params=pltpu.CompilerParams(
            collective_id=1, has_side_effects=True, vmem_limit_bytes=62 << 20
        ),
        name="front",
    )(small, w_qkv, w_out, w_in, w_down, x, variates, valid, cos_t, sin_t)


TILE = 512
BLOCK = 1024
KEPT, GIVEN, GOT, OVER_X, OVER_Y, OVER_Z, LATE, ENDS, WIDE = 13, 3, 4, 5, 5, 6, 4, 4, 3
STAGES = (0, 1, 3, 5, 7, 8, 9, 10, 11, 12)
SUBSTEPS = 6


def stream_scratch(line, shards, half):
    only, shared = reduce_split(TILE)
    both = only + shared
    low = jnp.bfloat16
    copies = 7
    return [
        pltpu.VMEM((KEPT, shards, half, TILE), low),
        pltpu.VMEM((GIVEN, shards, half, TILE), low),
        pltpu.VMEM((GOT, shards, half, TILE), low),
        pltpu.VMEM((OVER_X, shards, half, only), low),
        pltpu.VMEM((OVER_Y, line, half, both), low),
        pltpu.VMEM((OVER_Z, line + 1, half, both), low),
        pltpu.VMEM((LATE, half, both), low),
        pltpu.VMEM((ENDS, half, TILE), low),
        pltpu.VMEM((ENDS, half, TILE), low),
        pltpu.VMEM((WIDE, 2 * half, TILE), jnp.float32),
        pltpu.SemaphoreType.DMA((KEPT, 4)),
        pltpu.SemaphoreType.DMA((KEPT, copies)),
        pltpu.SemaphoreType.DMA((KEPT, copies)),
    ]


class Stream:
    def __init__(self, net, scratch, writes):
        self.net, self.writes = net, writes
        (
            self.kept,
            self.give,
            self.got,
            self.from_x,
            self.from_y,
            self.from_z,
            self.late,
            self.final,
            self.swapped,
            self.wide,
            self.local_sem,
            self.send_sem,
            self.recv_sem,
        ) = scratch
        self.shards, self.half = self.kept.shape[1], self.kept.shape[2]
        self.own = net.y * net.line + net.z
        self.only, self.shared = reduce_split(TILE)
        self.both = self.only + self.shared
        self.carried = pl.ds(aligned(net.x * self.only, 128), self.both)
        self.lone = pl.ds(aligned(net.x * self.both, 128), self.only)
        self.their_lone = pl.ds(aligned((1 - net.x) * self.both, 128), self.only)

    def remote(self, tile, origin, landing, index, target):
        slot = tile % KEPT
        return pltpu.make_async_remote_copy(
            src_ref=origin,
            dst_ref=landing,
            send_sem=self.send_sem.at[slot, index],
            recv_sem=self.recv_sem.at[slot, index],
            device_id=target,
            device_id_type=MESH,
        )

    def halves(self, tile):
        return self.remote(tile, self.give.at[tile % GIVEN], self.got.at[tile % GOT], 3, self.net.sibling)

    def over_x(self, tile):
        origin = self.kept.at[tile % KEPT, :, :, self.their_lone]
        return self.remote(tile, origin, self.from_x.at[tile % OVER_X], 4, self.net.across_x)

    def over_y(self, tile):
        net = self.net
        origin = self.kept.at[tile % KEPT, pl.ds((1 - net.y) * net.line, net.line), :, self.carried]
        return self.remote(tile, origin, self.from_y.at[tile % OVER_Y], 2, net.across_y)

    def up(self, tile, z):
        net, count = self.net, self.net.line - 1 - z
        origin = self.kept.at[tile % KEPT, pl.ds(net.y * net.line + z + 1, count), :, self.carried]
        return self.remote(tile, origin, self.from_z.at[tile % OVER_Z, pl.ds(z + 2, count)], 0, net.above)

    def down(self, tile, z):
        net = self.net
        origin = self.kept.at[tile % KEPT, pl.ds(net.y * net.line, z), :, self.carried]
        return self.remote(tile, origin, self.from_z.at[tile % OVER_Z, pl.ds(0, z)], 1, net.below)

    def end_x(self, tile):
        net = self.net
        origin = self.kept.at[tile % KEPT, self.own, :, self.carried]
        return self.remote(tile, origin, self.late.at[tile % LATE], 5, net.across_x)

    def to_core(self, tile):
        slot = tile % ENDS
        return self.remote(tile, self.final.at[slot], self.swapped.at[slot], 6, self.net.sibling)

    def add(self, tile, shard, part):
        slot = tile % KEPT
        self.kept[slot, shard, :, self.carried] = self.kept[slot, shard, :, self.carried] + part

    def born(self, tile):
        self.halves(tile).start()

    def meet_core(self, tile):
        copy = self.halves(tile)
        copy.wait_recv()
        copy.wait_send()
        slot, came = tile % KEPT, tile % GOT

        @pl.loop(0, self.shards)
        def _(shard):
            self.kept[slot, shard] = self.kept[slot, shard] + self.got[came, shard]

        self.over_x(tile).start()

    def meet_x(self, tile):
        self.over_x(tile).wait_recv()
        slot, came = tile % KEPT, tile % OVER_X

        @pl.loop(0, self.shards)
        def _(shard):
            self.kept[slot, shard, :, self.lone] = self.kept[slot, shard, :, self.lone] + self.from_x[came, shard]

        self.over_y(tile).start()

    def meet_y(self, tile):
        self.over_y(tile).wait_recv()
        came, base = tile % OVER_Y, self.net.y * self.net.line

        @pl.loop(0, self.net.line)
        def _(z):
            self.add(tile, base + z, self.from_y[came, z])

        self.hop(tile, 0)

    def hop(self, tile, step):
        net, came = self.net, tile % OVER_Z
        base, end = net.y * net.line, net.line - 1

        @pl.when(net.z == step)
        def _():
            if step > 0:
                self.up(tile, step - 1).wait_recv()
                for z in range(step + 1, net.line):
                    self.add(tile, base + z, self.from_z[came, z + 1])
            self.up(tile, step).start()

        @pl.when(net.z == end - step)
        def _():
            if step > 0:
                self.down(tile, end - step + 1).wait_recv()
                for z in range(end - step):
                    self.add(tile, base + z, self.from_z[came, z])
            self.down(tile, end - step).start()

    def land(self, tile):
        net, came, end = self.net, tile % OVER_Z, self.net.line - 1
        pl.when(net.z == end)(self.up(tile, end - 1).wait_recv)
        pl.when(net.z == 0)(self.down(tile, 1).wait_recv)

        @pl.when(net.has_below)
        def _():
            self.add(tile, self.own, self.from_z[came, net.z + 1])

        @pl.when(net.has_above)
        def _():
            self.add(tile, self.own, self.from_z[came, net.z])

        self.end_x(tile).start()

    def meet(self, tile):
        net, only, both, shared = self.net, self.only, self.both, self.shared
        slot, came, end = tile % KEPT, tile % LATE, tile % ENDS
        self.end_x(tile).wait_recv()
        self.final[end, :, self.lone] = self.kept[slot, self.own, :, self.lone]
        for x in range(2):

            @pl.when(net.x == x)
            def _():
                theirs = 0 if x == 1 else shared
                middle = only if x == 1 else 0
                at = (1 - x) * both
                self.final[end, :, at : at + only] = self.late[came, :, theirs : theirs + only]
                self.final[end, :, only:both] = (
                    self.kept[slot, self.own, :, only:both] + self.late[came, :, middle : middle + shared]
                )

        self.to_core(tile).start()
        mine = pl.ds(aligned(net.core * self.half, self.half), self.half)
        self.wide[tile % WIDE, mine, :] = self.final[end].astype(jnp.float32)

    def swap(self, tile):
        self.to_core(tile).wait_recv()
        theirs = pl.ds(aligned((1 - self.net.core) * self.half, self.half), self.half)
        self.wide[tile % WIDE, theirs, :] = self.swapped[tile % ENDS].astype(jnp.float32)
        self.writes(tile, self.wide.at[tile % WIDE], self.local_sem.at[tile % KEPT], True)

    def finish(self, tile):
        net = self.net
        self.writes(tile, self.wide.at[tile % WIDE], self.local_sem.at[tile % KEPT], False)
        self.over_x(tile).wait_send()
        self.over_y(tile).wait_send()
        for z in range(net.line - 1):
            pl.when(net.z == z)(self.up(tile, z).wait_send)
            pl.when(net.z == z + 1)(self.down(tile, z + 1).wait_send)
        self.end_x(tile).wait_send()
        self.to_core(tile).wait_send()

    def stages(self):
        return [
            self.born,
            self.meet_core,
            self.meet_x,
            self.meet_y,
            lambda tile: self.hop(tile, 1),
            lambda tile: self.hop(tile, 2),
            self.land,
            self.meet,
            self.swap,
            self.finish,
        ]


class Plan:
    def __init__(self, blocks, heads):
        self.blocks, self.heads = blocks, heads
        self.ffn = blocks * SUBSTEPS
        self.norm = self.ffn
        self.branch = self.ffn + 1
        self.attend = self.ffn + 2
        self.groups = 4
        self.per_group = heads // self.groups
        self.out = self.ffn + SUBSTEPS
        self.ready = [self.attend + self.per_group * (group + 1) for group in range(self.groups)]
        self.births = list(range(SUBSTEPS, self.out + 2))
        self.ffn_tiles = self.ffn
        self.keys_tiles, self.value_tiles = [], []
        for group in range(self.groups):
            self.keys_tiles.append(len(self.births))
            self.births.append(max(self.ready[group], self.births[-1] + 1))
            if group % 2 == 1:
                self.value_tiles.append(len(self.births))
                self.births.append(self.births[-1] + 1)
        self.last = self.births[-1]
        self.grid = self.last + STAGES[-1] + 1

    def tile_at(self, step):
        regular = self.out + 2 - SUBSTEPS
        tile = step - SUBSTEPS
        known = (step >= SUBSTEPS) & (step < self.out + 2)
        for index in range(regular, len(self.births)):
            hit = step == self.births[index]
            tile = jnp.where(hit, index, tile)
            known = known | hit
        return tile, known


def back_kernel(plan, line, shards, *refs):
    step = pl.program_id(0)
    refs = list(refs)

    def take(count):
        out = refs[:count]
        del refs[:count]
        return out

    normed_hbm, given_hbm, hidden_hbm = take(3)
    early = take(4)
    into_2, into_3, down_hbm = take(3)
    attended_hbm, out_hbm, normed_one_hbm, x_hbm, qkv_hbm = take(5)
    small_hbm, = take(1)
    length_ref, q_ref, k_ref, v_ref, wide_ref, lse_ref, var_ref, valid_ref, cos_ref, sin_ref = take(10)
    result_hbm, tokens_hbm, sum_in, sum_down, sum_out, sum_qkv, sum_small = take(7)
    gather_to = take(4)
    normed, turned, given, w_down, act, act_t = take(6)
    w_both, d_both, acc, through = take(4)
    w_gate, w_up = w_both.at[0], w_both.at[1]
    d_gate, d_up = d_both.at[pl.ds(0, 2)], d_both.at[pl.ds(2, 2)]
    query_ref, given_aug_ref, dk_acc, dv_acc = take(4)
    load_sem, = take(1)
    gather_local, gather_send, gather_recv = take(3)
    small_ref, bias_ref, grad_gain_one_ref, grad_gain_two_ref, grad_small = take(5)
    small_buffers = take(REDUCE_BUFFERS)
    small_local, small_send, small_recv = take(3)
    net = Net(line)
    piece = BLOCK // shards
    gather_from = [
        into_2,
        down_hbm.at[pl.ds(2 * piece, piece)],
        into_3,
        down_hbm.at[pl.ds(3 * piece, piece)],
    ]
    half = BLOCK // shards // 2
    heads_at = step - plan.attend

    def writes(tile, wide, sems, begin):
        rows = 2 * half

        def move(index, origin, landing):
            copy = pltpu.make_async_copy(origin, landing, sems.at[index])
            copy.start() if begin else copy.wait()

        block, kind = tile // SUBSTEPS, tile % SUBSTEPS
        in_ffn = tile < plan.ffn_tiles

        @pl.when(in_ffn & (kind < 2))
        def _():
            lines = pl.ds(aligned(block * rows, rows), rows)
            move(0, wide, sum_down.at[lines, pl.ds(aligned(kind * TILE, TILE), TILE)])

        @pl.when(in_ffn & (kind >= 2))
        def _():
            inner = plan.blocks * BLOCK
            base = ((kind - 2) // 2) * inner
            for piece in range(4):
                shard = (kind % 2) * 4 + piece
                start = base + shard * (inner // shards) + block * (BLOCK // shards)
                columns = pl.ds(aligned(start, 128), 128)
                move(piece, wide.at[:, piece * 128 : (piece + 1) * 128], sum_in.at[:, columns])

        @pl.when((tile >= plan.ffn_tiles) & (tile < plan.ffn_tiles + 2))
        def _():
            start = aligned((tile - plan.ffn_tiles) * TILE, TILE)
            move(0, wide, sum_out.at[:, pl.ds(start, TILE)])

        width = plan.heads * q_ref.shape[0]
        for group, number in enumerate(plan.keys_tiles):

            @pl.when(tile == number)
            def _():
                for part in range(2):
                    start = part * width + group * (TILE // 2)
                    columns = slice(part * (TILE // 2), (part + 1) * (TILE // 2))
                    move(part, wide.at[:, columns], sum_qkv.at[:, pl.ds(start, TILE // 2)])

        for pair, number in enumerate(plan.value_tiles):

            @pl.when(tile == number)
            def _():
                move(0, wide, sum_qkv.at[:, pl.ds(2 * width + pair * TILE, TILE)])

    stream = Stream(net, refs, writes)
    stages = stream.stages()

    def load(index, origin, landing):
        return pltpu.make_async_copy(origin, landing, load_sem.at[index])

    def weight_loads(block):
        if block < 2:
            into, down = early[2 * block], early[2 * block + 1]
        else:
            into, down = gather_to[2 * (block - 2)], gather_to[2 * (block - 2) + 1]
        return [
            load(0, into.at[:, pl.ds(0, BLOCK)], w_gate),
            load(1, into.at[:, pl.ds(BLOCK, BLOCK)], w_up),
            load(2, down, w_down),
        ]

    first_loads = [
        load(3, normed_hbm, normed),
        load(4, given_hbm, given),
        load(5, hidden_hbm, acc),
        load(15, small_hbm, small_ref),
        load(16, small_hbm, bias_ref),
    ]
    hidden_load = load(5, hidden_hbm, acc)
    result_store = load(6, act, result_hbm)
    attended_wait = load(7, attended_hbm, w_down)
    out_load = load(8, out_hbm, d_up.at[0])
    normed_one_wait = load(9, normed_one_hbm, turned)
    x_load = load(10, x_hbm, normed)
    tokens_store = load(11, acc, tokens_hbm)

    def placed():
        for shard in range(shards):
            order = (shard % 2) * line + shard // 2
            for part in range(2):
                which = net.core if part == 0 else 1 - net.core
                start = (shard * 2 + part) * half
                yield start, aligned((which * shards + order) * half, half)

    def in_order(index, origin, landing):
        return [load(index, origin.at[pl.ds(start, half)], landing.at[pl.ds(to, half)]) for start, to in placed()]

    def turn_into(page, value):
        flipped = value.T
        for start, to in placed():
            page[pl.ds(to, half), :] = flipped[start : start + half]

    def qkv_loads(group):
        width = qkv_hbm.shape[1] // 3
        part = width // plan.groups
        page = act_t if group % 2 == 0 else d_up.at[0]
        return [
            load(
                12 + index,
                qkv_hbm.at[:, pl.ds(index * width + group * part, part)],
                page.at[:, pl.ds(index * part, part)],
            )
            for index in range(3)
        ]

    def at(place):
        return pl.when(step == place)

    def start(copies):
        for copy in copies:
            copy.start()

    def wait(copies):
        for copy in copies:
            copy.wait()

    gathers = [
        gather_steps(
            net, gather_from[i], gather_to[i], gather_local.at[i], gather_send.at[i], gather_recv.at[i]
        )
        for i in range(4)
    ]
    gather_places = ((0, 2, 4, 6, 8, 9, 10), (7, 9, 11, 12, 14, 15, 16))

    @at(0)
    def _():
        net.greet()
        start(weight_loads(0) + first_loads)

    for pair, places in enumerate(gather_places):
        for index, place in enumerate(places):

            @at(place)
            def _():
                gathers[2 * pair][index]()
                gathers[2 * pair + 1][index]()

    for stage in range(len(STAGES) - 1, 0, -1):
        tile, known = plan.tile_at(step - STAGES[stage])
        pl.when(known)(functools.partial(stages[stage], tile))

    @at(0)
    def _():
        wait(first_loads)
        position = lax.broadcasted_iota(jnp.int32, (given.shape[0], 1), 0)
        counted = jnp.where(position < length_ref[0], 1.0, 0.0).astype(jnp.bfloat16)
        given[...] = given[...] * counted
        grad_small[...] = jnp.zeros_like(grad_small)
        turn_into(turned, normed[...])

    for block in range(plan.blocks):

        @at(block * SUBSTEPS)
        def _():
            wait(weight_loads(block))

        if block + 1 < plan.blocks:

            @at(block * SUBSTEPS + SUBSTEPS - 1)
            def _():
                start(weight_loads(block + 1))

    block, sub = step // SUBSTEPS, step % SUBSTEPS
    slot = block % 2
    in_ffn = step < plan.ffn

    @pl.when(in_ffn & (sub < 2))
    def _():
        columns = pl.ds(aligned(sub * TILE, TILE), TILE)
        d_act = product(given[...], w_down[columns, :], COLUMNS_BY_COLUMNS)
        gate = product(normed[...], w_gate[:, columns])
        up = product(normed[...], w_up[:, columns])
        sigmoid = jax.nn.sigmoid(gate)
        swish = gate * sigmoid
        act[:, columns] = (swish * up).astype(jnp.bfloat16)
        d_gate[slot, :, columns] = (d_act * up * sigmoid * (1.0 + gate * (1.0 - sigmoid))).astype(jnp.bfloat16)
        d_up[slot, :, columns] = (d_act * swish).astype(jnp.bfloat16)

    @pl.when(in_ffn & (sub == 2))
    def _():
        acc[...] += product(act[...], w_down[...])
        turn_into(act_t, act[...])

    @pl.when(in_ffn & ((sub == 3) | (sub == 4)))
    def _():
        which = jnp.clip(sub - 3, 0, 1)
        part = product(d_both[2 * which + slot], w_both[which], COLUMNS_BY_COLUMNS)
        first = (block == 0) & (sub == 3)

        @pl.when(first)
        def _():
            through[...] = part

        @pl.when(jnp.logical_not(first))
        def _():
            through[...] += part

    last_sum = plan.ffn - SUBSTEPS + 2

    @at(last_sum)
    def _():
        act[...] = acc[...].astype(jnp.bfloat16)
        result_store.start()

    @at(last_sum + 1)
    def _():
        start([hidden_load] + in_order(7, attended_hbm, w_down))

    @at(last_sum + 3)
    def _():
        result_store.wait()

    row_block = 128

    @at(plan.norm)
    def _():
        out_load.start()
        hidden_load.wait()
        grad_gain_two_ref[...] = jnp.zeros_like(grad_gain_two_ref)
        gain_two = gain_of(small_ref, shards, 1)

        @pl.loop(0, acc.shape[0] // row_block)
        def _(index):
            lines = pl.ds(aligned(index * row_block, row_block), row_block)
            back, grad_gain = norm_back(through[lines, :], acc[lines, :], gain_two)
            d_hidden = given[lines, :].astype(jnp.float32) + back
            acc[lines, :] = d_hidden
            d_gate[0, lines, :] = d_hidden.astype(jnp.bfloat16)
            grad_gain_two_ref[...] += grad_gain

    @at(plan.branch)
    def _():
        out_load.wait()
        act[...] = product(d_up[0], d_gate[0], COLUMNS_BY_COLUMNS).astype(jnp.bfloat16)
        through[...] = jnp.zeros_like(through)

    for group in range(plan.groups):
        ready = plan.ready[group]

        if group == 0:

            @at(plan.attend)
            def _():
                start(qkv_loads(0))

        @at(ready)
        def _():
            wait(qkv_loads(group))
            if group + 1 < plan.groups:
                start(qkv_loads(group + 1))

    quarter = TILE // 2
    for parity, page in enumerate((act_t, d_up.at[0])):
        base = parity * TILE
        now = (step == plan.ready[parity]) | (step == plan.ready[parity + 2])
        pair = jnp.where(step == plan.ready[parity + 2], 1, 0)
        value_at = pl.ds(aligned(pair * TILE + parity * quarter, quarter), quarter)

        @pl.when(now)
        def _():
            part = product(page[:, :TILE], w_gate[base : base + TILE, :])
            through[...] += part + product(page[:, TILE : TILE + quarter], w_up[value_at, :])

    @at(plan.out)
    def _():
        attended_wait.wait()
        start(in_order(9, normed_one_hbm, turned) + [x_load])

    @at(plan.births[plan.keys_tiles[0]])
    def _():
        normed_one_wait.wait()

    @pl.when((heads_at >= 0) & (heads_at < plan.heads))
    def _():
        depth = q_ref.shape[0]
        head = heads_at
        group = head // plan.per_group
        q_at = (group % 2) * TILE + (head % plan.per_group) * depth
        k_at = q_at + TILE // 2
        v_at = (group // 2) * TILE + (head % (2 * plan.per_group)) * depth

        def rows(start):
            return pl.ds(aligned(start, depth), depth)

        per_shard = plan.heads // shards
        same, other = bias_of(bias_ref, head, per_shard)
        sums = attend_back_head(
            2,
            same,
            other,
            q_ref,
            k_ref,
            v_ref,
            act.at[rows(head * depth)],
            wide_ref,
            lse_ref,
            var_ref,
            valid_ref,
            cos_ref,
            sin_ref,
            w_gate.at[rows(q_at)],
            w_gate.at[rows(k_at)],
            w_up.at[rows(v_at)],
            query_ref,
            given_aug_ref,
            dk_acc,
            dv_acc,
        )
        for which, lanes in enumerate(sums):
            folded = sum(lanes[:, start : start + 128] for start in range(0, lanes.shape[1], 128))
            grad_small[head // per_shard, pl.ds(2 + 2 * (head % per_shard) + which, 1), :] = folded

    tile, known = plan.tile_at(step)

    def birth(left, right, dims=(((1,), (0,)), ((), ()))):
        out = product(left[...], right, dims).astype(jnp.bfloat16)
        kept, give = stream.kept.at[tile % KEPT], stream.give.at[tile % GIVEN]
        for order in range(shards):
            kept[order] = out[order * half : (order + 1) * half]
            give[order] = out[(shards + order) * half : (shards + order + 1) * half]

    def chosen(numbers, bases):
        base, hit = 0, False
        for number, start in zip(numbers, bases):
            now = step == plan.births[number]
            base, hit = jnp.where(now, start, base), now | hit
        return base, hit

    kind, source = tile % SUBSTEPS, (tile // SUBSTEPS) % 2
    in_tiles = known & (tile < plan.ffn_tiles)
    columns = pl.ds(aligned((kind % 2) * TILE, TILE), TILE)
    pl.when(in_tiles & (kind < 2))(lambda: birth(act_t, given[:, columns]))
    page_at = jnp.where(kind >= 4, 2, 0) + source
    pl.when(in_tiles & (kind >= 2))(lambda: birth(turned, d_both[page_at, :, columns]))
    out_columns = pl.ds(aligned(jnp.clip(step - plan.out, 0, 1) * TILE, TILE), TILE)
    pl.when((step == plan.out) | (step == plan.out + 1))(lambda: birth(w_down, d_gate[0, :, out_columns]))
    key_base, key_hit = chosen(plan.keys_tiles, [(group % 2) * TILE for group in range(plan.groups)])
    value_base, value_hit = chosen(plan.value_tiles, [pair * TILE for pair in range(plan.groups // 2)])
    lines = pl.ds(aligned(key_base + value_base, TILE), TILE)
    late_page = jnp.where(value_hit, 1, 0)
    pl.when(key_hit | value_hit)(lambda: birth(turned, w_both[late_page, lines, :], COLUMNS_BY_COLUMNS))
    pl.when(known)(lambda: stream.born(tile))

    @at(plan.last + 1)
    def _():
        x_load.wait()
        grad_gain_one_ref[...] = jnp.zeros_like(grad_gain_one_ref)
        gain_one = gain_of(small_ref, shards, 0)

        @pl.loop(0, acc.shape[0] // row_block)
        def _(index):
            lines = pl.ds(aligned(index * row_block, row_block), row_block)
            values = normed[lines, :].astype(jnp.float32)
            back, grad_gain = norm_back(through[:, lines].T, values, gain_one)
            acc[lines, :] = acc[lines, :] + back
            grad_gain_one_ref[...] += grad_gain

        tokens_store.start()
        for shard in range(shards):
            columns = slice(shard * 128, (shard + 1) * 128)
            grad_small[shard, 0:1, :] = grad_gain_one_ref[:, columns]
            grad_small[shard, 1:2, :] = grad_gain_two_ref[:, columns]

    small_steps = reduce_steps(
        net, grad_small, sum_small, 0, 0, small_buffers, small_local, small_send, small_recv
    )
    for index, action in enumerate(small_steps):
        at(plan.last + 2 + index)(action)

    @at(plan.grid - 1)
    def _():
        tokens_store.wait()


def back(line, early, sources, own_down, normed_two, given, hidden, attended_t, out_weight, normed_t, x, qkv_weight,
         small, lengths, qkv_t, wide_t, log_sums, variates, valid, cos_t, sin_t):
    shards = lax.axis_size("shard")
    rows, width = x.shape
    heads = log_sums.shape[0]
    depth = width // heads
    blocks = 4
    plan = Plan(blocks, heads)
    low = jnp.bfloat16
    owned = width // shards
    inner = blocks * BLOCK

    def head_at(step):
        return jnp.clip(step - plan.attend, 0, heads - 1)

    def part(which):
        return pl.BlockSpec((depth, rows), lambda step: (which * heads + head_at(step), 0))

    page = pltpu.VMEM((BLOCK, BLOCK), low)
    copies = gather_count(line)
    return pl.pallas_call(
        functools.partial(back_kernel, plan, line, shards),
        grid=(plan.grid,),
        out_shape=[
            like((rows, width), low),
            like((rows, width), jnp.float32),
            like((owned, 2 * inner), jnp.float32),
            like((inner // shards, width), jnp.float32),
            like((owned, width), jnp.float32),
            like((owned, 3 * width), jnp.float32),
            like((16, 128), jnp.float32),
        ]
        + [like((width, 2 * BLOCK), low), like((BLOCK, width), low)] * 2
,
        in_specs=[ANY] * 16
        + [
            pl.BlockSpec(memory_space=pltpu.SMEM),
            part(0),
            part(1),
            part(2),
            pl.BlockSpec((depth, rows), lambda step: (head_at(step), 0)),
            pl.BlockSpec((1, 1, rows), lambda step: (head_at(step), 0, 0)),
            whole(1, rows),
            whole(1, rows),
            whole(*cos_t.shape),
            whole(*sin_t.shape),
        ],
        out_specs=[ANY] * 11,
        scratch_shapes=[page] * 6
        + [
            pltpu.VMEM((2, BLOCK, BLOCK), low),
            pltpu.VMEM((4, BLOCK, BLOCK), low),
            pltpu.VMEM((rows, width), jnp.float32),
            pltpu.VMEM((rows, width), jnp.float32),
            pltpu.VMEM((2 * depth + FEATURES, rows), low),
            pltpu.VMEM((depth + FEATURES, rows), low),
            pltpu.VMEM((rows, depth), jnp.float32),
            pltpu.VMEM((rows, depth), jnp.float32),
            pltpu.SemaphoreType.DMA((17,)),
            pltpu.SemaphoreType.DMA((4,)),
            pltpu.SemaphoreType.DMA((4, copies)),
            pltpu.SemaphoreType.DMA((4, copies)),
            pltpu.VMEM((16 * shards, 128), jnp.float32),
            pltpu.SMEM((16 * shards, 128), jnp.float32),
            pltpu.VMEM((1, width), jnp.float32),
            pltpu.VMEM((1, width), jnp.float32),
            pltpu.VMEM((shards, 16, 128), jnp.float32),
        ]
        + reduce_scratch(line, shards, 8, 128, jnp.float32)
        + [
            pltpu.SemaphoreType.DMA((2,)),
            pltpu.SemaphoreType.DMA((reduce_count(line),)),
            pltpu.SemaphoreType.DMA((reduce_count(line),)),
        ]
        + stream_scratch(line, shards, owned // 2),
        compiler_params=pltpu.CompilerParams(
            collective_id=9, has_side_effects=True, vmem_limit_bytes=64 << 20
        ),
        name="back",
    )(
        normed_two, given, hidden, *early, *sources, own_down, attended_t, out_weight, normed_t, x, qkv_weight,
        small, lengths, qkv_t, qkv_t, qkv_t, wide_t, log_sums, variates, valid, cos_t, sin_t,
    )


def rope_tables(time_ids):
    half = HEAD_DIM // 2
    exponent = jnp.arange(half).astype(jnp.float32) * (2.0 / HEAD_DIM)
    inverse = jnp.exp(-jnp.log(rope_base) * exponent)
    angles = inverse[:, None] * time_ids.astype(jnp.float32)
    return jnp.cos(angles), jnp.sin(angles)


def pack_small(attn_gain, ffn_gain, attn_bias):
    heads = attn_bias.shape[1]
    small = jnp.zeros((16, 128), jnp.float32)
    small = small.at[0].set(attn_gain.astype(jnp.float32)).at[1].set(ffn_gain.astype(jnp.float32))
    return small.at[2:4, :heads].set(attn_bias.astype(jnp.float32))


def shards(
    line,
    tokens,
    lengths,
    variate_ids,
    time_ids,
    attn_gain,
    w_qkv,
    attn_bias,
    w_out,
    ffn_gain,
    w_in,
    w_down,
    cotangent,
):
    length = variate_ids.shape[1]
    heads = attn_bias.shape[1]
    key_valid = jnp.arange(length)[None, :] < lengths[:, None]
    valid = key_valid.astype(jnp.float32)
    cos_t, sin_t = rope_tables(time_ids)
    if line:
        small, qkv_weight, out_weight, into_0, down_0, into_1, down_1, *rest = front(
            line,
            pack_small(attn_gain, ffn_gain, attn_bias),
            w_qkv,
            w_out,
            w_in,
            w_down,
            tokens,
            variate_ids,
            valid,
            cos_t,
            sin_t,
            HEADS,
        )
        intos, (qkv_t, normed_t, attended_t, hidden, normed_two, wide_t, log_sums) = rest[:4], rest[4:]
        result, grad_tokens, sum_in, sum_down, sum_out, sum_qkv, small = back(
            line,
            [into_0, down_0, into_1, down_1],
            [intos[2], intos[3]],
            w_down,
            normed_two,
            cotangent,
            hidden,
            attended_t,
            out_weight,
            normed_t,
            tokens,
            qkv_weight,
            small,
            lengths,
            qkv_t,
            wide_t,
            log_sums,
            variate_ids,
            valid,
            cos_t,
            sin_t,
        )[:7]
        return (
            result,
            grad_tokens,
            small[0],
            sum_qkv,
            jnp.sum(small[2 : 2 + 2 * heads], axis=1).reshape(heads, 2).T,
            sum_out,
            small[1],
            sum_in,
            sum_down,
        )
    given = jnp.where(key_valid.reshape(length, 1), cotangent, jnp.zeros_like(cotangent))
    gain_one, gain_two, qkv_weight, out_weight, in_weight, down_weight = (
        lax.all_gather(part, "shard", axis=0, tiled=True)
        for part in (attn_gain, ffn_gain, w_qkv, w_out, w_in, w_down)
    )
    bias = lax.all_gather(attn_bias, "shard", axis=1, tiled=True).astype(jnp.float32)
    gain_one = gain_one.astype(jnp.float32).reshape(1, -1)
    gain_two = gain_two.astype(jnp.float32).reshape(1, -1)
    qkv_t, normed_t = project(tokens, gain_one, qkv_weight, cos_t, sin_t)
    attended_t, wide_t, log_sums = attend_forward(qkv_t, variate_ids, valid, bias, HEADS)
    hidden, normed_two = branch(attended_t, out_weight, tokens, gain_two)
    act, to_gate, to_up = widen(normed_two, in_weight)
    result, grad_down, d_gate, d_up = narrow(act, to_gate, to_up, down_weight, given, hidden)
    grad_gate, grad_up = grad_into(normed_two, d_gate, d_up)
    d_hidden, d_branch, grad_gain_two = ffn_back(d_gate, d_up, in_weight, hidden, gain_two, given)
    grad_out, given_t = branch_back(attended_t, out_weight, d_branch)
    dq, dk, dv, bias_parts = attend_backward(
        qkv_t, given_t, wide_t, log_sums, variate_ids, valid, bias, cos_t, sin_t, HEADS
    )
    grad_qkv, grad_tokens, grad_gain_one = project_back(
        normed_t, dq, dk, dv, qkv_weight, tokens, gain_one, d_hidden
    )
    grads = (
        (grad_gain_one.reshape(-1), 0),
        (grad_qkv, 0),
        (jnp.sum(bias_parts, axis=2).T, 1),
        (grad_out, 0),
        (grad_gain_two.reshape(-1), 0),
        (jnp.concatenate([grad_gate, grad_up], axis=1), 0),
        (grad_down, 0),
    )
    owned = [
        lax.psum_scatter(grad.astype(jnp.bfloat16), "shard", scatter_dimension=axis, tiled=True)
        for grad, axis in grads
    ]
    return (result, grad_tokens) + tuple(lax.psum(part, "rep").astype(jnp.float32) for part in owned)


def solution(mesh):
    placed = (
        P(("shard", "rep"), None),
        P(("shard", "rep")),
        P(("shard", "rep"), None),
        P(("shard", "rep"), None),
        P("shard"),
        P("shard", None),
        P(None, "shard"),
        P("shard", None),
        P("shard"),
        P("shard", None),
        P("shard", None),
        P(("shard", "rep"), None),
    )
    line = mesh.shape["shard"] // 2 if (mesh.shape["shard"], mesh.shape["rep"]) == (8, 4) else 0
    return jax.shard_map(
        functools.partial(shards, line),
        mesh=mesh,
        in_specs=placed,
        out_specs=(
            P(("shard", "rep"), None),
            P(("shard", "rep"), None),
            P("shard"),
            P("shard", None),
            P(None, "shard"),
            P("shard", None),
            P("shard"),
            P("shard", None),
            P("shard", None),
        ),
        check_vma=False,
    )
```
